32 devices in a mesh: dp: 8 (over z, y), tensor: 4 (over x, core).
Axes of the slice: x: 2, y: 2, z: 4, core: 2. Of those that a mesh axis runs over, the one named last changes fastest.
Arguments:
- tokens: bfloat16 [8192, 2048], P(('dp', 'tensor')), may hold values from -6 to 6
- norm_gain: bfloat16 [2048], replicated, may hold values from 0.5 to 1.5
- norm_bias: bfloat16 [2048], replicated, may hold values from -3 to 3
- query_weight: bfloat16 [2048, 2048], P('dp', 'tensor'), may hold values from -0.1875 to 0.1875
- query_bias: bfloat16 [2048], P('tensor'), may hold values from -3 to 3
- key_weight: bfloat16 [2048, 2048], P('dp', 'tensor'), may hold values from -0.1875 to 0.1875
- key_bias: bfloat16 [2048], P('tensor'), may hold values from -3 to 3
- value_weight: bfloat16 [2048, 2048], P('dp', 'tensor'), may hold values from -0.125 to 0.125
- value_bias: bfloat16 [2048], P('tensor'), may hold values from -3 to 3
- output_weight: bfloat16 [2048, 2048], P('tensor', 'dp'), may hold values from -0.5 to 0.5
- output_bias: bfloat16 [2048], replicated, may hold values from -3 to 3
- up_weight: bfloat16 [2048, 8192], P('dp', 'tensor'), may hold values from -0.125 to 0.125
- up_bias: bfloat16 [8192], P('tensor'), may hold values from -3 to 3
- down_weight: bfloat16 [8192, 2048], P('tensor', 'dp'), may hold values from -0.0625 to 0.0625
- down_bias: bfloat16 [2048], replicated, may hold values from -3 to 3
- doc_split: int32 [8], P('dp'), may hold values from 256 to 768, as said below
- cotangent: bfloat16 [8192, 2048], P(('dp', 'tensor')), may hold values from -6 to 6
Outputs:
- out: bfloat16 [8192, 2048], P(('dp', 'tensor'))
- grad_tokens: float32 [8192, 2048], P(('dp', 'tensor'))
- grad_norm_gain: float32 [2048], replicated
- grad_norm_bias: float32 [2048], replicated
- grad_query_weight: float32 [2048, 2048], P('dp', 'tensor')
- grad_query_bias: float32 [2048], P('tensor')
- grad_key_weight: float32 [2048, 2048], P('dp', 'tensor')
- grad_key_bias: float32 [2048], P('tensor')
- grad_value_weight: float32 [2048, 2048], P('dp', 'tensor')
- grad_value_bias: float32 [2048], P('tensor')
- grad_output_weight: float32 [2048, 2048], P('tensor', 'dp')
- grad_output_bias: float32 [2048], replicated
- grad_up_weight: float32 [2048, 8192], P('dp', 'tensor')
- grad_up_bias: float32 [8192], P('tensor')
- grad_down_weight: float32 [8192, 2048], P('tensor', 'dp')
- grad_down_bias: float32 [2048], replicated
The draws below stay inside these ranges and needn't reach their ends.
Inputs may be any that keep to these rules, and one draw needn't show every extreme that they name: `doc_split`: each sequence holds two documents; the second begins at a multiple of 256, and every such start from 256 to 768 occurs in some sequence.
All inputs are finite; a program needn't handle non-finite values.
Results may differ from the reference program's by a relative error of at most 0.013.
The reference program's roundings to bfloat16 on the way count: a program that leaves them out, or rounds other values in their place, can miss the bound.
Values may be sent and summed in bfloat16 or wider, within the bound.
A program may use at most 256 MiB of HBM per device.

```python
import jax
import jax.numpy as jnp
from jax import lax

D = 2048
HEADS = 32
HEAD_DIM = 64
ROT = 32
FF = 8192
BLOCK = 256
SEQ = 1024
SEQUENCES = 8
TOKENS = 8192


def draw_doc_split(key, part):
    order = jax.random.permutation(key, SEQUENCES)
    return (BLOCK * (1 + order % (SEQ // BLOCK - 1))).astype(jnp.int32)


def with_spikes(entries, key, source, target, parts, factor):
    owner, partner = [(jnp.arange(entries.shape[dim]) // (entries.shape[dim] // parts)).reshape([-1 if axis == dim else 1 for axis in range(entries.ndim)]) for dim in (source, target)]
    chosen = jax.random.permutation(key, parts)[partner]
    strong = (owner == chosen) | (owner == (partner + parts // 2) % parts)
    return jnp.where(strong, factor * entries, entries)


def shard_levels(stream_key, extent, split, least, high):
    loudness = 1.0
    for dim, blocks in split:
        draws = jax.random.uniform(jax.random.fold_in(jax.random.fold_in(stream_key, 6), dim), (blocks,), jnp.float32, least / len(split), high / len(split))
        loudness = loudness * jnp.repeat(jnp.exp(draws), extent[dim] // blocks).reshape((-1,) + (1,) * (len(extent) - 1 - dim))
    return loudness


def gaussian(own_key, shape, spread, limit, shards=(), kind=jnp.bfloat16):
    values = spread * jax.random.normal(own_key, shape, jnp.float32)
    if shards:
        values = values * shard_levels(own_key, shape, shards, -0.22, 0.18)
    return jnp.clip(values, -limit, limit).astype(kind)


def gaussian_with(rng, shape, deviation, most, shards, heavy, kind=jnp.bfloat16):
    drawn = deviation * jax.random.normal(rng, shape, jnp.float32)
    if shards:
        drawn = drawn * shard_levels(rng, shape, shards, -0.22, 0.18)
    return jnp.clip(with_spikes(drawn, jax.random.fold_in(rng, 3), *heavy), -most, most).astype(kind)


def setup_inputs(seed: int = 0) -> dict:
    streams_of = jax.random.split(jax.random.key(seed), 18)
    tokens = gaussian_with(streams_of[0], (TOKENS, D), 1.0, 6.0, ((0, 32),), (0, 1, 32, 2.75))
    norm_gain = jnp.clip(1.0 + 0.1 * jax.random.normal(streams_of[1], (D,), jnp.float32), 0.5, 1.5).astype(jnp.bfloat16)
    norm_bias = gaussian(streams_of[2], (D,), 0.3, 3.0)
    query_weight = gaussian(streams_of[3], (D, D), (D // 2) ** -0.5, 0.1875, ((0, 8), (1, 4)))
    query_bias = gaussian(streams_of[4], (D,), 0.5, 3.0, ((0, 4),))
    key_weight = gaussian(streams_of[5], (D, D), (D // 2) ** -0.5, 0.1875, ((0, 8), (1, 4)))
    key_bias = gaussian(streams_of[6], (D,), 0.5, 3.0, ((0, 4),))
    value_weight = gaussian(streams_of[7], (D, D), D ** -0.5, 0.125, ((0, 8), (1, 4)))
    value_bias = gaussian(streams_of[8], (D,), 0.5, 3.0, ((0, 4),))
    output_weight = gaussian(streams_of[9], (D, D), (D // 16) ** -0.5, 0.5, ((0, 4), (1, 8)))
    output_bias = gaussian(streams_of[10], (D,), 0.5, 3.0)
    up_weight = gaussian(streams_of[11], (D, FF), D ** -0.5, 0.125, ((0, 8), (1, 4)))
    up_bias = gaussian(streams_of[12], (FF,), 0.5, 3.0, ((0, 4),))
    down_weight = gaussian(streams_of[13], (FF, D), FF ** -0.5, 0.0625, ((0, 4), (1, 8)))
    down_bias = gaussian(streams_of[14], (D,), 0.5, 3.0)
    doc_split = draw_doc_split(jax.random.fold_in(streams_of[17], 71), 0)
    cotangent = gaussian_with(streams_of[16], (TOKENS, D), 1.0, 6.0, ((0, 32),), (0, 1, 32, 2.75))
    return {"tokens": tokens, "norm_gain": norm_gain, "norm_bias": norm_bias, "query_weight": query_weight, "query_bias": query_bias, "key_weight": key_weight, "key_bias": key_bias, "value_weight": value_weight, "value_bias": value_bias, "output_weight": output_weight, "output_bias": output_bias, "up_weight": up_weight, "up_bias": up_bias, "down_weight": down_weight, "down_bias": down_bias, "doc_split": doc_split, "cotangent": cotangent}


EPS = 1e-05
NEG = -1000000000.0

@jax.custom_vjp
def low(v):
    return lax.optimization_barrier(v.astype(jnp.bfloat16)).astype(jnp.float32)

@jax.custom_vjp
def low_back(v):
    return v

def low_keep(v):
    return (low(v), None)

def low_pass(kept, grad):
    return (grad,)

def back_keep(v):
    return (v, None)

def back_low(kept, grad):
    return (low(grad),)
low.defvjp(low_keep, low_pass)
low_back.defvjp(back_keep, back_low)

def matmul(left, right):
    return jnp.dot(left, right, precision=lax.Precision.HIGHEST, preferred_element_type=jnp.float32)

def tables(split_at, seq_len):
    token_index = jnp.arange(seq_len, dtype=jnp.int32)
    later_doc = token_index >= split_at
    position = (token_index - jnp.where(later_doc, split_at, 0)).astype(jnp.float32)
    frequency = 10000.0 ** (-(2.0 * jnp.arange(ROT // 2, dtype=jnp.float32)) / ROT)
    angles = position[:, None] * frequency[None, :]
    return (jnp.cos(angles), jnp.sin(angles), later_doc)

def rotate(values, cosine, sine_table):
    half_rot = ROT // 2
    front_part = values[..., :half_rot]
    back_part = values[..., half_rot:ROT]
    cos_wide = cosine[..., None, :]
    sin_wide = sine_table[..., None, :]
    return jnp.concatenate([front_part * cos_wide - back_part * sin_wide, back_part * cos_wide + front_part * sin_wide, values[..., ROT:]], axis=-1)

def one_sequence(tokens_seq, split_at, params):
    norm_gain, norm_bias, query_weight, query_bias, key_weight, key_bias, value_weight, value_bias, output_weight, output_bias, up_weight, up_bias, down_weight, down_bias = params
    seq_len = tokens_seq.shape[0]
    cosine, sine_table, later_doc = tables(split_at, seq_len)
    block_ids = jnp.arange(seq_len, dtype=jnp.int32) // BLOCK
    allowed = (block_ids[None, :] <= block_ids[:, None]) & (later_doc[None, :] == later_doc[:, None])
    row_mean = lax.optimization_barrier(jnp.mean(tokens_seq, -1, keepdims=True))
    centred = tokens_seq - row_mean
    variance = lax.optimization_barrier(jnp.mean(centred * centred, -1, keepdims=True))
    normed = low(centred * lax.rsqrt(variance + EPS) * norm_gain + norm_bias)
    shaped = (seq_len, HEADS, HEAD_DIM)
    queries = low(rotate(low_back(matmul(normed, query_weight) + query_bias).reshape(shaped), cosine, sine_table))
    keys_rot = low(rotate(low_back(matmul(normed, key_weight) + key_bias).reshape(shaped), cosine, sine_table))
    values_all = low(low_back(matmul(normed, value_weight) + value_bias)).reshape(shaped)
    raw_scores = jnp.einsum('qhd,khd->hqk', queries, keys_rot, precision=lax.Precision.HIGHEST)
    scores = jnp.where(allowed[None], low_back(raw_scores) * HEAD_DIM ** (-0.5), NEG)
    row_top = lax.optimization_barrier(jnp.max(scores, -1, keepdims=True))
    exponent = jnp.exp(scores - row_top)
    probability = exponent / lax.optimization_barrier(jnp.sum(exponent, -1, keepdims=True))
    attended = jnp.einsum('hqk,khd->qhd', low(probability), values_all, precision=lax.Precision.HIGHEST)
    attended = low(low_back(attended)).reshape(seq_len, HEADS * HEAD_DIM)
    hidden = low_back(matmul(normed, up_weight) + up_bias)
    activated = low(jax.nn.gelu(hidden, approximate=True))
    attn_branch = matmul(attended, output_weight) + output_bias
    mlp_branch = matmul(activated, down_weight) + down_bias
    return tokens_seq + attn_branch + mlp_branch

def reference(tokens, norm_gain, norm_bias, query_weight, query_bias, key_weight, key_bias, value_weight, value_bias, output_weight, output_bias, up_weight, up_bias, down_weight, down_bias, doc_split, cotangent):
    params_low = (norm_gain, norm_bias, query_weight, query_bias, key_weight, key_bias, value_weight, value_bias, output_weight, output_bias, up_weight, up_bias, down_weight, down_bias)
    params_wide = tuple((array.astype(jnp.float32) for array in params_low))
    checkpointed = jax.checkpoint(one_sequence)

    def forward(tokens_wide, params):
        sequences = tokens_wide.reshape(SEQUENCES, SEQ, D)
        results = lax.map(lambda pair: checkpointed(pair[0], pair[1], params), (sequences, doc_split))
        return results.reshape(TOKENS, D)
    out_wide, pullback = jax.vjp(forward, tokens.astype(jnp.float32), params_wide)
    grad_tokens, grads = pullback(cotangent.astype(jnp.float32))
    grad_norm_gain, grad_norm_bias, grad_query_weight, grad_query_bias, grad_key_weight, grad_key_bias, grad_value_weight, grad_value_bias, grad_output_weight, grad_output_bias, grad_up_weight, grad_up_bias, grad_down_weight, grad_down_bias = grads
    return (out_wide.astype(jnp.bfloat16), grad_tokens, grad_norm_gain, grad_norm_bias, grad_query_weight, grad_query_bias, grad_key_weight, grad_key_bias, grad_value_weight, grad_value_bias, grad_output_weight, grad_output_bias, grad_up_weight, grad_up_bias, grad_down_weight, grad_down_bias)
```

```python
import functools

import jax
import jax.numpy as jnp
from jax import lax
from jax.experimental import pallas as pl
from jax.experimental.pallas import tpu as pltpu
from jax.sharding import Mesh, PartitionSpec as P

HEAD_DIM = 64
ROT = 32
BLOCK = 256
EPS = 1e-05
LANES = 128
F32 = jnp.float32
BF16 = jnp.bfloat16


SWAP = [(0, 1), (1, 0)]
NT = (((1,), (1,)), ((), ()))
TN = (((0,), (0,)), ((), ()))
NN = (((1,), (0,)), ((), ()))


def dot(left, right, dims=NN):
    return lax.dot_general(left, right, dims, preferred_element_type=F32)


def spin(value, cosine, sine):
    lane = lax.broadcasted_iota(jnp.int32, value.shape, 1) % HEAD_DIM
    half = ROT // 2
    ahead = pltpu.roll(value, LANES - half, 1)
    behind = pltpu.roll(value, half, 1)
    return value * cosine + jnp.where(lane < half, ahead, behind) * sine


def attention_kernel(
    split_ref, qkv_ref, grad_ref, cos_ref, sin_ref, att_ref, dqkv_ref,
    q_s, k_s, v_s, g_s, kt_s, vt_s, ot_s, dqt_s, dk_s, dv_s,
):
    seq_len, width = grad_ref.shape
    first = split_ref[pl.program_id(0)] // BLOCK
    scale = HEAD_DIM ** (-0.5)
    per = LANES // HEAD_DIM

    def one_pair(pair, carry):
        def cols(part):
            return pl.ds(pl.multiple_of(part * width + pair * LANES, LANES), LANES)

        cosine, sine = cos_ref[...], sin_ref[...]
        head_of = lax.broadcasted_iota(jnp.int32, (seq_len, LANES), 1) // HEAD_DIM
        query = spin(qkv_ref[:, cols(0)], cosine, sine).astype(BF16)
        key = spin(qkv_ref[:, cols(1)], cosine, sine).astype(BF16)
        value = qkv_ref[:, cols(2)].astype(BF16)
        grad = grad_ref[:, cols(0)]
        kt_s[...] = key.T
        vt_s[...] = value.T
        for head in range(per):
            here = head_of == head
            q_s[head] = jnp.where(here, query, 0).astype(BF16)
            k_s[head] = jnp.where(here, key, 0).astype(BF16)
            v_s[head] = jnp.where(here, value, 0).astype(BF16)
            g_s[head] = jnp.where(here, grad, 0).astype(BF16)
        dk_s[...] = jnp.zeros_like(dk_s)
        dv_s[...] = jnp.zeros_like(dv_s)

        def one_block(block, inner):
            begin = jnp.where(block >= first, first, 0)
            rows = pl.ds(pl.multiple_of(block * BLOCK, BLOCK), BLOCK)

            def work(count):
                span = pl.ds(pl.multiple_of(begin * BLOCK, BLOCK), count * BLOCK)
                dk, dv = None, None
                for head in range(per):
                    q, g = q_s[head, rows, :], g_s[head, rows, :]
                    own = slice(head * HEAD_DIM, (head + 1) * HEAD_DIM)
                    scores = dot(k_s[head, span, :], q, NT) * scale
                    top = jnp.max(scores, 0, keepdims=True)
                    power = jnp.exp(scores - top)
                    prob = power * (1.0 / jnp.sum(power, 0, keepdims=True))
                    low = prob.astype(BF16)
                    ot_s[own, rows] = dot(vt_s[own, span], low)
                    dprob = dot(v_s[head, span, :], g, NT)
                    mean = jnp.sum(prob * dprob, 0, keepdims=True)
                    dscore = (prob * (dprob - mean) * scale).astype(BF16)
                    dqt_s[own, rows] = dot(kt_s[own, span], dscore)
                    dk_h, dv_h = dot(dscore, q), dot(low, g)
                    dk = dk_h if dk is None else dk + dk_h
                    dv = dv_h if dv is None else dv + dv_h
                dk_s[span, :] += dk
                dv_s[span, :] += dv

            for count in range(1, seq_len // BLOCK):
                pl.when(block - begin == count - 1)(functools.partial(work, count))
            return inner

        lax.fori_loop(0, seq_len // BLOCK, one_block, 0)
        att_ref[:, cols(0)] = ot_s[...].T.astype(BF16)
        dqkv_ref[:, cols(0)] = spin(dqt_s[...].T, cosine, -sine).astype(BF16)
        dqkv_ref[:, cols(1)] = spin(dk_s[...], cosine, -sine).astype(BF16)
        dqkv_ref[:, cols(2)] = dv_s[...].astype(BF16)
        return carry

    lax.fori_loop(0, width // LANES, one_pair, 0)


def attention(splits, qkv, grad, cosine, sine):
    count = splits.shape[0]
    rows, width = grad.shape
    seq_len = rows // count
    per = LANES // HEAD_DIM

    def spec(columns):
        return pl.BlockSpec((seq_len, columns), lambda s, split: (s, 0))

    masked = pltpu.VMEM((per, seq_len, LANES), BF16)
    turned = pltpu.VMEM((LANES, seq_len), BF16)
    return pl.pallas_call(
        attention_kernel,
        grid_spec=pltpu.PrefetchScalarGridSpec(
            num_scalar_prefetch=1,
            grid=(count,),
            in_specs=[spec(3 * width), spec(width), spec(LANES), spec(LANES)],
            out_specs=[spec(width), spec(3 * width)],
            scratch_shapes=[
                masked, masked, masked, masked, turned, turned,
                pltpu.VMEM((LANES, seq_len), F32),
                pltpu.VMEM((LANES, seq_len), F32),
                pltpu.VMEM((seq_len, LANES), F32),
                pltpu.VMEM((seq_len, LANES), F32),
            ],
        ),
        out_shape=[
            jax.ShapeDtypeStruct((rows, width), BF16),
            jax.ShapeDtypeStruct((rows, 3 * width), BF16),
        ],
        cost_estimate=pl.CostEstimate(
            flops=40 * rows * seq_len * width // 4,
            transcendentals=rows * seq_len * width // HEAD_DIM // 2,
            bytes_accessed=rows * width * 24,
        ),
        compiler_params=pltpu.CompilerParams(vmem_limit_bytes=48 << 20),
    )(splits, qkv, grad, cosine, sine)


def turn_tables(splits, seq_len):
    shape = (splits.shape[0], seq_len, LANES)
    token = lax.broadcasted_iota(jnp.int32, shape, 1)
    start = splits[:, None, None]
    position = (token - jnp.where(token >= start, start, 0)).astype(F32)
    lane = jnp.arange(LANES, dtype=jnp.int32) % HEAD_DIM
    entry = (lane % (ROT // 2)).astype(F32)
    angle = position * (10000.0 ** (-(2.0 * entry) / ROT))
    cosine = jnp.where(lane < ROT, jnp.cos(angle), 1.0)
    sine = jnp.sin(angle)
    sine = jnp.where(lane < ROT // 2, -sine, jnp.where(lane < ROT, sine, 0.0))
    return cosine.reshape(-1, LANES), sine.reshape(-1, LANES)


def chain_gather(unit, n, z):
    right, left = [None] * n, [None] * n
    going_right = going_left = unit
    for k in range(1, n):
        going_right = lax.ppermute(going_right, "z", [(i, i + 1) for i in range(k - 1, n - 1)])
        going_left = lax.ppermute(going_left, "z", [(i, i - 1) for i in range(1, n - k + 1)])
        right[k], left[k] = going_right, going_left
    return [unit] + [jnp.where(z >= k, right[k], left[n - k]) for k in range(1, n)]


def place(buffer, pieces, n, z, rows_each, offset):
    for k, piece in enumerate(pieces):
        row = lax.rem(z - k + n, n) * rows_each + offset
        buffer = lax.dynamic_update_slice(buffer, piece, (row, jnp.int32(0)))
    return buffer


def chain_scatter(grads, n, z):
    rows = grads.shape[0] // n

    def block(index):
        return lax.dynamic_slice_in_dim(grads, jnp.clip(index, 0, n - 1) * rows, rows, 0)

    def send(index, received, pairs):
        piece = block(index)
        if received is not None:
            piece = (piece.astype(F32) + received.astype(F32)).astype(BF16)
        return lax.ppermute(piece, "z", pairs)

    from_right = from_left = None
    for k in range(n - 1, 0, -1):
        from_right = send(z - k, from_right, [(r, r - 1) for r in range(k, n)])
        from_left = send(z + k, from_left, [(r, r + 1) for r in range(0, n - k)])
    return block(z).astype(F32) + from_right.astype(F32) + from_left.astype(F32)


def plane_gather(block, y, x, c):
    rows = block.shape[0]
    half = rows // 2
    by_x = lax.ppermute(block, "x", SWAP)
    by_y = lax.ppermute(block, "y", SWAP)
    far_top = lax.ppermute(by_y[:half], "x", SWAP)
    far_low = lax.ppermute(by_x[half:], "y", SWAP)
    pieces = [
        (block, y, x, 0), (by_x, y, 1 - x, 0), (by_y, 1 - y, x, 0),
        (far_top, 1 - y, 1 - x, 0), (far_low, 1 - y, 1 - x, half),
    ]
    whole = jnp.zeros((8 * rows, block.shape[1]), block.dtype)
    for piece, row_y, row_x, shift in pieces:
        other = lax.ppermute(piece, "c", SWAP)
        for part, row_c in ((piece, c), (other, 1 - c)):
            row = (row_y * 4 + row_x * 2 + row_c) * rows + shift
            whole = lax.dynamic_update_slice(whole, part, (row, jnp.int32(0)))
    return whole


def pick(array, index, axis):
    return lax.dynamic_index_in_dim(array, index, axis, keepdims=False)


def add_low(left, right):
    return (left.astype(F32) + right.astype(F32)).astype(BF16)


def plane_scatter(partial, y, x, c):
    rows, columns = partial.shape[0] // 8, partial.shape[1]
    half = rows // 2
    parts = partial.reshape(2, 2, 2, rows, columns)
    acc = add_low(pick(parts, c, 2), lax.ppermute(pick(parts, 1 - c, 2), "c", SWAP))
    top, low = acc[:, :, :half], acc[:, :, half:]
    top = add_low(pick(top, x, 1), lax.ppermute(pick(top, 1 - x, 1), "x", SWAP))
    low = add_low(pick(low, y, 0), lax.ppermute(pick(low, 1 - y, 0), "y", SWAP))
    top = pick(top, y, 0).astype(F32) + lax.ppermute(pick(top, 1 - y, 0), "y", SWAP).astype(F32)
    low = pick(low, x, 0).astype(F32) + lax.ppermute(pick(low, 1 - x, 0), "x", SWAP).astype(F32)
    return jnp.concatenate([top, low], 0)


def in_order(y, own, other, axis):
    return jnp.where(
        y == 0, jnp.concatenate([own, other], axis), jnp.concatenate([other, own], axis)
    )


def gelu_tanh(hidden):
    return jax.nn.gelu(hidden, approximate=True)


def on_device(
    n,
    tokens, norm_gain, norm_bias,
    query_weight, query_bias, key_weight, key_bias, value_weight, value_bias,
    output_weight, output_bias, up_weight, up_bias, down_weight, down_bias,
    doc_split, cotangent,
):
    z, y, x, c = (lax.axis_index(name) for name in ("z", "y", "x", "c"))
    shard_rows = query_weight.shape[0]
    width = query_weight.shape[1] // 2
    hidden_width = up_weight.shape[1] // 2
    chunks = 2
    piece = hidden_width // chunks

    def col(array, start, size):
        return lax.dynamic_slice_in_dim(array, start, size, 1)

    def row(array, start, size):
        return lax.dynamic_slice_in_dim(array, start, size, 0)

    def pack_heads(side):
        return jnp.concatenate(
            [col(w, side * width, width) for w in (query_weight, key_weight, value_weight)]
            + [row(output_weight, side * width, width).T],
            1,
        )

    def pack_hidden(side, chunk):
        start = side * hidden_width + chunk * piece
        return jnp.concatenate(
            [col(up_weight, start, piece), row(down_weight, start, piece).T], 1
        )

    heads_own = pack_heads(y)
    heads_other = lax.ppermute(pack_heads(1 - y), "y", SWAP)
    head_weights = jnp.zeros((2 * n * shard_rows, heads_own.shape[1]), BF16)
    for unit, side in ((heads_own, y), (heads_other, 1 - y)):
        head_weights = place(
            head_weights, chain_gather(unit, n, z), n, z, 2 * shard_rows, side * shard_rows
        )
    qkv_weight, output_turned = head_weights[:, : 3 * width], head_weights[:, 3 * width :]

    gain_wide = norm_gain.astype(F32)
    tokens_wide = tokens.astype(F32)
    row_mean = jnp.mean(tokens_wide, -1, keepdims=True)
    centred = tokens_wide - row_mean
    inv_scale = lax.rsqrt(jnp.mean(centred * centred, -1, keepdims=True) + EPS)
    standard = centred * inv_scale
    normed = (standard * gain_wide + norm_bias.astype(F32)).astype(BF16)
    normed_all = plane_gather(normed, y, x, c)
    cot_all = lax.all_gather(cotangent, ("y", "x", "c"), axis=0, tiled=True)

    other_split = lax.ppermute(doc_split, "y", SWAP)
    splits = in_order(y, doc_split, other_split, 0)
    seq_len = normed_all.shape[0] // splits.shape[0]
    cosine, sine = turn_tables(splits, seq_len)

    hidden_weights = []
    for chunk in range(chunks):
        own = pack_hidden(y, chunk)
        other = lax.ppermute(pack_hidden(1 - y, chunk), "y", SWAP)
        unit = in_order(y, own, other, 0)
        buffer = jnp.zeros((2 * n * shard_rows, own.shape[1]), BF16)
        hidden_weights.append(
            place(buffer, chain_gather(unit, n, z), n, z, 2 * shard_rows, jnp.int32(0))
        )

    qkv_bias = jnp.concatenate(
        [row(b, y * width, width) for b in (query_bias, key_bias, value_bias)]
    ).astype(F32)
    qkv = dot(normed_all, qkv_weight) + qkv_bias
    grad_attended = dot(cot_all, output_turned).astype(BF16)
    attended, grad_qkv = attention(splits, qkv, grad_attended, cosine, sine)
    grads_heads = jnp.concatenate(
        [dot(normed_all, grad_qkv, TN).astype(BF16), dot(cot_all, attended, TN).astype(BF16)], 1
    )
    heads_sum = chain_scatter(grads_heads, n, z)
    partial_out = dot(attended, output_turned, NT)
    grad_normed_part = dot(grad_qkv, qkv_weight, NT)
    bias_parts = [jnp.sum(grad_qkv, 0, dtype=F32)]

    hidden_sums = []
    for chunk in range(chunks):
        weights = hidden_weights[chunk]
        up, down_turned = weights[:, :piece], weights[:, piece:]
        hidden = dot(normed_all, up) + row(up_bias, y * hidden_width + chunk * piece, piece).astype(F32)
        activated = gelu_tanh(hidden).astype(BF16)
        grad_activated = dot(cot_all, down_turned)
        grad_hidden = jax.vjp(gelu_tanh, hidden)[1](grad_activated)[0].astype(BF16)
        grads = jnp.concatenate(
            [dot(normed_all, grad_hidden, TN).astype(BF16), dot(cot_all, activated, TN).astype(BF16)],
            1,
        )
        hidden_sums.append(chain_scatter(grads, n, z))
        grad_normed_part = grad_normed_part + dot(grad_hidden, up, NT)
        partial_out = partial_out + dot(activated, down_turned, NT)
        bias_parts.append(jnp.sum(grad_hidden, 0, dtype=F32))

    grad_normed = plane_scatter(grad_normed_part.astype(BF16), y, x, c)
    mixed = lax.psum_scatter(
        partial_out.astype(BF16), ("y", "x", "c"), scatter_dimension=0, tiled=True
    ).astype(F32)
    out_bias = output_bias.astype(F32) + down_bias.astype(F32)
    out = (tokens_wide + mixed + out_bias).astype(BF16)

    def halves(total):
        keep = row(total, y * shard_rows, shard_rows)
        give = row(total, (1 - y) * shard_rows, shard_rows).astype(BF16)
        return keep, lax.ppermute(give, "y", SWAP).astype(F32)

    heads_keep, heads_take = halves(heads_sum)

    def joined(start, size):
        return in_order(
            y, heads_keep[:, start : start + size], heads_take[:, start : start + size], 1
        )

    grad_query_weight, grad_key_weight, grad_value_weight, grad_output_turned = (
        joined(part * width, width) for part in range(4)
    )
    hidden_halves = [halves(total) for total in hidden_sums]

    def side(which, start):
        return jnp.concatenate([pair[which][:, start : start + piece] for pair in hidden_halves], 1)

    grad_up_weight = in_order(y, side(0, 0), side(1, 0), 1)
    grad_down_turned = in_order(y, side(0, piece), side(1, piece), 1)

    bias_row = jnp.concatenate(bias_parts)[None]
    bias_rows = jnp.where(lax.broadcasted_iota(jnp.int32, (2, 1), 0) == y, bias_row, 0.0)
    bias_rows = lax.psum(bias_rows, ("z", "y"))
    grad_query_bias, grad_key_bias, grad_value_bias = (
        bias_rows[:, part * width : (part + 1) * width].reshape(-1) for part in range(3)
    )
    grad_up_bias = bias_rows[:, 3 * width :].reshape(-1)

    cot_wide = cotangent.astype(F32)
    grad_scaled = grad_normed * gain_wide
    grad_tokens = cot_wide + inv_scale * (
        grad_scaled
        - jnp.mean(grad_scaled, -1, keepdims=True)
        - standard * jnp.mean(grad_scaled * standard, -1, keepdims=True)
    )
    grad_norm_gain, grad_norm_bias, grad_out_bias = lax.psum(
        (jnp.sum(grad_normed * standard, 0), jnp.sum(grad_normed, 0), jnp.sum(cot_wide, 0)),
        ("z", "y", "x", "c"),
    )
    return (
        out, grad_tokens, grad_norm_gain, grad_norm_bias,
        grad_query_weight, grad_query_bias, grad_key_weight, grad_key_bias,
        grad_value_weight, grad_value_bias, grad_output_turned.T, grad_out_bias,
        grad_up_weight, grad_up_bias, grad_down_turned.T, grad_out_bias,
    )


def solution(mesh):
    n = mesh.shape["dp"] // 2
    grid = Mesh(mesh.devices.reshape(n, 2, mesh.shape["tensor"] // 2, 2), ("z", "y", "x", "c"))
    dp, tensor = ("z", "y"), ("x", "c")
    rows = P(dp + tensor, None)
    whole, split = P(), P(tensor)
    wide, tall = P(dp, tensor), P(tensor, dp)
    in_specs = (
        rows, whole, whole, wide, split, wide, split, wide, split,
        tall, whole, wide, split, tall, whole, P(dp), rows,
    )
    out_specs = (
        rows, rows, whole, whole, wide, split, wide, split, wide, split,
        tall, whole, wide, split, tall, whole,
    )
    return jax.shard_map(
        functools.partial(on_device, n),
        mesh=grid, in_specs=in_specs, out_specs=out_specs, check_vma=False,
    )
```

```python
import functools

import jax
import jax.numpy as jnp
from jax import lax
from jax.experimental import pallas as pl
from jax.experimental.pallas import tpu as pltpu
from jax.sharding import Mesh, PartitionSpec as P

HEAD_DIM = 64
ROT = 32
BLOCK = 256
EPS = 1e-05
LANES = 128
F32 = jnp.float32
BF16 = jnp.bfloat16


SWAP = [(0, 1), (1, 0)]
NT = (((1,), (1,)), ((), ()))
TN = (((0,), (0,)), ((), ()))
NN = (((1,), (0,)), ((), ()))


def dot(left, right, dims=NN):
    return lax.dot_general(left, right, dims, preferred_element_type=F32)


def spin(value, cosine, sine):
    lane = lax.broadcasted_iota(jnp.int32, value.shape, 1) % HEAD_DIM
    half = ROT // 2
    ahead = pltpu.roll(value, LANES - half, 1)
    behind = pltpu.roll(value, half, 1)
    return value * cosine + jnp.where(lane < half, ahead, behind) * sine


def attention_kernel(
    split_ref, qkv_ref, grad_ref, cos_ref, sin_ref, att_ref, dqkv_ref,
    q_s, k_s, v_s, g_s, kt_s, vt_s, ot_s, dqt_s, dk_s, dv_s, cos_s, sin_s,
):
    seq_len, width = grad_ref.shape
    first = split_ref[pl.program_id(0)] // BLOCK
    scale = HEAD_DIM ** (-0.5)
    per = LANES // HEAD_DIM
    rest = jnp.zeros((HEAD_DIM - ROT, seq_len), F32)
    cos_part, sin_part = cos_ref[...], sin_ref[...]
    cos_s[...] = jnp.concatenate([cos_part, cos_part, rest + 1.0] * per, 0).T
    sin_s[...] = jnp.concatenate([-sin_part, sin_part, rest] * per, 0).T

    def one_pair(pair, carry):
        def cols(part):
            return pl.ds(pl.multiple_of(part * width + pair * LANES, LANES), LANES)

        cosine, sine = cos_s[...], sin_s[...]
        head_of = lax.broadcasted_iota(jnp.int32, (seq_len, LANES), 1) // HEAD_DIM
        query = spin(qkv_ref[:, cols(0)], cosine, sine).astype(BF16)
        key = spin(qkv_ref[:, cols(1)], cosine, sine).astype(BF16)
        value = qkv_ref[:, cols(2)].astype(BF16)
        grad = grad_ref[:, cols(0)]
        kt_s[...] = key.T
        vt_s[...] = value.T
        for head in range(per):
            here = head_of == head
            q_s[head] = jnp.where(here, query, 0).astype(BF16)
            k_s[head] = jnp.where(here, key, 0).astype(BF16)
            v_s[head] = jnp.where(here, value, 0).astype(BF16)
            g_s[head] = jnp.where(here, grad, 0).astype(BF16)
        dk_s[...] = jnp.zeros_like(dk_s)
        dv_s[...] = jnp.zeros_like(dv_s)

        def one_block(block, inner):
            begin = jnp.where(block >= first, first, 0)
            rows = pl.ds(pl.multiple_of(block * BLOCK, BLOCK), BLOCK)

            def work(count):
                span = pl.ds(pl.multiple_of(begin * BLOCK, BLOCK), count * BLOCK)
                dk, dv = None, None
                for head in range(per):
                    q, g = q_s[head, rows, :], g_s[head, rows, :]
                    own = slice(head * HEAD_DIM, (head + 1) * HEAD_DIM)
                    scores = dot(k_s[head, span, :], q, NT) * scale
                    top = jnp.max(scores, 0, keepdims=True)
                    power = jnp.exp(scores - top)
                    prob = power * (1.0 / jnp.sum(power, 0, keepdims=True))
                    low = prob.astype(BF16)
                    ot_s[own, rows] = dot(vt_s[own, span], low)
                    dprob = dot(v_s[head, span, :], g, NT)
                    mean = jnp.sum(prob * dprob, 0, keepdims=True)
                    dscore = (prob * (dprob - mean) * scale).astype(BF16)
                    dqt_s[own, rows] = dot(kt_s[own, span], dscore)
                    dk_h, dv_h = dot(dscore, q), dot(low, g)
                    dk = dk_h if dk is None else dk + dk_h
                    dv = dv_h if dv is None else dv + dv_h
                dk_s[span, :] += dk
                dv_s[span, :] += dv

            for count in range(1, seq_len // BLOCK):
                pl.when(block - begin == count - 1)(functools.partial(work, count))
            return inner

        lax.fori_loop(0, seq_len // BLOCK, one_block, 0)
        att_ref[:, cols(0)] = ot_s[...].T.astype(BF16)
        dqkv_ref[:, cols(0)] = spin(dqt_s[...].T, cosine, -sine).astype(BF16)
        dqkv_ref[:, cols(1)] = spin(dk_s[...], cosine, -sine).astype(BF16)
        dqkv_ref[:, cols(2)] = dv_s[...].astype(BF16)
        return carry

    lax.fori_loop(0, width // LANES, one_pair, 0)


def attention(splits, qkv, grad, cosine, sine):
    count = splits.shape[0]
    rows, width = grad.shape
    seq_len = rows // count
    per = LANES // HEAD_DIM

    def spec(columns):
        return pl.BlockSpec((seq_len, columns), lambda s, split: (s, 0))

    table = pl.BlockSpec((ROT // 2, seq_len), lambda s, split: (0, s))
    masked = pltpu.VMEM((per, seq_len, LANES), BF16)
    turned = pltpu.VMEM((LANES, seq_len), BF16)
    return pl.pallas_call(
        attention_kernel,
        grid_spec=pltpu.PrefetchScalarGridSpec(
            num_scalar_prefetch=1,
            grid=(count,),
            in_specs=[spec(3 * width), spec(width), table, table],
            out_specs=[spec(width), spec(3 * width)],
            scratch_shapes=[
                masked, masked, masked, masked, turned, turned,
                pltpu.VMEM((LANES, seq_len), F32),
                pltpu.VMEM((LANES, seq_len), F32),
                pltpu.VMEM((seq_len, LANES), F32),
                pltpu.VMEM((seq_len, LANES), F32),
                pltpu.VMEM((seq_len, LANES), F32),
                pltpu.VMEM((seq_len, LANES), F32),
            ],
        ),
        out_shape=[
            jax.ShapeDtypeStruct((rows, width), BF16),
            jax.ShapeDtypeStruct((rows, 3 * width), BF16),
        ],
        cost_estimate=pl.CostEstimate(
            flops=40 * rows * seq_len * width // 4,
            transcendentals=rows * seq_len * width // HEAD_DIM // 2,
            bytes_accessed=rows * width * 24,
        ),
        compiler_params=pltpu.CompilerParams(vmem_limit_bytes=48 << 20),
    )(splits, qkv, grad, cosine, sine)


def turn_tables(splits, seq_len):
    shape = (ROT // 2, splits.shape[0], seq_len)
    token = lax.broadcasted_iota(jnp.int32, shape, 2)
    start = splits[None, :, None]
    position = (token - jnp.where(token >= start, start, 0)).astype(F32)
    entry = jnp.arange(ROT // 2, dtype=F32)
    angle = position * (10000.0 ** (-(2.0 * entry) / ROT))[:, None, None]
    return jnp.cos(angle).reshape(ROT // 2, -1), jnp.sin(angle).reshape(ROT // 2, -1)


def sum_dots_kernel(count, *refs):
    out_ref = refs[-1]
    total = None
    for i in range(count):
        part = dot(refs[i][...], refs[count + i][...], NT)
        total = part if total is None else total + part
    out_ref[...] = total.astype(out_ref.dtype)


def sum_dots(lefts, rights, tile=512):
    rows, columns = lefts[0].shape[0], rights[0][0].shape[0]
    tile = min(tile, rows)
    depth = sum(left.shape[1] for left in lefts)
    return pl.pallas_call(
        functools.partial(sum_dots_kernel, len(lefts)),
        grid=(rows // tile,),
        in_specs=[pl.BlockSpec((tile, left.shape[1]), lambda i: (i, 0)) for left in lefts] + [
            pl.BlockSpec((columns, size), functools.partial(lambda at, i: (0, at), at))
            for _, size, at in rights
        ],
        out_specs=pl.BlockSpec((tile, columns), lambda i: (i, 0)),
        out_shape=jax.ShapeDtypeStruct((rows, columns), BF16),
        cost_estimate=pl.CostEstimate(
            flops=2 * rows * columns * depth, transcendentals=0,
            bytes_accessed=2 * (rows * columns + depth * (rows + columns)),
        ),
        compiler_params=pltpu.CompilerParams(vmem_limit_bytes=56 << 20),
        name="sum_dots",
    )(*lefts, *(right[0] for right in rights))


def hidden_kernel(n_ref, c_ref, w_ref, bias_ref, act_ref, dh_ref, sum_ref):
    piece = act_ref.shape[1]
    hidden = dot(n_ref[...], w_ref[:, :piece]) + bias_ref[...]
    grad = dot(c_ref[...], w_ref[:, piece:])
    rate = (2.0 / jnp.pi) ** 0.5
    square = hidden * hidden
    bent = jnp.tanh(rate * hidden * (1.0 + 0.044715 * square))
    act_ref[...] = (0.5 * hidden * (1.0 + bent)).astype(BF16)
    slope = 0.5 * (1.0 + bent) + 0.5 * hidden * (1.0 - bent * bent) * (
        rate * (1.0 + 3.0 * 0.044715 * square)
    )
    low = (grad * slope).astype(BF16)
    dh_ref[...] = low

    @pl.when(pl.program_id(0) == 0)
    def _():
        sum_ref[...] = jnp.zeros_like(sum_ref)

    sum_ref[...] += jnp.sum(low.astype(F32), 0, keepdims=True)


def hidden_part(normed_all, cot_all, weights, bias, tile=512):
    rows, depth = normed_all.shape
    piece = weights.shape[1] // 2
    tile = min(tile, rows)
    wide = pl.BlockSpec((tile, depth), lambda i: (i, 0))
    thin = pl.BlockSpec((tile, piece), lambda i: (i, 0))
    line = pl.BlockSpec((1, piece), lambda i: (0, 0))
    return pl.pallas_call(
        hidden_kernel,
        grid=(rows // tile,),
        in_specs=[wide, wide, pl.BlockSpec(weights.shape, lambda i: (0, 0)), line],
        out_specs=[thin, thin, line],
        out_shape=[
            jax.ShapeDtypeStruct((rows, piece), BF16),
            jax.ShapeDtypeStruct((rows, piece), BF16),
            jax.ShapeDtypeStruct((1, piece), F32),
        ],
        cost_estimate=pl.CostEstimate(
            flops=4 * rows * depth * piece, transcendentals=rows * piece,
            bytes_accessed=4 * rows * depth + 4 * depth * piece + 4 * rows * piece,
        ),
        compiler_params=pltpu.CompilerParams(vmem_limit_bytes=48 << 20),
        name="hidden_part",
    )(normed_all, cot_all, weights, bias)


def gather_kernel(
    n, own_ref, other_ref, second_ref, second_other_ref, next_ref, norm_ref, cot_ref,
    w_ref, unit_ref, right_ref, left_ref, swapped_ref, n_ref, c_ref, send_sem, recv_sem, local_sem,
):
    z, y, x, c = (lax.axis_index(name) for name in ("z", "y", "x", "c"))
    rows = norm_ref.shape[0]
    half = 3 * rows // 4
    mine = y * 4 + x * 2 + c
    has_right, has_left = z < n - 1, z > 0
    number = {}

    def remote(key, src, dst, axis, target):
        slot = number.setdefault(key, len(number))
        return pltpu.make_async_remote_copy(
            src_ref=src, dst_ref=dst, send_sem=send_sem.at[slot], recv_sem=recv_sem.at[slot],
            device_id={axis: target}, device_id_type=pl.DeviceIdType.MESH,
        )

    def when(condition, action):
        if condition is None:
            action()
        else:
            pl.when(condition)(action)

    started = []

    def start(condition, copy):
        when(condition, copy.start)
        started.append((condition, copy))

    def shard(index, unit):
        return w_ref.at[index * 2 + (y if unit == 0 else 1 - y)]

    def along(step, unit, sign, receiving=False):
        index = z - sign * step if receiving else z - sign * (step - 1)
        source = own_ref if step == 1 and unit == 0 and not receiving else shard(index, unit)
        return remote((step, unit, sign), source, shard(index, unit), "z", z + sign)


    full, top, low = pl.ds(0, rows), pl.ds(0, half), pl.ds(half, rows - half)
    arrays = ((n_ref, norm_ref, "n"), (c_ref, cot_ref, "c"))
    at_x, at_y, at_xy = y * 4 + (1 - x) * 2 + c, (1 - y) * 4 + x * 2 + c, (1 - y) * 4 + (1 - x) * 2 + c

    barrier = pltpu.get_barrier_semaphore()
    for axis, target in (("x", 1 - x), ("y", 1 - y), ("c", 1 - c)):
        pl.semaphore_signal(
            barrier, inc=1, device_id={axis: target}, device_id_type=pl.DeviceIdType.MESH
        )
    for condition, target in ((has_right, z + 1), (has_left, z - 1)):
        when(condition, functools.partial(
            pl.semaphore_signal, barrier, inc=1, device_id={"z": target},
            device_id_type=pl.DeviceIdType.MESH,
        ))
    pl.semaphore_wait(barrier, 3 + has_right.astype(jnp.int32) + has_left.astype(jnp.int32))

    for condition, sign in ((has_right, 1), (has_left, -1)):
        start(condition, along(1, 0, sign))
    swap = remote("swap", other_ref, w_ref.at[z * 2 + y], "y", 1 - y)
    swap_in = remote("swap", other_ref, w_ref.at[z * 2 + 1 - y], "y", 1 - y)
    start(None, swap)
    for array, source, name in arrays:
        for axis in ("x", "y", "c"):
            start(None, remote((name, axis), source, array.at[mine], axis,
                               {"x": 1 - x, "y": 1 - y, "c": 1 - c}[axis]))
    unit_swap = remote("unit", second_other_ref, unit_ref.at[y], "y", 1 - y)
    unit_swap_in = remote("unit", second_other_ref, unit_ref.at[1 - y], "y", 1 - y)
    start(None, unit_swap)
    late_swap = remote("late", next_ref, swapped_ref, "y", 1 - y)
    start(None, late_swap)
    local = [
        pltpu.make_async_copy(own_ref, shard(z, 0), local_sem.at[0]),
        pltpu.make_async_copy(norm_ref, n_ref.at[mine], local_sem.at[1]),
        pltpu.make_async_copy(cot_ref, c_ref.at[mine], local_sem.at[2]),
        pltpu.make_async_copy(second_ref, unit_ref.at[y], local_sem.at[3]),
    ]
    for copy in local:
        copy.start()

    def arrive_swap():
        swap_in.wait_recv()
        for condition, sign in ((has_right, 1), (has_left, -1)):
            start(condition, along(1, 1, sign))

    def arrive_shard(step, unit, sign):
        inside = z - sign * step >= 0 if sign > 0 else z + step < n
        further = has_right if sign > 0 else has_left
        when(inside, along(step, unit, sign, True).wait_recv)
        if step + 1 < n:
            start(inside & further, along(step + 1, unit, sign))

    def arrive_rows(array, name, axis):
        index = {"x": at_x, "y": at_y, "c": None}[axis]
        block = array.at[index]
        remote((name, axis), block, block, axis, 0).wait_recv()
        part, on = (low, "y") if axis == "x" else (top, "x")
        piece = array.at[index, part]
        start(None, remote((name, "far", on), piece, piece, on, {"x": 1 - x, "y": 1 - y}[on]))
        start(None, remote((name, "core", axis), block, block, "c", 1 - c))

    def arrive_far(array, name, on):
        part = low if on == "y" else top
        piece = array.at[at_xy, part]
        remote((name, "far", on), piece, piece, on, 0).wait_recv()
        start(None, remote((name, "core", "far", on), piece, piece, "c", 1 - c))

    def arrive_steps(step):
        for unit in (0, 1):
            for sign in (1, -1):
                arrive_shard(step, unit, sign)

    def second_step(half_of, receiving):
        index = y if half_of == 0 else 1 - y
        source = second_ref if half_of == 0 else unit_ref.at[index]
        ways = ((1, has_left if receiving else has_right, right_ref),
                (-1, has_right if receiving else has_left, left_ref))
        for sign, condition, target in ways:
            copy = remote(("second", half_of, sign), source, target.at[index], "z", z + sign)
            if receiving:
                when(condition, copy.wait_recv)
            else:
                start(condition, copy)

    (norm, _, norm_name), (cot, _, cot_name) = arrays
    arrive_swap()
    arrive_rows(norm, norm_name, "x")
    for sign in (1, -1):
        arrive_shard(1, 0, sign)
    arrive_rows(norm, norm_name, "y")
    for sign in (1, -1):
        arrive_shard(1, 1, sign)
    arrive_rows(cot, cot_name, "x")
    if n > 2:
        arrive_steps(2)
    second_step(0, False)
    arrive_rows(cot, cot_name, "y")
    unit_swap_in.wait_recv()
    second_step(1, False)
    for step in range(3, n):
        arrive_steps(step)
    for array, _, name in arrays:
        for on in ("x", "y"):
            arrive_far(array, name, on)
    for array, _, name in arrays:
        for key, index, part in (
            ((name, "c"), y * 4 + x * 2 + 1 - c, full),
            ((name, "core", "x"), y * 4 + (1 - x) * 2 + 1 - c, full),
            ((name, "core", "y"), (1 - y) * 4 + x * 2 + 1 - c, full),
            ((name, "core", "far", "x"), (1 - y) * 4 + (1 - x) * 2 + 1 - c, top),
            ((name, "core", "far", "y"), (1 - y) * 4 + (1 - x) * 2 + 1 - c, low),
        ):
            piece = array.at[index, part]
            remote(key, piece, piece, "c", 0).wait_recv()
    late_swap.wait_recv()
    for half_of in (0, 1):
        second_step(half_of, True)
    for copy in local:
        copy.wait()
    for condition, copy in started:
        when(condition, copy.wait_send)


def gather_all(n, own, other, second, second_other, following, normed, cotangent):
    rows, columns = normed.shape
    copies = 4 * (n - 1) + 8 + 2 * 9
    anywhere = pl.BlockSpec(memory_space=pl.ANY)
    pair = jax.ShapeDtypeStruct((2,) + second.shape, second.dtype)
    weights, unit, right, left, swapped, normed_all, cot_all = pl.pallas_call(
        functools.partial(gather_kernel, n),
        in_specs=[anywhere] * 7,
        out_specs=[anywhere] * 7,
        out_shape=[
            jax.ShapeDtypeStruct((2 * n,) + own.shape, own.dtype),
            pair, pair, pair,
            jax.ShapeDtypeStruct(following.shape, following.dtype),
            jax.ShapeDtypeStruct((8, rows, columns), normed.dtype),
            jax.ShapeDtypeStruct((8, rows, columns), cotangent.dtype),
        ],
        scratch_shapes=[
            pltpu.SemaphoreType.DMA((copies,)),
            pltpu.SemaphoreType.DMA((copies,)),
            pltpu.SemaphoreType.DMA((4,)),
        ],
        cost_estimate=pl.CostEstimate(flops=0, transcendentals=0, bytes_accessed=200 << 20),
        compiler_params=pltpu.CompilerParams(collective_id=0, has_side_effects=True),
        name="gather_rows",
    )(own, other, second, second_other, following, normed, cotangent)
    flat = lambda array: array.reshape(-1, array.shape[-1])
    return tuple(map(flat, (weights, unit, right, left, swapped, normed_all, cot_all)))


def chain_step(step, n, right, left):
    return (
        lax.ppermute(right, "z", [(i, i + 1) for i in range(step - 1, n - 1)]),
        lax.ppermute(left, "z", [(i, i - 1) for i in range(1, n - step + 1)]),
    )


def assemble(unit, right, left, n, z):
    rows, columns = unit.shape
    whole = jnp.zeros((n * rows, columns), unit.dtype)
    for k in range(n):
        piece = unit if k == 0 else jnp.where(z >= k, right[k], left[n - k])
        row = lax.rem(z - k + n, n) * rows
        whole = lax.dynamic_update_slice(whole, piece, (row, jnp.int32(0)))
    return whole


def scatter_step(k, grads, n, z, received):
    rows = grads.shape[0] // n

    def send(index, got, pairs):
        piece = lax.dynamic_slice_in_dim(grads, jnp.clip(index, 0, n - 1) * rows, rows, 0)
        if got is not None:
            piece = add_low(piece, got)
        return lax.ppermute(piece, "z", pairs)

    from_right, from_left = received
    return (
        send(z - k, from_right, [(r, r - 1) for r in range(k, n)]),
        send(z + k, from_left, [(r, r + 1) for r in range(0, n - k)]),
    )


def scatter_end(grads, n, z, received):
    rows = grads.shape[0] // n
    own = lax.dynamic_slice_in_dim(grads, z * rows, rows, 0).astype(F32)
    return own + received[0].astype(F32) + received[1].astype(F32)


def tail_kernel(
    n, g_ref, dn_ref, po_ref, std_ref, vec_ref, keep_ref, take_ref, out_ref, mixed_ref, sums_ref,
    zrecv, zstage, total, give, own_2, crecv_2, xtop_2, ylow_2, ytop_2, xlow_2, top_2, low_2,
    vstage, vrecv, send_sem, recv_sem, local_sem,
):
    z, y, x, c = (lax.axis_index(name) for name in ("z", "y", "x", "c"))
    rows = out_ref.shape[0]
    half = rows // 2
    number, started = {}, []

    def remote(key, src, dst, axis, target):
        slot = number.setdefault(key, len(number))
        return pltpu.make_async_remote_copy(
            src_ref=src, dst_ref=dst, send_sem=send_sem.at[slot], recv_sem=recv_sem.at[slot],
            device_id={axis: target}, device_id_type=pl.DeviceIdType.MESH,
        )

    def when(condition, action):
        if condition is None:
            action()
        else:
            pl.when(condition)(action)

    def start(condition, copy):
        when(condition, copy.start)
        started.append((condition, copy))

    def each(count, size, body):
        def step(i, carry):
            body(pl.ds(pl.multiple_of(i * size, size), size))
            return carry
        lax.fori_loop(0, count // size, step, 0)

    barrier = pltpu.get_barrier_semaphore()
    greet = [(None, "x", 1 - x), (None, "y", 1 - y), (None, "c", 1 - c)]
    greet += [(z < n - 1, "z", z + 1), (z > 0, "z", z - 1)]
    for step in (2 ** i for i in range(1, n.bit_length() - 1)):
        greet.append((None, "z", jnp.bitwise_xor(z, step)))
    for condition, axis, target in greet:
        when(condition, functools.partial(
            pl.semaphore_signal, barrier, inc=1, device_id={axis: target},
            device_id_type=pl.DeviceIdType.MESH))
    always = sum(condition is None for condition, _, _ in greet)
    pl.semaphore_wait(barrier, always + sum(
        condition.astype(jnp.int32) for condition, _, _ in greet if condition is not None))

    sides = (1 - y, y)

    local = {}

    def core_send(a):
        source = (dn_ref, po_ref)[a]
        for i in range(4):
            block = (i // 2) * 4 + (i % 2) * 2
            start(None, remote(
                ("core", a, i), source.at[block + 1 - c], crecv_2.at[a, i], "c", 1 - c))
            local[a, i] = pltpu.make_async_copy(
                source.at[block + c], own_2.at[a, i], local_sem.at[a * 4 + i])
            local[a, i].start()

    def first_copy(a, name, j):
        if name == "xtop":
            source = own_2.at[a, j * 2 + 1 - x, pl.ds(0, half)]
            return remote((name, a, j), source, xtop_2.at[a, j], "x", 1 - x)
        source = own_2.at[a, (1 - y) * 2 + j, pl.ds(half, half)]
        return remote((name, a, j), source, ylow_2.at[a, j], "y", 1 - y)

    def second_copy(a, name):
        if name == "ytop":
            return remote((name, a), top_2.at[a], ytop_2.at[a], "y", 1 - y)
        return remote((name, a), low_2.at[a], xlow_2.at[a], "x", 1 - x)

    def core_arrive(a):
        for i in range(4):
            local[a, i].wait()
            remote(("core", a, i), crecv_2.at[a, i], crecv_2.at[a, i], "c", 1 - c).wait_recv()

            def body(part, i=i):
                own_2[a, i, part, :] = (
                    own_2[a, i, part, :].astype(F32) + crecv_2[a, i, part, :].astype(F32)
                ).astype(BF16)

            each(rows, 32, body)
        for j in (0, 1):
            start(None, first_copy(a, "xtop", j))
            start(None, first_copy(a, "ylow", j))

    def first_arrive(a):
        for j in (0, 1):
            first_copy(a, "xtop", j).wait_recv()
            first_copy(a, "ylow", j).wait_recv()

        def body(part):
            low_part = pl.ds(part.start + half, part.size)
            top_2[a, part, :] = (
                own_2[a, (1 - y) * 2 + x, part, :].astype(F32)
                + xtop_2[a, 1 - y, part, :].astype(F32)
            ).astype(BF16)
            low_2[a, part, :] = (
                own_2[a, y * 2 + 1 - x, low_part, :].astype(F32)
                + ylow_2[a, 1 - x, part, :].astype(F32)
            ).astype(BF16)

        each(half, 32, body)
        start(None, second_copy(a, "ytop"))
        start(None, second_copy(a, "xlow"))

    def second_arrive(a):
        second_copy(a, "ytop").wait_recv()
        second_copy(a, "xlow").wait_recv()
        target = (out_ref, mixed_ref)[a]

        def joined(left, right, last):
            return left.astype(F32) + right.astype(F32) + last.astype(F32)

        def body(part):
            low_part = pl.ds(part.start + half, part.size)
            top = joined(own_2[a, y * 2 + x, part, :], xtop_2[a, y, part, :], ytop_2[a, part, :])
            low = joined(
                own_2[a, y * 2 + x, low_part, :], ylow_2[a, x, part, :], xlow_2[a, part, :])
            target[part, :] = top
            target[low_part, :] = low
            if a == 0:
                scaled = top * std_ref[part, :] + low * std_ref[low_part, :]
                vstage[0, 0:1, :] += jnp.sum(scaled, 0, keepdims=True)
                vstage[0, 1:2, :] += jnp.sum(top + low, 0, keepdims=True)

        each(half, 16, body)

    core_send(0)

    def mine(direction, k):
        return z - k if direction == 0 else z + k

    def z_copy(direction, k, u, src):
        target = z - 1 if direction == 0 else z + 1
        return remote((direction, k, u), src, zrecv.at[direction, k - 1, u], "z", target)

    def z_first(direction):
        edge = z == n - 1 if direction == 0 else z == 0
        for k in range(n - 1, 0, -1):
            for u in (0, 1):
                start(edge, z_copy(direction, k, u, g_ref.at[mine(direction, k) * 2 + sides[u]]))

    def z_step(k, u):
        for direction in (0, 1):
            if direction == 0:
                inside = (z >= k) & (z < n - 1)
            else:
                inside = (n - 1 - z >= k) & (z > 0)
            stage = zstage.at[direction, k - 1, u]

            def add():
                z_copy(direction, k + 1, u, stage).wait_recv()
                block = mine(direction, k) * 2 + sides[u]

                def body(part):
                    stage[part, :] = (
                        g_ref[block, part, :].astype(F32)
                        + zrecv[direction, k, u, part, :].astype(F32)
                    ).astype(BF16)

                each(rows, 64, body)

            when(inside, add)
            start(inside, z_copy(direction, k, u, stage))

    def z_last(u, target):
        def first(part):
            target[part, :] = g_ref[z * 2 + sides[u], part, :].astype(F32)

        each(rows, 64, first)
        for direction in (0, 1):
            def add():
                z_copy(direction, 1, u, zstage.at[direction, 0, u]).wait_recv()

                def body(part):
                    target[part, :] += zrecv[direction, 0, u, part, :].astype(F32)

                each(rows, 64, body)

            when(z < n - 1 if direction == 0 else z > 0, add)

    for direction in (0, 1):
        z_first(direction)

    core_send(1)
    vstage[0] = vec_ref[...]
    core_arrive(0)
    if n > 2:
        for u in (0, 1):
            z_step(n - 2, u)
    first_arrive(0)
    core_arrive(1)
    for k in range(n - 3, 0, -1):
        for u in (0, 1):
            z_step(k, u)
    second_arrive(0)

    steps = [("z", jnp.bitwise_xor(z, 2 ** i)) for i in range(n.bit_length() - 1)]
    steps += [("y", 1 - y), ("x", 1 - x), ("c", 1 - c)]
    line = lax.broadcasted_iota(jnp.int32, vec_ref.shape, 0)
    for i, (axis, target) in enumerate(steps):
        copy = remote(("vec", i), vstage.at[i], vrecv.at[i], axis, target)
        start(None, copy)
        copy.wait_recv()
        old, new = vstage[i], vrecv[i]
        joined = old + jnp.where((line < 3) | (axis == "z"), new, 0.0)
        result = sums_ref if i == len(steps) - 1 else vstage.at[i + 1]
        result[...] = joined
        if axis == "y":
            result[4:5, :] = new[3:4, :]

    first_arrive(1)
    z_last(0, total)

    def lower(part):
        give[part, :] = total[part, :].astype(BF16)

    each(rows, 64, lower)
    swap = remote("swap", give, take_ref, "y", 1 - y)
    start(None, swap)
    z_last(1, keep_ref)
    second_arrive(1)
    swap.wait_recv()
    for condition, copy in started:
        when(condition, copy.wait_send)


def tail(n, grads, partial, partial_out, standard, vector):
    rows, columns = standard.shape
    wide = grads.shape[1]
    inside = pl.BlockSpec(memory_space=pltpu.VMEM)
    copies = 4 * (n - 1) + 40
    anywhere = pl.BlockSpec(memory_space=pl.ANY)
    low = lambda *shape: pltpu.VMEM(shape, BF16)
    small = vector.shape
    return pl.pallas_call(
        functools.partial(tail_kernel, n),
        in_specs=[inside, anywhere, anywhere, inside, inside],
        out_specs=[inside] * 5,
        out_shape=[
            jax.ShapeDtypeStruct((rows, wide), F32),
            jax.ShapeDtypeStruct((rows, wide), BF16),
            jax.ShapeDtypeStruct((rows, columns), F32),
            jax.ShapeDtypeStruct((rows, columns), F32),
            jax.ShapeDtypeStruct(small, F32),
        ],
        scratch_shapes=[
            low(2, n - 1, 2, rows, wide), low(2, n - 1, 2, rows, wide),
            pltpu.VMEM((rows, wide), F32), low(rows, wide),
            low(2, 4, rows, columns), low(2, 4, rows, columns),
            low(2, 2, rows // 2, columns), low(2, 2, rows // 2, columns),
            low(2, rows // 2, columns), low(2, rows // 2, columns),
            low(2, rows // 2, columns), low(2, rows // 2, columns),
            pltpu.VMEM((8,) + small, F32), pltpu.VMEM((8,) + small, F32),
            pltpu.SemaphoreType.DMA((copies,)),
            pltpu.SemaphoreType.DMA((copies,)),
            pltpu.SemaphoreType.DMA((8,)),
        ],
        cost_estimate=pl.CostEstimate(flops=0, transcendentals=0, bytes_accessed=200 << 20),
        compiler_params=pltpu.CompilerParams(
            collective_id=1, has_side_effects=True, vmem_limit_bytes=62 << 20
        ),
        name="scatter_rest",
    )(
        grads.reshape(2 * n, rows, wide), partial.reshape(8, rows, columns),
        partial_out.reshape(8, rows, columns), standard, vector,
    )


def sum_small(array, axes):
    for axis in axes:
        size = lax.axis_size(axis)
        if size & (size - 1):
            array = lax.psum(array, axis)
            continue
        step = 1
        while step < size:
            array = array + lax.ppermute(array, axis, [(i, i ^ step) for i in range(size)])
            step *= 2
    return array


def pick(array, index, axis):
    return lax.dynamic_index_in_dim(array, index, axis, keepdims=False)


def add_low(left, right):
    return (left.astype(F32) + right.astype(F32)).astype(BF16)


def plane_scatter(partial, y, x, c):
    rows, columns = partial.shape[0] // 8, partial.shape[1]
    half = rows // 2
    parts = partial.reshape(2, 2, 2, rows, columns)
    acc = add_low(pick(parts, c, 2), lax.ppermute(pick(parts, 1 - c, 2), "c", SWAP))
    top, low = acc[:, :, :half], acc[:, :, half:]
    top = add_low(pick(top, x, 1), lax.ppermute(pick(top, 1 - x, 1), "x", SWAP))
    low = add_low(pick(low, y, 0), lax.ppermute(pick(low, 1 - y, 0), "y", SWAP))
    top = pick(top, y, 0).astype(F32) + lax.ppermute(pick(top, 1 - y, 0), "y", SWAP).astype(F32)
    low = pick(low, x, 0).astype(F32) + lax.ppermute(pick(low, 1 - x, 0), "x", SWAP).astype(F32)
    return jnp.concatenate([top, low], 0)


def in_order(y, own, other, axis):
    return jnp.where(
        y == 0, jnp.concatenate([own, other], axis), jnp.concatenate([other, own], axis)
    )


def on_device(
    n,
    tokens, norm_gain, norm_bias,
    query_weight, query_bias, key_weight, key_bias, value_weight, value_bias,
    output_weight, output_bias, up_weight, up_bias, down_weight, down_bias,
    doc_split, cotangent,
):
    z, y, x, c = (lax.axis_index(name) for name in ("z", "y", "x", "c"))
    shard_rows = query_weight.shape[0]
    width = query_weight.shape[1] // 2
    hidden_width = up_weight.shape[1] // 2
    chunks = 2
    piece = hidden_width // chunks

    def col(array, start, size):
        return lax.dynamic_slice_in_dim(array, start, size, 1)

    def row(array, start, size):
        return lax.dynamic_slice_in_dim(array, start, size, 0)

    def pack_heads(side):
        return jnp.concatenate(
            [col(w, side * width, width) for w in (query_weight, key_weight, value_weight)]
            + [row(output_weight, side * width, width).T],
            1,
        )

    def pack_hidden(side, chunk):
        start = side * hidden_width + chunk * piece
        return jnp.concatenate(
            [col(up_weight, start, piece), row(down_weight, start, piece).T], 1
        )

    gain_wide = norm_gain.astype(F32)
    tokens_wide = tokens.astype(F32)
    row_mean = jnp.mean(tokens_wide, -1, keepdims=True)
    centred = tokens_wide - row_mean
    inv_scale = lax.rsqrt(jnp.mean(centred * centred, -1, keepdims=True) + EPS)
    standard = centred * inv_scale
    normed = (standard * gain_wide + norm_bias.astype(F32)).astype(BF16)
    phase = lax.optimization_barrier
    packed = (
        pack_hidden(y, 0), pack_hidden(1 - y, 0), pack_heads(y), pack_heads(1 - y),
        pack_hidden(1 - y, 1), normed,
    )
    last_own = pack_hidden(y, 1)
    other_split = lax.ppermute(doc_split, "y", SWAP)
    splits = in_order(y, doc_split, other_split, 0)
    seq_len = 4 * normed.shape[0]
    cosine, sine = turn_tables(splits, seq_len)

    right, left = [None] * n, [None] * n
    first_weights, heads_unit, right[1], left[1], last_swapped, normed_all, cot_all = gather_all(
        n, *packed, cotangent
    )
    last_unit = in_order(y, last_own, last_swapped, 0)
    first_weights, heads_unit, last_unit, normed_all, cot_all, right[1], left[1], cosine, sine = phase(
        (first_weights, heads_unit, last_unit, normed_all, cot_all, right[1], left[1], cosine, sine)
    )

    def hidden_local(weights, chunk):
        bias = row(up_bias, y * hidden_width + chunk * piece, piece).astype(F32)[None]
        return hidden_part(normed_all, cot_all, weights, bias)

    def weight_grads(grad_columns, columns):
        return jnp.concatenate(
            [dot(normed_all, grad_columns, TN).astype(BF16), dot(cot_all, columns, TN).astype(BF16)], 1
        )

    def gather_step(step, source):
        return chain_step(step, n, right[step - 1], left[step - 1]) if step > 1 else chain_step(
            1, n, source, source)

    activated_0, grad_hidden_0, hidden_sum_0 = hidden_local(first_weights, 0)
    right[2], left[2] = gather_step(2, None)
    activated_0, grad_hidden_0, normed_all, cot_all, right[2], left[2] = phase(
        (activated_0, grad_hidden_0, normed_all, cot_all, right[2], left[2])
    )
    grads_first = weight_grads(grad_hidden_0, activated_0)
    for step in range(3, n):
        right[step], left[step] = gather_step(step, None)
    grads_first, activated_0, last_unit, normed_all, cot_all, right[3:], left[3:] = phase(
        (grads_first, activated_0, last_unit, normed_all, cot_all, right[3:], left[3:])
    )
    head_weights = assemble(heads_unit, right, left, n, z)
    qkv_weight, output_turned = head_weights[:, : 3 * width], head_weights[:, 3 * width :]

    qkv_bias = jnp.concatenate(
        [row(b, y * width, width) for b in (query_bias, key_bias, value_bias)]
    ).astype(F32)
    qkv = dot(normed_all, qkv_weight) + qkv_bias
    grad_attended = dot(cot_all, output_turned).astype(BF16)
    right[1], left[1] = gather_step(1, last_unit)
    qkv, grad_attended, normed_all, cot_all, right[1], left[1] = phase(
        (qkv, grad_attended, normed_all, cot_all, right[1], left[1])
    )
    attended, grad_qkv = attention(splits, qkv, grad_attended, cosine, sine)
    right[2], left[2] = gather_step(2, None)
    first_in = scatter_step(n - 1, grads_first, n, z, (None, None))
    attended, grad_qkv, normed_all, cot_all, right[2], left[2], first_in, grads_first = phase(
        (attended, grad_qkv, normed_all, cot_all, right[2], left[2], first_in, grads_first)
    )
    grads_heads = weight_grads(grad_qkv, attended)
    for step in range(3, n):
        right[step], left[step] = gather_step(step, None)
    for k in range(n - 2, n - 3, -1):
        first_in = scatter_step(k, grads_first, n, z, first_in)
    (grads_heads, attended, grad_qkv, normed_all, cot_all, right[3:], left[3:],
     first_in, grads_first) = phase(
        (grads_heads, attended, grad_qkv, normed_all, cot_all, right[3:], left[3:],
         first_in, grads_first)
    )

    last_weights = assemble(last_unit, right, left, n, z)
    activated_1, grad_hidden_1, hidden_sum_1 = hidden_local(last_weights, 1)
    for k in range(n - 3, 0, -1):
        first_in = scatter_step(k, grads_first, n, z, first_in)
    last_weights, activated_1, grad_hidden_1, attended, first_in, grads_heads = phase(
        (last_weights, activated_1, grad_hidden_1, attended, first_in, grads_heads)
    )
    first_sum = scatter_end(grads_first, n, z, first_in)
    partial_out = sum_dots(
        (attended, activated_0, activated_1),
        ((head_weights, width, 3), (first_weights, piece, 1), (last_weights, piece, 1)),
    )
    heads_in = scatter_step(n - 1, grads_heads, n, z, (None, None))
    partial_out, heads_in, grads_heads, grad_qkv, grad_hidden_1 = phase(
        (partial_out, heads_in, grads_heads, grad_qkv, grad_hidden_1)
    )
    grad_normed_part = sum_dots(
        (grad_qkv, grad_hidden_0, grad_hidden_1),
        ((head_weights, 3 * width, 0), (first_weights, piece, 0), (last_weights, piece, 0)),
    )
    for k in range(n - 2, n - 3, -1):
        heads_in = scatter_step(k, grads_heads, n, z, heads_in)
    grad_normed_part, heads_in, grads_heads, grad_hidden_1, activated_1, normed_all, cot_all = phase(
        (grad_normed_part, heads_in, grads_heads, grad_hidden_1, activated_1, normed_all, cot_all)
    )
    grads_last = weight_grads(grad_hidden_1, activated_1)
    for k in range(n - 3, 0, -1):
        heads_in = scatter_step(k, grads_heads, n, z, heads_in)
    qkv_sum = jnp.sum(grad_qkv, 0, dtype=F32)[None]
    bias_row = jnp.concatenate([qkv_sum, hidden_sum_0, hidden_sum_1], 1)
    cot_wide = cotangent.astype(F32)
    cot_sum = jnp.sum(cot_wide, 0)[None]
    grads_last, grad_normed_part, heads_in, grads_heads, bias_row, cot_sum = phase(
        (grads_last, grad_normed_part, heads_in, grads_heads, bias_row, cot_sum)
    )
    heads_sum = scatter_end(grads_heads, n, z, heads_in)

    def halves(total):
        keep = row(total, y * shard_rows, shard_rows)
        give = row(total, (1 - y) * shard_rows, shard_rows).astype(BF16)
        return keep, lax.ppermute(give, "y", SWAP).astype(F32)

    heads_keep, heads_take = halves(heads_sum)
    first_keep, first_take = halves(first_sum)

    if n in (2, 4) and bias_row.shape[1] <= cot_sum.shape[1]:
        spread = cot_sum.shape[1]
        vector = jnp.concatenate([
            jnp.zeros((2, spread), F32), cot_sum,
            jnp.pad(bias_row, ((0, 0), (0, spread - bias_row.shape[1]))),
            jnp.zeros((4, spread), F32),
        ])
        last_keep, last_take, grad_normed, mixed, sums = tail(
            n, grads_last, grad_normed_part, partial_out, standard, vector
        )
        last_take = last_take.astype(F32)
        norm_sums = sums[:3]
        bias_rows = in_order(y, sums[3:4], sums[4:5], 0)[:, : bias_row.shape[1]]
    else:
        last_in = (None, None)
        for k in range(n - 1, 0, -1):
            last_in = scatter_step(k, grads_last, n, z, last_in)
        last_keep, last_take = halves(scatter_end(grads_last, n, z, last_in))
        grad_normed = plane_scatter(grad_normed_part, y, x, c)
        mixed = plane_scatter(partial_out, y, x, c)
        norm_sums = sum_small(
            jnp.concatenate([
                jnp.sum(grad_normed * standard, 0)[None], jnp.sum(grad_normed, 0)[None], cot_sum
            ]),
            ("c", "x", "y", "z"),
        )
        bias_row = sum_small(bias_row, ("z",))
        bias_rows = in_order(y, bias_row, lax.ppermute(bias_row, "y", SWAP), 0)
    grad_norm_gain, grad_norm_bias, grad_out_bias = norm_sums

    out_bias = output_bias.astype(F32) + down_bias.astype(F32)
    out = (tokens_wide + mixed + out_bias).astype(BF16)

    def joined(start, size):
        return in_order(
            y, heads_keep[:, start : start + size], heads_take[:, start : start + size], 1
        )

    grad_query_weight, grad_key_weight, grad_value_weight, grad_output_turned = (
        joined(part * width, width) for part in range(4)
    )
    hidden_halves = [(first_keep, first_take), (last_keep, last_take)]

    def side(which, start):
        return jnp.concatenate([pair[which][:, start : start + piece] for pair in hidden_halves], 1)

    grad_up_weight = in_order(y, side(0, 0), side(1, 0), 1)
    grad_down_turned = in_order(y, side(0, piece), side(1, piece), 1)

    grad_query_bias, grad_key_bias, grad_value_bias = (
        bias_rows[:, part * width : (part + 1) * width].reshape(-1) for part in range(3)
    )
    grad_up_bias = bias_rows[:, 3 * width :].reshape(-1)

    grad_scaled = grad_normed * gain_wide
    grad_tokens = cot_wide + inv_scale * (
        grad_scaled
        - jnp.mean(grad_scaled, -1, keepdims=True)
        - standard * jnp.mean(grad_scaled * standard, -1, keepdims=True)
    )
    return (
        out, grad_tokens, grad_norm_gain, grad_norm_bias,
        grad_query_weight, grad_query_bias, grad_key_weight, grad_key_bias,
        grad_value_weight, grad_value_bias, grad_output_turned.T, grad_out_bias,
        grad_up_weight, grad_up_bias, grad_down_turned.T, grad_out_bias,
    )


def solution(mesh):
    n = mesh.shape["dp"] // 2
    grid = Mesh(mesh.devices.reshape(n, 2, mesh.shape["tensor"] // 2, 2), ("z", "y", "x", "c"))
    dp, tensor = ("z", "y"), ("x", "c")
    rows = P(dp + tensor, None)
    whole, split = P(), P(tensor)
    wide, tall = P(dp, tensor), P(tensor, dp)
    in_specs = (
        rows, whole, whole, wide, split, wide, split, wide, split,
        tall, whole, wide, split, tall, whole, P(dp), rows,
    )
    out_specs = (
        rows, rows, whole, whole, wide, split, wide, split, wide, split,
        tall, whole, wide, split, tall, whole,
    )
    return jax.shard_map(
        functools.partial(on_device, n),
        mesh=grid, in_specs=in_specs, out_specs=out_specs, check_vma=False,
    )
```

```python
import functools

import jax
import jax.numpy as jnp
from jax import lax
from jax.experimental import pallas as pl
from jax.experimental.pallas import tpu as pltpu
from jax.sharding import Mesh, PartitionSpec as P

HEAD_DIM = 64
ROT = 32
BLOCK = 256
EPS = 1e-05
LANES = 128
F32 = jnp.float32
BF16 = jnp.bfloat16


SWAP = [(0, 1), (1, 0)]
NT = (((1,), (1,)), ((), ()))
TN = (((0,), (0,)), ((), ()))
NN = (((1,), (0,)), ((), ()))


def dot(left, right, dims=NN):
    return lax.dot_general(left, right, dims, preferred_element_type=F32)


def spin(value, cosine, sine):
    lane = lax.broadcasted_iota(jnp.int32, value.shape, 1) % HEAD_DIM
    half = ROT // 2
    ahead = pltpu.roll(value, LANES - half, 1)
    behind = pltpu.roll(value, half, 1)
    return value * cosine + jnp.where(lane < half, ahead, behind) * sine


def attention_kernel(
    index, earlier, split_ref, qkv_ref, grad_ref, cos_ref, sin_ref, *refs
):
    (att_ref, dqkv_ref, *scratch) = refs[earlier:]
    attention_body(index, split_ref, qkv_ref, grad_ref, cos_ref, sin_ref, att_ref, dqkv_ref, *scratch)


def attention_body(
    index, split_ref, qkv_ref, grad_ref, cos_ref, sin_ref, att_ref, dqkv_ref,
    q_s, k_s, v_s, g_s, kt_s, vt_s, ot_s, dqt_s, dk_s, dv_s, cos_s, sin_s,
):
    seq_len, width = grad_ref.shape
    first = split_ref[index] // BLOCK
    scale = HEAD_DIM ** (-0.5)
    per = LANES // HEAD_DIM
    rest = jnp.zeros((HEAD_DIM - ROT, seq_len), F32)
    cos_part, sin_part = cos_ref[...], sin_ref[...]
    cos_s[...] = jnp.concatenate([cos_part, cos_part, rest + 1.0] * per, 0).T
    sin_s[...] = jnp.concatenate([-sin_part, sin_part, rest] * per, 0).T

    def one_pair(pair, carry):
        def cols(part):
            return pl.ds(pl.multiple_of(part * width + pair * LANES, LANES), LANES)

        cosine, sine = cos_s[...], sin_s[...]
        head_of = lax.broadcasted_iota(jnp.int32, (seq_len, LANES), 1) // HEAD_DIM
        query = spin(qkv_ref[:, cols(0)], cosine, sine).astype(BF16)
        key = spin(qkv_ref[:, cols(1)], cosine, sine).astype(BF16)
        value = qkv_ref[:, cols(2)].astype(BF16)
        grad = grad_ref[:, cols(0)]
        kt_s[...] = key.T
        vt_s[...] = value.T
        for head in range(per):
            here = head_of == head
            q_s[head] = jnp.where(here, query, 0).astype(BF16)
            k_s[head] = jnp.where(here, key, 0).astype(BF16)
            v_s[head] = jnp.where(here, value, 0).astype(BF16)
            g_s[head] = jnp.where(here, grad, 0).astype(BF16)
        dk_s[...] = jnp.zeros_like(dk_s)
        dv_s[...] = jnp.zeros_like(dv_s)

        def one_block(block, inner):
            begin = jnp.where(block >= first, first, 0)
            rows = pl.ds(pl.multiple_of(block * BLOCK, BLOCK), BLOCK)

            def work(count):
                span = pl.ds(pl.multiple_of(begin * BLOCK, BLOCK), count * BLOCK)
                dk, dv = None, None
                for head in range(per):
                    q, g = q_s[head, rows, :], g_s[head, rows, :]
                    own = slice(head * HEAD_DIM, (head + 1) * HEAD_DIM)
                    scores = dot(k_s[head, span, :], q, NT) * scale
                    top = jnp.max(scores, 0, keepdims=True)
                    power = jnp.exp(scores - top)
                    prob = power * (1.0 / jnp.sum(power, 0, keepdims=True))
                    low = prob.astype(BF16)
                    ot_s[own, rows] = dot(vt_s[own, span], low)
                    dprob = dot(v_s[head, span, :], g, NT)
                    mean = jnp.sum(prob * dprob, 0, keepdims=True)
                    dscore = (prob * (dprob - mean) * scale).astype(BF16)
                    dqt_s[own, rows] = dot(kt_s[own, span], dscore)
                    dk_h, dv_h = dot(dscore, q), dot(low, g)
                    dk = dk_h if dk is None else dk + dk_h
                    dv = dv_h if dv is None else dv + dv_h
                dk_s[span, :] += dk
                dv_s[span, :] += dv

            for count in range(1, seq_len // BLOCK):
                pl.when(block - begin == count - 1)(functools.partial(work, count))
            return inner

        lax.fori_loop(0, seq_len // BLOCK, one_block, 0)
        att_ref[:, cols(0)] = ot_s[...].T.astype(BF16)
        dqkv_ref[:, cols(0)] = spin(dqt_s[...].T, cosine, -sine).astype(BF16)
        dqkv_ref[:, cols(1)] = spin(dk_s[...], cosine, -sine).astype(BF16)
        dqkv_ref[:, cols(2)] = dv_s[...].astype(BF16)
        return carry

    lax.fori_loop(0, width // LANES, one_pair, 0)


def attention(index, splits, qkv, grad, cosine, sine, earlier):
    count = splits.shape[0]
    rows, width = grad.shape
    seq_len = rows // count
    per = LANES // HEAD_DIM

    def spec(columns):
        return pl.BlockSpec((seq_len, columns), lambda i, split: (index, 0))

    table = pl.BlockSpec((ROT // 2, seq_len), lambda i, split: (0, index))
    masked = pltpu.VMEM((per, seq_len, LANES), BF16)
    turned = pltpu.VMEM((LANES, seq_len), BF16)
    return pl.pallas_call(
        functools.partial(attention_kernel, index, len(earlier)),
        grid_spec=pltpu.PrefetchScalarGridSpec(
            num_scalar_prefetch=1,
            grid=(1,),
            in_specs=[spec(3 * width), spec(width), table, table]
            + [pl.BlockSpec(memory_space=pl.ANY)] * len(earlier),
            out_specs=[spec(width), spec(3 * width)],
            scratch_shapes=[
                masked, masked, masked, masked, turned, turned,
                pltpu.VMEM((LANES, seq_len), F32),
                pltpu.VMEM((LANES, seq_len), F32),
                pltpu.VMEM((seq_len, LANES), F32),
                pltpu.VMEM((seq_len, LANES), F32),
                pltpu.VMEM((seq_len, LANES), F32),
                pltpu.VMEM((seq_len, LANES), F32),
            ],
        ),
        out_shape=[
            jax.ShapeDtypeStruct((rows, width), BF16),
            jax.ShapeDtypeStruct((rows, 3 * width), BF16),
        ],
        cost_estimate=pl.CostEstimate(
            flops=40 * seq_len * seq_len * width // 4,
            transcendentals=seq_len * seq_len * width // HEAD_DIM // 2,
            bytes_accessed=seq_len * width * 24,
        ),
        input_output_aliases={5 + i: i for i in range(len(earlier))},
        compiler_params=pltpu.CompilerParams(vmem_limit_bytes=48 << 20),
        name="attention",
    )(splits, qkv, grad, cosine, sine, *earlier)


def turn_tables(splits, seq_len):
    shape = (ROT // 2, splits.shape[0], seq_len)
    token = lax.broadcasted_iota(jnp.int32, shape, 2)
    start = splits[None, :, None]
    position = (token - jnp.where(token >= start, start, 0)).astype(F32)
    entry = jnp.arange(ROT // 2, dtype=F32)
    angle = position * (10000.0 ** (-(2.0 * entry) / ROT))[:, None, None]
    return jnp.cos(angle).reshape(ROT // 2, -1), jnp.sin(angle).reshape(ROT // 2, -1)


def sum_dots_kernel(count, *refs):
    out_ref = refs[-1]
    total = None
    for i in range(count):
        part = dot(refs[i][...], refs[count + i][...], NT)
        total = part if total is None else total + part
    out_ref[...] = total.astype(out_ref.dtype)


def sum_dots(lefts, rights, tile=512):
    rows, columns = lefts[0].shape[0], rights[0][0].shape[0]
    tile = min(tile, rows)
    depth = sum(left.shape[1] for left in lefts)
    return pl.pallas_call(
        functools.partial(sum_dots_kernel, len(lefts)),
        grid=(rows // tile,),
        in_specs=[pl.BlockSpec((tile, left.shape[1]), lambda i: (i, 0)) for left in lefts] + [
            pl.BlockSpec((columns, size), functools.partial(lambda at, i: (0, at), at))
            for _, size, at in rights
        ],
        out_specs=pl.BlockSpec((tile, columns), lambda i: (i, 0)),
        out_shape=jax.ShapeDtypeStruct((rows, columns), BF16),
        cost_estimate=pl.CostEstimate(
            flops=2 * rows * columns * depth, transcendentals=0,
            bytes_accessed=2 * (rows * columns + depth * (rows + columns)),
        ),
        compiler_params=pltpu.CompilerParams(vmem_limit_bytes=56 << 20),
        name="sum_dots",
    )(*lefts, *(right[0] for right in rights))


def hidden_kernel(n_ref, c_ref, w_ref, bias_ref, act_ref, dh_ref, sum_ref):
    piece = act_ref.shape[1]
    hidden = dot(n_ref[...], w_ref[:, :piece]) + bias_ref[...]
    grad = dot(c_ref[...], w_ref[:, piece:])
    rate = (2.0 / jnp.pi) ** 0.5
    square = hidden * hidden
    bent = jnp.tanh(rate * hidden * (1.0 + 0.044715 * square))
    act_ref[...] = (0.5 * hidden * (1.0 + bent)).astype(BF16)
    slope = 0.5 * (1.0 + bent) + 0.5 * hidden * (1.0 - bent * bent) * (
        rate * (1.0 + 3.0 * 0.044715 * square)
    )
    low = (grad * slope).astype(BF16)
    dh_ref[...] = low

    @pl.when(pl.program_id(0) == 0)
    def _():
        sum_ref[...] = jnp.zeros_like(sum_ref)

    sum_ref[...] += jnp.sum(low.astype(F32), 0, keepdims=True)


def hidden_part(normed_all, cot_all, weights, bias, tile=512):
    rows, depth = normed_all.shape
    piece = weights.shape[1] // 2
    tile = min(tile, rows)
    wide = pl.BlockSpec((tile, depth), lambda i: (i, 0))
    thin = pl.BlockSpec((tile, piece), lambda i: (i, 0))
    line = pl.BlockSpec((1, piece), lambda i: (0, 0))
    return pl.pallas_call(
        hidden_kernel,
        grid=(rows // tile,),
        in_specs=[wide, wide, pl.BlockSpec(weights.shape, lambda i: (0, 0)), line],
        out_specs=[thin, thin, line],
        out_shape=[
            jax.ShapeDtypeStruct((rows, piece), BF16),
            jax.ShapeDtypeStruct((rows, piece), BF16),
            jax.ShapeDtypeStruct((1, piece), F32),
        ],
        cost_estimate=pl.CostEstimate(
            flops=4 * rows * depth * piece, transcendentals=rows * piece,
            bytes_accessed=4 * rows * depth + 4 * depth * piece + 4 * rows * piece,
        ),
        compiler_params=pltpu.CompilerParams(vmem_limit_bytes=48 << 20),
        name="hidden_part",
    )(normed_all, cot_all, weights, bias)


def gather_kernel(
    n, own_ref, other_ref, second_ref, second_other_ref, next_ref, norm_ref, cot_ref,
    w_ref, unit_ref, right_ref, left_ref, swapped_ref, n_ref, c_ref, send_sem, recv_sem, local_sem,
):
    z, y, x, c = (lax.axis_index(name) for name in ("z", "y", "x", "c"))
    rows = norm_ref.shape[0]
    half = 3 * rows // 4
    mine = y * 4 + x * 2 + c
    has_right, has_left = z < n - 1, z > 0
    number = {}

    def remote(key, src, dst, axis, target):
        slot = number.setdefault(key, len(number))
        return pltpu.make_async_remote_copy(
            src_ref=src, dst_ref=dst, send_sem=send_sem.at[slot], recv_sem=recv_sem.at[slot],
            device_id={axis: target}, device_id_type=pl.DeviceIdType.MESH,
        )

    def when(condition, action):
        if condition is None:
            action()
        else:
            pl.when(condition)(action)

    started = []

    def start(condition, copy):
        when(condition, copy.start)
        started.append((condition, copy))

    def shard(index, unit):
        return w_ref.at[index * 2 + (y if unit == 0 else 1 - y)]

    def along(step, unit, sign, receiving=False):
        index = z - sign * step if receiving else z - sign * (step - 1)
        source = own_ref if step == 1 and unit == 0 and not receiving else shard(index, unit)
        return remote((step, unit, sign), source, shard(index, unit), "z", z + sign)


    full, top, low = pl.ds(0, rows), pl.ds(0, half), pl.ds(half, rows - half)
    arrays = ((n_ref, norm_ref, "n"), (c_ref, cot_ref, "c"))
    at_x, at_y, at_xy = y * 4 + (1 - x) * 2 + c, (1 - y) * 4 + x * 2 + c, (1 - y) * 4 + (1 - x) * 2 + c

    barrier = pltpu.get_barrier_semaphore()
    for axis, target in (("x", 1 - x), ("y", 1 - y), ("c", 1 - c)):
        pl.semaphore_signal(
            barrier, inc=1, device_id={axis: target}, device_id_type=pl.DeviceIdType.MESH
        )
    for condition, target in ((has_right, z + 1), (has_left, z - 1)):
        when(condition, functools.partial(
            pl.semaphore_signal, barrier, inc=1, device_id={"z": target},
            device_id_type=pl.DeviceIdType.MESH,
        ))
    pl.semaphore_wait(barrier, 3 + has_right.astype(jnp.int32) + has_left.astype(jnp.int32))

    for condition, sign in ((has_right, 1), (has_left, -1)):
        start(condition, along(1, 0, sign))
    swap = remote("swap", other_ref, w_ref.at[z * 2 + y], "y", 1 - y)
    swap_in = remote("swap", other_ref, w_ref.at[z * 2 + 1 - y], "y", 1 - y)
    start(None, swap)
    for array, source, name in arrays:
        for axis in ("x", "y", "c"):
            start(None, remote((name, axis), source, array.at[mine], axis,
                               {"x": 1 - x, "y": 1 - y, "c": 1 - c}[axis]))
    unit_swap = remote("unit", second_other_ref, unit_ref.at[y], "y", 1 - y)
    unit_swap_in = remote("unit", second_other_ref, unit_ref.at[1 - y], "y", 1 - y)
    start(None, unit_swap)
    late_swap = remote("late", next_ref, swapped_ref, "y", 1 - y)
    start(None, late_swap)
    local = [
        pltpu.make_async_copy(own_ref, shard(z, 0), local_sem.at[0]),
        pltpu.make_async_copy(norm_ref, n_ref.at[mine], local_sem.at[1]),
        pltpu.make_async_copy(cot_ref, c_ref.at[mine], local_sem.at[2]),
        pltpu.make_async_copy(second_ref, unit_ref.at[y], local_sem.at[3]),
    ]
    for copy in local:
        copy.start()

    def arrive_swap():
        swap_in.wait_recv()
        for condition, sign in ((has_right, 1), (has_left, -1)):
            start(condition, along(1, 1, sign))

    def arrive_shard(step, unit, sign):
        inside = z - sign * step >= 0 if sign > 0 else z + step < n
        further = has_right if sign > 0 else has_left
        when(inside, along(step, unit, sign, True).wait_recv)
        if step + 1 < n:
            start(inside & further, along(step + 1, unit, sign))

    def arrive_rows(array, name, axis):
        index = {"x": at_x, "y": at_y, "c": None}[axis]
        block = array.at[index]
        remote((name, axis), block, block, axis, 0).wait_recv()
        part, on = (low, "y") if axis == "x" else (top, "x")
        piece = array.at[index, part]
        start(None, remote((name, "far", on), piece, piece, on, {"x": 1 - x, "y": 1 - y}[on]))
        start(None, remote((name, "core", axis), block, block, "c", 1 - c))

    def arrive_far(array, name, on):
        part = low if on == "y" else top
        piece = array.at[at_xy, part]
        remote((name, "far", on), piece, piece, on, 0).wait_recv()
        start(None, remote((name, "core", "far", on), piece, piece, "c", 1 - c))

    def arrive_steps(step):
        for unit in (0, 1):
            for sign in (1, -1):
                arrive_shard(step, unit, sign)

    def second_step(half_of, receiving):
        index = y if half_of == 0 else 1 - y
        source = second_ref if half_of == 0 else unit_ref.at[index]
        ways = ((1, has_left if receiving else has_right, right_ref),
                (-1, has_right if receiving else has_left, left_ref))
        for sign, condition, target in ways:
            copy = remote(("second", half_of, sign), source, target.at[index], "z", z + sign)
            if receiving:
                when(condition, copy.wait_recv)
            else:
                start(condition, copy)

    (norm, _, norm_name), (cot, _, cot_name) = arrays
    arrive_swap()
    arrive_rows(norm, norm_name, "x")
    for sign in (1, -1):
        arrive_shard(1, 0, sign)
    arrive_rows(norm, norm_name, "y")
    for sign in (1, -1):
        arrive_shard(1, 1, sign)
    arrive_rows(cot, cot_name, "x")
    if n > 2:
        arrive_steps(2)
    second_step(0, False)
    arrive_rows(cot, cot_name, "y")
    unit_swap_in.wait_recv()
    second_step(1, False)
    for step in range(3, n):
        arrive_steps(step)
    for array, _, name in arrays:
        for on in ("x", "y"):
            arrive_far(array, name, on)
    for array, _, name in arrays:
        for key, index, part in (
            ((name, "c"), y * 4 + x * 2 + 1 - c, full),
            ((name, "core", "x"), y * 4 + (1 - x) * 2 + 1 - c, full),
            ((name, "core", "y"), (1 - y) * 4 + x * 2 + 1 - c, full),
            ((name, "core", "far", "x"), (1 - y) * 4 + (1 - x) * 2 + 1 - c, top),
            ((name, "core", "far", "y"), (1 - y) * 4 + (1 - x) * 2 + 1 - c, low),
        ):
            piece = array.at[index, part]
            remote(key, piece, piece, "c", 0).wait_recv()
    late_swap.wait_recv()
    for half_of in (0, 1):
        second_step(half_of, True)
    for copy in local:
        copy.wait()
    for condition, copy in started:
        when(condition, copy.wait_send)


def gather_all(n, own, other, second, second_other, following, normed, cotangent):
    rows, columns = normed.shape
    copies = 4 * (n - 1) + 8 + 2 * 9
    anywhere = pl.BlockSpec(memory_space=pl.ANY)
    pair = jax.ShapeDtypeStruct((2,) + second.shape, second.dtype)
    weights, unit, right, left, swapped, normed_all, cot_all = pl.pallas_call(
        functools.partial(gather_kernel, n),
        in_specs=[anywhere] * 7,
        out_specs=[anywhere] * 7,
        out_shape=[
            jax.ShapeDtypeStruct((2 * n,) + own.shape, own.dtype),
            pair, pair, pair,
            jax.ShapeDtypeStruct(following.shape, following.dtype),
            jax.ShapeDtypeStruct((8, rows, columns), normed.dtype),
            jax.ShapeDtypeStruct((8, rows, columns), cotangent.dtype),
        ],
        scratch_shapes=[
            pltpu.SemaphoreType.DMA((copies,)),
            pltpu.SemaphoreType.DMA((copies,)),
            pltpu.SemaphoreType.DMA((4,)),
        ],
        cost_estimate=pl.CostEstimate(flops=0, transcendentals=0, bytes_accessed=200 << 20),
        compiler_params=pltpu.CompilerParams(collective_id=0, has_side_effects=True),
        name="gather_rows",
    )(own, other, second, second_other, following, normed, cotangent)
    flat = lambda array: array.reshape(-1, array.shape[-1])
    return tuple(map(flat, (weights, unit, right, left, swapped, normed_all, cot_all)))


def chain_step(step, n, right, left):
    return (
        lax.ppermute(right, "z", [(i, i + 1) for i in range(step - 1, n - 1)]),
        lax.ppermute(left, "z", [(i, i - 1) for i in range(1, n - step + 1)]),
    )


def assemble(unit, right, left, n, z):
    rows, columns = unit.shape
    whole = jnp.zeros((n * rows, columns), unit.dtype)
    for k in range(n):
        piece = unit if k == 0 else jnp.where(z >= k, right[k], left[n - k])
        row = lax.rem(z - k + n, n) * rows
        whole = lax.dynamic_update_slice(whole, piece, (row, jnp.int32(0)))
    return whole


def scatter_step(k, grads, n, z, received):
    rows = grads.shape[0] // n

    def send(index, got, pairs):
        piece = lax.dynamic_slice_in_dim(grads, jnp.clip(index, 0, n - 1) * rows, rows, 0)
        if got is not None:
            piece = add_low(piece, got)
        return lax.ppermute(piece, "z", pairs)

    from_right, from_left = received
    return (
        send(z - k, from_right, [(r, r - 1) for r in range(k, n)]),
        send(z + k, from_left, [(r, r + 1) for r in range(0, n - k)]),
    )


def scatter_end(grads, n, z, received):
    rows = grads.shape[0] // n
    own = lax.dynamic_slice_in_dim(grads, z * rows, rows, 0).astype(F32)
    return own + received[0].astype(F32) + received[1].astype(F32)


def tail_kernel(
    n, g_ref, hw_ref, fw_ref, lw_ref, dq_ref, d0_ref, d1_ref, at_ref, a0_ref, a1_ref,
    std_ref, vec_ref, keep_ref, take_ref, out_ref, mixed_ref, sums_ref,
    hw_s, fw_s, lw_s, rows_s, stage, zrecv, total, give, both, xtop_2, ylow_2, ytop_2, xlow_2,
    top_2, low_2, vstage, vrecv, send_sem, recv_sem, load_sem, rows_sem,
):
    z, y, x, c = (lax.axis_index(name) for name in ("z", "y", "x", "c"))
    rows, columns = out_ref.shape
    wide = give.shape[0]
    half = 5 * rows // 8
    rest = rows - half
    number, started = {}, []

    def remote(key, src, dst, axis, target):
        slot = number.setdefault(key, len(number))
        return pltpu.make_async_remote_copy(
            src_ref=src, dst_ref=dst, send_sem=send_sem.at[slot], recv_sem=recv_sem.at[slot],
            device_id={axis: target}, device_id_type=pl.DeviceIdType.MESH,
        )

    def when(condition, action):
        if condition is None:
            action()
        else:
            pl.when(condition)(action)

    def start(condition, copy):
        when(condition, copy.start)
        started.append((condition, copy))

    def each(count, size, body):
        def step(i, carry):
            body(pl.ds(pl.multiple_of(i * size, size), size))
            return carry
        lax.fori_loop(0, count // size, step, 0)

    barrier = pltpu.get_barrier_semaphore()
    greet = [(None, "x", 1 - x), (None, "y", 1 - y), (None, "c", 1 - c)]
    greet += [(z < n - 1, "z", z + 1), (z > 0, "z", z - 1)]
    for step in (2 ** i for i in range(1, n.bit_length() - 1)):
        greet.append((None, "z", jnp.bitwise_xor(z, step)))
    for condition, axis, target in greet:
        when(condition, functools.partial(
            pl.semaphore_signal, barrier, inc=1, device_id={axis: target},
            device_id_type=pl.DeviceIdType.MESH))

    loads = [
        pltpu.make_async_copy(source, target, load_sem.at[i])
        for i, (source, target) in enumerate(((hw_ref, hw_s), (fw_ref, fw_s), (lw_ref, lw_s)))
    ]
    for load in loads:
        load.start()

    firsts, lasts = fw_ref.shape[1] // 2, lw_ref.shape[1] // 2
    heads = dq_ref.shape[1]
    sums = (
        ((dq_ref, heads, hw_s, 0), (d0_ref, firsts, fw_s, 0), (d1_ref, lasts, lw_s, 0)),
        ((at_ref, heads // 3, hw_s, heads), (a0_ref, firsts, fw_s, firsts),
         (a1_ref, lasts, lw_s, lasts)),
    )
    jobs = [(a, own, j) for a in (0, 1) for own in (False, True) for j in (0, 1)]

    def row_loads(number_of):
        a, own, j = jobs[number_of]
        slot, core, copies, at = number_of % 2, c if own else 1 - c, [], 0
        for p, (left, width, _, _) in enumerate(sums[a]):
            for i in (0, 1):
                block = j * 4 + i * 2 + core
                source = left.at[pl.ds(pl.multiple_of(block * rows, rows), rows)]
                target = rows_s.at[slot, pl.ds(i * rows, rows), pl.ds(at, width)]
                copies.append(pltpu.make_async_copy(source, target, rows_sem.at[slot, p * 2 + i]))
            at += width
        return copies

    def job(number_of):
        a, own, j = jobs[number_of]
        slot = number_of % 2
        if number_of + 1 < len(jobs):
            for copy in row_loads(number_of + 1):
                copy.start()
        for copy in row_loads(number_of):
            copy.wait()
        if own:
            for i in (0, 1):
                core_copy(a, j * 2 + i).wait_recv()
        elif a == 1:
            for i in (0, 1):
                core_copy(0, j * 2 + i).wait_send()
        size = min(512, columns)

        def tile(t, carry):
            span = pl.ds(pl.multiple_of(t * size, size), size)
            acc, at = None, 0
            for left, width, weights, column in sums[a]:
                part = dot(
                    rows_s[slot, :, at : at + width], weights[span, column : column + width], NT)
                acc = part if acc is None else acc + part
                at += width
            for i in (0, 1):
                piece = acc[i * rows : (i + 1) * rows]
                if own:
                    both[a, j * 2 + i, :, span] = (
                        piece + both[a, j * 2 + i, :, span].astype(F32)).astype(BF16)
                else:
                    stage[j * 2 + i, :, span] = piece.astype(BF16)
            return carry

        lax.fori_loop(0, columns // size, tile, 0)
        if not own:
            for i in (0, 1):
                copy = core_copy(a, j * 2 + i)
                copy.start()
                if a == 1:
                    started.append((None, copy))

    def core_copy(a, i):
        return remote(("core", a, i), stage.at[i], both.at[a, i], "c", 1 - c)

    for copy in row_loads(0):
        copy.start()
    always = sum(condition is None for condition, _, _ in greet)
    pl.semaphore_wait(barrier, always + sum(
        condition.astype(jnp.int32) for condition, _, _ in greet if condition is not None))

    def first_copy(a, name, j):
        if name == "xtop":
            source = both.at[a, j * 2 + 1 - x, pl.ds(0, half)]
            return remote((name, a, j), source, xtop_2.at[a, j], "x", 1 - x)
        source = both.at[a, (1 - y) * 2 + j, pl.ds(half, rest)]
        return remote((name, a, j), source, ylow_2.at[a, j], "y", 1 - y)

    def second_copy(a, name):
        if name == "ytop":
            return remote((name, a), top_2.at[a], ytop_2.at[a], "y", 1 - y)
        return remote((name, a), low_2.at[a], xlow_2.at[a], "x", 1 - x)

    def first_send(a):
        for j in (0, 1):
            start(None, first_copy(a, "xtop", j))
            start(None, first_copy(a, "ylow", j))

    def first_arrive(a):
        for j in (0, 1):
            first_copy(a, "xtop", j).wait_recv()
            first_copy(a, "ylow", j).wait_recv()

        def upper(part):
            top_2[a, part, :] = (
                both[a, (1 - y) * 2 + x, part, :].astype(F32)
                + xtop_2[a, 1 - y, part, :].astype(F32)
            ).astype(BF16)

        def lower(part):
            low_part = pl.ds(part.start + half, part.size)
            low_2[a, part, :] = (
                both[a, y * 2 + 1 - x, low_part, :].astype(F32)
                + ylow_2[a, 1 - x, part, :].astype(F32)
            ).astype(BF16)

        each(half, 32, upper)
        each(rest, 32, lower)
        start(None, second_copy(a, "ytop"))
        start(None, second_copy(a, "xlow"))

    def second_arrive(a):
        second_copy(a, "ytop").wait_recv()
        second_copy(a, "xlow").wait_recv()
        target = (out_ref, mixed_ref)[a]

        def finish(first, part, placed, last):
            value = (
                both[a, y * 2 + x, placed, :].astype(F32) + first[part, :].astype(F32)
                + last[part, :].astype(F32)
            )
            target[placed, :] = value
            if a == 0:
                scaled = value * std_ref[placed, :]
                vstage[0, 0:1, :] += jnp.sum(scaled, 0, keepdims=True)
                vstage[0, 1:2, :] += jnp.sum(value, 0, keepdims=True)

        def upper(part):
            finish(xtop_2.at[a, y], part, part, ytop_2.at[a])

        def lower(part):
            finish(ylow_2.at[a, x], part, pl.ds(part.start + half, part.size), xlow_2.at[a])

        each(half, 32, upper)
        each(rest, 32, lower)

    sides = (1 - y, y)

    def block_of(direction, k, u):
        index = (z - k if direction == 0 else z + k) * 2 + sides[u]
        return pl.ds(pl.multiple_of(index * rows, rows), rows)

    def z_copy(direction, k, u, src):
        target = z - 1 if direction == 0 else z + 1
        return remote((direction, k, u), src, zrecv.at[direction, k - 1, u], "z", target)

    def z_first(direction):
        edge = z == n - 1 if direction == 0 else z == 0
        for k in range(n - 1, 0, -1):
            for u in (0, 1):
                start(edge, z_copy(direction, k, u, g_ref.at[:, block_of(direction, k, u)]))

    def z_step(k, u):
        for direction in (0, 1):
            if direction == 0:
                inside = (z >= k) & (z < n - 1)
            else:
                inside = (n - 1 - z >= k) & (z > 0)
            held = zrecv.at[direction, k, u]

            def add():
                z_copy(direction, k + 1, u, held).wait_recv()
                block = block_of(direction, k, u)

                def body(part):
                    held[part, :] = (
                        g_ref[part, block].astype(F32) + held[part, :].astype(F32)
                    ).astype(BF16)

                each(wide, 256, body)

            when(inside, add)
            start(inside, z_copy(direction, k, u, held))

    def z_last(u, target):
        block = block_of(0, 0, u)

        def first(part):
            target[part, :] = g_ref[part, block].astype(F32)

        each(wide, 256, first)
        for direction in (0, 1):
            held = zrecv.at[direction, 0, u]

            def add():
                z_copy(direction, 1, u, held).wait_recv()

                def body(part):
                    target[part, :] += held[part, :].astype(F32)

                each(wide, 256, body)

            when(z < n - 1 if direction == 0 else z > 0, add)

    steps = [(k, u) for k in range(n - 2, 0, -1) for u in (0, 1)]

    def z_next():
        if steps:
            z_step(*steps.pop(0))

    for direction in (0, 1):
        z_first(direction)
    vstage[0] = vec_ref[...]
    for load in loads:
        load.wait()
    job(0)
    job(1)
    z_next()
    job(2)
    job(3)
    first_send(0)
    z_next()
    job(4)
    job(5)
    z_next()
    job(6)
    job(7)
    first_arrive(0)
    first_send(1)
    while steps:
        z_next()
    second_arrive(0)

    turns = [("z", jnp.bitwise_xor(z, 2 ** i)) for i in range(n.bit_length() - 1)]
    turns += [("y", 1 - y), ("x", 1 - x), ("c", 1 - c)]
    line = lax.broadcasted_iota(jnp.int32, vec_ref.shape, 0)
    for i, (axis, target) in enumerate(turns):
        copy = remote(("vec", i), vstage.at[i], vrecv.at[i], axis, target)
        start(None, copy)
        copy.wait_recv()
        old, new = vstage[i], vrecv[i]
        joined = old + jnp.where((line < 3) | (axis == "z"), new, 0.0)
        result = sums_ref if i == len(turns) - 1 else vstage.at[i + 1]
        result[...] = joined
        if axis == "y":
            result[4:5, :] = new[3:4, :]

    z_last(0, total)

    def lower_precision(part):
        give[part, :] = total[part, :].astype(BF16)

    each(wide, 256, lower_precision)
    swap = remote("swap", give, take_ref, "y", 1 - y)
    start(None, swap)
    first_arrive(1)
    z_last(1, keep_ref)
    second_arrive(1)
    swap.wait_recv()
    for condition, copy in started:
        when(condition, copy.wait_send)


def tail(n, grads_turned, weights, lefts, lefts_out, standard, vector):
    rows, columns = standard.shape
    wide = grads_turned.shape[0]
    half = 5 * rows // 8
    inside = pl.BlockSpec(memory_space=pltpu.VMEM)
    anywhere = pl.BlockSpec(memory_space=pl.ANY)
    copies = 4 * (n - 1) + 40
    low = lambda *shape: pltpu.VMEM(shape, BF16)
    small = vector.shape
    depth = sum(left.shape[1] for left in lefts)
    return pl.pallas_call(
        functools.partial(tail_kernel, n),
        in_specs=[inside] + [anywhere] * 9 + [inside, inside],
        out_specs=[inside] * 5,
        out_shape=[
            jax.ShapeDtypeStruct((wide, rows), F32),
            jax.ShapeDtypeStruct((wide, rows), BF16),
            jax.ShapeDtypeStruct((rows, columns), F32),
            jax.ShapeDtypeStruct((rows, columns), F32),
            jax.ShapeDtypeStruct(small, F32),
        ],
        scratch_shapes=[low(*array.shape) for array in weights] + [
            low(2, 2 * rows, depth), low(4, rows, columns),
            low(2, n - 1, 2, wide, rows), pltpu.VMEM((wide, rows), F32), low(wide, rows),
            low(2, 4, rows, columns),
            low(2, 2, half, columns), low(2, 2, rows - half, columns),
            low(2, half, columns), low(2, rows - half, columns),
            low(2, half, columns), low(2, rows - half, columns),
            pltpu.VMEM((8,) + small, F32), pltpu.VMEM((8,) + small, F32),
            pltpu.SemaphoreType.DMA((copies,)),
            pltpu.SemaphoreType.DMA((copies,)),
            pltpu.SemaphoreType.DMA((3,)),
            pltpu.SemaphoreType.DMA((2, 6)),
        ],
        cost_estimate=pl.CostEstimate(flops=0, transcendentals=0, bytes_accessed=200 << 20),
        compiler_params=pltpu.CompilerParams(
            collective_id=1, has_side_effects=True, vmem_limit_bytes=63 << 20
        ),
        name="scatter_rest",
    )(grads_turned, *weights, *lefts, *lefts_out, standard, vector)


def sum_small(array, axes):
    for axis in axes:
        size = lax.axis_size(axis)
        if size & (size - 1):
            array = lax.psum(array, axis)
            continue
        step = 1
        while step < size:
            array = array + lax.ppermute(array, axis, [(i, i ^ step) for i in range(size)])
            step *= 2
    return array


def pick(array, index, axis):
    return lax.dynamic_index_in_dim(array, index, axis, keepdims=False)


def add_low(left, right):
    return (left.astype(F32) + right.astype(F32)).astype(BF16)


def plane_scatter(partial, y, x, c):
    rows, columns = partial.shape[0] // 8, partial.shape[1]
    half = rows // 2
    parts = partial.reshape(2, 2, 2, rows, columns)
    acc = add_low(pick(parts, c, 2), lax.ppermute(pick(parts, 1 - c, 2), "c", SWAP))
    top, low = acc[:, :, :half], acc[:, :, half:]
    top = add_low(pick(top, x, 1), lax.ppermute(pick(top, 1 - x, 1), "x", SWAP))
    low = add_low(pick(low, y, 0), lax.ppermute(pick(low, 1 - y, 0), "y", SWAP))
    top = pick(top, y, 0).astype(F32) + lax.ppermute(pick(top, 1 - y, 0), "y", SWAP).astype(F32)
    low = pick(low, x, 0).astype(F32) + lax.ppermute(pick(low, 1 - x, 0), "x", SWAP).astype(F32)
    return jnp.concatenate([top, low], 0)


def in_order(y, own, other, axis):
    return jnp.where(
        y == 0, jnp.concatenate([own, other], axis), jnp.concatenate([other, own], axis)
    )


def on_device(
    n,
    tokens, norm_gain, norm_bias,
    query_weight, query_bias, key_weight, key_bias, value_weight, value_bias,
    output_weight, output_bias, up_weight, up_bias, down_weight, down_bias,
    doc_split, cotangent,
):
    z, y, x, c = (lax.axis_index(name) for name in ("z", "y", "x", "c"))
    shard_rows = query_weight.shape[0]
    width = query_weight.shape[1] // 2
    hidden_width = up_weight.shape[1] // 2
    chunks = 2
    piece = hidden_width // chunks

    def col(array, start, size):
        return lax.dynamic_slice_in_dim(array, start, size, 1)

    def row(array, start, size):
        return lax.dynamic_slice_in_dim(array, start, size, 0)

    def pack_heads(side):
        return jnp.concatenate(
            [col(w, side * width, width) for w in (query_weight, key_weight, value_weight)]
            + [row(output_weight, side * width, width).T],
            1,
        )

    def pack_hidden(side, chunk):
        start = side * hidden_width + chunk * piece
        return jnp.concatenate(
            [col(up_weight, start, piece), row(down_weight, start, piece).T], 1
        )

    gain_wide = norm_gain.astype(F32)
    tokens_wide = tokens.astype(F32)
    row_mean = jnp.mean(tokens_wide, -1, keepdims=True)
    centred = tokens_wide - row_mean
    inv_scale = lax.rsqrt(jnp.mean(centred * centred, -1, keepdims=True) + EPS)
    standard = centred * inv_scale
    normed = (standard * gain_wide + norm_bias.astype(F32)).astype(BF16)
    phase = lax.optimization_barrier
    packed = (
        pack_hidden(y, 0), pack_hidden(1 - y, 0), pack_heads(y), pack_heads(1 - y),
        pack_hidden(1 - y, 1), normed,
    )
    last_own = pack_hidden(y, 1)
    other_split = lax.ppermute(doc_split, "y", SWAP)
    splits = in_order(y, doc_split, other_split, 0)
    seq_len = 4 * normed.shape[0]
    cosine, sine = turn_tables(splits, seq_len)

    right, left = [None] * n, [None] * n
    first_weights, heads_unit, right[1], left[1], last_swapped, normed_all, cot_all = gather_all(
        n, *packed, cotangent
    )
    last_unit = in_order(y, last_own, last_swapped, 0)
    first_weights, heads_unit, last_unit, normed_all, cot_all, right[1], left[1], cosine, sine = phase(
        (first_weights, heads_unit, last_unit, normed_all, cot_all, right[1], left[1], cosine, sine)
    )

    def hidden_local(weights, chunk):
        bias = row(up_bias, y * hidden_width + chunk * piece, piece).astype(F32)[None]
        return hidden_part(normed_all, cot_all, weights, bias)

    def weight_grads(grad_columns, columns):
        return jnp.concatenate(
            [dot(normed_all, grad_columns, TN).astype(BF16), dot(cot_all, columns, TN).astype(BF16)], 1
        )

    def gather_step(step, source):
        return chain_step(step, n, right[step - 1], left[step - 1]) if step > 1 else chain_step(
            1, n, source, source)

    activated_0, grad_hidden_0, hidden_sum_0 = hidden_local(first_weights, 0)
    right[2], left[2] = gather_step(2, None)
    activated_0, grad_hidden_0, normed_all, cot_all, right[2], left[2] = phase(
        (activated_0, grad_hidden_0, normed_all, cot_all, right[2], left[2])
    )
    grads_first = weight_grads(grad_hidden_0, activated_0)
    for step in range(3, n):
        right[step], left[step] = gather_step(step, None)
    grads_first, activated_0, last_unit, normed_all, cot_all, right[3:], left[3:] = phase(
        (grads_first, activated_0, last_unit, normed_all, cot_all, right[3:], left[3:])
    )
    head_weights = assemble(heads_unit, right, left, n, z)
    qkv_weight, output_turned = head_weights[:, : 3 * width], head_weights[:, 3 * width :]

    qkv_bias = jnp.concatenate(
        [row(b, y * width, width) for b in (query_bias, key_bias, value_bias)]
    ).astype(F32)
    qkv = dot(normed_all, qkv_weight) + qkv_bias
    grad_attended = dot(cot_all, output_turned).astype(BF16)
    right[1], left[1] = gather_step(1, last_unit)
    qkv, grad_attended, normed_all, cot_all, right[1], left[1] = phase(
        (qkv, grad_attended, normed_all, cot_all, right[1], left[1])
    )
    found = attention(0, splits, qkv, grad_attended, cosine, sine, ())
    right[2], left[2] = gather_step(2, None)
    first_in = scatter_step(n - 1, grads_first, n, z, (None, None))
    found, qkv, grad_attended, normed_all, cot_all, right[2], left[2], first_in, grads_first = phase(
        (found, qkv, grad_attended, normed_all, cot_all, right[2], left[2], first_in, grads_first)
    )
    for index in range(1, splits.shape[0]):
        found = attention(index, splits, qkv, grad_attended, cosine, sine, found)
    for step in range(3, n):
        right[step], left[step] = gather_step(step, None)
    for k in range(n - 2, n - 3, -1):
        first_in = scatter_step(k, grads_first, n, z, first_in)
    found, normed_all, cot_all, right[3:], left[3:], first_in, grads_first = phase(
        (found, normed_all, cot_all, right[3:], left[3:], first_in, grads_first)
    )
    attended, grad_qkv = found
    grads_heads = weight_grads(grad_qkv, attended)
    for k in range(n - 3, 0, -1):
        first_in = scatter_step(k, grads_first, n, z, first_in)
    grads_heads, attended, grad_qkv, normed_all, cot_all, last_unit, first_in, grads_first = phase(
        (grads_heads, attended, grad_qkv, normed_all, cot_all, last_unit, first_in, grads_first)
    )
    first_sum = scatter_end(grads_first, n, z, first_in)

    last_weights = assemble(last_unit, right, left, n, z)
    activated_1, grad_hidden_1, hidden_sum_1 = hidden_local(last_weights, 1)
    heads_in = scatter_step(n - 1, grads_heads, n, z, (None, None))
    (last_weights, activated_1, grad_hidden_1, attended, grad_qkv, heads_in, grads_heads,
     normed_all, cot_all) = phase(
        (last_weights, activated_1, grad_hidden_1, attended, grad_qkv, heads_in, grads_heads,
         normed_all, cot_all)
    )
    for k in range(n - 2, n - 3, -1):
        heads_in = scatter_step(k, grads_heads, n, z, heads_in)
    grads_last = weight_grads(grad_hidden_1, activated_1)
    qkv_sum = jnp.sum(grad_qkv, 0, dtype=F32)[None]
    bias_row = jnp.concatenate([qkv_sum, hidden_sum_0, hidden_sum_1], 1)
    cot_wide = cotangent.astype(F32)
    cot_sum = jnp.sum(cot_wide, 0)[None]
    grads_last, heads_in, grads_heads, bias_row, cot_sum = phase(
        (grads_last, heads_in, grads_heads, bias_row, cot_sum)
    )
    for k in range(n - 3, 0, -1):
        heads_in = scatter_step(k, grads_heads, n, z, heads_in)
    heads_sum = scatter_end(grads_heads, n, z, heads_in)

    def halves(total):
        keep = row(total, y * shard_rows, shard_rows)
        give = row(total, (1 - y) * shard_rows, shard_rows).astype(BF16)
        return keep, lax.ppermute(give, "y", SWAP).astype(F32)

    heads_keep, heads_take = halves(heads_sum)
    first_keep, first_take = halves(first_sum)

    if n in (2, 4) and bias_row.shape[1] <= cot_sum.shape[1]:
        spread = cot_sum.shape[1]
        vector = jnp.concatenate([
            jnp.zeros((2, spread), F32), cot_sum,
            jnp.pad(bias_row, ((0, 0), (0, spread - bias_row.shape[1]))),
            jnp.zeros((4, spread), F32),
        ])
        last_keep, last_take, grad_normed, mixed, sums = tail(
            n, grads_last.T, (head_weights, first_weights, last_weights),
            (grad_qkv, grad_hidden_0, grad_hidden_1), (attended, activated_0, activated_1),
            standard, vector,
        )
        last_keep, last_take = last_keep.T, last_take.astype(F32).T
        norm_sums = sums[:3]
        bias_rows = in_order(y, sums[3:4], sums[4:5], 0)[:, : bias_row.shape[1]]
    else:
        partial_out = sum_dots(
            (attended, activated_0, activated_1),
            ((head_weights, width, 3), (first_weights, piece, 1), (last_weights, piece, 1)),
        )
        grad_normed_part = sum_dots(
            (grad_qkv, grad_hidden_0, grad_hidden_1),
            ((head_weights, 3 * width, 0), (first_weights, piece, 0), (last_weights, piece, 0)),
        )
        last_in = (None, None)
        for k in range(n - 1, 0, -1):
            last_in = scatter_step(k, grads_last, n, z, last_in)
        last_keep, last_take = halves(scatter_end(grads_last, n, z, last_in))
        grad_normed = plane_scatter(grad_normed_part, y, x, c)
        mixed = plane_scatter(partial_out, y, x, c)
        norm_sums = sum_small(
            jnp.concatenate([
                jnp.sum(grad_normed * standard, 0)[None], jnp.sum(grad_normed, 0)[None], cot_sum
            ]),
            ("c", "x", "y", "z"),
        )
        bias_row = sum_small(bias_row, ("z",))
        bias_rows = in_order(y, bias_row, lax.ppermute(bias_row, "y", SWAP), 0)
    grad_norm_gain, grad_norm_bias, grad_out_bias = norm_sums

    out_bias = output_bias.astype(F32) + down_bias.astype(F32)
    out = (tokens_wide + mixed + out_bias).astype(BF16)

    def joined(start, size):
        return in_order(
            y, heads_keep[:, start : start + size], heads_take[:, start : start + size], 1
        )

    grad_query_weight, grad_key_weight, grad_value_weight, grad_output_turned = (
        joined(part * width, width) for part in range(4)
    )
    hidden_halves = [(first_keep, first_take), (last_keep, last_take)]

    def side(which, start):
        return jnp.concatenate([pair[which][:, start : start + piece] for pair in hidden_halves], 1)

    grad_up_weight = in_order(y, side(0, 0), side(1, 0), 1)
    grad_down_turned = in_order(y, side(0, piece), side(1, piece), 1)

    grad_query_bias, grad_key_bias, grad_value_bias = (
        bias_rows[:, part * width : (part + 1) * width].reshape(-1) for part in range(3)
    )
    grad_up_bias = bias_rows[:, 3 * width :].reshape(-1)

    grad_scaled = grad_normed * gain_wide
    grad_tokens = cot_wide + inv_scale * (
        grad_scaled
        - jnp.mean(grad_scaled, -1, keepdims=True)
        - standard * jnp.mean(grad_scaled * standard, -1, keepdims=True)
    )
    return (
        out, grad_tokens, grad_norm_gain, grad_norm_bias,
        grad_query_weight, grad_query_bias, grad_key_weight, grad_key_bias,
        grad_value_weight, grad_value_bias, grad_output_turned.T, grad_out_bias,
        grad_up_weight, grad_up_bias, grad_down_turned.T, grad_out_bias,
    )


def solution(mesh):
    n = mesh.shape["dp"] // 2
    grid = Mesh(mesh.devices.reshape(n, 2, mesh.shape["tensor"] // 2, 2), ("z", "y", "x", "c"))
    dp, tensor = ("z", "y"), ("x", "c")
    rows = P(dp + tensor, None)
    whole, split = P(), P(tensor)
    wide, tall = P(dp, tensor), P(tensor, dp)
    in_specs = (
        rows, whole, whole, wide, split, wide, split, wide, split,
        tall, whole, wide, split, tall, whole, P(dp), rows,
    )
    out_specs = (
        rows, rows, whole, whole, wide, split, wide, split, wide, split,
        tall, whole, wide, split, tall, whole,
    )
    return jax.shard_map(
        functools.partial(on_device, n),
        mesh=grid, in_specs=in_specs, out_specs=out_specs, check_vma=False,
    )
```

```python
import functools

import jax
import jax.numpy as jnp
from jax import lax
from jax.experimental import pallas as pl
from jax.experimental.pallas import tpu as pltpu
from jax.sharding import Mesh, PartitionSpec as P

HEAD_DIM = 64
ROT = 32
BLOCK = 256
EPS = 1e-05
LANES = 128
F32 = jnp.float32
BF16 = jnp.bfloat16


SWAP = [(0, 1), (1, 0)]
NT = (((1,), (1,)), ((), ()))
TN = (((0,), (0,)), ((), ()))
NN = (((1,), (0,)), ((), ()))


def dot(left, right, dims=NN):
    return lax.dot_general(left, right, dims, preferred_element_type=F32)


def spin(value, cosine, sine):
    lane = lax.broadcasted_iota(jnp.int32, value.shape, 1) % HEAD_DIM
    half = ROT // 2
    ahead = pltpu.roll(value, LANES - half, 1)
    behind = pltpu.roll(value, half, 1)
    return value * cosine + jnp.where(lane < half, ahead, behind) * sine


def attention_kernel(
    index, earlier, split_ref, qkv_ref, grad_ref, cos_ref, sin_ref, *refs
):
    (att_ref, dqkv_ref, *scratch) = refs[earlier:]
    attention_body(index, split_ref, qkv_ref, grad_ref, cos_ref, sin_ref, att_ref, dqkv_ref, *scratch)


def attention_body(
    index, split_ref, qkv_ref, grad_ref, cos_ref, sin_ref, att_ref, dqkv_ref,
    q_s, k_s, v_s, g_s, kt_s, vt_s, ot_s, dqt_s, dk_s, dv_s, cos_s, sin_s,
):
    seq_len, width = grad_ref.shape
    first = split_ref[index] // BLOCK
    scale = HEAD_DIM ** (-0.5)
    per = LANES // HEAD_DIM
    rest = jnp.zeros((HEAD_DIM - ROT, seq_len), F32)
    cos_part, sin_part = cos_ref[...], sin_ref[...]
    cos_s[...] = jnp.concatenate([cos_part, cos_part, rest + 1.0] * per, 0).T
    sin_s[...] = jnp.concatenate([-sin_part, sin_part, rest] * per, 0).T

    def one_pair(pair, carry):
        def cols(part):
            return pl.ds(pl.multiple_of(part * width + pair * LANES, LANES), LANES)

        cosine, sine = cos_s[...], sin_s[...]
        head_of = lax.broadcasted_iota(jnp.int32, (seq_len, LANES), 1) // HEAD_DIM
        query = spin(qkv_ref[:, cols(0)], cosine, sine).astype(BF16)
        key = spin(qkv_ref[:, cols(1)], cosine, sine).astype(BF16)
        value = qkv_ref[:, cols(2)].astype(BF16)
        grad = grad_ref[:, cols(0)]
        kt_s[...] = key.T
        vt_s[...] = value.T
        for head in range(per):
            here = head_of == head
            q_s[head] = jnp.where(here, query, 0).astype(BF16)
            k_s[head] = jnp.where(here, key, 0).astype(BF16)
            v_s[head] = jnp.where(here, value, 0).astype(BF16)
            g_s[head] = jnp.where(here, grad, 0).astype(BF16)
        dk_s[...] = jnp.zeros_like(dk_s)
        dv_s[...] = jnp.zeros_like(dv_s)

        def one_block(block, inner):
            begin = jnp.where(block >= first, first, 0)
            rows = pl.ds(pl.multiple_of(block * BLOCK, BLOCK), BLOCK)

            def work(count):
                span = pl.ds(pl.multiple_of(begin * BLOCK, BLOCK), count * BLOCK)
                dk, dv = None, None
                for head in range(per):
                    q, g = q_s[head, rows, :], g_s[head, rows, :]
                    own = slice(head * HEAD_DIM, (head + 1) * HEAD_DIM)
                    scores = dot(k_s[head, span, :], q, NT) * scale
                    top = jnp.max(scores, 0, keepdims=True)
                    power = jnp.exp(scores - top)
                    prob = power * (1.0 / jnp.sum(power, 0, keepdims=True))
                    low = prob.astype(BF16)
                    ot_s[own, rows] = dot(vt_s[own, span], low)
                    dprob = dot(v_s[head, span, :], g, NT)
                    mean = jnp.sum(prob * dprob, 0, keepdims=True)
                    dscore = (prob * (dprob - mean) * scale).astype(BF16)
                    dqt_s[own, rows] = dot(kt_s[own, span], dscore)
                    dk_h, dv_h = dot(dscore, q), dot(low, g)
                    dk = dk_h if dk is None else dk + dk_h
                    dv = dv_h if dv is None else dv + dv_h
                dk_s[span, :] += dk
                dv_s[span, :] += dv

            for count in range(1, seq_len // BLOCK):
                pl.when(block - begin == count - 1)(functools.partial(work, count))
            return inner

        lax.fori_loop(0, seq_len // BLOCK, one_block, 0)
        att_ref[:, cols(0)] = ot_s[...].T.astype(BF16)
        dqkv_ref[:, cols(0)] = spin(dqt_s[...].T, cosine, -sine).astype(BF16)
        dqkv_ref[:, cols(1)] = spin(dk_s[...], cosine, -sine).astype(BF16)
        dqkv_ref[:, cols(2)] = dv_s[...].astype(BF16)
        return carry

    lax.fori_loop(0, width // LANES, one_pair, 0)


def attention(index, splits, qkv, grad, cosine, sine, earlier):
    count = splits.shape[0]
    rows, width = grad.shape
    seq_len = rows // count
    per = LANES // HEAD_DIM

    def spec(columns):
        return pl.BlockSpec((seq_len, columns), lambda i, split: (index, 0))

    table = pl.BlockSpec((ROT // 2, seq_len), lambda i, split: (0, index))
    masked = pltpu.VMEM((per, seq_len, LANES), BF16)
    turned = pltpu.VMEM((LANES, seq_len), BF16)
    return pl.pallas_call(
        functools.partial(attention_kernel, index, len(earlier)),
        grid_spec=pltpu.PrefetchScalarGridSpec(
            num_scalar_prefetch=1,
            grid=(1,),
            in_specs=[spec(3 * width), spec(width), table, table]
            + [pl.BlockSpec(memory_space=pl.ANY)] * len(earlier),
            out_specs=[spec(width), spec(3 * width)],
            scratch_shapes=[
                masked, masked, masked, masked, turned, turned,
                pltpu.VMEM((LANES, seq_len), F32),
                pltpu.VMEM((LANES, seq_len), F32),
                pltpu.VMEM((seq_len, LANES), F32),
                pltpu.VMEM((seq_len, LANES), F32),
                pltpu.VMEM((seq_len, LANES), F32),
                pltpu.VMEM((seq_len, LANES), F32),
            ],
        ),
        out_shape=[
            jax.ShapeDtypeStruct((rows, width), BF16),
            jax.ShapeDtypeStruct((rows, 3 * width), BF16),
        ],
        cost_estimate=pl.CostEstimate(
            flops=40 * seq_len * seq_len * width // 4,
            transcendentals=seq_len * seq_len * width // HEAD_DIM // 2,
            bytes_accessed=seq_len * width * 24,
        ),
        input_output_aliases={5 + i: i for i in range(len(earlier))},
        compiler_params=pltpu.CompilerParams(vmem_limit_bytes=48 << 20),
        name="attention",
    )(splits, qkv, grad, cosine, sine, *earlier)


def turn_tables(splits, seq_len):
    shape = (ROT // 2, splits.shape[0], seq_len)
    token = lax.broadcasted_iota(jnp.int32, shape, 2)
    start = splits[None, :, None]
    position = (token - jnp.where(token >= start, start, 0)).astype(F32)
    entry = jnp.arange(ROT // 2, dtype=F32)
    angle = position * (10000.0 ** (-(2.0 * entry) / ROT))[:, None, None]
    return jnp.cos(angle).reshape(ROT // 2, -1), jnp.sin(angle).reshape(ROT // 2, -1)


def sum_dots_kernel(count, *refs):
    out_ref = refs[-1]
    total = None
    for i in range(count):
        part = dot(refs[i][...], refs[count + i][...], NT)
        total = part if total is None else total + part
    out_ref[...] = total.astype(out_ref.dtype)


def sum_dots(lefts, rights, tile=512):
    rows, columns = lefts[0].shape[0], rights[0][0].shape[0]
    tile = min(tile, rows)
    depth = sum(left.shape[1] for left in lefts)
    return pl.pallas_call(
        functools.partial(sum_dots_kernel, len(lefts)),
        grid=(rows // tile,),
        in_specs=[pl.BlockSpec((tile, left.shape[1]), lambda i: (i, 0)) for left in lefts] + [
            pl.BlockSpec((columns, size), functools.partial(lambda at, i: (0, at), at))
            for _, size, at in rights
        ],
        out_specs=pl.BlockSpec((tile, columns), lambda i: (i, 0)),
        out_shape=jax.ShapeDtypeStruct((rows, columns), BF16),
        cost_estimate=pl.CostEstimate(
            flops=2 * rows * columns * depth, transcendentals=0,
            bytes_accessed=2 * (rows * columns + depth * (rows + columns)),
        ),
        compiler_params=pltpu.CompilerParams(vmem_limit_bytes=56 << 20),
        name="sum_dots",
    )(*lefts, *(right[0] for right in rights))


def hidden_kernel(n_ref, c_ref, w_ref, bias_ref, act_ref, dh_ref, sum_ref):
    piece = act_ref.shape[1]
    hidden = dot(n_ref[...], w_ref[:, :piece]) + bias_ref[...]
    grad = dot(c_ref[...], w_ref[:, piece:])
    rate = (2.0 / jnp.pi) ** 0.5
    square = hidden * hidden
    bent = jnp.tanh(rate * hidden * (1.0 + 0.044715 * square))
    act_ref[...] = (0.5 * hidden * (1.0 + bent)).astype(BF16)
    slope = 0.5 * (1.0 + bent) + 0.5 * hidden * (1.0 - bent * bent) * (
        rate * (1.0 + 3.0 * 0.044715 * square)
    )
    low = (grad * slope).astype(BF16)
    dh_ref[...] = low

    @pl.when(pl.program_id(0) == 0)
    def _():
        sum_ref[...] = jnp.zeros_like(sum_ref)

    sum_ref[...] += jnp.sum(low.astype(F32), 0, keepdims=True)


def hidden_part(normed_all, cot_all, weights, bias, tile=512):
    rows, depth = normed_all.shape
    piece = weights.shape[1] // 2
    tile = min(tile, rows)
    wide = pl.BlockSpec((tile, depth), lambda i: (i, 0))
    thin = pl.BlockSpec((tile, piece), lambda i: (i, 0))
    line = pl.BlockSpec((1, piece), lambda i: (0, 0))
    return pl.pallas_call(
        hidden_kernel,
        grid=(rows // tile,),
        in_specs=[wide, wide, pl.BlockSpec(weights.shape, lambda i: (0, 0)), line],
        out_specs=[thin, thin, line],
        out_shape=[
            jax.ShapeDtypeStruct((rows, piece), BF16),
            jax.ShapeDtypeStruct((rows, piece), BF16),
            jax.ShapeDtypeStruct((1, piece), F32),
        ],
        cost_estimate=pl.CostEstimate(
            flops=4 * rows * depth * piece, transcendentals=rows * piece,
            bytes_accessed=4 * rows * depth + 4 * depth * piece + 4 * rows * piece,
        ),
        compiler_params=pltpu.CompilerParams(vmem_limit_bytes=48 << 20),
        name="hidden_part",
    )(normed_all, cot_all, weights, bias)


def gather_kernel(
    n, own_ref, other_ref, second_ref, second_other_ref, next_ref, norm_ref, cot_ref,
    w_ref, unit_ref, right_ref, left_ref, swapped_ref, n_ref, c_ref, send_sem, recv_sem, local_sem,
):
    z, y, x, c = (lax.axis_index(name) for name in ("z", "y", "x", "c"))
    rows = norm_ref.shape[0]
    half = 3 * rows // 4
    mine = y * 4 + x * 2 + c
    has_right, has_left = z < n - 1, z > 0
    number = {}

    def remote(key, src, dst, axis, target):
        slot = number.setdefault(key, len(number))
        return pltpu.make_async_remote_copy(
            src_ref=src, dst_ref=dst, send_sem=send_sem.at[slot], recv_sem=recv_sem.at[slot],
            device_id={axis: target}, device_id_type=pl.DeviceIdType.MESH,
        )

    def when(condition, action):
        if condition is None:
            action()
        else:
            pl.when(condition)(action)

    started = []

    def start(condition, copy):
        when(condition, copy.start)
        started.append((condition, copy))

    def shard(index, unit):
        return w_ref.at[index * 2 + (y if unit == 0 else 1 - y)]

    def along(step, unit, sign, receiving=False):
        index = z - sign * step if receiving else z - sign * (step - 1)
        source = own_ref if step == 1 and unit == 0 and not receiving else shard(index, unit)
        return remote((step, unit, sign), source, shard(index, unit), "z", z + sign)


    full, top, low = pl.ds(0, rows), pl.ds(0, half), pl.ds(half, rows - half)
    arrays = ((n_ref, norm_ref, "n"), (c_ref, cot_ref, "c"))
    at_x, at_y, at_xy = y * 4 + (1 - x) * 2 + c, (1 - y) * 4 + x * 2 + c, (1 - y) * 4 + (1 - x) * 2 + c

    barrier = pltpu.get_barrier_semaphore()
    for axis, target in (("x", 1 - x), ("y", 1 - y), ("c", 1 - c)):
        pl.semaphore_signal(
            barrier, inc=1, device_id={axis: target}, device_id_type=pl.DeviceIdType.MESH
        )
    for condition, target in ((has_right, z + 1), (has_left, z - 1)):
        when(condition, functools.partial(
            pl.semaphore_signal, barrier, inc=1, device_id={"z": target},
            device_id_type=pl.DeviceIdType.MESH,
        ))
    pl.semaphore_wait(barrier, 3 + has_right.astype(jnp.int32) + has_left.astype(jnp.int32))

    for condition, sign in ((has_right, 1), (has_left, -1)):
        start(condition, along(1, 0, sign))
    swap = remote("swap", other_ref, w_ref.at[z * 2 + y], "y", 1 - y)
    swap_in = remote("swap", other_ref, w_ref.at[z * 2 + 1 - y], "y", 1 - y)
    start(None, swap)
    for array, source, name in arrays:
        for axis in ("x", "y", "c"):
            start(None, remote((name, axis), source, array.at[mine], axis,
                               {"x": 1 - x, "y": 1 - y, "c": 1 - c}[axis]))
    unit_swap = remote("unit", second_other_ref, unit_ref.at[y], "y", 1 - y)
    unit_swap_in = remote("unit", second_other_ref, unit_ref.at[1 - y], "y", 1 - y)
    start(None, unit_swap)
    late_swap = remote("late", next_ref, swapped_ref, "y", 1 - y)
    start(None, late_swap)
    local = [
        pltpu.make_async_copy(own_ref, shard(z, 0), local_sem.at[0]),
        pltpu.make_async_copy(norm_ref, n_ref.at[mine], local_sem.at[1]),
        pltpu.make_async_copy(cot_ref, c_ref.at[mine], local_sem.at[2]),
        pltpu.make_async_copy(second_ref, unit_ref.at[y], local_sem.at[3]),
    ]
    for copy in local:
        copy.start()

    def arrive_swap():
        swap_in.wait_recv()
        for condition, sign in ((has_right, 1), (has_left, -1)):
            start(condition, along(1, 1, sign))

    def arrive_shard(step, unit, sign):
        inside = z - sign * step >= 0 if sign > 0 else z + step < n
        further = has_right if sign > 0 else has_left
        when(inside, along(step, unit, sign, True).wait_recv)
        if step + 1 < n:
            start(inside & further, along(step + 1, unit, sign))

    def arrive_rows(array, name, axis):
        index = {"x": at_x, "y": at_y, "c": None}[axis]
        block = array.at[index]
        remote((name, axis), block, block, axis, 0).wait_recv()
        part, on = (low, "y") if axis == "x" else (top, "x")
        piece = array.at[index, part]
        start(None, remote((name, "far", on), piece, piece, on, {"x": 1 - x, "y": 1 - y}[on]))
        start(None, remote((name, "core", axis), block, block, "c", 1 - c))

    def arrive_far(array, name, on):
        part = low if on == "y" else top
        piece = array.at[at_xy, part]
        remote((name, "far", on), piece, piece, on, 0).wait_recv()
        start(None, remote((name, "core", "far", on), piece, piece, "c", 1 - c))

    def arrive_steps(step):
        for unit in (0, 1):
            for sign in (1, -1):
                arrive_shard(step, unit, sign)

    def second_step(half_of, receiving):
        index = y if half_of == 0 else 1 - y
        source = second_ref if half_of == 0 else unit_ref.at[index]
        ways = ((1, has_left if receiving else has_right, right_ref),
                (-1, has_right if receiving else has_left, left_ref))
        for sign, condition, target in ways:
            copy = remote(("second", half_of, sign), source, target.at[index], "z", z + sign)
            if receiving:
                when(condition, copy.wait_recv)
            else:
                start(condition, copy)

    (norm, _, norm_name), (cot, _, cot_name) = arrays
    arrive_swap()
    arrive_rows(norm, norm_name, "x")
    for sign in (1, -1):
        arrive_shard(1, 0, sign)
    arrive_rows(norm, norm_name, "y")
    for sign in (1, -1):
        arrive_shard(1, 1, sign)
    arrive_rows(cot, cot_name, "x")
    if n > 2:
        arrive_steps(2)
    second_step(0, False)
    arrive_rows(cot, cot_name, "y")
    unit_swap_in.wait_recv()
    second_step(1, False)
    for step in range(3, n):
        arrive_steps(step)
    for array, _, name in arrays:
        for on in ("x", "y"):
            arrive_far(array, name, on)
    for array, _, name in arrays:
        for key, index, part in (
            ((name, "c"), y * 4 + x * 2 + 1 - c, full),
            ((name, "core", "x"), y * 4 + (1 - x) * 2 + 1 - c, full),
            ((name, "core", "y"), (1 - y) * 4 + x * 2 + 1 - c, full),
            ((name, "core", "far", "x"), (1 - y) * 4 + (1 - x) * 2 + 1 - c, top),
            ((name, "core", "far", "y"), (1 - y) * 4 + (1 - x) * 2 + 1 - c, low),
        ):
            piece = array.at[index, part]
            remote(key, piece, piece, "c", 0).wait_recv()
    late_swap.wait_recv()
    for half_of in (0, 1):
        second_step(half_of, True)
    for copy in local:
        copy.wait()
    for condition, copy in started:
        when(condition, copy.wait_send)


def gather_all(n, own, other, second, second_other, following, normed, cotangent):
    rows, columns = normed.shape
    copies = 4 * (n - 1) + 8 + 2 * 9
    anywhere = pl.BlockSpec(memory_space=pl.ANY)
    pair = jax.ShapeDtypeStruct((2,) + second.shape, second.dtype)
    weights, unit, right, left, swapped, normed_all, cot_all = pl.pallas_call(
        functools.partial(gather_kernel, n),
        in_specs=[anywhere] * 7,
        out_specs=[anywhere] * 7,
        out_shape=[
            jax.ShapeDtypeStruct((2 * n,) + own.shape, own.dtype),
            pair, pair, pair,
            jax.ShapeDtypeStruct(following.shape, following.dtype),
            jax.ShapeDtypeStruct((8, rows, columns), normed.dtype),
            jax.ShapeDtypeStruct((8, rows, columns), cotangent.dtype),
        ],
        scratch_shapes=[
            pltpu.SemaphoreType.DMA((copies,)),
            pltpu.SemaphoreType.DMA((copies,)),
            pltpu.SemaphoreType.DMA((4,)),
        ],
        cost_estimate=pl.CostEstimate(flops=0, transcendentals=0, bytes_accessed=200 << 20),
        compiler_params=pltpu.CompilerParams(collective_id=0, has_side_effects=True),
        name="gather_rows",
    )(own, other, second, second_other, following, normed, cotangent)
    flat = lambda array: array.reshape(-1, array.shape[-1])
    return tuple(map(flat, (weights, unit, right, left, swapped, normed_all, cot_all)))


def chain_step(step, n, right, left):
    return (
        lax.ppermute(right, "z", [(i, i + 1) for i in range(step - 1, n - 1)]),
        lax.ppermute(left, "z", [(i, i - 1) for i in range(1, n - step + 1)]),
    )


def assemble(unit, right, left, n, z):
    rows, columns = unit.shape
    whole = jnp.zeros((n * rows, columns), unit.dtype)
    for k in range(n):
        piece = unit if k == 0 else jnp.where(z >= k, right[k], left[n - k])
        row = lax.rem(z - k + n, n) * rows
        whole = lax.dynamic_update_slice(whole, piece, (row, jnp.int32(0)))
    return whole


def scatter_pieces(k, grads, n, z, received):
    rows = grads.shape[0] // n

    def piece(index, got):
        own = lax.dynamic_slice_in_dim(grads, jnp.clip(index, 0, n - 1) * rows, rows, 0)
        return own if got is None else add_low(own, got)

    return piece(z - k, received[0]), piece(z + k, received[1])


def scatter_step(k, grads, n, z, received):
    to_left, to_right = scatter_pieces(k, grads, n, z, received)
    return (
        lax.ppermute(to_left, "z", [(r, r - 1) for r in range(k, n)]),
        lax.ppermute(to_right, "z", [(r, r + 1) for r in range(0, n - k)]),
    )


def scatter_end(grads, n, z, received):
    rows = grads.shape[0] // n
    own = lax.dynamic_slice_in_dim(grads, z * rows, rows, 0).astype(F32)
    return own + received[0].astype(F32) + received[1].astype(F32)


def tail_kernel(
    n, g_ref, hw_ref, fw_ref, lw_ref, dq_ref, d0_ref, d1_ref, at_ref, a0_ref, a1_ref,
    left_ref, right_ref, own_ref, std_ref, vec_ref,
    keep_ref, take_ref, heads_keep_ref, heads_take_ref, out_ref, mixed_ref, sums_ref,
    hw_s, fw_s, lw_s, rows_s, stage, zrecv, give, heads_recv, heads_own, heads_give, both, xtop_2, ylow_2, ytop_2, xlow_2,
    top_2, low_2, vstage, vrecv, send_sem, recv_sem, load_sem, rows_sem,
):
    z, y, x, c = (lax.axis_index(name) for name in ("z", "y", "x", "c"))
    rows, columns = out_ref.shape
    wide, wide_heads = give.shape[0], heads_give.shape[0]
    half = 5 * rows // 8
    rest = rows - half
    number, started = {}, []

    def remote(key, src, dst, axis, target):
        slot = number.setdefault(key, len(number))
        return pltpu.make_async_remote_copy(
            src_ref=src, dst_ref=dst, send_sem=send_sem.at[slot], recv_sem=recv_sem.at[slot],
            device_id={axis: target}, device_id_type=pl.DeviceIdType.MESH,
        )

    def when(condition, action):
        if condition is None:
            action()
        else:
            pl.when(condition)(action)

    def start(condition, copy):
        when(condition, copy.start)
        started.append((condition, copy))

    def each(count, size, body):
        def step(i, carry):
            body(pl.ds(pl.multiple_of(i * size, size), size))
            return carry
        lax.fori_loop(0, count // size, step, 0)

    barrier = pltpu.get_barrier_semaphore()
    greet = [(None, "x", 1 - x), (None, "y", 1 - y), (None, "c", 1 - c)]
    greet += [(z < n - 1, "z", z + 1), (z > 0, "z", z - 1)]
    for step in (2 ** i for i in range(1, n.bit_length() - 1)):
        greet.append((None, "z", jnp.bitwise_xor(z, step)))
    for condition, axis, target in greet:
        when(condition, functools.partial(
            pl.semaphore_signal, barrier, inc=1, device_id={axis: target},
            device_id_type=pl.DeviceIdType.MESH))

    loads = [
        pltpu.make_async_copy(source, target, load_sem.at[i])
        for i, (source, target) in enumerate(
            ((hw_ref, hw_s), (fw_ref, fw_s), (lw_ref, lw_s), (own_ref, heads_own)))
    ]
    for load in loads:
        load.start()

    firsts, lasts = fw_ref.shape[1] // 2, lw_ref.shape[1] // 2
    heads = dq_ref.shape[1]
    sums = (
        ((dq_ref, heads, hw_s, 0), (d0_ref, firsts, fw_s, 0), (d1_ref, lasts, lw_s, 0)),
        ((at_ref, heads // 3, hw_s, heads), (a0_ref, firsts, fw_s, firsts),
         (a1_ref, lasts, lw_s, lasts)),
    )
    jobs = [(a, own, j) for a in (0, 1) for own in (False, True) for j in (0, 1)]

    def row_loads(number_of):
        a, own, j = jobs[number_of]
        slot, core, copies, at = number_of % 2, c if own else 1 - c, [], 0
        for p, (left, width, _, _) in enumerate(sums[a]):
            for i in (0, 1):
                block = j * 4 + i * 2 + core
                source = left.at[pl.ds(pl.multiple_of(block * rows, rows), rows)]
                target = rows_s.at[slot, pl.ds(i * rows, rows), pl.ds(at, width)]
                copies.append(pltpu.make_async_copy(source, target, rows_sem.at[slot, p * 2 + i]))
            at += width
        return copies

    def job(number_of):
        a, own, j = jobs[number_of]
        slot = number_of % 2
        if number_of + 1 < len(jobs):
            for copy in row_loads(number_of + 1):
                copy.start()
        for copy in row_loads(number_of):
            copy.wait()
        if own:
            for i in (0, 1):
                core_copy(a, j * 2 + i).wait_recv()
        elif a == 1:
            for i in (0, 1):
                core_copy(0, j * 2 + i).wait_send()
        size = min(512, columns)

        def tile(t, carry):
            span = pl.ds(pl.multiple_of(t * size, size), size)
            acc, at = None, 0
            for left, width, weights, column in sums[a]:
                part = dot(
                    rows_s[slot, :, at : at + width], weights[span, column : column + width], NT)
                acc = part if acc is None else acc + part
                at += width
            for i in (0, 1):
                piece = acc[i * rows : (i + 1) * rows]
                if own:
                    both[a, j * 2 + i, :, span] = (
                        piece + both[a, j * 2 + i, :, span].astype(F32)).astype(BF16)
                else:
                    stage[j * 2 + i, :, span] = piece.astype(BF16)
            return carry

        lax.fori_loop(0, columns // size, tile, 0)
        if not own:
            for i in (0, 1):
                copy = core_copy(a, j * 2 + i)
                copy.start()
                if a == 1:
                    started.append((None, copy))

    def core_copy(a, i):
        return remote(("core", a, i), stage.at[i], both.at[a, i], "c", 1 - c)

    for copy in row_loads(0):
        copy.start()
    always = sum(condition is None for condition, _, _ in greet)
    pl.semaphore_wait(barrier, always + sum(
        condition.astype(jnp.int32) for condition, _, _ in greet if condition is not None))

    def first_copy(a, name, j):
        if name == "xtop":
            source = both.at[a, j * 2 + 1 - x, pl.ds(0, half)]
            return remote((name, a, j), source, xtop_2.at[a, j], "x", 1 - x)
        source = both.at[a, (1 - y) * 2 + j, pl.ds(half, rest)]
        return remote((name, a, j), source, ylow_2.at[a, j], "y", 1 - y)

    def second_copy(a, name):
        if name == "ytop":
            return remote((name, a), top_2.at[a], ytop_2.at[a], "y", 1 - y)
        return remote((name, a), low_2.at[a], xlow_2.at[a], "x", 1 - x)

    def first_send(a):
        for j in (0, 1):
            start(None, first_copy(a, "xtop", j))
            start(None, first_copy(a, "ylow", j))

    def first_arrive(a):
        for j in (0, 1):
            first_copy(a, "xtop", j).wait_recv()
            first_copy(a, "ylow", j).wait_recv()

        def upper(part):
            top_2[a, part, :] = (
                both[a, (1 - y) * 2 + x, part, :].astype(F32)
                + xtop_2[a, 1 - y, part, :].astype(F32)
            ).astype(BF16)

        def lower(part):
            low_part = pl.ds(part.start + half, part.size)
            low_2[a, part, :] = (
                both[a, y * 2 + 1 - x, low_part, :].astype(F32)
                + ylow_2[a, 1 - x, part, :].astype(F32)
            ).astype(BF16)

        each(half, 32, upper)
        each(rest, 32, lower)
        start(None, second_copy(a, "ytop"))
        start(None, second_copy(a, "xlow"))

    def second_arrive(a):
        second_copy(a, "ytop").wait_recv()
        second_copy(a, "xlow").wait_recv()
        target = (out_ref, mixed_ref)[a]

        def finish(first, part, placed, last):
            value = (
                both[a, y * 2 + x, placed, :].astype(F32) + first[part, :].astype(F32)
                + last[part, :].astype(F32)
            )
            target[placed, :] = value
            if a == 0:
                scaled = value * std_ref[placed, :]
                vstage[0, 0:1, :] += jnp.sum(scaled, 0, keepdims=True)
                vstage[0, 1:2, :] += jnp.sum(value, 0, keepdims=True)

        def upper(part):
            finish(xtop_2.at[a, y], part, part, ytop_2.at[a])

        def lower(part):
            finish(ylow_2.at[a, x], part, pl.ds(part.start + half, part.size), xlow_2.at[a])

        each(half, 32, upper)
        each(rest, 32, lower)

    sides = (1 - y, y)

    def block_of(direction, k, u):
        index = (z - k if direction == 0 else z + k) * 2 + sides[u]
        return pl.ds(pl.multiple_of(index * rows, rows), rows)

    def z_copy(direction, k, u, src):
        target = z - 1 if direction == 0 else z + 1
        return remote((direction, k, u), src, zrecv.at[direction, k - 1, u], "z", target)

    def z_first(direction):
        edge = z == n - 1 if direction == 0 else z == 0
        for k in range(n - 1, 0, -1):
            for u in (0, 1):
                start(edge, z_copy(direction, k, u, g_ref.at[:, block_of(direction, k, u)]))

    def z_step(k, u):
        for direction in (0, 1):
            if direction == 0:
                inside = (z >= k) & (z < n - 1)
            else:
                inside = (n - 1 - z >= k) & (z > 0)
            held = zrecv.at[direction, k, u]

            def add():
                z_copy(direction, k + 1, u, held).wait_recv()
                block = block_of(direction, k, u)

                def body(part):
                    held[part, :] = (
                        g_ref[part, block].astype(F32) + held[part, :].astype(F32)
                    ).astype(BF16)

                each(wide, 256, body)

            when(inside, add)
            start(inside, z_copy(direction, k, u, held))

    def z_last(u, target):
        block = block_of(0, 0, u)

        def first(part):
            target[part, :] = g_ref[part, block].astype(F32)

        each(wide, 256, first)
        for direction in (0, 1):
            held = zrecv.at[direction, 0, u]

            def add():
                z_copy(direction, 1, u, held).wait_recv()

                def body(part):
                    target[part, :] += held[part, :].astype(F32)

                each(wide, 256, body)

            when(z < n - 1 if direction == 0 else z > 0, add)

    def heads_copy(direction, u):
        span = pl.ds(pl.multiple_of(sides[u] * rows, rows), rows)
        source = (left_ref, right_ref)[direction].at[:, span]
        return remote(
            ("heads", direction, u), source, heads_recv.at[direction, :, span], "z",
            z - 1 if direction == 0 else z + 1)

    def heads_send():
        for u in (0, 1):
            start(z > 0, heads_copy(0, u))
            start(z < n - 1, heads_copy(1, u))

    def heads_last(u, target):
        span = pl.ds(pl.multiple_of(sides[u] * rows, rows), rows)

        def first(part):
            target[part, :] = heads_own[part, span].astype(F32)

        each(wide_heads, 256, first)
        for direction in (0, 1):
            def add():
                heads_copy(direction, u).wait_recv()

                def body(part):
                    target[part, :] += heads_recv[direction, part, span].astype(F32)

                each(wide_heads, 256, body)

            when(z < n - 1 if direction == 0 else z > 0, add)

    steps = [(k, u) for k in range(n - 2, 0, -1) for u in (0, 1)]

    def z_next():
        if steps:
            z_step(*steps.pop(0))

    for direction in (0, 1):
        z_first(direction)
    vstage[0] = vec_ref[...]
    for load in loads:
        load.wait()
    job(0)
    job(1)
    z_next()
    job(2)
    job(3)
    first_send(0)
    heads_send()
    z_next()
    job(4)
    job(5)
    z_next()
    job(6)
    job(7)
    first_arrive(0)
    first_send(1)
    while steps:
        z_next()
    second_arrive(0)

    turns = [("z", jnp.bitwise_xor(z, 2 ** i)) for i in range(n.bit_length() - 1)]
    turns += [("y", 1 - y), ("x", 1 - x), ("c", 1 - c)]
    line = lax.broadcasted_iota(jnp.int32, vec_ref.shape, 0)
    for i, (axis, target) in enumerate(turns):
        copy = remote(("vec", i), vstage.at[i], vrecv.at[i], axis, target)
        start(None, copy)
        copy.wait_recv()
        old, new = vstage[i], vrecv[i]
        joined = old + jnp.where((line < 3) | (axis == "z"), new, 0.0)
        result = sums_ref if i == len(turns) - 1 else vstage.at[i + 1]
        result[...] = joined
        if axis == "y":
            result[4:5, :] = new[3:4, :]

    def swapped(key, source, target, length, received):
        def lower_precision(part):
            target[part, :] = source[part, :].astype(BF16)

        each(length, 256, lower_precision)
        copy = remote(key, target, received, "y", 1 - y)
        start(None, copy)
        return copy

    z_last(0, keep_ref)
    swap = swapped("swap", keep_ref, give, wide, take_ref)
    first_arrive(1)
    heads_last(0, heads_keep_ref)
    heads_swap = swapped("heads swap", heads_keep_ref, heads_give, wide_heads, heads_take_ref)
    z_last(1, keep_ref)
    heads_last(1, heads_keep_ref)
    second_arrive(1)
    swap.wait_recv()
    heads_swap.wait_recv()
    for condition, copy in started:
        when(condition, copy.wait_send)


def tail(n, grads_turned, weights, lefts, lefts_out, heads_turned, standard, vector):
    rows, columns = standard.shape
    wide, wide_heads = grads_turned.shape[0], heads_turned[0].shape[0]
    half = 5 * rows // 8
    inside = pl.BlockSpec(memory_space=pltpu.VMEM)
    anywhere = pl.BlockSpec(memory_space=pl.ANY)
    copies = 4 * (n - 1) + 46
    low = lambda *shape: pltpu.VMEM(shape, BF16)
    small = vector.shape
    depth = sum(left.shape[1] for left in lefts)
    return pl.pallas_call(
        functools.partial(tail_kernel, n),
        in_specs=[inside] + [anywhere] * 12 + [inside, inside],
        out_specs=[inside] * 7,
        out_shape=[
            jax.ShapeDtypeStruct((wide, rows), F32),
            jax.ShapeDtypeStruct((wide, rows), BF16),
            jax.ShapeDtypeStruct((wide_heads, rows), F32),
            jax.ShapeDtypeStruct((wide_heads, rows), BF16),
            jax.ShapeDtypeStruct((rows, columns), F32),
            jax.ShapeDtypeStruct((rows, columns), F32),
            jax.ShapeDtypeStruct(small, F32),
        ],
        scratch_shapes=[low(*array.shape) for array in weights] + [
            low(2, 2 * rows, depth), low(4, rows, columns),
            low(2, n - 1, 2, wide, rows), low(wide, rows),
            low(2, wide_heads, 2 * rows), low(wide_heads, 2 * rows), low(wide_heads, rows),
            low(2, 4, rows, columns),
            low(2, 2, half, columns), low(2, 2, rows - half, columns),
            low(2, half, columns), low(2, rows - half, columns),
            low(2, half, columns), low(2, rows - half, columns),
            pltpu.VMEM((8,) + small, F32), pltpu.VMEM((8,) + small, F32),
            pltpu.SemaphoreType.DMA((copies,)),
            pltpu.SemaphoreType.DMA((copies,)),
            pltpu.SemaphoreType.DMA((4,)),
            pltpu.SemaphoreType.DMA((2, 6)),
        ],
        cost_estimate=pl.CostEstimate(flops=0, transcendentals=0, bytes_accessed=200 << 20),
        compiler_params=pltpu.CompilerParams(
            collective_id=1, has_side_effects=True, vmem_limit_bytes=63 << 20
        ),
        name="scatter_rest",
    )(grads_turned, *weights, *lefts, *lefts_out, *heads_turned, standard, vector)


def sum_small(array, axes):
    for axis in axes:
        size = lax.axis_size(axis)
        if size & (size - 1):
            array = lax.psum(array, axis)
            continue
        step = 1
        while step < size:
            array = array + lax.ppermute(array, axis, [(i, i ^ step) for i in range(size)])
            step *= 2
    return array


def pick(array, index, axis):
    return lax.dynamic_index_in_dim(array, index, axis, keepdims=False)


def add_low(left, right):
    return (left.astype(F32) + right.astype(F32)).astype(BF16)


def plane_scatter(partial, y, x, c):
    rows, columns = partial.shape[0] // 8, partial.shape[1]
    half = rows // 2
    parts = partial.reshape(2, 2, 2, rows, columns)
    acc = add_low(pick(parts, c, 2), lax.ppermute(pick(parts, 1 - c, 2), "c", SWAP))
    top, low = acc[:, :, :half], acc[:, :, half:]
    top = add_low(pick(top, x, 1), lax.ppermute(pick(top, 1 - x, 1), "x", SWAP))
    low = add_low(pick(low, y, 0), lax.ppermute(pick(low, 1 - y, 0), "y", SWAP))
    top = pick(top, y, 0).astype(F32) + lax.ppermute(pick(top, 1 - y, 0), "y", SWAP).astype(F32)
    low = pick(low, x, 0).astype(F32) + lax.ppermute(pick(low, 1 - x, 0), "x", SWAP).astype(F32)
    return jnp.concatenate([top, low], 0)


def in_order(y, own, other, axis):
    return jnp.where(
        y == 0, jnp.concatenate([own, other], axis), jnp.concatenate([other, own], axis)
    )


def on_device(
    n,
    tokens, norm_gain, norm_bias,
    query_weight, query_bias, key_weight, key_bias, value_weight, value_bias,
    output_weight, output_bias, up_weight, up_bias, down_weight, down_bias,
    doc_split, cotangent,
):
    z, y, x, c = (lax.axis_index(name) for name in ("z", "y", "x", "c"))
    shard_rows = query_weight.shape[0]
    width = query_weight.shape[1] // 2
    hidden_width = up_weight.shape[1] // 2
    chunks = 2
    piece = hidden_width // chunks

    def col(array, start, size):
        return lax.dynamic_slice_in_dim(array, start, size, 1)

    def row(array, start, size):
        return lax.dynamic_slice_in_dim(array, start, size, 0)

    def pack_heads(side):
        return jnp.concatenate(
            [col(w, side * width, width) for w in (query_weight, key_weight, value_weight)]
            + [row(output_weight, side * width, width).T],
            1,
        )

    def pack_hidden(side, chunk):
        start = side * hidden_width + chunk * piece
        return jnp.concatenate(
            [col(up_weight, start, piece), row(down_weight, start, piece).T], 1
        )

    gain_wide = norm_gain.astype(F32)
    tokens_wide = tokens.astype(F32)
    row_mean = jnp.mean(tokens_wide, -1, keepdims=True)
    centred = tokens_wide - row_mean
    inv_scale = lax.rsqrt(jnp.mean(centred * centred, -1, keepdims=True) + EPS)
    standard = centred * inv_scale
    normed = (standard * gain_wide + norm_bias.astype(F32)).astype(BF16)
    phase = lax.optimization_barrier
    packed = (
        pack_hidden(y, 0), pack_hidden(1 - y, 0), pack_heads(y), pack_heads(1 - y),
        pack_hidden(1 - y, 1), normed,
    )
    last_own = pack_hidden(y, 1)
    other_split = lax.ppermute(doc_split, "y", SWAP)
    splits = in_order(y, doc_split, other_split, 0)
    seq_len = 4 * normed.shape[0]
    cosine, sine = turn_tables(splits, seq_len)

    right, left = [None] * n, [None] * n
    first_weights, heads_unit, right[1], left[1], last_swapped, normed_all, cot_all = gather_all(
        n, *packed, cotangent
    )
    last_unit = in_order(y, last_own, last_swapped, 0)
    first_weights, heads_unit, last_unit, normed_all, cot_all, right[1], left[1], cosine, sine = phase(
        (first_weights, heads_unit, last_unit, normed_all, cot_all, right[1], left[1], cosine, sine)
    )

    def hidden_local(weights, chunk):
        bias = row(up_bias, y * hidden_width + chunk * piece, piece).astype(F32)[None]
        return hidden_part(normed_all, cot_all, weights, bias)

    def weight_grads(grad_columns, columns):
        return jnp.concatenate(
            [dot(normed_all, grad_columns, TN).astype(BF16), dot(cot_all, columns, TN).astype(BF16)], 1
        )

    def gather_step(step, source):
        return chain_step(step, n, right[step - 1], left[step - 1]) if step > 1 else chain_step(
            1, n, source, source)

    activated_0, grad_hidden_0, hidden_sum_0 = hidden_local(first_weights, 0)
    right[2], left[2] = gather_step(2, None)
    activated_0, grad_hidden_0, normed_all, cot_all, right[2], left[2] = phase(
        (activated_0, grad_hidden_0, normed_all, cot_all, right[2], left[2])
    )
    grads_first = weight_grads(grad_hidden_0, activated_0)
    for step in range(3, n):
        right[step], left[step] = gather_step(step, None)
    grads_first, activated_0, last_unit, normed_all, cot_all, right[3:], left[3:] = phase(
        (grads_first, activated_0, last_unit, normed_all, cot_all, right[3:], left[3:])
    )
    head_weights = assemble(heads_unit, right, left, n, z)
    qkv_weight, output_turned = head_weights[:, : 3 * width], head_weights[:, 3 * width :]

    qkv_bias = jnp.concatenate(
        [row(b, y * width, width) for b in (query_bias, key_bias, value_bias)]
    ).astype(F32)
    qkv = dot(normed_all, qkv_weight) + qkv_bias
    grad_attended = dot(cot_all, output_turned).astype(BF16)
    right[1], left[1] = gather_step(1, last_unit)
    qkv, grad_attended, normed_all, cot_all, right[1], left[1] = phase(
        (qkv, grad_attended, normed_all, cot_all, right[1], left[1])
    )
    found = attention(0, splits, qkv, grad_attended, cosine, sine, ())
    right[2], left[2] = gather_step(2, None)
    first_in = scatter_step(n - 1, grads_first, n, z, (None, None))
    found, qkv, grad_attended, normed_all, cot_all, right[2], left[2], first_in, grads_first = phase(
        (found, qkv, grad_attended, normed_all, cot_all, right[2], left[2], first_in, grads_first)
    )
    for index in range(1, splits.shape[0]):
        found = attention(index, splits, qkv, grad_attended, cosine, sine, found)
    for step in range(3, n):
        right[step], left[step] = gather_step(step, None)
    for k in range(n - 2, n - 3, -1):
        first_in = scatter_step(k, grads_first, n, z, first_in)
    found, normed_all, cot_all, right[3:], left[3:], first_in, grads_first = phase(
        (found, normed_all, cot_all, right[3:], left[3:], first_in, grads_first)
    )
    attended, grad_qkv = found
    grads_heads = weight_grads(grad_qkv, attended)
    for k in range(n - 3, 0, -1):
        first_in = scatter_step(k, grads_first, n, z, first_in)
    grads_heads, attended, grad_qkv, normed_all, cot_all, last_unit, first_in, grads_first = phase(
        (grads_heads, attended, grad_qkv, normed_all, cot_all, last_unit, first_in, grads_first)
    )
    first_sum = scatter_end(grads_first, n, z, first_in)

    last_weights = assemble(last_unit, right, left, n, z)
    activated_1, grad_hidden_1, hidden_sum_1 = hidden_local(last_weights, 1)
    heads_in = scatter_step(n - 1, grads_heads, n, z, (None, None))
    (last_weights, activated_1, grad_hidden_1, attended, grad_qkv, heads_in, grads_heads,
     normed_all, cot_all) = phase(
        (last_weights, activated_1, grad_hidden_1, attended, grad_qkv, heads_in, grads_heads,
         normed_all, cot_all)
    )
    for k in range(n - 2, max(n - 3, 1), -1):
        heads_in = scatter_step(k, grads_heads, n, z, heads_in)
    grads_last = weight_grads(grad_hidden_1, activated_1)
    qkv_sum = jnp.sum(grad_qkv, 0, dtype=F32)[None]
    bias_row = jnp.concatenate([qkv_sum, hidden_sum_0, hidden_sum_1], 1)
    cot_wide = cotangent.astype(F32)
    cot_sum = jnp.sum(cot_wide, 0)[None]
    grads_last, heads_in, grads_heads, bias_row, cot_sum = phase(
        (grads_last, heads_in, grads_heads, bias_row, cot_sum)
    )
    def halves(total):
        keep = row(total, y * shard_rows, shard_rows)
        give = row(total, (1 - y) * shard_rows, shard_rows).astype(BF16)
        return keep, lax.ppermute(give, "y", SWAP).astype(F32)

    first_keep, first_take = halves(first_sum)

    if n == 4 and bias_row.shape[1] <= cot_sum.shape[1]:
        spread = cot_sum.shape[1]
        vector = jnp.concatenate([
            jnp.zeros((2, spread), F32), cot_sum,
            jnp.pad(bias_row, ((0, 0), (0, spread - bias_row.shape[1]))),
            jnp.zeros((4, spread), F32),
        ])
        left_piece, right_piece = scatter_pieces(1, grads_heads, n, z, heads_in)
        own_piece = row(grads_heads, z * 2 * shard_rows, 2 * shard_rows)
        last_keep, last_take, heads_keep, heads_take, grad_normed, mixed, sums = tail(
            n, grads_last.T, (head_weights, first_weights, last_weights),
            (grad_qkv, grad_hidden_0, grad_hidden_1), (attended, activated_0, activated_1),
            (left_piece.T, right_piece.T, own_piece.T), standard, vector,
        )
        last_keep, last_take = last_keep.T, last_take.astype(F32).T
        heads_keep, heads_take = heads_keep.T, heads_take.astype(F32).T
        norm_sums = sums[:3]
        bias_rows = in_order(y, sums[3:4], sums[4:5], 0)[:, : bias_row.shape[1]]
    else:
        for k in range(n - 3, 0, -1):
            heads_in = scatter_step(k, grads_heads, n, z, heads_in)
        heads_keep, heads_take = halves(scatter_end(grads_heads, n, z, heads_in))
        partial_out = sum_dots(
            (attended, activated_0, activated_1),
            ((head_weights, width, 3), (first_weights, piece, 1), (last_weights, piece, 1)),
        )
        grad_normed_part = sum_dots(
            (grad_qkv, grad_hidden_0, grad_hidden_1),
            ((head_weights, 3 * width, 0), (first_weights, piece, 0), (last_weights, piece, 0)),
        )
        last_in = (None, None)
        for k in range(n - 1, 0, -1):
            last_in = scatter_step(k, grads_last, n, z, last_in)
        last_keep, last_take = halves(scatter_end(grads_last, n, z, last_in))
        grad_normed = plane_scatter(grad_normed_part, y, x, c)
        mixed = plane_scatter(partial_out, y, x, c)
        norm_sums = sum_small(
            jnp.concatenate([
                jnp.sum(grad_normed * standard, 0)[None], jnp.sum(grad_normed, 0)[None], cot_sum
            ]),
            ("c", "x", "y", "z"),
        )
        bias_row = sum_small(bias_row, ("z",))
        bias_rows = in_order(y, bias_row, lax.ppermute(bias_row, "y", SWAP), 0)
    grad_norm_gain, grad_norm_bias, grad_out_bias = norm_sums

    out_bias = output_bias.astype(F32) + down_bias.astype(F32)
    out = (tokens_wide + mixed + out_bias).astype(BF16)

    def joined(start, size):
        return in_order(
            y, heads_keep[:, start : start + size], heads_take[:, start : start + size], 1
        )

    grad_query_weight, grad_key_weight, grad_value_weight, grad_output_turned = (
        joined(part * width, width) for part in range(4)
    )
    hidden_halves = [(first_keep, first_take), (last_keep, last_take)]

    def side(which, start):
        return jnp.concatenate([pair[which][:, start : start + piece] for pair in hidden_halves], 1)

    grad_up_weight = in_order(y, side(0, 0), side(1, 0), 1)
    grad_down_turned = in_order(y, side(0, piece), side(1, piece), 1)

    grad_query_bias, grad_key_bias, grad_value_bias = (
        bias_rows[:, part * width : (part + 1) * width].reshape(-1) for part in range(3)
    )
    grad_up_bias = bias_rows[:, 3 * width :].reshape(-1)

    grad_scaled = grad_normed * gain_wide
    grad_tokens = cot_wide + inv_scale * (
        grad_scaled
        - jnp.mean(grad_scaled, -1, keepdims=True)
        - standard * jnp.mean(grad_scaled * standard, -1, keepdims=True)
    )
    return (
        out, grad_tokens, grad_norm_gain, grad_norm_bias,
        grad_query_weight, grad_query_bias, grad_key_weight, grad_key_bias,
        grad_value_weight, grad_value_bias, grad_output_turned.T, grad_out_bias,
        grad_up_weight, grad_up_bias, grad_down_turned.T, grad_out_bias,
    )


def solution(mesh):
    n = mesh.shape["dp"] // 2
    grid = Mesh(mesh.devices.reshape(n, 2, mesh.shape["tensor"] // 2, 2), ("z", "y", "x", "c"))
    dp, tensor = ("z", "y"), ("x", "c")
    rows = P(dp + tensor, None)
    whole, split = P(), P(tensor)
    wide, tall = P(dp, tensor), P(tensor, dp)
    in_specs = (
        rows, whole, whole, wide, split, wide, split, wide, split,
        tall, whole, wide, split, tall, whole, P(dp), rows,
    )
    out_specs = (
        rows, rows, whole, whole, wide, split, wide, split, wide, split,
        tall, whole, wide, split, tall, whole,
    )
    return jax.shard_map(
        functools.partial(on_device, n),
        mesh=grid, in_specs=in_specs, out_specs=out_specs, check_vma=False,
    )
```

```python
import functools

import jax
import jax.numpy as jnp
from jax import lax
from jax.experimental import pallas as pl
from jax.experimental.pallas import tpu as pltpu
from jax.sharding import Mesh, PartitionSpec as P

HEAD_DIM = 64
ROT = 32
BLOCK = 256
EPS = 1e-05
LANES = 128
F32 = jnp.float32
BF16 = jnp.bfloat16


SWAP = [(0, 1), (1, 0)]
NT = (((1,), (1,)), ((), ()))
TN = (((0,), (0,)), ((), ()))
NN = (((1,), (0,)), ((), ()))


def dot(left, right, dims=NN):
    return lax.dot_general(left, right, dims, preferred_element_type=F32)


def spin(value, cosine, sine):
    lane = lax.broadcasted_iota(jnp.int32, value.shape, 1) % HEAD_DIM
    half = ROT // 2
    ahead = pltpu.roll(value, LANES - half, 1)
    behind = pltpu.roll(value, half, 1)
    return value * cosine + jnp.where(lane < half, ahead, behind) * sine


def attention_kernel(
    index, earlier, split_ref, qkv_ref, grad_ref, cos_ref, sin_ref, *refs
):
    (att_ref, dqkv_ref, *scratch) = refs[earlier:]
    attention_body(index, split_ref, qkv_ref, grad_ref, cos_ref, sin_ref, att_ref, dqkv_ref, *scratch)


def attention_body(
    index, split_ref, qkv_ref, grad_ref, cos_ref, sin_ref, att_ref, dqkv_ref,
    q_s, k_s, v_s, g_s, kt_s, vt_s, ot_s, dqt_s, dk_s, dv_s, cos_s, sin_s,
):
    seq_len, width = grad_ref.shape
    first = split_ref[index] // BLOCK
    scale = HEAD_DIM ** (-0.5)
    per = LANES // HEAD_DIM
    rest = jnp.zeros((HEAD_DIM - ROT, seq_len), F32)
    cos_part, sin_part = cos_ref[...], sin_ref[...]
    cos_s[...] = jnp.concatenate([cos_part, cos_part, rest + 1.0] * per, 0).T
    sin_s[...] = jnp.concatenate([-sin_part, sin_part, rest] * per, 0).T

    def one_pair(pair, carry):
        def cols(part):
            return pl.ds(pl.multiple_of(part * width + pair * LANES, LANES), LANES)

        cosine, sine = cos_s[...], sin_s[...]
        head_of = lax.broadcasted_iota(jnp.int32, (seq_len, LANES), 1) // HEAD_DIM
        query = spin(qkv_ref[:, cols(0)], cosine, sine).astype(BF16)
        key = spin(qkv_ref[:, cols(1)], cosine, sine).astype(BF16)
        value = qkv_ref[:, cols(2)].astype(BF16)
        grad = grad_ref[:, cols(0)]
        kt_s[...] = key.T
        vt_s[...] = value.T
        for head in range(per):
            here = head_of == head
            q_s[head] = jnp.where(here, query, 0).astype(BF16)
            k_s[head] = jnp.where(here, key, 0).astype(BF16)
            v_s[head] = jnp.where(here, value, 0).astype(BF16)
            g_s[head] = jnp.where(here, grad, 0).astype(BF16)
        dk_s[...] = jnp.zeros_like(dk_s)
        dv_s[...] = jnp.zeros_like(dv_s)

        def one_block(block, inner):
            begin = jnp.where(block >= first, first, 0)
            rows = pl.ds(pl.multiple_of(block * BLOCK, BLOCK), BLOCK)

            def work(count):
                span = pl.ds(pl.multiple_of(begin * BLOCK, BLOCK), count * BLOCK)
                dk, dv = None, None
                for head in range(per):
                    q, g = q_s[head, rows, :], g_s[head, rows, :]
                    own = slice(head * HEAD_DIM, (head + 1) * HEAD_DIM)
                    scores = dot(k_s[head, span, :], q, NT) * scale
                    top = jnp.max(scores, 0, keepdims=True)
                    power = jnp.exp(scores - top)
                    prob = power * (1.0 / jnp.sum(power, 0, keepdims=True))
                    low = prob.astype(BF16)
                    ot_s[own, rows] = dot(vt_s[own, span], low)
                    dprob = dot(v_s[head, span, :], g, NT)
                    mean = jnp.sum(prob * dprob, 0, keepdims=True)
                    dscore = (prob * (dprob - mean) * scale).astype(BF16)
                    dqt_s[own, rows] = dot(kt_s[own, span], dscore)
                    dk_h, dv_h = dot(dscore, q), dot(low, g)
                    dk = dk_h if dk is None else dk + dk_h
                    dv = dv_h if dv is None else dv + dv_h
                dk_s[span, :] += dk
                dv_s[span, :] += dv

            for count in range(1, seq_len // BLOCK):
                pl.when(block - begin == count - 1)(functools.partial(work, count))
            return inner

        lax.fori_loop(0, seq_len // BLOCK, one_block, 0)
        att_ref[:, cols(0)] = ot_s[...].T.astype(BF16)
        dqkv_ref[:, cols(0)] = spin(dqt_s[...].T, cosine, -sine).astype(BF16)
        dqkv_ref[:, cols(1)] = spin(dk_s[...], cosine, -sine).astype(BF16)
        dqkv_ref[:, cols(2)] = dv_s[...].astype(BF16)
        return carry

    lax.fori_loop(0, width // LANES, one_pair, 0)


def attention(index, splits, qkv, grad, cosine, sine, earlier):
    count = splits.shape[0]
    rows, width = grad.shape
    seq_len = rows // count
    per = LANES // HEAD_DIM

    def spec(columns):
        return pl.BlockSpec((seq_len, columns), lambda i, split: (index, 0))

    table = pl.BlockSpec((ROT // 2, seq_len), lambda i, split: (0, index))
    masked = pltpu.VMEM((per, seq_len, LANES), BF16)
    turned = pltpu.VMEM((LANES, seq_len), BF16)
    return pl.pallas_call(
        functools.partial(attention_kernel, index, len(earlier)),
        grid_spec=pltpu.PrefetchScalarGridSpec(
            num_scalar_prefetch=1,
            grid=(1,),
            in_specs=[spec(3 * width), spec(width), table, table]
            + [pl.BlockSpec(memory_space=pl.ANY)] * len(earlier),
            out_specs=[spec(width), spec(3 * width)],
            scratch_shapes=[
                masked, masked, masked, masked, turned, turned,
                pltpu.VMEM((LANES, seq_len), F32),
                pltpu.VMEM((LANES, seq_len), F32),
                pltpu.VMEM((seq_len, LANES), F32),
                pltpu.VMEM((seq_len, LANES), F32),
                pltpu.VMEM((seq_len, LANES), F32),
                pltpu.VMEM((seq_len, LANES), F32),
            ],
        ),
        out_shape=[
            jax.ShapeDtypeStruct((rows, width), BF16),
            jax.ShapeDtypeStruct((rows, 3 * width), BF16),
        ],
        cost_estimate=pl.CostEstimate(
            flops=40 * seq_len * seq_len * width // 4,
            transcendentals=seq_len * seq_len * width // HEAD_DIM // 2,
            bytes_accessed=seq_len * width * 24,
        ),
        input_output_aliases={5 + i: i for i in range(len(earlier))},
        compiler_params=pltpu.CompilerParams(vmem_limit_bytes=48 << 20),
        name="attention",
    )(splits, qkv, grad, cosine, sine, *earlier)


def turn_tables(splits, seq_len):
    shape = (ROT // 2, splits.shape[0], seq_len)
    token = lax.broadcasted_iota(jnp.int32, shape, 2)
    start = splits[None, :, None]
    position = (token - jnp.where(token >= start, start, 0)).astype(F32)
    entry = jnp.arange(ROT // 2, dtype=F32)
    angle = position * (10000.0 ** (-(2.0 * entry) / ROT))[:, None, None]
    return jnp.cos(angle).reshape(ROT // 2, -1), jnp.sin(angle).reshape(ROT // 2, -1)


def sum_dots_kernel(count, *refs):
    out_ref = refs[-1]
    total = None
    for i in range(count):
        part = dot(refs[i][...], refs[count + i][...], NT)
        total = part if total is None else total + part
    out_ref[...] = total.astype(out_ref.dtype)


def sum_dots(lefts, rights, tile=512):
    rows, columns = lefts[0].shape[0], rights[0][0].shape[0]
    tile = min(tile, rows)
    depth = sum(left.shape[1] for left in lefts)
    return pl.pallas_call(
        functools.partial(sum_dots_kernel, len(lefts)),
        grid=(rows // tile,),
        in_specs=[pl.BlockSpec((tile, left.shape[1]), lambda i: (i, 0)) for left in lefts] + [
            pl.BlockSpec((columns, size), functools.partial(lambda at, i: (0, at), at))
            for _, size, at in rights
        ],
        out_specs=pl.BlockSpec((tile, columns), lambda i: (i, 0)),
        out_shape=jax.ShapeDtypeStruct((rows, columns), BF16),
        cost_estimate=pl.CostEstimate(
            flops=2 * rows * columns * depth, transcendentals=0,
            bytes_accessed=2 * (rows * columns + depth * (rows + columns)),
        ),
        compiler_params=pltpu.CompilerParams(vmem_limit_bytes=56 << 20),
        name="sum_dots",
    )(*lefts, *(right[0] for right in rights))


def hidden_kernel(n_ref, c_ref, w_ref, bias_ref, act_ref, dh_ref, sum_ref):
    piece = act_ref.shape[1]
    hidden = dot(n_ref[...], w_ref[:, :piece]) + bias_ref[...]
    grad = dot(c_ref[...], w_ref[:, piece:])
    rate = (2.0 / jnp.pi) ** 0.5
    square = hidden * hidden
    bent = jnp.tanh(rate * hidden * (1.0 + 0.044715 * square))
    act_ref[...] = (0.5 * hidden * (1.0 + bent)).astype(BF16)
    slope = 0.5 * (1.0 + bent) + 0.5 * hidden * (1.0 - bent * bent) * (
        rate * (1.0 + 3.0 * 0.044715 * square)
    )
    low = (grad * slope).astype(BF16)
    dh_ref[...] = low

    @pl.when(pl.program_id(0) == 0)
    def _():
        sum_ref[...] = jnp.zeros_like(sum_ref)

    sum_ref[...] += jnp.sum(low.astype(F32), 0, keepdims=True)


def hidden_part(normed_all, cot_all, weights, bias, tile=512):
    rows, depth = normed_all.shape
    piece = weights.shape[1] // 2
    tile = min(tile, rows)
    wide = pl.BlockSpec((tile, depth), lambda i: (i, 0))
    thin = pl.BlockSpec((tile, piece), lambda i: (i, 0))
    line = pl.BlockSpec((1, piece), lambda i: (0, 0))
    return pl.pallas_call(
        hidden_kernel,
        grid=(rows // tile,),
        in_specs=[wide, wide, pl.BlockSpec(weights.shape, lambda i: (0, 0)), line],
        out_specs=[thin, thin, line],
        out_shape=[
            jax.ShapeDtypeStruct((rows, piece), BF16),
            jax.ShapeDtypeStruct((rows, piece), BF16),
            jax.ShapeDtypeStruct((1, piece), F32),
        ],
        cost_estimate=pl.CostEstimate(
            flops=4 * rows * depth * piece, transcendentals=rows * piece,
            bytes_accessed=4 * rows * depth + 4 * depth * piece + 4 * rows * piece,
        ),
        compiler_params=pltpu.CompilerParams(vmem_limit_bytes=48 << 20),
        name="hidden_part",
    )(normed_all, cot_all, weights, bias)


def gather_kernel(
    n, own_ref, other_ref, second_ref, second_other_ref, next_ref, norm_ref, cot_ref,
    w_ref, unit_ref, right_ref, left_ref, swapped_ref, n_ref, c_ref, send_sem, recv_sem, local_sem,
):
    z, y, x, c = (lax.axis_index(name) for name in ("z", "y", "x", "c"))
    rows = norm_ref.shape[0]
    half = 3 * rows // 4
    mine = y * 4 + x * 2 + c
    has_right, has_left = z < n - 1, z > 0
    number = {}

    def remote(key, src, dst, axis, target):
        slot = number.setdefault(key, len(number))
        return pltpu.make_async_remote_copy(
            src_ref=src, dst_ref=dst, send_sem=send_sem.at[slot], recv_sem=recv_sem.at[slot],
            device_id={axis: target}, device_id_type=pl.DeviceIdType.MESH,
        )

    def when(condition, action):
        if condition is None:
            action()
        else:
            pl.when(condition)(action)

    started = []

    def start(condition, copy):
        when(condition, copy.start)
        started.append((condition, copy))

    def shard(index, unit):
        return w_ref.at[index * 2 + (y if unit == 0 else 1 - y)]

    def along(step, unit, sign, receiving=False):
        index = z - sign * step if receiving else z - sign * (step - 1)
        source = own_ref if step == 1 and unit == 0 and not receiving else shard(index, unit)
        return remote((step, unit, sign), source, shard(index, unit), "z", z + sign)


    full, top, low = pl.ds(0, rows), pl.ds(0, half), pl.ds(half, rows - half)
    arrays = ((n_ref, norm_ref, "n"), (c_ref, cot_ref, "c"))
    at_x, at_y, at_xy = y * 4 + (1 - x) * 2 + c, (1 - y) * 4 + x * 2 + c, (1 - y) * 4 + (1 - x) * 2 + c

    barrier = pltpu.get_barrier_semaphore()
    for axis, target in (("x", 1 - x), ("y", 1 - y), ("c", 1 - c)):
        pl.semaphore_signal(
            barrier, inc=1, device_id={axis: target}, device_id_type=pl.DeviceIdType.MESH
        )
    for condition, target in ((has_right, z + 1), (has_left, z - 1)):
        when(condition, functools.partial(
            pl.semaphore_signal, barrier, inc=1, device_id={"z": target},
            device_id_type=pl.DeviceIdType.MESH,
        ))
    pl.semaphore_wait(barrier, 3 + has_right.astype(jnp.int32) + has_left.astype(jnp.int32))

    for condition, sign in ((has_right, 1), (has_left, -1)):
        start(condition, along(1, 0, sign))
    swap = remote("swap", other_ref, w_ref.at[z * 2 + y], "y", 1 - y)
    swap_in = remote("swap", other_ref, w_ref.at[z * 2 + 1 - y], "y", 1 - y)
    start(None, swap)
    for array, source, name in arrays:
        for axis in ("x", "y", "c"):
            start(None, remote((name, axis), source, array.at[mine], axis,
                               {"x": 1 - x, "y": 1 - y, "c": 1 - c}[axis]))
    unit_swap = remote("unit", second_other_ref, unit_ref.at[y], "y", 1 - y)
    unit_swap_in = remote("unit", second_other_ref, unit_ref.at[1 - y], "y", 1 - y)
    start(None, unit_swap)
    late_swap = remote("late", next_ref, swapped_ref, "y", 1 - y)
    start(None, late_swap)
    local = [
        pltpu.make_async_copy(own_ref, shard(z, 0), local_sem.at[0]),
        pltpu.make_async_copy(norm_ref, n_ref.at[mine], local_sem.at[1]),
        pltpu.make_async_copy(cot_ref, c_ref.at[mine], local_sem.at[2]),
        pltpu.make_async_copy(second_ref, unit_ref.at[y], local_sem.at[3]),
    ]
    for copy in local:
        copy.start()

    def arrive_swap():
        swap_in.wait_recv()
        for condition, sign in ((has_right, 1), (has_left, -1)):
            start(condition, along(1, 1, sign))

    def arrive_shard(step, unit, sign):
        inside = z - sign * step >= 0 if sign > 0 else z + step < n
        further = has_right if sign > 0 else has_left
        when(inside, along(step, unit, sign, True).wait_recv)
        if step + 1 < n:
            start(inside & further, along(step + 1, unit, sign))

    def arrive_rows(array, name, axis):
        index = {"x": at_x, "y": at_y, "c": None}[axis]
        block = array.at[index]
        remote((name, axis), block, block, axis, 0).wait_recv()
        part, on = (low, "y") if axis == "x" else (top, "x")
        piece = array.at[index, part]
        start(None, remote((name, "far", on), piece, piece, on, {"x": 1 - x, "y": 1 - y}[on]))
        start(None, remote((name, "core", axis), block, block, "c", 1 - c))

    def arrive_far(array, name, on):
        part = low if on == "y" else top
        piece = array.at[at_xy, part]
        remote((name, "far", on), piece, piece, on, 0).wait_recv()
        start(None, remote((name, "core", "far", on), piece, piece, "c", 1 - c))

    def arrive_steps(step):
        for unit in (0, 1):
            for sign in (1, -1):
                arrive_shard(step, unit, sign)

    def second_step(half_of, receiving):
        index = y if half_of == 0 else 1 - y
        source = second_ref if half_of == 0 else unit_ref.at[index]
        ways = ((1, has_left if receiving else has_right, right_ref),
                (-1, has_right if receiving else has_left, left_ref))
        for sign, condition, target in ways:
            copy = remote(("second", half_of, sign), source, target.at[index], "z", z + sign)
            if receiving:
                when(condition, copy.wait_recv)
            else:
                start(condition, copy)

    (norm, _, norm_name), (cot, _, cot_name) = arrays
    arrive_swap()
    arrive_rows(norm, norm_name, "x")
    for sign in (1, -1):
        arrive_shard(1, 0, sign)
    arrive_rows(norm, norm_name, "y")
    for sign in (1, -1):
        arrive_shard(1, 1, sign)
    arrive_rows(cot, cot_name, "x")
    if n > 2:
        arrive_steps(2)
    second_step(0, False)
    arrive_rows(cot, cot_name, "y")
    unit_swap_in.wait_recv()
    second_step(1, False)
    for step in range(3, n):
        arrive_steps(step)
    for array, _, name in arrays:
        for on in ("x", "y"):
            arrive_far(array, name, on)
    for array, _, name in arrays:
        for key, index, part in (
            ((name, "c"), y * 4 + x * 2 + 1 - c, full),
            ((name, "core", "x"), y * 4 + (1 - x) * 2 + 1 - c, full),
            ((name, "core", "y"), (1 - y) * 4 + x * 2 + 1 - c, full),
            ((name, "core", "far", "x"), (1 - y) * 4 + (1 - x) * 2 + 1 - c, top),
            ((name, "core", "far", "y"), (1 - y) * 4 + (1 - x) * 2 + 1 - c, low),
        ):
            piece = array.at[index, part]
            remote(key, piece, piece, "c", 0).wait_recv()
    late_swap.wait_recv()
    for half_of in (0, 1):
        second_step(half_of, True)
    for copy in local:
        copy.wait()
    for condition, copy in started:
        when(condition, copy.wait_send)


def gather_all(n, own, other, second, second_other, following, normed, cotangent):
    rows, columns = normed.shape
    copies = 4 * (n - 1) + 8 + 2 * 9
    anywhere = pl.BlockSpec(memory_space=pl.ANY)
    pair = jax.ShapeDtypeStruct((2,) + second.shape, second.dtype)
    weights, unit, right, left, swapped, normed_all, cot_all = pl.pallas_call(
        functools.partial(gather_kernel, n),
        in_specs=[anywhere] * 7,
        out_specs=[anywhere] * 7,
        out_shape=[
            jax.ShapeDtypeStruct((2 * n,) + own.shape, own.dtype),
            pair, pair, pair,
            jax.ShapeDtypeStruct(following.shape, following.dtype),
            jax.ShapeDtypeStruct((8, rows, columns), normed.dtype),
            jax.ShapeDtypeStruct((8, rows, columns), cotangent.dtype),
        ],
        scratch_shapes=[
            pltpu.SemaphoreType.DMA((copies,)),
            pltpu.SemaphoreType.DMA((copies,)),
            pltpu.SemaphoreType.DMA((4,)),
        ],
        cost_estimate=pl.CostEstimate(flops=0, transcendentals=0, bytes_accessed=200 << 20),
        compiler_params=pltpu.CompilerParams(collective_id=0, has_side_effects=True),
        name="gather_rows",
    )(own, other, second, second_other, following, normed, cotangent)
    flat = lambda array: array.reshape(-1, array.shape[-1])
    return tuple(map(flat, (weights, unit, right, left, swapped, normed_all, cot_all)))


def chain_step(step, n, right, left):
    return (
        lax.ppermute(right, "z", [(i, i + 1) for i in range(step - 1, n - 1)]),
        lax.ppermute(left, "z", [(i, i - 1) for i in range(1, n - step + 1)]),
    )


def assemble(unit, right, left, n, z):
    rows, columns = unit.shape
    whole = jnp.zeros((n * rows, columns), unit.dtype)
    for k in range(n):
        piece = unit if k == 0 else jnp.where(z >= k, right[k], left[n - k])
        row = lax.rem(z - k + n, n) * rows
        whole = lax.dynamic_update_slice(whole, piece, (row, jnp.int32(0)))
    return whole


def scatter_pieces(k, grads, n, z, received):
    rows = grads.shape[0] // n

    def piece(index, got):
        own = lax.dynamic_slice_in_dim(grads, jnp.clip(index, 0, n - 1) * rows, rows, 0)
        return own if got is None else add_low(own, got)

    return piece(z - k, received[0]), piece(z + k, received[1])


def scatter_step(k, grads, n, z, received):
    to_left, to_right = scatter_pieces(k, grads, n, z, received)
    return (
        lax.ppermute(to_left, "z", [(r, r - 1) for r in range(k, n)]),
        lax.ppermute(to_right, "z", [(r, r + 1) for r in range(0, n - k)]),
    )


def scatter_end(grads, n, z, received):
    rows = grads.shape[0] // n
    own = lax.dynamic_slice_in_dim(grads, z * rows, rows, 0).astype(F32)
    return own + received[0].astype(F32) + received[1].astype(F32)


def tail_kernel(
    n, g_any, hw_ref, fw_ref, lw_ref, dq_ref, d0_ref, d1_ref, at_ref, a0_ref, a1_ref,
    left_ref, right_ref, own_ref, std_any, vec_ref,
    keep_ref, take_ref, heads_keep_ref, heads_take_ref, out_ref, mixed_ref, sums_ref,
    g_ref, std_ref, hw_s, fw_s, lw_s, rows_s, stage, zrecv, give, heads_recv, heads_own, heads_give, both, xtop_2, ylow_2, ytop_2, xlow_2,
    top_2, low_2, vstage, vrecv, send_sem, recv_sem, load_sem, rows_sem,
):
    z, y, x, c = (lax.axis_index(name) for name in ("z", "y", "x", "c"))
    rows, columns = out_ref.shape
    wide, wide_heads = give.shape[0], heads_give.shape[0]
    half = rows // 2
    rest = rows - half
    number, started = {}, []

    def remote(key, src, dst, axis, target):
        slot = number.setdefault(key, len(number))
        return pltpu.make_async_remote_copy(
            src_ref=src, dst_ref=dst, send_sem=send_sem.at[slot], recv_sem=recv_sem.at[slot],
            device_id={axis: target}, device_id_type=pl.DeviceIdType.MESH,
        )

    def when(condition, action):
        if condition is None:
            action()
        else:
            pl.when(condition)(action)

    def start(condition, copy):
        when(condition, copy.start)
        started.append((condition, copy))

    def each(count, size, body):
        def step(i, carry):
            body(pl.ds(pl.multiple_of(i * size, size), size))
            return carry
        lax.fori_loop(0, count // size, step, 0)

    barrier = pltpu.get_barrier_semaphore()
    greet = [(None, "x", 1 - x), (None, "y", 1 - y), (None, "c", 1 - c)]
    greet += [(z < n - 1, "z", z + 1), (z > 0, "z", z - 1)]
    for step in (2 ** i for i in range(1, n.bit_length() - 1)):
        greet.append((None, "z", jnp.bitwise_xor(z, step)))
    for condition, axis, target in greet:
        when(condition, functools.partial(
            pl.semaphore_signal, barrier, inc=1, device_id={axis: target},
            device_id_type=pl.DeviceIdType.MESH))

    loads = [
        pltpu.make_async_copy(source, target, load_sem.at[i])
        for i, (source, target) in enumerate(
            ((hw_ref, hw_s), (fw_ref, fw_s), (lw_ref, lw_s), (g_any, g_ref), (std_any, std_ref),
             (own_ref, heads_own)))
    ]
    for load in loads:
        load.start()

    firsts, lasts = fw_ref.shape[1] // 2, lw_ref.shape[1] // 2
    heads = dq_ref.shape[1]
    sums = (
        ((dq_ref, heads, hw_s, 0), (d0_ref, firsts, fw_s, 0), (d1_ref, lasts, lw_s, 0)),
        ((at_ref, heads // 3, hw_s, heads), (a0_ref, firsts, fw_s, firsts),
         (a1_ref, lasts, lw_s, lasts)),
    )
    sides = (1 - y, y)
    jobs = [(a, own, j) for a in (0, 1) for own in (False, True) for j in sides]

    def row_loads(number_of):
        a, own, j = jobs[number_of]
        slot, core, copies, at = number_of % 2, c if own else 1 - c, [], 0
        for p, (left, width, _, _) in enumerate(sums[a]):
            for i in (0, 1):
                block = j * 4 + i * 2 + core
                source = left.at[pl.ds(pl.multiple_of(block * rows, rows), rows)]
                target = rows_s.at[slot, pl.ds(i * rows, rows), pl.ds(at, width)]
                copies.append(pltpu.make_async_copy(source, target, rows_sem.at[slot, p * 2 + i]))
            at += width
        return copies

    def job(number_of):
        a, own, j = jobs[number_of]
        slot = number_of % 2
        if number_of + 1 < len(jobs):
            for copy in row_loads(number_of + 1):
                copy.start()
        for copy in row_loads(number_of):
            copy.wait()
        if own:
            for i in (0, 1):
                core_copy(a, number_of % 2, i).wait_recv()
        elif a == 1:
            for i in (0, 1):
                core_copy(0, number_of % 2, i).wait_send()
        size = min(512, columns)

        def tile(t, carry):
            span = pl.ds(pl.multiple_of(t * size, size), size)
            acc, at = None, 0
            for left, width, weights, column in sums[a]:
                part = dot(
                    rows_s[slot, :, at : at + width], weights[span, column : column + width], NT)
                acc = part if acc is None else acc + part
                at += width
            for i in (0, 1):
                piece = acc[i * rows : (i + 1) * rows]
                if own:
                    both[a, j * 2 + i, :, span] = (
                        piece + both[a, j * 2 + i, :, span].astype(F32)).astype(BF16)
                else:
                    stage[j * 2 + i, :, span] = piece.astype(BF16)
            return carry

        lax.fori_loop(0, columns // size, tile, 0)
        if own and a == 0:
            start(None, first_copy(a, "xtop", number_of % 2))
            if number_of % 2 == 0:
                for i in (0, 1):
                    start(None, first_copy(a, "ylow", i))
        if not own:
            for i in (0, 1):
                copy = core_copy(a, number_of % 2, i)
                copy.start()
                if a == 1:
                    started.append((None, copy))

    def core_copy(a, u, i):
        place = sides[u] * 2 + i
        return remote(("core", a, u, i), stage.at[place], both.at[a, place], "c", 1 - c)

    for copy in row_loads(0):
        copy.start()
    always = sum(condition is None for condition, _, _ in greet)
    pl.semaphore_wait(barrier, always + sum(
        condition.astype(jnp.int32) for condition, _, _ in greet if condition is not None))

    def first_copy(a, name, j):
        if name == "xtop":
            source = both.at[a, sides[j] * 2 + 1 - x, pl.ds(0, half)]
            return remote((name, a, j), source, xtop_2.at[a, j], "x", 1 - x)
        source = both.at[a, (1 - y) * 2 + j, pl.ds(half, rest)]
        return remote((name, a, j), source, ylow_2.at[a, j], "y", 1 - y)

    def second_copy(a, name):
        if name == "ytop":
            return remote((name, a), top_2.at[a], ytop_2.at[a], "y", 1 - y)
        return remote((name, a), low_2.at[a], xlow_2.at[a], "x", 1 - x)

    def first_send(a):
        for j in (0, 1):
            start(None, first_copy(a, "xtop", j))
            start(None, first_copy(a, "ylow", j))

    def first_arrive(a):
        for j in (0, 1):
            first_copy(a, "xtop", j).wait_recv()
            first_copy(a, "ylow", j).wait_recv()

        def upper(part):
            top_2[a, part, :] = (
                both[a, (1 - y) * 2 + x, part, :].astype(F32)
                + xtop_2[a, 0, part, :].astype(F32)
            ).astype(BF16)

        def lower(part):
            low_part = pl.ds(part.start + half, part.size)
            low_2[a, part, :] = (
                both[a, y * 2 + 1 - x, low_part, :].astype(F32)
                + ylow_2[a, 1 - x, part, :].astype(F32)
            ).astype(BF16)

        each(half, 32, upper)
        each(rest, 32, lower)
        start(None, second_copy(a, "ytop"))
        start(None, second_copy(a, "xlow"))

    def second_arrive(a):
        second_copy(a, "ytop").wait_recv()
        second_copy(a, "xlow").wait_recv()
        target = (out_ref, mixed_ref)[a]

        def finish(first, part, placed, last):
            value = (
                both[a, y * 2 + x, placed, :].astype(F32) + first[part, :].astype(F32)
                + last[part, :].astype(F32)
            )
            target[placed, :] = value
            if a == 0:
                scaled = value * std_ref[placed, :]
                vstage[0, 0:1, :] += jnp.sum(scaled, 0, keepdims=True)
                vstage[0, 1:2, :] += jnp.sum(value, 0, keepdims=True)

        def upper(part):
            finish(xtop_2.at[a, 1], part, part, ytop_2.at[a])

        def lower(part):
            finish(ylow_2.at[a, x], part, pl.ds(part.start + half, part.size), xlow_2.at[a])

        each(half, 32, upper)
        each(rest, 32, lower)

    def block_of(direction, k, u):
        index = (z - k if direction == 0 else z + k) * 2 + sides[u]
        return pl.ds(pl.multiple_of(index * rows, rows), rows)

    def z_copy(direction, k, u, src):
        target = z - 1 if direction == 0 else z + 1
        return remote((direction, k, u), src, zrecv.at[direction, k - 1, u], "z", target)

    def z_first(direction):
        edge = z == n - 1 if direction == 0 else z == 0
        for k in range(n - 1, 0, -1):
            for u in (0, 1):
                start(edge, z_copy(direction, k, u, g_any.at[:, block_of(direction, k, u)]))

    def z_step(k, u):
        for direction in (0, 1):
            if direction == 0:
                inside = (z >= k) & (z < n - 1)
            else:
                inside = (n - 1 - z >= k) & (z > 0)
            held = zrecv.at[direction, k, u]

            def add():
                z_copy(direction, k + 1, u, held).wait_recv()
                block = block_of(direction, k, u)

                def body(part):
                    held[part, :] = (
                        g_ref[part, block].astype(F32) + held[part, :].astype(F32)
                    ).astype(BF16)

                each(wide, 256, body)

            when(inside, add)
            start(inside, z_copy(direction, k, u, held))

    def z_last(u, target):
        block = block_of(0, 0, u)

        def first(part):
            target[part, :] = g_ref[part, block].astype(F32)

        each(wide, 256, first)
        for direction in (0, 1):
            held = zrecv.at[direction, 0, u]

            def add():
                z_copy(direction, 1, u, held).wait_recv()

                def body(part):
                    target[part, :] += held[part, :].astype(F32)

                each(wide, 256, body)

            when(z < n - 1 if direction == 0 else z > 0, add)

    def heads_copy(direction, u):
        span = pl.ds(pl.multiple_of(sides[u] * rows, rows), rows)
        source = (left_ref, right_ref)[direction].at[:, span]
        return remote(
            ("heads", direction, u), source, heads_recv.at[direction, :, span], "z",
            z - 1 if direction == 0 else z + 1)

    def heads_send():
        for u in (0, 1):
            start(z > 0, heads_copy(0, u))
            start(z < n - 1, heads_copy(1, u))

    def heads_last(u, target):
        span = pl.ds(pl.multiple_of(sides[u] * rows, rows), rows)

        def first(part):
            target[part, :] = heads_own[part, span].astype(F32)

        each(wide_heads, 256, first)
        for direction in (0, 1):
            def add():
                heads_copy(direction, u).wait_recv()

                def body(part):
                    target[part, :] += heads_recv[direction, part, span].astype(F32)

                each(wide_heads, 256, body)

            when(z < n - 1 if direction == 0 else z > 0, add)

    steps = [(k, u) for k in range(n - 2, 0, -1) for u in (0, 1)]

    def z_next():
        if steps:
            z_step(*steps.pop(0))

    for direction in (0, 1):
        z_first(direction)
    vstage[0] = vec_ref[...]
    for load in loads[:3]:
        load.wait()
    job(0)
    job(1)
    for load in loads[3:]:
        load.wait()
    z_next()
    job(2)
    job(3)
    heads_send()
    z_next()
    job(4)
    job(5)
    z_next()
    job(6)
    job(7)
    first_arrive(0)
    first_send(1)
    while steps:
        z_next()
    second_arrive(0)

    turns = [("z", jnp.bitwise_xor(z, 2 ** i)) for i in range(n.bit_length() - 1)]
    turns += [("y", 1 - y), ("x", 1 - x), ("c", 1 - c)]
    line = lax.broadcasted_iota(jnp.int32, vec_ref.shape, 0)

    def exchange(i):
        axis, target = turns[i]
        return remote(("vec", i), vstage.at[i], vrecv.at[i], axis, target)

    def turn(i):
        exchange(i).wait_recv()
        axis, _ = turns[i]
        old, new = vstage[i], vrecv[i]
        result = sums_ref if i == len(turns) - 1 else vstage.at[i + 1]
        result[...] = old + jnp.where((line < 3) | (axis == "z"), new, 0.0)
        if axis == "y":
            result[4:5, :] = new[3:4, :]
        if i + 1 < len(turns):
            start(None, exchange(i + 1))

    start(None, exchange(0))

    def swapped(key, source, target, length, received):
        def lower_precision(part):
            target[part, :] = source[part, :].astype(BF16)

        each(length, 256, lower_precision)
        copy = remote(key, target, received, "y", 1 - y)
        start(None, copy)
        return copy

    first_arrive(1)
    z_last(0, keep_ref)
    swap = swapped("swap", keep_ref, give, wide, take_ref)
    turn(0)
    turn(1)
    heads_last(0, heads_keep_ref)
    heads_swap = swapped("heads swap", heads_keep_ref, heads_give, wide_heads, heads_take_ref)
    turn(2)
    z_last(1, keep_ref)
    turn(3)
    heads_last(1, heads_keep_ref)
    for i in range(4, len(turns)):
        turn(i)
    second_arrive(1)
    swap.wait_recv()
    heads_swap.wait_recv()
    for condition, copy in started:
        when(condition, copy.wait_send)


def tail(n, grads_turned, weights, lefts, lefts_out, heads_turned, standard, vector):
    rows, columns = standard.shape
    wide, wide_heads = grads_turned.shape[0], heads_turned[0].shape[0]
    half = rows // 2
    inside = pl.BlockSpec(memory_space=pltpu.VMEM)
    anywhere = pl.BlockSpec(memory_space=pl.ANY)
    copies = 4 * (n - 1) + 46
    low = lambda *shape: pltpu.VMEM(shape, BF16)
    small = vector.shape
    depth = sum(left.shape[1] for left in lefts)
    return pl.pallas_call(
        functools.partial(tail_kernel, n),
        in_specs=[anywhere] * 14 + [inside],
        out_specs=[inside] * 7,
        out_shape=[
            jax.ShapeDtypeStruct((wide, rows), F32),
            jax.ShapeDtypeStruct((wide, rows), BF16),
            jax.ShapeDtypeStruct((wide_heads, rows), F32),
            jax.ShapeDtypeStruct((wide_heads, rows), BF16),
            jax.ShapeDtypeStruct((rows, columns), F32),
            jax.ShapeDtypeStruct((rows, columns), F32),
            jax.ShapeDtypeStruct(small, F32),
        ],
        scratch_shapes=[low(*grads_turned.shape), pltpu.VMEM(standard.shape, F32)] + [
            low(*array.shape) for array in weights
        ] + [
            low(2, 2 * rows, depth), low(4, rows, columns),
            low(2, n - 1, 2, wide, rows), low(wide, rows),
            low(2, wide_heads, 2 * rows), low(wide_heads, 2 * rows), low(wide_heads, rows),
            low(2, 4, rows, columns),
            low(2, 2, half, columns), low(2, 2, rows - half, columns),
            low(2, half, columns), low(2, rows - half, columns),
            low(2, half, columns), low(2, rows - half, columns),
            pltpu.VMEM((8,) + small, F32), pltpu.VMEM((8,) + small, F32),
            pltpu.SemaphoreType.DMA((copies,)),
            pltpu.SemaphoreType.DMA((copies,)),
            pltpu.SemaphoreType.DMA((6,)),
            pltpu.SemaphoreType.DMA((2, 6)),
        ],
        cost_estimate=pl.CostEstimate(flops=0, transcendentals=0, bytes_accessed=200 << 20),
        compiler_params=pltpu.CompilerParams(
            collective_id=1, has_side_effects=True, vmem_limit_bytes=63 << 20
        ),
        name="scatter_rest",
    )(grads_turned, *weights, *lefts, *lefts_out, *heads_turned, standard, vector)


def sum_small(array, axes):
    for axis in axes:
        size = lax.axis_size(axis)
        if size & (size - 1):
            array = lax.psum(array, axis)
            continue
        step = 1
        while step < size:
            array = array + lax.ppermute(array, axis, [(i, i ^ step) for i in range(size)])
            step *= 2
    return array


def pick(array, index, axis):
    return lax.dynamic_index_in_dim(array, index, axis, keepdims=False)


def add_low(left, right):
    return (left.astype(F32) + right.astype(F32)).astype(BF16)


def plane_scatter(partial, y, x, c):
    rows, columns = partial.shape[0] // 8, partial.shape[1]
    half = rows // 2
    parts = partial.reshape(2, 2, 2, rows, columns)
    acc = add_low(pick(parts, c, 2), lax.ppermute(pick(parts, 1 - c, 2), "c", SWAP))
    top, low = acc[:, :, :half], acc[:, :, half:]
    top = add_low(pick(top, x, 1), lax.ppermute(pick(top, 1 - x, 1), "x", SWAP))
    low = add_low(pick(low, y, 0), lax.ppermute(pick(low, 1 - y, 0), "y", SWAP))
    top = pick(top, y, 0).astype(F32) + lax.ppermute(pick(top, 1 - y, 0), "y", SWAP).astype(F32)
    low = pick(low, x, 0).astype(F32) + lax.ppermute(pick(low, 1 - x, 0), "x", SWAP).astype(F32)
    return jnp.concatenate([top, low], 0)


def in_order(y, own, other, axis):
    return jnp.where(
        y == 0, jnp.concatenate([own, other], axis), jnp.concatenate([other, own], axis)
    )


def on_device(
    n,
    tokens, norm_gain, norm_bias,
    query_weight, query_bias, key_weight, key_bias, value_weight, value_bias,
    output_weight, output_bias, up_weight, up_bias, down_weight, down_bias,
    doc_split, cotangent,
):
    z, y, x, c = (lax.axis_index(name) for name in ("z", "y", "x", "c"))
    shard_rows = query_weight.shape[0]
    width = query_weight.shape[1] // 2
    hidden_width = up_weight.shape[1] // 2
    chunks = 2
    piece = hidden_width // chunks

    def col(array, start, size):
        return lax.dynamic_slice_in_dim(array, start, size, 1)

    def row(array, start, size):
        return lax.dynamic_slice_in_dim(array, start, size, 0)

    def pack_heads(side):
        return jnp.concatenate(
            [col(w, side * width, width) for w in (query_weight, key_weight, value_weight)]
            + [row(output_weight, side * width, width).T],
            1,
        )

    def pack_hidden(side, chunk):
        start = side * hidden_width + chunk * piece
        return jnp.concatenate(
            [col(up_weight, start, piece), row(down_weight, start, piece).T], 1
        )

    gain_wide = norm_gain.astype(F32)
    tokens_wide = tokens.astype(F32)
    row_mean = jnp.mean(tokens_wide, -1, keepdims=True)
    centred = tokens_wide - row_mean
    inv_scale = lax.rsqrt(jnp.mean(centred * centred, -1, keepdims=True) + EPS)
    standard = centred * inv_scale
    normed = (standard * gain_wide + norm_bias.astype(F32)).astype(BF16)
    phase = lax.optimization_barrier
    packed = (
        pack_hidden(y, 0), pack_hidden(1 - y, 0), pack_heads(y), pack_heads(1 - y),
        pack_hidden(1 - y, 1), normed,
    )
    last_own = pack_hidden(y, 1)
    other_split = lax.ppermute(doc_split, "y", SWAP)
    splits = in_order(y, doc_split, other_split, 0)
    seq_len = 4 * normed.shape[0]
    cosine, sine = turn_tables(splits, seq_len)

    right, left = [None] * n, [None] * n
    first_weights, heads_unit, right[1], left[1], last_swapped, normed_all, cot_all = gather_all(
        n, *packed, cotangent
    )
    last_unit = in_order(y, last_own, last_swapped, 0)
    first_weights, heads_unit, last_unit, normed_all, cot_all, right[1], left[1], cosine, sine = phase(
        (first_weights, heads_unit, last_unit, normed_all, cot_all, right[1], left[1], cosine, sine)
    )

    def hidden_local(weights, chunk):
        bias = row(up_bias, y * hidden_width + chunk * piece, piece).astype(F32)[None]
        return hidden_part(normed_all, cot_all, weights, bias)

    def weight_grads(grad_columns, columns):
        return jnp.concatenate(
            [dot(normed_all, grad_columns, TN).astype(BF16), dot(cot_all, columns, TN).astype(BF16)], 1
        )

    def gather_step(step, source):
        return chain_step(step, n, right[step - 1], left[step - 1]) if step > 1 else chain_step(
            1, n, source, source)

    activated_0, grad_hidden_0, hidden_sum_0 = hidden_local(first_weights, 0)
    right[2], left[2] = gather_step(2, None)
    activated_0, grad_hidden_0, normed_all, cot_all, right[2], left[2] = phase(
        (activated_0, grad_hidden_0, normed_all, cot_all, right[2], left[2])
    )
    grads_first = weight_grads(grad_hidden_0, activated_0)
    for step in range(3, n):
        right[step], left[step] = gather_step(step, None)
    grads_first, activated_0, last_unit, normed_all, cot_all, right[3:], left[3:] = phase(
        (grads_first, activated_0, last_unit, normed_all, cot_all, right[3:], left[3:])
    )
    head_weights = assemble(heads_unit, right, left, n, z)
    qkv_weight, output_turned = head_weights[:, : 3 * width], head_weights[:, 3 * width :]

    qkv_bias = jnp.concatenate(
        [row(b, y * width, width) for b in (query_bias, key_bias, value_bias)]
    ).astype(F32)
    qkv = dot(normed_all, qkv_weight) + qkv_bias
    grad_attended = dot(cot_all, output_turned).astype(BF16)
    right[1], left[1] = gather_step(1, last_unit)
    qkv, grad_attended, normed_all, cot_all, right[1], left[1] = phase(
        (qkv, grad_attended, normed_all, cot_all, right[1], left[1])
    )
    found = attention(0, splits, qkv, grad_attended, cosine, sine, ())
    right[2], left[2] = gather_step(2, None)
    first_in = scatter_step(n - 1, grads_first, n, z, (None, None))
    found, qkv, grad_attended, normed_all, cot_all, right[2], left[2], first_in, grads_first = phase(
        (found, qkv, grad_attended, normed_all, cot_all, right[2], left[2], first_in, grads_first)
    )
    for index in range(1, splits.shape[0]):
        found = attention(index, splits, qkv, grad_attended, cosine, sine, found)
    for step in range(3, n):
        right[step], left[step] = gather_step(step, None)
    for k in range(n - 2, n - 3, -1):
        first_in = scatter_step(k, grads_first, n, z, first_in)
    found, normed_all, cot_all, right[3:], left[3:], first_in, grads_first = phase(
        (found, normed_all, cot_all, right[3:], left[3:], first_in, grads_first)
    )
    attended, grad_qkv = found
    grads_heads = weight_grads(grad_qkv, attended)
    for k in range(n - 3, 0, -1):
        first_in = scatter_step(k, grads_first, n, z, first_in)
    grads_heads, attended, grad_qkv, normed_all, cot_all, last_unit, first_in, grads_first = phase(
        (grads_heads, attended, grad_qkv, normed_all, cot_all, last_unit, first_in, grads_first)
    )
    first_sum = scatter_end(grads_first, n, z, first_in)

    last_weights = assemble(last_unit, right, left, n, z)
    activated_1, grad_hidden_1, hidden_sum_1 = hidden_local(last_weights, 1)
    heads_in = scatter_step(n - 1, grads_heads, n, z, (None, None))
    (last_weights, activated_1, grad_hidden_1, attended, grad_qkv, heads_in, grads_heads,
     normed_all, cot_all) = phase(
        (last_weights, activated_1, grad_hidden_1, attended, grad_qkv, heads_in, grads_heads,
         normed_all, cot_all)
    )
    for k in range(n - 2, max(n - 3, 1), -1):
        heads_in = scatter_step(k, grads_heads, n, z, heads_in)
    grads_last = weight_grads(grad_hidden_1, activated_1)
    qkv_sum = jnp.sum(grad_qkv, 0, dtype=F32)[None]
    bias_row = jnp.concatenate([qkv_sum, hidden_sum_0, hidden_sum_1], 1)
    cot_wide = cotangent.astype(F32)
    cot_sum = jnp.sum(cot_wide, 0)[None]
    grads_last, heads_in, grads_heads, bias_row, cot_sum = phase(
        (grads_last, heads_in, grads_heads, bias_row, cot_sum)
    )
    def halves(total):
        keep = row(total, y * shard_rows, shard_rows)
        give = row(total, (1 - y) * shard_rows, shard_rows).astype(BF16)
        return keep, lax.ppermute(give, "y", SWAP).astype(F32)

    first_keep, first_take = halves(first_sum)

    if n == 4 and bias_row.shape[1] <= cot_sum.shape[1]:
        spread = cot_sum.shape[1]
        vector = jnp.concatenate([
            jnp.zeros((2, spread), F32), cot_sum,
            jnp.pad(bias_row, ((0, 0), (0, spread - bias_row.shape[1]))),
            jnp.zeros((4, spread), F32),
        ])
        left_piece, right_piece = scatter_pieces(1, grads_heads, n, z, heads_in)
        own_piece = row(grads_heads, z * 2 * shard_rows, 2 * shard_rows)
        last_keep, last_take, heads_keep, heads_take, grad_normed, mixed, sums = tail(
            n, grads_last.T, (head_weights, first_weights, last_weights),
            (grad_qkv, grad_hidden_0, grad_hidden_1), (attended, activated_0, activated_1),
            (left_piece.T, right_piece.T, own_piece.T), standard, vector,
        )
        last_keep, last_take = last_keep.T, last_take.astype(F32).T
        heads_keep, heads_take = heads_keep.T, heads_take.astype(F32).T
        norm_sums = sums[:3]
        bias_rows = in_order(y, sums[3:4], sums[4:5], 0)[:, : bias_row.shape[1]]
    else:
        for k in range(n - 3, 0, -1):
            heads_in = scatter_step(k, grads_heads, n, z, heads_in)
        heads_keep, heads_take = halves(scatter_end(grads_heads, n, z, heads_in))
        partial_out = sum_dots(
            (attended, activated_0, activated_1),
            ((head_weights, width, 3), (first_weights, piece, 1), (last_weights, piece, 1)),
        )
        grad_normed_part = sum_dots(
            (grad_qkv, grad_hidden_0, grad_hidden_1),
            ((head_weights, 3 * width, 0), (first_weights, piece, 0), (last_weights, piece, 0)),
        )
        last_in = (None, None)
        for k in range(n - 1, 0, -1):
            last_in = scatter_step(k, grads_last, n, z, last_in)
        last_keep, last_take = halves(scatter_end(grads_last, n, z, last_in))
        grad_normed = plane_scatter(grad_normed_part, y, x, c)
        mixed = plane_scatter(partial_out, y, x, c)
        norm_sums = sum_small(
            jnp.concatenate([
                jnp.sum(grad_normed * standard, 0)[None], jnp.sum(grad_normed, 0)[None], cot_sum
            ]),
            ("c", "x", "y", "z"),
        )
        bias_row = sum_small(bias_row, ("z",))
        bias_rows = in_order(y, bias_row, lax.ppermute(bias_row, "y", SWAP), 0)
    grad_norm_gain, grad_norm_bias, grad_out_bias = norm_sums

    out_bias = output_bias.astype(F32) + down_bias.astype(F32)
    out = (tokens_wide + mixed + out_bias).astype(BF16)

    def joined(start, size):
        return in_order(
            y, heads_keep[:, start : start + size], heads_take[:, start : start + size], 1
        )

    grad_query_weight, grad_key_weight, grad_value_weight, grad_output_turned = (
        joined(part * width, width) for part in range(4)
    )
    hidden_halves = [(first_keep, first_take), (last_keep, last_take)]

    def side(which, start):
        return jnp.concatenate([pair[which][:, start : start + piece] for pair in hidden_halves], 1)

    grad_up_weight = in_order(y, side(0, 0), side(1, 0), 1)
    grad_down_turned = in_order(y, side(0, piece), side(1, piece), 1)

    grad_query_bias, grad_key_bias, grad_value_bias = (
        bias_rows[:, part * width : (part + 1) * width].reshape(-1) for part in range(3)
    )
    grad_up_bias = bias_rows[:, 3 * width :].reshape(-1)

    grad_scaled = grad_normed * gain_wide
    grad_tokens = cot_wide + inv_scale * (
        grad_scaled
        - jnp.mean(grad_scaled, -1, keepdims=True)
        - standard * jnp.mean(grad_scaled * standard, -1, keepdims=True)
    )
    return (
        out, grad_tokens, grad_norm_gain, grad_norm_bias,
        grad_query_weight, grad_query_bias, grad_key_weight, grad_key_bias,
        grad_value_weight, grad_value_bias, grad_output_turned.T, grad_out_bias,
        grad_up_weight, grad_up_bias, grad_down_turned.T, grad_out_bias,
    )


def solution(mesh):
    n = mesh.shape["dp"] // 2
    grid = Mesh(mesh.devices.reshape(n, 2, mesh.shape["tensor"] // 2, 2), ("z", "y", "x", "c"))
    dp, tensor = ("z", "y"), ("x", "c")
    rows = P(dp + tensor, None)
    whole, split = P(), P(tensor)
    wide, tall = P(dp, tensor), P(tensor, dp)
    in_specs = (
        rows, whole, whole, wide, split, wide, split, wide, split,
        tall, whole, wide, split, tall, whole, P(dp), rows,
    )
    out_specs = (
        rows, rows, whole, whole, wide, split, wide, split, wide, split,
        tall, whole, wide, split, tall, whole,
    )
    return jax.shard_map(
        functools.partial(on_device, n),
        mesh=grid, in_specs=in_specs, out_specs=out_specs, check_vma=False,
    )
```

```python
import functools

import jax
import jax.numpy as jnp
from jax import lax
from jax.experimental import pallas as pl
from jax.experimental.pallas import tpu as pltpu
from jax.sharding import Mesh, PartitionSpec as P

HEAD_DIM = 64
ROT = 32
BLOCK = 256
EPS = 1e-05
LANES = 128
F32 = jnp.float32
BF16 = jnp.bfloat16


SWAP = [(0, 1), (1, 0)]
NT = (((1,), (1,)), ((), ()))
TN = (((0,), (0,)), ((), ()))
NN = (((1,), (0,)), ((), ()))


def dot(left, right, dims=NN):
    return lax.dot_general(left, right, dims, preferred_element_type=F32)


def spin(value, cosine, sine):
    lane = lax.broadcasted_iota(jnp.int32, value.shape, 1) % HEAD_DIM
    half = ROT // 2
    ahead = pltpu.roll(value, LANES - half, 1)
    behind = pltpu.roll(value, half, 1)
    return value * cosine + jnp.where(lane < half, ahead, behind) * sine


def attention_kernel(
    index, earlier, split_ref, qkv_ref, grad_ref, cos_ref, sin_ref, *refs
):
    (att_ref, dqkv_ref, *scratch) = refs[earlier:]
    attention_body(index, split_ref, qkv_ref, grad_ref, cos_ref, sin_ref, att_ref, dqkv_ref, *scratch)


def attention_body(
    index, split_ref, qkv_ref, grad_ref, cos_ref, sin_ref, att_ref, dqkv_ref,
    q_s, k_s, v_s, g_s, b_s, dq_s, dk_s, dv_s, cos_s, sin_s,
):
    seq_len, width = grad_ref.shape
    first = split_ref[index] // BLOCK
    scale = HEAD_DIM ** (-0.5)
    per = LANES // HEAD_DIM
    rest = jnp.zeros((HEAD_DIM - ROT, seq_len), F32)
    cos_part, sin_part = cos_ref[...], sin_ref[...]
    cos_s[...] = jnp.concatenate([cos_part, cos_part, rest + 1.0] * per, 0).T
    sin_s[...] = jnp.concatenate([-sin_part, sin_part, rest] * per, 0).T

    def one_pair(pair, carry):
        def cols(part):
            return pl.ds(pl.multiple_of(part * width + pair * LANES, LANES), LANES)

        cosine, sine = cos_s[...], sin_s[...]
        head_of = lax.broadcasted_iota(jnp.int32, (seq_len, LANES), 1) // HEAD_DIM
        query = spin(qkv_ref[:, cols(0)], cosine, sine).astype(BF16)
        key = spin(qkv_ref[:, cols(1)], cosine, sine).astype(BF16)
        value = qkv_ref[:, cols(2)].astype(BF16)
        grad = grad_ref[:, cols(0)]
        query = (query.astype(F32) * scale).astype(BF16)
        turned_back = (key.astype(F32) * scale).astype(BF16)
        for head in range(per):
            here = head_of == head
            q_s[head] = jnp.where(here, query, 0).astype(BF16)
            k_s[head] = jnp.where(here, key, 0).astype(BF16)
            b_s[head] = jnp.where(here, turned_back, 0).astype(BF16)
            v_s[head] = jnp.where(here, value, 0).astype(BF16)
            g_s[head] = jnp.where(here, grad, 0).astype(BF16)
        dk_s[...] = jnp.zeros_like(dk_s)
        dv_s[...] = jnp.zeros_like(dv_s)

        def one_block(block, inner):
            begin = jnp.where(block >= first, first, 0)
            rows = pl.ds(pl.multiple_of(block * BLOCK, BLOCK), BLOCK)

            def work(count):
                span = pl.ds(pl.multiple_of(begin * BLOCK, BLOCK), count * BLOCK)
                held = None
                for head in range(per):
                    q, g = q_s[head, rows, :], g_s[head, rows, :]
                    scores = dot(k_s[head, span, :], q, NT)
                    top = jnp.max(scores, 0, keepdims=True)
                    power = jnp.exp(scores - top)
                    prob = power * (1.0 / jnp.sum(power, 0, keepdims=True))
                    low = prob.astype(BF16)
                    dprob = dot(v_s[head, span, :], g, NT)
                    mean = jnp.sum(prob * dprob, 0, keepdims=True)
                    dscore = (prob * (dprob - mean)).astype(BF16)
                    parts = (
                        dot(dscore, q), dot(low, g),
                        dot(dscore, b_s[head, span, :], TN), dot(low, v_s[head, span, :], TN),
                    )
                    held = parts if held is None else [a + b for a, b in zip(held, parts)]
                dk, dv, dq, found = held
                dq_s[rows, :] = dq
                att_ref[rows, cols(0)] = found.astype(BF16)
                dk_s[span, :] += dk
                dv_s[span, :] += dv

            for count in range(1, seq_len // BLOCK):
                pl.when(block - begin == count - 1)(functools.partial(work, count))
            return inner

        lax.fori_loop(0, seq_len // BLOCK, one_block, 0)
        dqkv_ref[:, cols(0)] = spin(dq_s[...], cosine, -sine).astype(BF16)
        dqkv_ref[:, cols(1)] = spin(dk_s[...], cosine, -sine).astype(BF16)
        dqkv_ref[:, cols(2)] = dv_s[...].astype(BF16)
        return carry

    lax.fori_loop(0, width // LANES, one_pair, 0)


def attention(index, splits, qkv, grad, cosine, sine, earlier):
    count = splits.shape[0]
    rows, width = grad.shape
    seq_len = rows // count
    per = LANES // HEAD_DIM

    def spec(columns):
        return pl.BlockSpec((seq_len, columns), lambda i, split: (index, 0))

    table = pl.BlockSpec((ROT // 2, seq_len), lambda i, split: (0, index))
    masked = pltpu.VMEM((per, seq_len, LANES), BF16)
    return pl.pallas_call(
        functools.partial(attention_kernel, index, len(earlier)),
        grid_spec=pltpu.PrefetchScalarGridSpec(
            num_scalar_prefetch=1,
            grid=(1,),
            in_specs=[spec(3 * width), spec(width), table, table]
            + [pl.BlockSpec(memory_space=pl.ANY)] * len(earlier),
            out_specs=[spec(width), spec(3 * width)],
            scratch_shapes=[
                masked, masked, masked, masked, masked,
                pltpu.VMEM((seq_len, LANES), F32),
                pltpu.VMEM((seq_len, LANES), F32),
                pltpu.VMEM((seq_len, LANES), F32),
                pltpu.VMEM((seq_len, LANES), F32),
                pltpu.VMEM((seq_len, LANES), F32),
            ],
        ),
        out_shape=[
            jax.ShapeDtypeStruct((rows, width), BF16),
            jax.ShapeDtypeStruct((rows, 3 * width), BF16),
        ],
        cost_estimate=pl.CostEstimate(
            flops=40 * seq_len * seq_len * width // 4,
            transcendentals=seq_len * seq_len * width // HEAD_DIM // 2,
            bytes_accessed=seq_len * width * 24,
        ),
        input_output_aliases={5 + i: i for i in range(len(earlier))},
        compiler_params=pltpu.CompilerParams(vmem_limit_bytes=48 << 20),
        name="attention",
    )(splits, qkv, grad, cosine, sine, *earlier)


def turn_tables(splits, seq_len):
    shape = (ROT // 2, splits.shape[0], seq_len)
    token = lax.broadcasted_iota(jnp.int32, shape, 2)
    start = splits[None, :, None]
    position = (token - jnp.where(token >= start, start, 0)).astype(F32)
    entry = jnp.arange(ROT // 2, dtype=F32)
    angle = position * (10000.0 ** (-(2.0 * entry) / ROT))[:, None, None]
    return jnp.cos(angle).reshape(ROT // 2, -1), jnp.sin(angle).reshape(ROT // 2, -1)


def sum_dots_kernel(count, *refs):
    out_ref = refs[-1]
    total = None
    for i in range(count):
        part = dot(refs[i][...], refs[count + i][...], NT)
        total = part if total is None else total + part
    out_ref[...] = total.astype(out_ref.dtype)


def sum_dots(lefts, rights, tile=512):
    rows, columns = lefts[0].shape[0], rights[0][0].shape[0]
    tile = min(tile, rows)
    depth = sum(left.shape[1] for left in lefts)
    return pl.pallas_call(
        functools.partial(sum_dots_kernel, len(lefts)),
        grid=(rows // tile,),
        in_specs=[pl.BlockSpec((tile, left.shape[1]), lambda i: (i, 0)) for left in lefts] + [
            pl.BlockSpec((columns, size), functools.partial(lambda at, i: (0, at), at))
            for _, size, at in rights
        ],
        out_specs=pl.BlockSpec((tile, columns), lambda i: (i, 0)),
        out_shape=jax.ShapeDtypeStruct((rows, columns), BF16),
        cost_estimate=pl.CostEstimate(
            flops=2 * rows * columns * depth, transcendentals=0,
            bytes_accessed=2 * (rows * columns + depth * (rows + columns)),
        ),
        compiler_params=pltpu.CompilerParams(vmem_limit_bytes=56 << 20),
        name="sum_dots",
    )(*lefts, *(right[0] for right in rights))


def hidden_kernel(n_ref, c_ref, w_ref, bias_ref, act_ref, dh_ref, sum_ref, *grads):
    piece = act_ref.shape[1]
    hidden = dot(n_ref[...], w_ref[:, :piece]) + bias_ref[...]
    grad = dot(c_ref[...], w_ref[:, piece:])
    rate = (2.0 / jnp.pi) ** 0.5
    square = hidden * hidden
    bent = jnp.tanh(rate * hidden * (1.0 + 0.044715 * square))
    act = (0.5 * hidden * (1.0 + bent)).astype(BF16)
    act_ref[...] = act
    slope = 0.5 * (1.0 + bent) + 0.5 * hidden * (1.0 - bent * bent) * (
        rate * (1.0 + 3.0 * 0.044715 * square)
    )
    low = (grad * slope).astype(BF16)
    dh_ref[...] = low

    @pl.when(pl.program_id(0) == 0)
    def _():
        sum_ref[...] = jnp.zeros_like(sum_ref)

    sum_ref[...] += jnp.sum(low.astype(F32), 0, keepdims=True)
    if not grads:
        return

    grads_ref, acc_s = grads
    depth = n_ref.shape[1]
    width = min(512, depth)
    low_turned, act_turned = low.T, act.T
    first = pl.program_id(0) == 0

    def columns(t, carry):
        span = pl.ds(pl.multiple_of(t * width, width), width)
        for turned, right, where in ((low_turned, n_ref, 0), (act_turned, c_ref, piece)):
            rows = slice(where, where + piece)
            part = dot(turned, right[:, span])
            total = jnp.where(first, part, part + acc_s[rows, span])
            acc_s[rows, span] = total
            grads_ref[rows, span] = total.astype(BF16)
        return carry

    lax.fori_loop(0, depth // width, columns, 0)


def hidden_part(normed_all, cot_all, weights, bias, with_grads=False):
    tile = 1024 if with_grads else 512
    rows, depth = normed_all.shape
    piece = weights.shape[1] // 2
    tile = min(tile, rows)
    wide = pl.BlockSpec((tile, depth), lambda i: (i, 0))
    thin = pl.BlockSpec((tile, piece), lambda i: (i, 0))
    line = pl.BlockSpec((1, piece), lambda i: (0, 0))
    return pl.pallas_call(
        hidden_kernel,
        grid=(rows // tile,),
        in_specs=[wide, wide, pl.BlockSpec(weights.shape, lambda i: (0, 0)), line],
        out_specs=[thin, thin, line]
        + [pl.BlockSpec((2 * piece, depth), lambda i: (0, 0))] * with_grads,
        out_shape=[
            jax.ShapeDtypeStruct((rows, piece), BF16),
            jax.ShapeDtypeStruct((rows, piece), BF16),
            jax.ShapeDtypeStruct((1, piece), F32),
        ] + [jax.ShapeDtypeStruct((2 * piece, depth), BF16)] * with_grads,
        scratch_shapes=[pltpu.VMEM((2 * piece, depth), F32)] * with_grads,
        cost_estimate=pl.CostEstimate(
            flops=(8 if with_grads else 4) * rows * depth * piece, transcendentals=rows * piece,
            bytes_accessed=4 * rows * depth + 4 * depth * piece + 4 * rows * piece,
        ),
        compiler_params=pltpu.CompilerParams(vmem_limit_bytes=60 << 20),
        name="hidden_part",
    )(normed_all, cot_all, weights, bias)


def gather_kernel(
    n, own_ref, other_ref, second_ref, second_other_ref, next_ref, norm_ref, cot_ref,
    w_ref, unit_ref, right_ref, left_ref, swapped_ref, n_ref, c_ref, send_sem, recv_sem, local_sem,
):
    z, y, x, c = (lax.axis_index(name) for name in ("z", "y", "x", "c"))
    rows = norm_ref.shape[0]
    half = 3 * rows // 4
    mine = y * 4 + x * 2 + c
    has_right, has_left = z < n - 1, z > 0
    number = {}

    def remote(key, src, dst, axis, target):
        slot = number.setdefault(key, len(number))
        return pltpu.make_async_remote_copy(
            src_ref=src, dst_ref=dst, send_sem=send_sem.at[slot], recv_sem=recv_sem.at[slot],
            device_id={axis: target}, device_id_type=pl.DeviceIdType.MESH,
        )

    def when(condition, action):
        if condition is None:
            action()
        else:
            pl.when(condition)(action)

    started = []

    def start(condition, copy):
        when(condition, copy.start)
        started.append((condition, copy))

    def shard(index, unit):
        return w_ref.at[index * 2 + (y if unit == 0 else 1 - y)]

    def along(step, unit, sign, receiving=False):
        index = z - sign * step if receiving else z - sign * (step - 1)
        source = own_ref if step == 1 and unit == 0 and not receiving else shard(index, unit)
        return remote((step, unit, sign), source, shard(index, unit), "z", z + sign)


    full, top, low = pl.ds(0, rows), pl.ds(0, half), pl.ds(half, rows - half)
    arrays = ((n_ref, norm_ref, "n"), (c_ref, cot_ref, "c"))
    at_x, at_y, at_xy = y * 4 + (1 - x) * 2 + c, (1 - y) * 4 + x * 2 + c, (1 - y) * 4 + (1 - x) * 2 + c

    barrier = pltpu.get_barrier_semaphore()
    for axis, target in (("x", 1 - x), ("y", 1 - y), ("c", 1 - c)):
        pl.semaphore_signal(
            barrier, inc=1, device_id={axis: target}, device_id_type=pl.DeviceIdType.MESH
        )
    for condition, target in ((has_right, z + 1), (has_left, z - 1)):
        when(condition, functools.partial(
            pl.semaphore_signal, barrier, inc=1, device_id={"z": target},
            device_id_type=pl.DeviceIdType.MESH,
        ))
    pl.semaphore_wait(barrier, 3 + has_right.astype(jnp.int32) + has_left.astype(jnp.int32))

    for condition, sign in ((has_right, 1), (has_left, -1)):
        start(condition, along(1, 0, sign))
    swap = remote("swap", other_ref, w_ref.at[z * 2 + y], "y", 1 - y)
    swap_in = remote("swap", other_ref, w_ref.at[z * 2 + 1 - y], "y", 1 - y)
    start(None, swap)
    for array, source, name in arrays:
        for axis in ("x", "y", "c"):
            start(None, remote((name, axis), source, array.at[mine], axis,
                               {"x": 1 - x, "y": 1 - y, "c": 1 - c}[axis]))
    unit_swap = remote("unit", second_other_ref, unit_ref.at[y], "y", 1 - y)
    unit_swap_in = remote("unit", second_other_ref, unit_ref.at[1 - y], "y", 1 - y)
    start(None, unit_swap)
    late_swap = remote("late", next_ref, swapped_ref, "y", 1 - y)
    start(None, late_swap)
    local = [
        pltpu.make_async_copy(own_ref, shard(z, 0), local_sem.at[0]),
        pltpu.make_async_copy(norm_ref, n_ref.at[mine], local_sem.at[1]),
        pltpu.make_async_copy(cot_ref, c_ref.at[mine], local_sem.at[2]),
        pltpu.make_async_copy(second_ref, unit_ref.at[y], local_sem.at[3]),
    ]
    for copy in local:
        copy.start()

    def arrive_swap():
        swap_in.wait_recv()
        for condition, sign in ((has_right, 1), (has_left, -1)):
            start(condition, along(1, 1, sign))

    def arrive_shard(step, unit, sign):
        inside = z - sign * step >= 0 if sign > 0 else z + step < n
        further = has_right if sign > 0 else has_left
        when(inside, along(step, unit, sign, True).wait_recv)
        if step + 1 < n:
            start(inside & further, along(step + 1, unit, sign))

    def arrive_rows(array, name, axis):
        index = {"x": at_x, "y": at_y, "c": None}[axis]
        block = array.at[index]
        remote((name, axis), block, block, axis, 0).wait_recv()
        part, on = (low, "y") if axis == "x" else (top, "x")
        piece = array.at[index, part]
        start(None, remote((name, "far", on), piece, piece, on, {"x": 1 - x, "y": 1 - y}[on]))
        start(None, remote((name, "core", axis), block, block, "c", 1 - c))

    def arrive_far(array, name, on):
        part = low if on == "y" else top
        piece = array.at[at_xy, part]
        remote((name, "far", on), piece, piece, on, 0).wait_recv()
        start(None, remote((name, "core", "far", on), piece, piece, "c", 1 - c))

    def arrive_steps(step):
        for unit in (0, 1):
            for sign in (1, -1):
                arrive_shard(step, unit, sign)

    def second_step(half_of, receiving):
        index = y if half_of == 0 else 1 - y
        source = second_ref if half_of == 0 else unit_ref.at[index]
        ways = ((1, has_left if receiving else has_right, right_ref),
                (-1, has_right if receiving else has_left, left_ref))
        for sign, condition, target in ways:
            copy = remote(("second", half_of, sign), source, target.at[index], "z", z + sign)
            if receiving:
                when(condition, copy.wait_recv)
            else:
                start(condition, copy)

    (norm, _, norm_name), (cot, _, cot_name) = arrays
    arrive_swap()
    arrive_rows(norm, norm_name, "x")
    for sign in (1, -1):
        arrive_shard(1, 0, sign)
    arrive_rows(norm, norm_name, "y")
    for sign in (1, -1):
        arrive_shard(1, 1, sign)
    arrive_rows(cot, cot_name, "x")
    if n > 2:
        arrive_steps(2)
    second_step(0, False)
    arrive_rows(cot, cot_name, "y")
    unit_swap_in.wait_recv()
    second_step(1, False)
    for step in range(3, n):
        arrive_steps(step)
    for array, _, name in arrays:
        for on in ("x", "y"):
            arrive_far(array, name, on)
    for array, _, name in arrays:
        for key, index, part in (
            ((name, "c"), y * 4 + x * 2 + 1 - c, full),
            ((name, "core", "x"), y * 4 + (1 - x) * 2 + 1 - c, full),
            ((name, "core", "y"), (1 - y) * 4 + x * 2 + 1 - c, full),
            ((name, "core", "far", "x"), (1 - y) * 4 + (1 - x) * 2 + 1 - c, top),
            ((name, "core", "far", "y"), (1 - y) * 4 + (1 - x) * 2 + 1 - c, low),
        ):
            piece = array.at[index, part]
            remote(key, piece, piece, "c", 0).wait_recv()
    late_swap.wait_recv()
    for half_of in (0, 1):
        second_step(half_of, True)
    for copy in local:
        copy.wait()
    for condition, copy in started:
        when(condition, copy.wait_send)


def gather_all(n, own, other, second, second_other, following, normed, cotangent):
    rows, columns = normed.shape
    copies = 4 * (n - 1) + 8 + 2 * 9
    anywhere = pl.BlockSpec(memory_space=pl.ANY)
    pair = jax.ShapeDtypeStruct((2,) + second.shape, second.dtype)
    weights, unit, right, left, swapped, normed_all, cot_all = pl.pallas_call(
        functools.partial(gather_kernel, n),
        in_specs=[anywhere] * 7,
        out_specs=[anywhere] * 7,
        out_shape=[
            jax.ShapeDtypeStruct((2 * n,) + own.shape, own.dtype),
            pair, pair, pair,
            jax.ShapeDtypeStruct(following.shape, following.dtype),
            jax.ShapeDtypeStruct((8, rows, columns), normed.dtype),
            jax.ShapeDtypeStruct((8, rows, columns), cotangent.dtype),
        ],
        scratch_shapes=[
            pltpu.SemaphoreType.DMA((copies,)),
            pltpu.SemaphoreType.DMA((copies,)),
            pltpu.SemaphoreType.DMA((4,)),
        ],
        cost_estimate=pl.CostEstimate(flops=0, transcendentals=0, bytes_accessed=200 << 20),
        compiler_params=pltpu.CompilerParams(collective_id=0, has_side_effects=True),
        name="gather_rows",
    )(own, other, second, second_other, following, normed, cotangent)
    flat = lambda array: array.reshape(-1, array.shape[-1])
    return tuple(map(flat, (weights, unit, right, left, swapped, normed_all, cot_all)))


def chain_step(step, n, right, left):
    return (
        lax.ppermute(right, "z", [(i, i + 1) for i in range(step - 1, n - 1)]),
        lax.ppermute(left, "z", [(i, i - 1) for i in range(1, n - step + 1)]),
    )


def assemble(unit, right, left, n, z):
    rows, columns = unit.shape
    whole = jnp.zeros((n * rows, columns), unit.dtype)
    for k in range(n):
        piece = unit if k == 0 else jnp.where(z >= k, right[k], left[n - k])
        row = lax.rem(z - k + n, n) * rows
        whole = lax.dynamic_update_slice(whole, piece, (row, jnp.int32(0)))
    return whole


def scatter_pieces(k, grads, n, z, received):
    rows = grads.shape[0] // n

    def piece(index, got):
        own = lax.dynamic_slice_in_dim(grads, jnp.clip(index, 0, n - 1) * rows, rows, 0)
        return own if got is None else add_low(own, got)

    return piece(z - k, received[0]), piece(z + k, received[1])


def scatter_step(k, grads, n, z, received):
    to_left, to_right = scatter_pieces(k, grads, n, z, received)
    return (
        lax.ppermute(to_left, "z", [(r, r - 1) for r in range(k, n)]),
        lax.ppermute(to_right, "z", [(r, r + 1) for r in range(0, n - k)]),
    )


def scatter_end(grads, n, z, received):
    rows = grads.shape[0] // n
    own = lax.dynamic_slice_in_dim(grads, z * rows, rows, 0).astype(F32)
    return own + received[0].astype(F32) + received[1].astype(F32)


def tail_kernel(
    n, g_any, hw_ref, fw_ref, lw_ref, dq_ref, d0_ref, d1_ref, at_ref, a0_ref, a1_ref,
    left_ref, right_ref, own_ref, std_any, vec_ref,
    keep_ref, take_ref, heads_keep_ref, heads_take_ref, out_ref, mixed_ref, sums_ref,
    g_ref, std_ref, hw_s, fw_s, lw_s, rows_s, stage, zrecv, give, heads_recv, heads_own, heads_give, both, xtop_2, ylow_2, ytop_2, xlow_2,
    top_2, low_2, vstage, vrecv, send_sem, recv_sem, load_sem, rows_sem,
):
    z, y, x, c = (lax.axis_index(name) for name in ("z", "y", "x", "c"))
    rows, columns = out_ref.shape
    wide, wide_heads = give.shape[0], heads_give.shape[0]
    half = rows // 2
    rest = rows - half
    number, started = {}, []

    def remote(key, src, dst, axis, target):
        slot = number.setdefault(key, len(number))
        return pltpu.make_async_remote_copy(
            src_ref=src, dst_ref=dst, send_sem=send_sem.at[slot], recv_sem=recv_sem.at[slot],
            device_id={axis: target}, device_id_type=pl.DeviceIdType.MESH,
        )

    def when(condition, action):
        if condition is None:
            action()
        else:
            pl.when(condition)(action)

    def start(condition, copy):
        when(condition, copy.start)
        started.append((condition, copy))

    def each(count, size, body):
        def step(i, carry):
            body(pl.ds(pl.multiple_of(i * size, size), size))
            return carry
        lax.fori_loop(0, count // size, step, 0)

    barrier = pltpu.get_barrier_semaphore()
    greet = [(None, "x", 1 - x), (None, "y", 1 - y), (None, "c", 1 - c)]
    greet += [(z < n - 1, "z", z + 1), (z > 0, "z", z - 1)]
    for step in (2 ** i for i in range(1, n.bit_length() - 1)):
        greet.append((None, "z", jnp.bitwise_xor(z, step)))
    for condition, axis, target in greet:
        when(condition, functools.partial(
            pl.semaphore_signal, barrier, inc=1, device_id={axis: target},
            device_id_type=pl.DeviceIdType.MESH))

    loads = [
        pltpu.make_async_copy(source, target, load_sem.at[i])
        for i, (source, target) in enumerate(
            ((hw_ref, hw_s), (fw_ref, fw_s), (lw_ref, lw_s), (g_any, g_ref), (std_any, std_ref),
             (own_ref, heads_own)))
    ]
    for load in loads:
        load.start()

    firsts, lasts = fw_ref.shape[1] // 2, lw_ref.shape[1] // 2
    heads = dq_ref.shape[1]
    sums = (
        ((dq_ref, heads, hw_s, 0), (d0_ref, firsts, fw_s, 0), (d1_ref, lasts, lw_s, 0)),
        ((at_ref, heads // 3, hw_s, heads), (a0_ref, firsts, fw_s, firsts),
         (a1_ref, lasts, lw_s, lasts)),
    )
    sides = (1 - y, y)
    jobs = [(a, own, j) for a in (0, 1) for own in (False, True) for j in sides]

    def row_loads(number_of):
        a, own, j = jobs[number_of]
        slot, core, copies, at = number_of % 2, c if own else 1 - c, [], 0
        for p, (left, width, _, _) in enumerate(sums[a]):
            for i in (0, 1):
                block = j * 4 + i * 2 + core
                source = left.at[pl.ds(pl.multiple_of(block * rows, rows), rows)]
                target = rows_s.at[slot, pl.ds(i * rows, rows), pl.ds(at, width)]
                copies.append(pltpu.make_async_copy(source, target, rows_sem.at[slot, p * 2 + i]))
            at += width
        return copies

    def job(number_of):
        a, own, j = jobs[number_of]
        slot = number_of % 2
        if number_of + 1 < len(jobs):
            for copy in row_loads(number_of + 1):
                copy.start()
        for copy in row_loads(number_of):
            copy.wait()
        if own:
            for i in (0, 1):
                core_copy(a, number_of % 2, i).wait_recv()
        elif a == 1:
            for i in (0, 1):
                core_copy(0, number_of % 2, i).wait_send()
        size = min(512, columns)

        def tile(t, carry):
            span = pl.ds(pl.multiple_of(t * size, size), size)
            acc, at = None, 0
            for left, width, weights, column in sums[a]:
                part = dot(
                    rows_s[slot, :, at : at + width], weights[span, column : column + width], NT)
                acc = part if acc is None else acc + part
                at += width
            for i in (0, 1):
                piece = acc[i * rows : (i + 1) * rows]
                if own:
                    both[a, j * 2 + i, :, span] = (
                        piece + both[a, j * 2 + i, :, span].astype(F32)).astype(BF16)
                else:
                    stage[j * 2 + i, :, span] = piece.astype(BF16)
            return carry

        lax.fori_loop(0, columns // size, tile, 0)
        if own and a == 0:
            start(None, first_copy(a, "xtop", number_of % 2))
            if number_of % 2 == 0:
                for i in (0, 1):
                    start(None, first_copy(a, "ylow", i))
        if not own:
            for i in (0, 1):
                copy = core_copy(a, number_of % 2, i)
                copy.start()
                if a == 1:
                    started.append((None, copy))

    def core_copy(a, u, i):
        place = sides[u] * 2 + i
        return remote(("core", a, u, i), stage.at[place], both.at[a, place], "c", 1 - c)

    for copy in row_loads(0):
        copy.start()
    always = sum(condition is None for condition, _, _ in greet)
    pl.semaphore_wait(barrier, always + sum(
        condition.astype(jnp.int32) for condition, _, _ in greet if condition is not None))

    def first_copy(a, name, j):
        if name == "xtop":
            source = both.at[a, sides[j] * 2 + 1 - x, pl.ds(0, half)]
            return remote((name, a, j), source, xtop_2.at[a, j], "x", 1 - x)
        source = both.at[a, (1 - y) * 2 + j, pl.ds(half, rest)]
        return remote((name, a, j), source, ylow_2.at[a, j], "y", 1 - y)

    def second_copy(a, name):
        if name == "ytop":
            return remote((name, a), top_2.at[a], ytop_2.at[a], "y", 1 - y)
        return remote((name, a), low_2.at[a], xlow_2.at[a], "x", 1 - x)

    def first_send(a):
        for j in (0, 1):
            start(None, first_copy(a, "xtop", j))
            start(None, first_copy(a, "ylow", j))

    def first_arrive(a):
        for j in (0, 1):
            first_copy(a, "xtop", j).wait_recv()
            first_copy(a, "ylow", j).wait_recv()

        def upper(part):
            top_2[a, part, :] = (
                both[a, (1 - y) * 2 + x, part, :].astype(F32)
                + xtop_2[a, 0, part, :].astype(F32)
            ).astype(BF16)

        def lower(part):
            low_part = pl.ds(part.start + half, part.size)
            low_2[a, part, :] = (
                both[a, y * 2 + 1 - x, low_part, :].astype(F32)
                + ylow_2[a, 1 - x, part, :].astype(F32)
            ).astype(BF16)

        each(half, 32, upper)
        each(rest, 32, lower)
        start(None, second_copy(a, "ytop"))
        start(None, second_copy(a, "xlow"))

    def second_arrive(a):
        second_copy(a, "ytop").wait_recv()
        second_copy(a, "xlow").wait_recv()
        target = (out_ref, mixed_ref)[a]

        def finish(first, part, placed, last):
            value = (
                both[a, y * 2 + x, placed, :].astype(F32) + first[part, :].astype(F32)
                + last[part, :].astype(F32)
            )
            target[placed, :] = value
            if a == 0:
                scaled = value * std_ref[placed, :]
                vstage[0, 0:1, :] += jnp.sum(scaled, 0, keepdims=True)
                vstage[0, 1:2, :] += jnp.sum(value, 0, keepdims=True)

        def upper(part):
            finish(xtop_2.at[a, 1], part, part, ytop_2.at[a])

        def lower(part):
            finish(ylow_2.at[a, x], part, pl.ds(part.start + half, part.size), xlow_2.at[a])

        each(half, 32, upper)
        each(rest, 32, lower)

    def block_of(direction, k, u):
        index = (z - k if direction == 0 else z + k) * 2 + sides[u]
        return pl.ds(pl.multiple_of(index * rows, rows), rows)

    def z_copy(direction, k, u, src):
        target = z - 1 if direction == 0 else z + 1
        return remote((direction, k, u), src, zrecv.at[direction, k - 1, u], "z", target)

    def z_first(direction):
        edge = z == n - 1 if direction == 0 else z == 0
        for k in range(n - 1, 0, -1):
            for u in (0, 1):
                start(edge, z_copy(direction, k, u, g_any.at[:, block_of(direction, k, u)]))

    def z_step(k, u):
        for direction in (0, 1):
            if direction == 0:
                inside = (z >= k) & (z < n - 1)
            else:
                inside = (n - 1 - z >= k) & (z > 0)
            held = zrecv.at[direction, k, u]

            def add():
                z_copy(direction, k + 1, u, held).wait_recv()
                block = block_of(direction, k, u)

                def body(part):
                    held[part, :] = (
                        g_ref[part, block].astype(F32) + held[part, :].astype(F32)
                    ).astype(BF16)

                each(wide, 256, body)

            when(inside, add)
            start(inside, z_copy(direction, k, u, held))

    def z_last(u, target):
        block = block_of(0, 0, u)

        def first(part):
            target[part, :] = g_ref[part, block].astype(F32)

        each(wide, 256, first)
        for direction in (0, 1):
            held = zrecv.at[direction, 0, u]

            def add():
                z_copy(direction, 1, u, held).wait_recv()

                def body(part):
                    target[part, :] += held[part, :].astype(F32)

                each(wide, 256, body)

            when(z < n - 1 if direction == 0 else z > 0, add)

    def heads_copy(direction, u):
        span = pl.ds(pl.multiple_of(sides[u] * rows, rows), rows)
        source = (left_ref, right_ref)[direction].at[:, span]
        return remote(
            ("heads", direction, u), source, heads_recv.at[direction, :, span], "z",
            z - 1 if direction == 0 else z + 1)

    def heads_send():
        for u in (0, 1):
            start(z > 0, heads_copy(0, u))
            start(z < n - 1, heads_copy(1, u))

    def heads_last(u, target):
        span = pl.ds(pl.multiple_of(sides[u] * rows, rows), rows)

        def first(part):
            target[part, :] = heads_own[part, span].astype(F32)

        each(wide_heads, 256, first)
        for direction in (0, 1):
            def add():
                heads_copy(direction, u).wait_recv()

                def body(part):
                    target[part, :] += heads_recv[direction, part, span].astype(F32)

                each(wide_heads, 256, body)

            when(z < n - 1 if direction == 0 else z > 0, add)

    steps = [(k, u) for k in range(n - 2, 0, -1) for u in (0, 1)]

    def z_next():
        if steps:
            z_step(*steps.pop(0))

    for direction in (0, 1):
        z_first(direction)
    vstage[0] = vec_ref[...]
    for load in loads[:3]:
        load.wait()
    job(0)
    job(1)
    for load in loads[3:]:
        load.wait()
    z_next()
    job(2)
    job(3)
    heads_send()
    z_next()
    job(4)
    job(5)
    z_next()
    job(6)
    job(7)
    first_arrive(0)
    first_send(1)
    while steps:
        z_next()
    second_arrive(0)

    turns = [("z", jnp.bitwise_xor(z, 2 ** i)) for i in range(n.bit_length() - 1)]
    turns += [("y", 1 - y), ("x", 1 - x), ("c", 1 - c)]
    line = lax.broadcasted_iota(jnp.int32, vec_ref.shape, 0)

    def exchange(i):
        axis, target = turns[i]
        return remote(("vec", i), vstage.at[i], vrecv.at[i], axis, target)

    def turn(i):
        exchange(i).wait_recv()
        axis, _ = turns[i]
        old, new = vstage[i], vrecv[i]
        result = sums_ref if i == len(turns) - 1 else vstage.at[i + 1]
        result[...] = old + jnp.where((line < 3) | (axis == "z"), new, 0.0)
        if axis == "y":
            result[4:5, :] = new[3:4, :]
        if i + 1 < len(turns):
            start(None, exchange(i + 1))

    start(None, exchange(0))

    def swapped(key, source, target, length, received):
        def lower_precision(part):
            target[part, :] = source[part, :].astype(BF16)

        each(length, 256, lower_precision)
        copy = remote(key, target, received, "y", 1 - y)
        start(None, copy)
        return copy

    first_arrive(1)
    z_last(0, keep_ref)
    swap = swapped("swap", keep_ref, give, wide, take_ref)
    turn(0)
    turn(1)
    heads_last(0, heads_keep_ref)
    heads_swap = swapped("heads swap", heads_keep_ref, heads_give, wide_heads, heads_take_ref)
    turn(2)
    z_last(1, keep_ref)
    turn(3)
    heads_last(1, heads_keep_ref)
    for i in range(4, len(turns)):
        turn(i)
    second_arrive(1)
    swap.wait_recv()
    heads_swap.wait_recv()
    for condition, copy in started:
        when(condition, copy.wait_send)


def tail(n, grads_turned, weights, lefts, lefts_out, heads_turned, standard, vector):
    rows, columns = standard.shape
    wide, wide_heads = grads_turned.shape[0], heads_turned[0].shape[0]
    half = rows // 2
    inside = pl.BlockSpec(memory_space=pltpu.VMEM)
    anywhere = pl.BlockSpec(memory_space=pl.ANY)
    copies = 4 * (n - 1) + 46
    low = lambda *shape: pltpu.VMEM(shape, BF16)
    small = vector.shape
    depth = sum(left.shape[1] for left in lefts)
    return pl.pallas_call(
        functools.partial(tail_kernel, n),
        in_specs=[anywhere] * 14 + [inside],
        out_specs=[inside] * 7,
        out_shape=[
            jax.ShapeDtypeStruct((wide, rows), F32),
            jax.ShapeDtypeStruct((wide, rows), BF16),
            jax.ShapeDtypeStruct((wide_heads, rows), F32),
            jax.ShapeDtypeStruct((wide_heads, rows), BF16),
            jax.ShapeDtypeStruct((rows, columns), F32),
            jax.ShapeDtypeStruct((rows, columns), F32),
            jax.ShapeDtypeStruct(small, F32),
        ],
        scratch_shapes=[low(*grads_turned.shape), pltpu.VMEM(standard.shape, F32)] + [
            low(*array.shape) for array in weights
        ] + [
            low(2, 2 * rows, depth), low(4, rows, columns),
            low(2, n - 1, 2, wide, rows), low(wide, rows),
            low(2, wide_heads, 2 * rows), low(wide_heads, 2 * rows), low(wide_heads, rows),
            low(2, 4, rows, columns),
            low(2, 2, half, columns), low(2, 2, rows - half, columns),
            low(2, half, columns), low(2, rows - half, columns),
            low(2, half, columns), low(2, rows - half, columns),
            pltpu.VMEM((8,) + small, F32), pltpu.VMEM((8,) + small, F32),
            pltpu.SemaphoreType.DMA((copies,)),
            pltpu.SemaphoreType.DMA((copies,)),
            pltpu.SemaphoreType.DMA((6,)),
            pltpu.SemaphoreType.DMA((2, 6)),
        ],
        cost_estimate=pl.CostEstimate(flops=0, transcendentals=0, bytes_accessed=200 << 20),
        compiler_params=pltpu.CompilerParams(
            collective_id=1, has_side_effects=True, vmem_limit_bytes=63 << 20
        ),
        name="scatter_rest",
    )(grads_turned, *weights, *lefts, *lefts_out, *heads_turned, standard, vector)


def sum_small(array, axes):
    for axis in axes:
        size = lax.axis_size(axis)
        if size & (size - 1):
            array = lax.psum(array, axis)
            continue
        step = 1
        while step < size:
            array = array + lax.ppermute(array, axis, [(i, i ^ step) for i in range(size)])
            step *= 2
    return array


def pick(array, index, axis):
    return lax.dynamic_index_in_dim(array, index, axis, keepdims=False)


def add_low(left, right):
    return (left.astype(F32) + right.astype(F32)).astype(BF16)


def plane_scatter(partial, y, x, c):
    rows, columns = partial.shape[0] // 8, partial.shape[1]
    half = rows // 2
    parts = partial.reshape(2, 2, 2, rows, columns)
    acc = add_low(pick(parts, c, 2), lax.ppermute(pick(parts, 1 - c, 2), "c", SWAP))
    top, low = acc[:, :, :half], acc[:, :, half:]
    top = add_low(pick(top, x, 1), lax.ppermute(pick(top, 1 - x, 1), "x", SWAP))
    low = add_low(pick(low, y, 0), lax.ppermute(pick(low, 1 - y, 0), "y", SWAP))
    top = pick(top, y, 0).astype(F32) + lax.ppermute(pick(top, 1 - y, 0), "y", SWAP).astype(F32)
    low = pick(low, x, 0).astype(F32) + lax.ppermute(pick(low, 1 - x, 0), "x", SWAP).astype(F32)
    return jnp.concatenate([top, low], 0)


def in_order(y, own, other, axis):
    return jnp.where(
        y == 0, jnp.concatenate([own, other], axis), jnp.concatenate([other, own], axis)
    )


def on_device(
    n,
    tokens, norm_gain, norm_bias,
    query_weight, query_bias, key_weight, key_bias, value_weight, value_bias,
    output_weight, output_bias, up_weight, up_bias, down_weight, down_bias,
    doc_split, cotangent,
):
    z, y, x, c = (lax.axis_index(name) for name in ("z", "y", "x", "c"))
    shard_rows = query_weight.shape[0]
    width = query_weight.shape[1] // 2
    hidden_width = up_weight.shape[1] // 2
    chunks = 2
    piece = hidden_width // chunks

    def col(array, start, size):
        return lax.dynamic_slice_in_dim(array, start, size, 1)

    def row(array, start, size):
        return lax.dynamic_slice_in_dim(array, start, size, 0)

    def pack_heads(side):
        return jnp.concatenate(
            [col(w, side * width, width) for w in (query_weight, key_weight, value_weight)]
            + [row(output_weight, side * width, width).T],
            1,
        )

    def pack_hidden(side, chunk):
        start = side * hidden_width + chunk * piece
        return jnp.concatenate(
            [col(up_weight, start, piece), row(down_weight, start, piece).T], 1
        )

    gain_wide = norm_gain.astype(F32)
    tokens_wide = tokens.astype(F32)
    row_mean = jnp.mean(tokens_wide, -1, keepdims=True)
    centred = tokens_wide - row_mean
    inv_scale = lax.rsqrt(jnp.mean(centred * centred, -1, keepdims=True) + EPS)
    standard = centred * inv_scale
    normed = (standard * gain_wide + norm_bias.astype(F32)).astype(BF16)
    phase = lax.optimization_barrier
    packed = (
        pack_hidden(y, 0), pack_hidden(1 - y, 0), pack_heads(y), pack_heads(1 - y),
        pack_hidden(1 - y, 1), normed,
    )
    last_own = pack_hidden(y, 1)
    other_split = lax.ppermute(doc_split, "y", SWAP)
    splits = in_order(y, doc_split, other_split, 0)
    seq_len = 4 * normed.shape[0]
    cosine, sine = turn_tables(splits, seq_len)

    right, left = [None] * n, [None] * n
    first_weights, heads_unit, right[1], left[1], last_swapped, normed_all, cot_all = gather_all(
        n, *packed, cotangent
    )
    last_unit = in_order(y, last_own, last_swapped, 0)
    first_weights, heads_unit, last_unit, normed_all, cot_all, right[1], left[1], cosine, sine = phase(
        (first_weights, heads_unit, last_unit, normed_all, cot_all, right[1], left[1], cosine, sine)
    )

    def hidden_local(weights, chunk, with_grads=False):
        bias = row(up_bias, y * hidden_width + chunk * piece, piece).astype(F32)[None]
        return hidden_part(normed_all, cot_all, weights, bias, with_grads)

    def weight_grads(grad_columns, columns):
        return jnp.concatenate(
            [dot(normed_all, grad_columns, TN).astype(BF16), dot(cot_all, columns, TN).astype(BF16)], 1
        )

    def gather_step(step, source):
        return chain_step(step, n, right[step - 1], left[step - 1]) if step > 1 else chain_step(
            1, n, source, source)

    activated_0, grad_hidden_0, hidden_sum_0, grads_first = hidden_local(first_weights, 0, True)
    grads_first = grads_first.T
    right[2], left[2] = gather_step(2, None)
    activated_0, grad_hidden_0, grads_first, normed_all, cot_all, right[2], left[2] = phase(
        (activated_0, grad_hidden_0, grads_first, normed_all, cot_all, right[2], left[2])
    )
    for step in range(3, n):
        right[step], left[step] = gather_step(step, None)
    first_in = scatter_step(n - 1, grads_first, n, z, (None, None))
    (grads_first, activated_0, last_unit, normed_all, cot_all, right[3:], left[3:]) = phase(
        (grads_first, activated_0, last_unit, normed_all, cot_all, right[3:], left[3:])
    )
    head_weights = assemble(heads_unit, right, left, n, z)
    qkv_weight, output_turned = head_weights[:, : 3 * width], head_weights[:, 3 * width :]

    qkv_bias = jnp.concatenate(
        [row(b, y * width, width) for b in (query_bias, key_bias, value_bias)]
    ).astype(F32)
    qkv = dot(normed_all, qkv_weight) + qkv_bias
    grad_attended = dot(cot_all, output_turned).astype(BF16)
    right[1], left[1] = gather_step(1, last_unit)
    qkv, grad_attended, normed_all, cot_all, right[1], left[1] = phase(
        (qkv, grad_attended, normed_all, cot_all, right[1], left[1])
    )
    found = attention(0, splits, qkv, grad_attended, cosine, sine, ())
    right[2], left[2] = gather_step(2, None)
    found, qkv, grad_attended, normed_all, cot_all, right[2], left[2], first_in, grads_first = phase(
        (found, qkv, grad_attended, normed_all, cot_all, right[2], left[2], first_in, grads_first)
    )
    for index in range(1, splits.shape[0]):
        found = attention(index, splits, qkv, grad_attended, cosine, sine, found)
    for step in range(3, n):
        right[step], left[step] = gather_step(step, None)
    for k in range(n - 2, n - 3, -1):
        first_in = scatter_step(k, grads_first, n, z, first_in)
    found, normed_all, cot_all, right[3:], left[3:], first_in, grads_first = phase(
        (found, normed_all, cot_all, right[3:], left[3:], first_in, grads_first)
    )
    attended, grad_qkv = found
    grads_heads = weight_grads(grad_qkv, attended)
    for k in range(n - 3, 0, -1):
        first_in = scatter_step(k, grads_first, n, z, first_in)
    grads_heads, attended, grad_qkv, normed_all, cot_all, last_unit, first_in, grads_first = phase(
        (grads_heads, attended, grad_qkv, normed_all, cot_all, last_unit, first_in, grads_first)
    )
    first_sum = scatter_end(grads_first, n, z, first_in)

    last_weights = assemble(last_unit, right, left, n, z)
    activated_1, grad_hidden_1, hidden_sum_1 = hidden_local(last_weights, 1)
    heads_in = scatter_step(n - 1, grads_heads, n, z, (None, None))
    (last_weights, activated_1, grad_hidden_1, attended, grad_qkv, heads_in, grads_heads,
     normed_all, cot_all) = phase(
        (last_weights, activated_1, grad_hidden_1, attended, grad_qkv, heads_in, grads_heads,
         normed_all, cot_all)
    )
    for k in range(n - 2, max(n - 3, 1), -1):
        heads_in = scatter_step(k, grads_heads, n, z, heads_in)
    grads_last = weight_grads(grad_hidden_1, activated_1)
    qkv_sum = jnp.sum(grad_qkv, 0, dtype=F32)[None]
    bias_row = jnp.concatenate([qkv_sum, hidden_sum_0, hidden_sum_1], 1)
    cot_wide = cotangent.astype(F32)
    cot_sum = jnp.sum(cot_wide, 0)[None]
    grads_last, heads_in, grads_heads, bias_row, cot_sum = phase(
        (grads_last, heads_in, grads_heads, bias_row, cot_sum)
    )
    def halves(total):
        keep = row(total, y * shard_rows, shard_rows)
        give = row(total, (1 - y) * shard_rows, shard_rows).astype(BF16)
        return keep, lax.ppermute(give, "y", SWAP).astype(F32)

    first_keep, first_take = halves(first_sum)

    if n == 4 and bias_row.shape[1] <= cot_sum.shape[1]:
        spread = cot_sum.shape[1]
        vector = jnp.concatenate([
            jnp.zeros((2, spread), F32), cot_sum,
            jnp.pad(bias_row, ((0, 0), (0, spread - bias_row.shape[1]))),
            jnp.zeros((4, spread), F32),
        ])
        left_piece, right_piece = scatter_pieces(1, grads_heads, n, z, heads_in)
        own_piece = row(grads_heads, z * 2 * shard_rows, 2 * shard_rows)
        last_keep, last_take, heads_keep, heads_take, grad_normed, mixed, sums = tail(
            n, grads_last.T, (head_weights, first_weights, last_weights),
            (grad_qkv, grad_hidden_0, grad_hidden_1), (attended, activated_0, activated_1),
            (left_piece.T, right_piece.T, own_piece.T), standard, vector,
        )
        last_keep, last_take = last_keep.T, last_take.astype(F32).T
        heads_keep, heads_take = heads_keep.T, heads_take.astype(F32).T
        norm_sums = sums[:3]
        bias_rows = in_order(y, sums[3:4], sums[4:5], 0)[:, : bias_row.shape[1]]
    else:
        for k in range(n - 3, 0, -1):
            heads_in = scatter_step(k, grads_heads, n, z, heads_in)
        heads_keep, heads_take = halves(scatter_end(grads_heads, n, z, heads_in))
        partial_out = sum_dots(
            (attended, activated_0, activated_1),
            ((head_weights, width, 3), (first_weights, piece, 1), (last_weights, piece, 1)),
        )
        grad_normed_part = sum_dots(
            (grad_qkv, grad_hidden_0, grad_hidden_1),
            ((head_weights, 3 * width, 0), (first_weights, piece, 0), (last_weights, piece, 0)),
        )
        last_in = (None, None)
        for k in range(n - 1, 0, -1):
            last_in = scatter_step(k, grads_last, n, z, last_in)
        last_keep, last_take = halves(scatter_end(grads_last, n, z, last_in))
        grad_normed = plane_scatter(grad_normed_part, y, x, c)
        mixed = plane_scatter(partial_out, y, x, c)
        norm_sums = sum_small(
            jnp.concatenate([
                jnp.sum(grad_normed * standard, 0)[None], jnp.sum(grad_normed, 0)[None], cot_sum
            ]),
            ("c", "x", "y", "z"),
        )
        bias_row = sum_small(bias_row, ("z",))
        bias_rows = in_order(y, bias_row, lax.ppermute(bias_row, "y", SWAP), 0)
    grad_norm_gain, grad_norm_bias, grad_out_bias = norm_sums

    out_bias = output_bias.astype(F32) + down_bias.astype(F32)
    out = (tokens_wide + mixed + out_bias).astype(BF16)

    def joined(start, size):
        return in_order(
            y, heads_keep[:, start : start + size], heads_take[:, start : start + size], 1
        )

    grad_query_weight, grad_key_weight, grad_value_weight, grad_output_turned = (
        joined(part * width, width) for part in range(4)
    )
    hidden_halves = [(first_keep, first_take), (last_keep, last_take)]

    def side(which, start):
        return jnp.concatenate([pair[which][:, start : start + piece] for pair in hidden_halves], 1)

    grad_up_weight = in_order(y, side(0, 0), side(1, 0), 1)
    grad_down_turned = in_order(y, side(0, piece), side(1, piece), 1)

    grad_query_bias, grad_key_bias, grad_value_bias = (
        bias_rows[:, part * width : (part + 1) * width].reshape(-1) for part in range(3)
    )
    grad_up_bias = bias_rows[:, 3 * width :].reshape(-1)

    grad_scaled = grad_normed * gain_wide
    grad_tokens = cot_wide + inv_scale * (
        grad_scaled
        - jnp.mean(grad_scaled, -1, keepdims=True)
        - standard * jnp.mean(grad_scaled * standard, -1, keepdims=True)
    )
    return (
        out, grad_tokens, grad_norm_gain, grad_norm_bias,
        grad_query_weight, grad_query_bias, grad_key_weight, grad_key_bias,
        grad_value_weight, grad_value_bias, grad_output_turned.T, grad_out_bias,
        grad_up_weight, grad_up_bias, grad_down_turned.T, grad_out_bias,
    )


def solution(mesh):
    n = mesh.shape["dp"] // 2
    grid = Mesh(mesh.devices.reshape(n, 2, mesh.shape["tensor"] // 2, 2), ("z", "y", "x", "c"))
    dp, tensor = ("z", "y"), ("x", "c")
    rows = P(dp + tensor, None)
    whole, split = P(), P(tensor)
    wide, tall = P(dp, tensor), P(tensor, dp)
    in_specs = (
        rows, whole, whole, wide, split, wide, split, wide, split,
        tall, whole, wide, split, tall, whole, P(dp), rows,
    )
    out_specs = (
        rows, rows, whole, whole, wide, split, wide, split, wide, split,
        tall, whole, wide, split, tall, whole,
    )
    return jax.shard_map(
        functools.partial(on_device, n),
        mesh=grid, in_specs=in_specs, out_specs=out_specs, check_vma=False,
    )
```

```python
import functools

import jax
import jax.numpy as jnp
from jax import lax
from jax.experimental import pallas as pl
from jax.experimental.pallas import tpu as pltpu
from jax.sharding import Mesh, PartitionSpec as P

HEAD_DIM = 64
ROT = 32
BLOCK = 256
EPS = 1e-05
LANES = 128
F32 = jnp.float32
BF16 = jnp.bfloat16


SWAP = [(0, 1), (1, 0)]
NT = (((1,), (1,)), ((), ()))
TN = (((0,), (0,)), ((), ()))
NN = (((1,), (0,)), ((), ()))


def dot(left, right, dims=NN):
    return lax.dot_general(left, right, dims, preferred_element_type=F32)


def spin(value, cosine, sine):
    lane = lax.broadcasted_iota(jnp.int32, value.shape, 1) % HEAD_DIM
    half = ROT // 2
    ahead = pltpu.roll(value, LANES - half, 1)
    behind = pltpu.roll(value, half, 1)
    return value * cosine + jnp.where(lane < half, ahead, behind) * sine


def attention_kernel(
    index, earlier, split_ref, qkv_ref, grad_ref, cos_ref, sin_ref, *refs
):
    (att_ref, dqkv_ref, *scratch) = refs[earlier:]
    attention_body(index, split_ref, qkv_ref, grad_ref, cos_ref, sin_ref, att_ref, dqkv_ref, *scratch)


def attention_body(
    index, split_ref, qkv_ref, grad_ref, cos_ref, sin_ref, att_ref, dqkv_ref,
    q_s, k_s, v_s, g_s, b_s, dq_s, dk_s, dv_s, cos_s, sin_s,
):
    seq_len, width = grad_ref.shape
    first = split_ref[index] // BLOCK
    scale = HEAD_DIM ** (-0.5)
    per = LANES // HEAD_DIM
    rest = jnp.zeros((HEAD_DIM - ROT, seq_len), F32)
    cos_part, sin_part = cos_ref[...], sin_ref[...]
    cos_s[...] = jnp.concatenate([cos_part, cos_part, rest + 1.0] * per, 0).T
    sin_s[...] = jnp.concatenate([-sin_part, sin_part, rest] * per, 0).T

    def one_pair(pair, carry):
        def cols(part):
            return pl.ds(pl.multiple_of(part * width + pair * LANES, LANES), LANES)

        cosine, sine = cos_s[...], sin_s[...]
        head_of = lax.broadcasted_iota(jnp.int32, (seq_len, LANES), 1) // HEAD_DIM
        query = spin(qkv_ref[:, cols(0)], cosine, sine).astype(BF16)
        key = spin(qkv_ref[:, cols(1)], cosine, sine).astype(BF16)
        value = qkv_ref[:, cols(2)].astype(BF16)
        grad = grad_ref[:, cols(0)]
        query = (query.astype(F32) * scale).astype(BF16)
        turned_back = (key.astype(F32) * scale).astype(BF16)
        for head in range(per):
            here = head_of == head
            q_s[head] = jnp.where(here, query, 0).astype(BF16)
            k_s[head] = jnp.where(here, key, 0).astype(BF16)
            b_s[head] = jnp.where(here, turned_back, 0).astype(BF16)
            v_s[head] = jnp.where(here, value, 0).astype(BF16)
            g_s[head] = jnp.where(here, grad, 0).astype(BF16)
        dk_s[...] = jnp.zeros_like(dk_s)
        dv_s[...] = jnp.zeros_like(dv_s)

        def one_block(block, inner):
            begin = jnp.where(block >= first, first, 0)
            rows = pl.ds(pl.multiple_of(block * BLOCK, BLOCK), BLOCK)

            def work(count):
                span = pl.ds(pl.multiple_of(begin * BLOCK, BLOCK), count * BLOCK)
                held = None
                for head in range(per):
                    q, g = q_s[head, rows, :], g_s[head, rows, :]
                    scores = dot(k_s[head, span, :], q, NT)
                    top = jnp.max(scores, 0, keepdims=True)
                    power = jnp.exp(scores - top)
                    prob = power * (1.0 / jnp.sum(power, 0, keepdims=True))
                    low = prob.astype(BF16)
                    dprob = dot(v_s[head, span, :], g, NT)
                    mean = jnp.sum(prob * dprob, 0, keepdims=True)
                    dscore = (prob * (dprob - mean)).astype(BF16)
                    parts = (
                        dot(dscore, q), dot(low, g),
                        dot(dscore, b_s[head, span, :], TN), dot(low, v_s[head, span, :], TN),
                    )
                    held = parts if held is None else [a + b for a, b in zip(held, parts)]
                dk, dv, dq, found = held
                dq_s[rows, :] = dq
                att_ref[rows, cols(0)] = found.astype(BF16)
                dk_s[span, :] += dk
                dv_s[span, :] += dv

            for count in range(1, seq_len // BLOCK):
                pl.when(block - begin == count - 1)(functools.partial(work, count))
            return inner

        lax.fori_loop(0, seq_len // BLOCK, one_block, 0)
        dqkv_ref[:, cols(0)] = spin(dq_s[...], cosine, -sine).astype(BF16)
        dqkv_ref[:, cols(1)] = spin(dk_s[...], cosine, -sine).astype(BF16)
        dqkv_ref[:, cols(2)] = dv_s[...].astype(BF16)
        return carry

    lax.fori_loop(0, width // LANES, one_pair, 0)


def attention(index, splits, qkv, grad, cosine, sine, earlier):
    count = splits.shape[0]
    rows, width = grad.shape
    seq_len = rows // count
    per = LANES // HEAD_DIM

    def spec(columns):
        return pl.BlockSpec((seq_len, columns), lambda i, split: (index, 0))

    table = pl.BlockSpec((ROT // 2, seq_len), lambda i, split: (0, index))
    masked = pltpu.VMEM((per, seq_len, LANES), BF16)
    return pl.pallas_call(
        functools.partial(attention_kernel, index, len(earlier)),
        grid_spec=pltpu.PrefetchScalarGridSpec(
            num_scalar_prefetch=1,
            grid=(1,),
            in_specs=[spec(3 * width), spec(width), table, table]
            + [pl.BlockSpec(memory_space=pl.ANY)] * len(earlier),
            out_specs=[spec(width), spec(3 * width)],
            scratch_shapes=[
                masked, masked, masked, masked, masked,
                pltpu.VMEM((seq_len, LANES), F32),
                pltpu.VMEM((seq_len, LANES), F32),
                pltpu.VMEM((seq_len, LANES), F32),
                pltpu.VMEM((seq_len, LANES), F32),
                pltpu.VMEM((seq_len, LANES), F32),
            ],
        ),
        out_shape=[
            jax.ShapeDtypeStruct((rows, width), BF16),
            jax.ShapeDtypeStruct((rows, 3 * width), BF16),
        ],
        cost_estimate=pl.CostEstimate(
            flops=40 * seq_len * seq_len * width // 4,
            transcendentals=seq_len * seq_len * width // HEAD_DIM // 2,
            bytes_accessed=seq_len * width * 24,
        ),
        input_output_aliases={5 + i: i for i in range(len(earlier))},
        compiler_params=pltpu.CompilerParams(vmem_limit_bytes=48 << 20),
        name="attention",
    )(splits, qkv, grad, cosine, sine, *earlier)


def turn_tables(splits, seq_len):
    shape = (ROT // 2, splits.shape[0], seq_len)
    token = lax.broadcasted_iota(jnp.int32, shape, 2)
    start = splits[None, :, None]
    position = (token - jnp.where(token >= start, start, 0)).astype(F32)
    entry = jnp.arange(ROT // 2, dtype=F32)
    angle = position * (10000.0 ** (-(2.0 * entry) / ROT))[:, None, None]
    return jnp.cos(angle).reshape(ROT // 2, -1), jnp.sin(angle).reshape(ROT // 2, -1)


def sum_dots_kernel(count, *refs):
    out_ref = refs[-1]
    total = None
    for i in range(count):
        part = dot(refs[i][...], refs[count + i][...], NT)
        total = part if total is None else total + part
    out_ref[...] = total.astype(out_ref.dtype)


def sum_dots(lefts, rights, tile=512):
    rows, columns = lefts[0].shape[0], rights[0][0].shape[0]
    tile = min(tile, rows)
    depth = sum(left.shape[1] for left in lefts)
    return pl.pallas_call(
        functools.partial(sum_dots_kernel, len(lefts)),
        grid=(rows // tile,),
        in_specs=[pl.BlockSpec((tile, left.shape[1]), lambda i: (i, 0)) for left in lefts] + [
            pl.BlockSpec((columns, size), functools.partial(lambda at, i: (0, at), at))
            for _, size, at in rights
        ],
        out_specs=pl.BlockSpec((tile, columns), lambda i: (i, 0)),
        out_shape=jax.ShapeDtypeStruct((rows, columns), BF16),
        cost_estimate=pl.CostEstimate(
            flops=2 * rows * columns * depth, transcendentals=0,
            bytes_accessed=2 * (rows * columns + depth * (rows + columns)),
        ),
        compiler_params=pltpu.CompilerParams(vmem_limit_bytes=56 << 20),
        name="sum_dots",
    )(*lefts, *(right[0] for right in rights))


def hidden_kernel(n_ref, c_ref, w_ref, bias_ref, act_ref, dh_ref, sum_ref):
    piece = act_ref.shape[1]
    hidden = dot(n_ref[...], w_ref[:, :piece]) + bias_ref[...]
    grad = dot(c_ref[...], w_ref[:, piece:])
    rate = (2.0 / jnp.pi) ** 0.5
    square = hidden * hidden
    bent = jnp.tanh(rate * hidden * (1.0 + 0.044715 * square))
    act_ref[...] = (0.5 * hidden * (1.0 + bent)).astype(BF16)
    slope = 0.5 * (1.0 + bent) + 0.5 * hidden * (1.0 - bent * bent) * (
        rate * (1.0 + 3.0 * 0.044715 * square)
    )
    low = (grad * slope).astype(BF16)
    dh_ref[...] = low

    @pl.when(pl.program_id(0) == 0)
    def _():
        sum_ref[...] = jnp.zeros_like(sum_ref)

    sum_ref[...] += jnp.sum(low.astype(F32), 0, keepdims=True)


def hidden_part(normed_all, cot_all, weights, bias, tile=512):
    rows, depth = normed_all.shape
    piece = weights.shape[1] // 2
    tile = min(tile, rows)
    wide = pl.BlockSpec((tile, depth), lambda i: (i, 0))
    thin = pl.BlockSpec((tile, piece), lambda i: (i, 0))
    line = pl.BlockSpec((1, piece), lambda i: (0, 0))
    return pl.pallas_call(
        hidden_kernel,
        grid=(rows // tile,),
        in_specs=[wide, wide, pl.BlockSpec(weights.shape, lambda i: (0, 0)), line],
        out_specs=[thin, thin, line],
        out_shape=[
            jax.ShapeDtypeStruct((rows, piece), BF16),
            jax.ShapeDtypeStruct((rows, piece), BF16),
            jax.ShapeDtypeStruct((1, piece), F32),
        ],
        cost_estimate=pl.CostEstimate(
            flops=4 * rows * depth * piece, transcendentals=rows * piece,
            bytes_accessed=4 * rows * depth + 4 * depth * piece + 4 * rows * piece,
        ),
        compiler_params=pltpu.CompilerParams(vmem_limit_bytes=48 << 20),
        name="hidden_part",
    )(normed_all, cot_all, weights, bias)


def gather_kernel(
    n, q_ref, k_ref, v_ref, o_ref, up_ref, down_ref, norm_ref, cot_ref,
    w_ref, unit_ref, right_ref, left_ref, last_ref, n_ref, c_ref, send_sem, recv_sem, local_sem,
):
    z, y, x, c = (lax.axis_index(name) for name in ("z", "y", "x", "c"))
    rows = norm_ref.shape[0]
    half = 3 * rows // 4
    mine = y * 4 + x * 2 + c
    has_right, has_left = z < n - 1, z > 0
    number = {}

    def remote(key, src, dst, axis, target):
        slot = number.setdefault(key, len(number))
        return pltpu.make_async_remote_copy(
            src_ref=src, dst_ref=dst, send_sem=send_sem.at[slot], recv_sem=recv_sem.at[slot],
            device_id={axis: target}, device_id_type=pl.DeviceIdType.MESH,
        )

    def when(condition, action):
        if condition is None:
            action()
        else:
            pl.when(condition)(action)

    started = []

    def start(condition, copy):
        when(condition, copy.start)
        started.append((condition, copy))

    def shard(index, unit):
        return w_ref.at[index * 2 + (y if unit == 0 else 1 - y)]

    width, hidden = q_ref.shape[1] // 2, up_ref.shape[1] // 2
    piece = hidden // 2

    def parts(kind, side):
        if kind == 2:
            sources, size, begin = (q_ref, k_ref, v_ref, o_ref), width, side * width
        else:
            sources, size, begin = (up_ref, down_ref), piece, side * hidden + kind * piece
        span = pl.ds(pl.multiple_of(begin, LANES), size)
        return [(ref.at[:, span], pl.ds(i * size, size)) for i, ref in enumerate(sources)]

    def packed(key, kind, side, block, axis, target):
        return [
            remote(key + (i,), source, block.at[:, columns], axis, target)
            for i, (source, columns) in enumerate(parts(kind, side))
        ]

    def along(step, unit, sign, receiving=False):
        index = z - sign * step if receiving else z - sign * (step - 1)
        if step == 1 and unit == 0:
            return packed((step, unit, sign), 0, y, shard(index, unit), "z", z + sign)
        return [remote((step, unit, sign), shard(index, unit), shard(index, unit), "z", z + sign)]

    def start_all(condition, copies):
        for copy in copies:
            start(condition, copy)

    def wait_all(copies):
        for copy in copies:
            copy.wait_recv()


    full, top, low = pl.ds(0, rows), pl.ds(0, half), pl.ds(half, rows - half)
    arrays = ((n_ref, norm_ref, "n"), (c_ref, cot_ref, "c"))
    at_x, at_y, at_xy = y * 4 + (1 - x) * 2 + c, (1 - y) * 4 + x * 2 + c, (1 - y) * 4 + (1 - x) * 2 + c

    barrier = pltpu.get_barrier_semaphore()
    for axis, target in (("x", 1 - x), ("y", 1 - y), ("c", 1 - c)):
        pl.semaphore_signal(
            barrier, inc=1, device_id={axis: target}, device_id_type=pl.DeviceIdType.MESH
        )
    for condition, target in ((has_right, z + 1), (has_left, z - 1)):
        when(condition, functools.partial(
            pl.semaphore_signal, barrier, inc=1, device_id={"z": target},
            device_id_type=pl.DeviceIdType.MESH,
        ))
    pl.semaphore_wait(barrier, 3 + has_right.astype(jnp.int32) + has_left.astype(jnp.int32))

    for condition, sign in ((has_right, 1), (has_left, -1)):
        start_all(condition, along(1, 0, sign))
    start_all(None, packed(("swap",), 0, 1 - y, shard(z, 0), "y", 1 - y))
    swap_in = packed(("swap",), 0, 1 - y, shard(z, 1), "y", 1 - y)
    for array, source, name in arrays:
        for axis in ("x", "y", "c"):
            start(None, remote((name, axis), source, array.at[mine], axis,
                               {"x": 1 - x, "y": 1 - y, "c": 1 - c}[axis]))
    start_all(None, packed(("unit",), 2, 1 - y, unit_ref.at[y], "y", 1 - y))
    unit_swap_in = packed(("unit",), 2, 1 - y, unit_ref.at[1 - y], "y", 1 - y)
    start_all(None, packed(("late",), 1, 1 - y, last_ref.at[y], "y", 1 - y))
    late_swap = packed(("late",), 1, 1 - y, last_ref.at[1 - y], "y", 1 - y)
    pairs = [(norm_ref, n_ref.at[mine]), (cot_ref, c_ref.at[mine])]
    for kind, block in ((0, shard(z, 0)), (2, unit_ref.at[y]), (1, last_ref.at[y])):
        pairs += [(source, block.at[:, columns]) for source, columns in parts(kind, y)]
    local = [
        pltpu.make_async_copy(source, target, local_sem.at[i])
        for i, (source, target) in enumerate(pairs)
    ]
    for copy in local:
        copy.start()

    def arrive_swap():
        wait_all(swap_in)
        for condition, sign in ((has_right, 1), (has_left, -1)):
            start_all(condition, along(1, 1, sign))

    def arrive_shard(step, unit, sign):
        inside = z - sign * step >= 0 if sign > 0 else z + step < n
        further = has_right if sign > 0 else has_left
        when(inside, functools.partial(wait_all, along(step, unit, sign, True)))
        if step + 1 < n:
            start_all(inside & further, along(step + 1, unit, sign))

    def arrive_rows(array, name, axis):
        index = {"x": at_x, "y": at_y, "c": None}[axis]
        block = array.at[index]
        remote((name, axis), block, block, axis, 0).wait_recv()
        part, on = (low, "y") if axis == "x" else (top, "x")
        piece = array.at[index, part]
        start(None, remote((name, "far", on), piece, piece, on, {"x": 1 - x, "y": 1 - y}[on]))
        start(None, remote((name, "core", axis), block, block, "c", 1 - c))

    def arrive_far(array, name, on):
        part = low if on == "y" else top
        piece = array.at[at_xy, part]
        remote((name, "far", on), piece, piece, on, 0).wait_recv()
        start(None, remote((name, "core", "far", on), piece, piece, "c", 1 - c))

    def arrive_steps(step):
        for unit in (0, 1):
            for sign in (1, -1):
                arrive_shard(step, unit, sign)

    def second_step(half_of, receiving):
        index = y if half_of == 0 else 1 - y
        ways = ((1, has_left if receiving else has_right, right_ref),
                (-1, has_right if receiving else has_left, left_ref))
        for sign, condition, target in ways:
            key = ("second", half_of, sign)
            if half_of == 0:
                copies = packed(key, 2, y, target.at[index], "z", z + sign)
            else:
                copies = [remote(key, unit_ref.at[index], target.at[index], "z", z + sign)]
            if receiving:
                when(condition, functools.partial(wait_all, copies))
            else:
                start_all(condition, copies)

    (norm, _, norm_name), (cot, _, cot_name) = arrays
    arrive_swap()
    arrive_rows(norm, norm_name, "x")
    for sign in (1, -1):
        arrive_shard(1, 0, sign)
    arrive_rows(norm, norm_name, "y")
    for sign in (1, -1):
        arrive_shard(1, 1, sign)
    arrive_rows(cot, cot_name, "x")
    if n > 2:
        arrive_steps(2)
    second_step(0, False)
    arrive_rows(cot, cot_name, "y")
    wait_all(unit_swap_in)
    second_step(1, False)
    for step in range(3, n):
        arrive_steps(step)
    for array, _, name in arrays:
        for on in ("x", "y"):
            arrive_far(array, name, on)
    for array, _, name in arrays:
        for key, index, part in (
            ((name, "c"), y * 4 + x * 2 + 1 - c, full),
            ((name, "core", "x"), y * 4 + (1 - x) * 2 + 1 - c, full),
            ((name, "core", "y"), (1 - y) * 4 + x * 2 + 1 - c, full),
            ((name, "core", "far", "x"), (1 - y) * 4 + (1 - x) * 2 + 1 - c, top),
            ((name, "core", "far", "y"), (1 - y) * 4 + (1 - x) * 2 + 1 - c, low),
        ):
            piece = array.at[index, part]
            remote(key, piece, piece, "c", 0).wait_recv()
    wait_all(late_swap)
    for half_of in (0, 1):
        second_step(half_of, True)
    for copy in local:
        copy.wait()
    for condition, copy in started:
        when(condition, copy.wait_send)


def gather_all(n, query, key, value, output_turned, up, down_turned, normed, cotangent):
    rows, columns = normed.shape
    copies = 4 * (n - 1) + 46
    anywhere = pl.BlockSpec(memory_space=pl.ANY)
    heads = 2 * query.shape[1]
    hidden, depth = up.shape[1] // 2, query.shape[0]
    pair = jax.ShapeDtypeStruct((2, depth, heads), query.dtype)
    weights, unit, right, left, last, normed_all, cot_all = pl.pallas_call(
        functools.partial(gather_kernel, n),
        in_specs=[anywhere] * 8,
        out_specs=[anywhere] * 7,
        out_shape=[
            jax.ShapeDtypeStruct((2 * n, depth, hidden), up.dtype),
            pair, pair, pair,
            jax.ShapeDtypeStruct((2, depth, hidden), up.dtype),
            jax.ShapeDtypeStruct((8, rows, columns), normed.dtype),
            jax.ShapeDtypeStruct((8, rows, columns), cotangent.dtype),
        ],
        scratch_shapes=[
            pltpu.SemaphoreType.DMA((copies,)),
            pltpu.SemaphoreType.DMA((copies,)),
            pltpu.SemaphoreType.DMA((10,)),
        ],
        cost_estimate=pl.CostEstimate(flops=0, transcendentals=0, bytes_accessed=200 << 20),
        compiler_params=pltpu.CompilerParams(collective_id=0, has_side_effects=True),
        name="gather_rows",
    )(query, key, value, output_turned, up, down_turned, normed, cotangent)
    flat = lambda array: array.reshape(-1, array.shape[-1])
    return tuple(map(flat, (weights, unit, right, left, last, normed_all, cot_all)))


def chain_step(step, n, right, left):
    return (
        lax.ppermute(right, "z", [(i, i + 1) for i in range(step - 1, n - 1)]),
        lax.ppermute(left, "z", [(i, i - 1) for i in range(1, n - step + 1)]),
    )


def assemble(unit, right, left, n, z):
    rows, columns = unit.shape
    whole = jnp.zeros((n * rows, columns), unit.dtype)
    for k in range(n):
        piece = unit if k == 0 else jnp.where(z >= k, right[k], left[n - k])
        row = lax.rem(z - k + n, n) * rows
        whole = lax.dynamic_update_slice(whole, piece, (row, jnp.int32(0)))
    return whole


def scatter_pieces(k, grads, n, z, received):
    rows = grads.shape[0] // n

    def piece(index, got):
        own = lax.dynamic_slice_in_dim(grads, jnp.clip(index, 0, n - 1) * rows, rows, 0)
        return own if got is None else add_low(own, got)

    return piece(z - k, received[0]), piece(z + k, received[1])


def scatter_step(k, grads, n, z, received):
    to_left, to_right = scatter_pieces(k, grads, n, z, received)
    return (
        lax.ppermute(to_left, "z", [(r, r - 1) for r in range(k, n)]),
        lax.ppermute(to_right, "z", [(r, r + 1) for r in range(0, n - k)]),
    )


def scatter_end(grads, n, z, received):
    rows = grads.shape[0] // n
    own = lax.dynamic_slice_in_dim(grads, z * rows, rows, 0).astype(F32)
    return own + received[0].astype(F32) + received[1].astype(F32)


def tail_kernel(
    n, g_any, hw_ref, fw_ref, lw_ref, dq_ref, d0_ref, d1_ref, at_ref, a0_ref, a1_ref,
    left_ref, right_ref, own_ref, std_any, vec_ref,
    keep_ref, take_ref, heads_keep_ref, heads_take_ref, out_ref, mixed_ref, sums_ref,
    g_ref, std_ref, hw_s, fw_s, lw_s, rows_s, stage, zrecv, give, heads_recv, heads_own, heads_give, both, xtop_2, ylow_2, ytop_2, xlow_2,
    top_2, low_2, vstage, vrecv, send_sem, recv_sem, load_sem, rows_sem,
):
    z, y, x, c = (lax.axis_index(name) for name in ("z", "y", "x", "c"))
    rows, columns = out_ref.shape
    wide, wide_heads = give.shape[0], heads_give.shape[0]
    half = rows // 2
    rest = rows - half
    number, started = {}, []

    def remote(key, src, dst, axis, target):
        slot = number.setdefault(key, len(number))
        return pltpu.make_async_remote_copy(
            src_ref=src, dst_ref=dst, send_sem=send_sem.at[slot], recv_sem=recv_sem.at[slot],
            device_id={axis: target}, device_id_type=pl.DeviceIdType.MESH,
        )

    def when(condition, action):
        if condition is None:
            action()
        else:
            pl.when(condition)(action)

    def start(condition, copy):
        when(condition, copy.start)
        started.append((condition, copy))

    def each(count, size, body):
        def step(i, carry):
            body(pl.ds(pl.multiple_of(i * size, size), size))
            return carry
        lax.fori_loop(0, count // size, step, 0)

    barrier = pltpu.get_barrier_semaphore()
    greet = [(None, "x", 1 - x), (None, "y", 1 - y), (None, "c", 1 - c)]
    greet += [(z < n - 1, "z", z + 1), (z > 0, "z", z - 1)]
    for step in (2 ** i for i in range(1, n.bit_length() - 1)):
        greet.append((None, "z", jnp.bitwise_xor(z, step)))
    for condition, axis, target in greet:
        when(condition, functools.partial(
            pl.semaphore_signal, barrier, inc=1, device_id={axis: target},
            device_id_type=pl.DeviceIdType.MESH))

    loads = [
        pltpu.make_async_copy(source, target, load_sem.at[i])
        for i, (source, target) in enumerate(
            ((hw_ref, hw_s), (fw_ref, fw_s), (lw_ref, lw_s), (g_any, g_ref), (std_any, std_ref),
             (own_ref, heads_own)))
    ]
    for load in loads:
        load.start()

    firsts, lasts = fw_ref.shape[1] // 2, lw_ref.shape[1] // 2
    heads = dq_ref.shape[1]
    sums = (
        ((dq_ref, heads, hw_s, 0), (d0_ref, firsts, fw_s, 0), (d1_ref, lasts, lw_s, 0)),
        ((at_ref, heads // 3, hw_s, heads), (a0_ref, firsts, fw_s, firsts),
         (a1_ref, lasts, lw_s, lasts)),
    )
    sides = (1 - y, y)
    jobs = [(a, own, j) for a in (0, 1) for own in (False, True) for j in sides]

    def row_loads(number_of):
        a, own, j = jobs[number_of]
        slot, core, copies, at = number_of % 2, c if own else 1 - c, [], 0
        for p, (left, width, _, _) in enumerate(sums[a]):
            for i in (0, 1):
                block = j * 4 + i * 2 + core
                source = left.at[pl.ds(pl.multiple_of(block * rows, rows), rows)]
                target = rows_s.at[slot, pl.ds(i * rows, rows), pl.ds(at, width)]
                copies.append(pltpu.make_async_copy(source, target, rows_sem.at[slot, p * 2 + i]))
            at += width
        return copies

    def job(number_of):
        a, own, j = jobs[number_of]
        slot = number_of % 2
        if number_of + 1 < len(jobs):
            for copy in row_loads(number_of + 1):
                copy.start()
        for copy in row_loads(number_of):
            copy.wait()
        if own:
            for i in (0, 1):
                core_copy(a, number_of % 2, i).wait_recv()
        elif a == 1:
            for i in (0, 1):
                core_copy(0, number_of % 2, i).wait_send()
        size = min(512, columns)

        def tile(t, carry):
            span = pl.ds(pl.multiple_of(t * size, size), size)
            acc, at = None, 0
            for left, width, weights, column in sums[a]:
                part = dot(
                    rows_s[slot, :, at : at + width], weights[span, column : column + width], NT)
                acc = part if acc is None else acc + part
                at += width
            for i in (0, 1):
                piece = acc[i * rows : (i + 1) * rows]
                if own:
                    both[a, j * 2 + i, :, span] = (
                        piece + both[a, j * 2 + i, :, span].astype(F32)).astype(BF16)
                else:
                    stage[j * 2 + i, :, span] = piece.astype(BF16)
            return carry

        lax.fori_loop(0, columns // size, tile, 0)
        if own and a == 0:
            start(None, first_copy(a, "xtop", number_of % 2))
            if number_of % 2 == 0:
                for i in (0, 1):
                    start(None, first_copy(a, "ylow", i))
        if not own:
            for i in (0, 1):
                copy = core_copy(a, number_of % 2, i)
                copy.start()
                if a == 1:
                    started.append((None, copy))

    def core_copy(a, u, i):
        place = sides[u] * 2 + i
        return remote(("core", a, u, i), stage.at[place], both.at[a, place], "c", 1 - c)

    for copy in row_loads(0):
        copy.start()
    always = sum(condition is None for condition, _, _ in greet)
    pl.semaphore_wait(barrier, always + sum(
        condition.astype(jnp.int32) for condition, _, _ in greet if condition is not None))

    def first_copy(a, name, j):
        if name == "xtop":
            source = both.at[a, sides[j] * 2 + 1 - x, pl.ds(0, half)]
            return remote((name, a, j), source, xtop_2.at[a, j], "x", 1 - x)
        source = both.at[a, (1 - y) * 2 + j, pl.ds(half, rest)]
        return remote((name, a, j), source, ylow_2.at[a, j], "y", 1 - y)

    def second_copy(a, name):
        if name == "ytop":
            return remote((name, a), top_2.at[a], ytop_2.at[a], "y", 1 - y)
        return remote((name, a), low_2.at[a], xlow_2.at[a], "x", 1 - x)

    def first_send(a):
        for j in (0, 1):
            start(None, first_copy(a, "xtop", j))
            start(None, first_copy(a, "ylow", j))

    def first_arrive(a):
        for j in (0, 1):
            first_copy(a, "xtop", j).wait_recv()
            first_copy(a, "ylow", j).wait_recv()

        def upper(part):
            top_2[a, part, :] = (
                both[a, (1 - y) * 2 + x, part, :].astype(F32)
                + xtop_2[a, 0, part, :].astype(F32)
            ).astype(BF16)

        def lower(part):
            low_part = pl.ds(part.start + half, part.size)
            low_2[a, part, :] = (
                both[a, y * 2 + 1 - x, low_part, :].astype(F32)
                + ylow_2[a, 1 - x, part, :].astype(F32)
            ).astype(BF16)

        each(half, 32, upper)
        each(rest, 32, lower)
        start(None, second_copy(a, "ytop"))
        start(None, second_copy(a, "xlow"))

    def second_arrive(a):
        second_copy(a, "ytop").wait_recv()
        second_copy(a, "xlow").wait_recv()
        target = (out_ref, mixed_ref)[a]

        def finish(first, part, placed, last):
            value = (
                both[a, y * 2 + x, placed, :].astype(F32) + first[part, :].astype(F32)
                + last[part, :].astype(F32)
            )
            target[placed, :] = value
            if a == 0:
                scaled = value * std_ref[placed, :]
                vstage[0, 0:1, :] += jnp.sum(scaled, 0, keepdims=True)
                vstage[0, 1:2, :] += jnp.sum(value, 0, keepdims=True)

        def upper(part):
            finish(xtop_2.at[a, 1], part, part, ytop_2.at[a])

        def lower(part):
            finish(ylow_2.at[a, x], part, pl.ds(part.start + half, part.size), xlow_2.at[a])

        each(half, 32, upper)
        each(rest, 32, lower)

    def block_of(direction, k, u):
        index = (z - k if direction == 0 else z + k) * 2 + sides[u]
        return pl.ds(pl.multiple_of(index * rows, rows), rows)

    def z_copy(direction, k, u, src):
        target = z - 1 if direction == 0 else z + 1
        return remote((direction, k, u), src, zrecv.at[direction, k - 1, u], "z", target)

    def z_first(direction):
        edge = z == n - 1 if direction == 0 else z == 0
        for k in range(n - 1, 0, -1):
            for u in (0, 1):
                start(edge, z_copy(direction, k, u, g_any.at[:, block_of(direction, k, u)]))

    def z_step(k, u):
        for direction in (0, 1):
            if direction == 0:
                inside = (z >= k) & (z < n - 1)
            else:
                inside = (n - 1 - z >= k) & (z > 0)
            held = zrecv.at[direction, k, u]

            def add():
                z_copy(direction, k + 1, u, held).wait_recv()
                block = block_of(direction, k, u)

                def body(part):
                    held[part, :] = (
                        g_ref[part, block].astype(F32) + held[part, :].astype(F32)
                    ).astype(BF16)

                each(wide, 256, body)

            when(inside, add)
            start(inside, z_copy(direction, k, u, held))

    def z_last(u, target):
        block = block_of(0, 0, u)

        def first(part):
            target[part, :] = g_ref[part, block].astype(F32)

        each(wide, 256, first)
        for direction in (0, 1):
            held = zrecv.at[direction, 0, u]

            def add():
                z_copy(direction, 1, u, held).wait_recv()

                def body(part):
                    target[part, :] += held[part, :].astype(F32)

                each(wide, 256, body)

            when(z < n - 1 if direction == 0 else z > 0, add)

    def heads_copy(direction, u):
        span = pl.ds(pl.multiple_of(sides[u] * rows, rows), rows)
        source = (left_ref, right_ref)[direction].at[:, span]
        return remote(
            ("heads", direction, u), source, heads_recv.at[direction, :, span], "z",
            z - 1 if direction == 0 else z + 1)

    def heads_send():
        for u in (0, 1):
            start(z > 0, heads_copy(0, u))
            start(z < n - 1, heads_copy(1, u))

    def heads_last(u, target):
        span = pl.ds(pl.multiple_of(sides[u] * rows, rows), rows)

        def first(part):
            target[part, :] = heads_own[part, span].astype(F32)

        each(wide_heads, 256, first)
        for direction in (0, 1):
            def add():
                heads_copy(direction, u).wait_recv()

                def body(part):
                    target[part, :] += heads_recv[direction, part, span].astype(F32)

                each(wide_heads, 256, body)

            when(z < n - 1 if direction == 0 else z > 0, add)

    steps = [(k, u) for k in range(n - 2, 0, -1) for u in (0, 1)]

    def z_next():
        if steps:
            z_step(*steps.pop(0))

    for direction in (0, 1):
        z_first(direction)
    vstage[0] = vec_ref[...]
    for load in loads[:3]:
        load.wait()
    job(0)
    job(1)
    for load in loads[3:]:
        load.wait()
    z_next()
    job(2)
    job(3)
    heads_send()
    z_next()
    job(4)
    job(5)
    z_next()
    job(6)
    job(7)
    first_arrive(0)
    first_send(1)
    while steps:
        z_next()
    second_arrive(0)

    turns = [("z", jnp.bitwise_xor(z, 2 ** i)) for i in range(n.bit_length() - 1)]
    turns += [("y", 1 - y), ("x", 1 - x), ("c", 1 - c)]
    line = lax.broadcasted_iota(jnp.int32, vec_ref.shape, 0)

    def exchange(i):
        axis, target = turns[i]
        return remote(("vec", i), vstage.at[i], vrecv.at[i], axis, target)

    def turn(i):
        exchange(i).wait_recv()
        axis, _ = turns[i]
        old, new = vstage[i], vrecv[i]
        result = sums_ref if i == len(turns) - 1 else vstage.at[i + 1]
        result[...] = old + jnp.where((line < 3) | (axis == "z"), new, 0.0)
        if axis == "y":
            result[4:5, :] = new[3:4, :]
        if i + 1 < len(turns):
            start(None, exchange(i + 1))

    start(None, exchange(0))

    def swapped(key, source, target, length, received):
        def lower_precision(part):
            target[part, :] = source[part, :].astype(BF16)

        each(length, 256, lower_precision)
        copy = remote(key, target, received, "y", 1 - y)
        start(None, copy)
        return copy

    first_arrive(1)
    z_last(0, keep_ref)
    swap = swapped("swap", keep_ref, give, wide, take_ref)
    turn(0)
    turn(1)
    heads_last(0, heads_keep_ref)
    heads_swap = swapped("heads swap", heads_keep_ref, heads_give, wide_heads, heads_take_ref)
    turn(2)
    z_last(1, keep_ref)
    turn(3)
    heads_last(1, heads_keep_ref)
    for i in range(4, len(turns)):
        turn(i)
    second_arrive(1)
    swap.wait_recv()
    heads_swap.wait_recv()
    for condition, copy in started:
        when(condition, copy.wait_send)


def tail(n, grads_turned, weights, lefts, lefts_out, heads_turned, standard, vector):
    rows, columns = standard.shape
    wide, wide_heads = grads_turned.shape[0], heads_turned[0].shape[0]
    half = rows // 2
    inside = pl.BlockSpec(memory_space=pltpu.VMEM)
    anywhere = pl.BlockSpec(memory_space=pl.ANY)
    copies = 4 * (n - 1) + 46
    low = lambda *shape: pltpu.VMEM(shape, BF16)
    small = vector.shape
    depth = sum(left.shape[1] for left in lefts)
    return pl.pallas_call(
        functools.partial(tail_kernel, n),
        in_specs=[anywhere] * 14 + [inside],
        out_specs=[inside] * 7,
        out_shape=[
            jax.ShapeDtypeStruct((wide, rows), F32),
            jax.ShapeDtypeStruct((wide, rows), BF16),
            jax.ShapeDtypeStruct((wide_heads, rows), F32),
            jax.ShapeDtypeStruct((wide_heads, rows), BF16),
            jax.ShapeDtypeStruct((rows, columns), F32),
            jax.ShapeDtypeStruct((rows, columns), F32),
            jax.ShapeDtypeStruct(small, F32),
        ],
        scratch_shapes=[low(*grads_turned.shape), pltpu.VMEM(standard.shape, F32)] + [
            low(*array.shape) for array in weights
        ] + [
            low(2, 2 * rows, depth), low(4, rows, columns),
            low(2, n - 1, 2, wide, rows), low(wide, rows),
            low(2, wide_heads, 2 * rows), low(wide_heads, 2 * rows), low(wide_heads, rows),
            low(2, 4, rows, columns),
            low(2, 2, half, columns), low(2, 2, rows - half, columns),
            low(2, half, columns), low(2, rows - half, columns),
            low(2, half, columns), low(2, rows - half, columns),
            pltpu.VMEM((8,) + small, F32), pltpu.VMEM((8,) + small, F32),
            pltpu.SemaphoreType.DMA((copies,)),
            pltpu.SemaphoreType.DMA((copies,)),
            pltpu.SemaphoreType.DMA((6,)),
            pltpu.SemaphoreType.DMA((2, 6)),
        ],
        cost_estimate=pl.CostEstimate(flops=0, transcendentals=0, bytes_accessed=200 << 20),
        compiler_params=pltpu.CompilerParams(
            collective_id=1, has_side_effects=True, vmem_limit_bytes=63 << 20
        ),
        name="scatter_rest",
    )(grads_turned, *weights, *lefts, *lefts_out, *heads_turned, standard, vector)


def sum_small(array, axes):
    for axis in axes:
        size = lax.axis_size(axis)
        if size & (size - 1):
            array = lax.psum(array, axis)
            continue
        step = 1
        while step < size:
            array = array + lax.ppermute(array, axis, [(i, i ^ step) for i in range(size)])
            step *= 2
    return array


def pick(array, index, axis):
    return lax.dynamic_index_in_dim(array, index, axis, keepdims=False)


def add_low(left, right):
    return (left.astype(F32) + right.astype(F32)).astype(BF16)


def plane_scatter(partial, y, x, c):
    rows, columns = partial.shape[0] // 8, partial.shape[1]
    half = rows // 2
    parts = partial.reshape(2, 2, 2, rows, columns)
    acc = add_low(pick(parts, c, 2), lax.ppermute(pick(parts, 1 - c, 2), "c", SWAP))
    top, low = acc[:, :, :half], acc[:, :, half:]
    top = add_low(pick(top, x, 1), lax.ppermute(pick(top, 1 - x, 1), "x", SWAP))
    low = add_low(pick(low, y, 0), lax.ppermute(pick(low, 1 - y, 0), "y", SWAP))
    top = pick(top, y, 0).astype(F32) + lax.ppermute(pick(top, 1 - y, 0), "y", SWAP).astype(F32)
    low = pick(low, x, 0).astype(F32) + lax.ppermute(pick(low, 1 - x, 0), "x", SWAP).astype(F32)
    return jnp.concatenate([top, low], 0)


def in_order(y, own, other, axis):
    return jnp.where(
        y == 0, jnp.concatenate([own, other], axis), jnp.concatenate([other, own], axis)
    )


def on_device(
    n,
    tokens, norm_gain, norm_bias,
    query_weight, query_bias, key_weight, key_bias, value_weight, value_bias,
    output_weight, output_bias, up_weight, up_bias, down_weight, down_bias,
    doc_split, cotangent,
):
    z, y, x, c = (lax.axis_index(name) for name in ("z", "y", "x", "c"))
    shard_rows = query_weight.shape[0]
    width = query_weight.shape[1] // 2
    hidden_width = up_weight.shape[1] // 2
    chunks = 2
    piece = hidden_width // chunks

    def row(array, start, size):
        return lax.dynamic_slice_in_dim(array, start, size, 0)

    gain_wide = norm_gain.astype(F32)
    tokens_wide = tokens.astype(F32)
    row_mean = jnp.mean(tokens_wide, -1, keepdims=True)
    centred = tokens_wide - row_mean
    inv_scale = lax.rsqrt(jnp.mean(centred * centred, -1, keepdims=True) + EPS)
    standard = centred * inv_scale
    normed = (standard * gain_wide + norm_bias.astype(F32)).astype(BF16)
    phase = lax.optimization_barrier
    other_split = lax.ppermute(doc_split, "y", SWAP)
    splits = in_order(y, doc_split, other_split, 0)
    seq_len = 4 * normed.shape[0]
    cosine, sine = turn_tables(splits, seq_len)

    right, left = [None] * n, [None] * n
    first_weights, heads_unit, right[1], left[1], last_unit, normed_all, cot_all = gather_all(
        n, query_weight, key_weight, value_weight, output_weight.T, up_weight, down_weight.T,
        normed, cotangent,
    )
    first_weights, heads_unit, last_unit, normed_all, cot_all, right[1], left[1], cosine, sine = phase(
        (first_weights, heads_unit, last_unit, normed_all, cot_all, right[1], left[1], cosine, sine)
    )

    def hidden_local(weights, chunk):
        bias = row(up_bias, y * hidden_width + chunk * piece, piece).astype(F32)[None]
        return hidden_part(normed_all, cot_all, weights, bias)

    def weight_grads(grad_columns, columns):
        return jnp.concatenate(
            [dot(normed_all, grad_columns, TN).astype(BF16), dot(cot_all, columns, TN).astype(BF16)], 1
        )

    def gather_step(step, source):
        return chain_step(step, n, right[step - 1], left[step - 1]) if step > 1 else chain_step(
            1, n, source, source)

    activated_0, grad_hidden_0, hidden_sum_0 = hidden_local(first_weights, 0)
    right[2], left[2] = gather_step(2, None)
    activated_0, grad_hidden_0, normed_all, cot_all, right[2], left[2] = phase(
        (activated_0, grad_hidden_0, normed_all, cot_all, right[2], left[2])
    )
    grads_first = weight_grads(grad_hidden_0, activated_0)
    for step in range(3, n):
        right[step], left[step] = gather_step(step, None)
    grads_first, activated_0, last_unit, normed_all, cot_all, right[3:], left[3:] = phase(
        (grads_first, activated_0, last_unit, normed_all, cot_all, right[3:], left[3:])
    )
    head_weights = assemble(heads_unit, right, left, n, z)
    qkv_weight, output_turned = head_weights[:, : 3 * width], head_weights[:, 3 * width :]

    qkv_bias = jnp.concatenate(
        [row(b, y * width, width) for b in (query_bias, key_bias, value_bias)]
    ).astype(F32)
    qkv = dot(normed_all, qkv_weight) + qkv_bias
    grad_attended = dot(cot_all, output_turned).astype(BF16)
    right[1], left[1] = gather_step(1, last_unit)
    qkv, grad_attended, normed_all, cot_all, right[1], left[1] = phase(
        (qkv, grad_attended, normed_all, cot_all, right[1], left[1])
    )
    found = attention(0, splits, qkv, grad_attended, cosine, sine, ())
    right[2], left[2] = gather_step(2, None)
    first_in = scatter_step(n - 1, grads_first, n, z, (None, None))
    found, qkv, grad_attended, normed_all, cot_all, right[2], left[2], first_in, grads_first = phase(
        (found, qkv, grad_attended, normed_all, cot_all, right[2], left[2], first_in, grads_first)
    )
    for index in range(1, splits.shape[0]):
        found = attention(index, splits, qkv, grad_attended, cosine, sine, found)
    for step in range(3, n):
        right[step], left[step] = gather_step(step, None)
    for k in range(n - 2, n - 3, -1):
        first_in = scatter_step(k, grads_first, n, z, first_in)
    found, normed_all, cot_all, right[3:], left[3:], first_in, grads_first = phase(
        (found, normed_all, cot_all, right[3:], left[3:], first_in, grads_first)
    )
    attended, grad_qkv = found
    grads_heads = weight_grads(grad_qkv, attended)
    for k in range(n - 3, 0, -1):
        first_in = scatter_step(k, grads_first, n, z, first_in)
    grads_heads, attended, grad_qkv, normed_all, cot_all, last_unit, first_in, grads_first = phase(
        (grads_heads, attended, grad_qkv, normed_all, cot_all, last_unit, first_in, grads_first)
    )
    first_sum = scatter_end(grads_first, n, z, first_in)

    last_weights = assemble(last_unit, right, left, n, z)
    activated_1, grad_hidden_1, hidden_sum_1 = hidden_local(last_weights, 1)
    heads_in = scatter_step(n - 1, grads_heads, n, z, (None, None))
    (last_weights, activated_1, grad_hidden_1, attended, grad_qkv, heads_in, grads_heads,
     normed_all, cot_all) = phase(
        (last_weights, activated_1, grad_hidden_1, attended, grad_qkv, heads_in, grads_heads,
         normed_all, cot_all)
    )
    for k in range(n - 2, max(n - 3, 1), -1):
        heads_in = scatter_step(k, grads_heads, n, z, heads_in)
    grads_last = weight_grads(grad_hidden_1, activated_1)
    qkv_sum = jnp.sum(grad_qkv, 0, dtype=F32)[None]
    bias_row = jnp.concatenate([qkv_sum, hidden_sum_0, hidden_sum_1], 1)
    cot_wide = cotangent.astype(F32)
    cot_sum = jnp.sum(cot_wide, 0)[None]
    grads_last, heads_in, grads_heads, bias_row, cot_sum = phase(
        (grads_last, heads_in, grads_heads, bias_row, cot_sum)
    )
    def halves(total):
        keep = row(total, y * shard_rows, shard_rows)
        give = row(total, (1 - y) * shard_rows, shard_rows).astype(BF16)
        return keep, lax.ppermute(give, "y", SWAP).astype(F32)

    first_keep, first_take = halves(first_sum)

    if n == 4 and bias_row.shape[1] <= cot_sum.shape[1]:
        spread = cot_sum.shape[1]
        vector = jnp.concatenate([
            jnp.zeros((2, spread), F32), cot_sum,
            jnp.pad(bias_row, ((0, 0), (0, spread - bias_row.shape[1]))),
            jnp.zeros((4, spread), F32),
        ])
        left_piece, right_piece = scatter_pieces(1, grads_heads, n, z, heads_in)
        own_piece = row(grads_heads, z * 2 * shard_rows, 2 * shard_rows)
        last_keep, last_take, heads_keep, heads_take, grad_normed, mixed, sums = tail(
            n, grads_last.T, (head_weights, first_weights, last_weights),
            (grad_qkv, grad_hidden_0, grad_hidden_1), (attended, activated_0, activated_1),
            (left_piece.T, right_piece.T, own_piece.T), standard, vector,
        )
        last_keep, last_take = last_keep.T, last_take.astype(F32).T
        heads_keep, heads_take = heads_keep.T, heads_take.astype(F32).T
        norm_sums = sums[:3]
        bias_rows = in_order(y, sums[3:4], sums[4:5], 0)[:, : bias_row.shape[1]]
    else:
        for k in range(n - 3, 0, -1):
            heads_in = scatter_step(k, grads_heads, n, z, heads_in)
        heads_keep, heads_take = halves(scatter_end(grads_heads, n, z, heads_in))
        partial_out = sum_dots(
            (attended, activated_0, activated_1),
            ((head_weights, width, 3), (first_weights, piece, 1), (last_weights, piece, 1)),
        )
        grad_normed_part = sum_dots(
            (grad_qkv, grad_hidden_0, grad_hidden_1),
            ((head_weights, 3 * width, 0), (first_weights, piece, 0), (last_weights, piece, 0)),
        )
        last_in = (None, None)
        for k in range(n - 1, 0, -1):
            last_in = scatter_step(k, grads_last, n, z, last_in)
        last_keep, last_take = halves(scatter_end(grads_last, n, z, last_in))
        grad_normed = plane_scatter(grad_normed_part, y, x, c)
        mixed = plane_scatter(partial_out, y, x, c)
        norm_sums = sum_small(
            jnp.concatenate([
                jnp.sum(grad_normed * standard, 0)[None], jnp.sum(grad_normed, 0)[None], cot_sum
            ]),
            ("c", "x", "y", "z"),
        )
        bias_row = sum_small(bias_row, ("z",))
        bias_rows = in_order(y, bias_row, lax.ppermute(bias_row, "y", SWAP), 0)
    grad_norm_gain, grad_norm_bias, grad_out_bias = norm_sums

    out_bias = output_bias.astype(F32) + down_bias.astype(F32)
    out = (tokens_wide + mixed + out_bias).astype(BF16)

    def joined(start, size):
        return in_order(
            y, heads_keep[:, start : start + size], heads_take[:, start : start + size], 1
        )

    grad_query_weight, grad_key_weight, grad_value_weight, grad_output_turned = (
        joined(part * width, width) for part in range(4)
    )
    hidden_halves = [(first_keep, first_take), (last_keep, last_take)]

    def side(which, start):
        return jnp.concatenate([pair[which][:, start : start + piece] for pair in hidden_halves], 1)

    grad_up_weight = in_order(y, side(0, 0), side(1, 0), 1)
    grad_down_turned = in_order(y, side(0, piece), side(1, piece), 1)

    grad_query_bias, grad_key_bias, grad_value_bias = (
        bias_rows[:, part * width : (part + 1) * width].reshape(-1) for part in range(3)
    )
    grad_up_bias = bias_rows[:, 3 * width :].reshape(-1)

    grad_scaled = grad_normed * gain_wide
    grad_tokens = cot_wide + inv_scale * (
        grad_scaled
        - jnp.mean(grad_scaled, -1, keepdims=True)
        - standard * jnp.mean(grad_scaled * standard, -1, keepdims=True)
    )
    return (
        out, grad_tokens, grad_norm_gain, grad_norm_bias,
        grad_query_weight, grad_query_bias, grad_key_weight, grad_key_bias,
        grad_value_weight, grad_value_bias, grad_output_turned.T, grad_out_bias,
        grad_up_weight, grad_up_bias, grad_down_turned.T, grad_out_bias,
    )


def solution(mesh):
    n = mesh.shape["dp"] // 2
    grid = Mesh(mesh.devices.reshape(n, 2, mesh.shape["tensor"] // 2, 2), ("z", "y", "x", "c"))
    dp, tensor = ("z", "y"), ("x", "c")
    rows = P(dp + tensor, None)
    whole, split = P(), P(tensor)
    wide, tall = P(dp, tensor), P(tensor, dp)
    in_specs = (
        rows, whole, whole, wide, split, wide, split, wide, split,
        tall, whole, wide, split, tall, whole, P(dp), rows,
    )
    out_specs = (
        rows, rows, whole, whole, wide, split, wide, split, wide, split,
        tall, whole, wide, split, tall, whole,
    )
    return jax.shard_map(
        functools.partial(on_device, n),
        mesh=grid, in_specs=in_specs, out_specs=out_specs, check_vma=False,
    )
```

```python
import functools

import jax
import jax.numpy as jnp
from jax import lax
from jax.experimental import pallas as pl
from jax.experimental.pallas import tpu as pltpu
from jax.sharding import Mesh, PartitionSpec as P

HEAD_DIM = 64
ROT = 32
BLOCK = 256
EPS = 1e-05
LANES = 128
F32 = jnp.float32
BF16 = jnp.bfloat16


SWAP = [(0, 1), (1, 0)]
NT = (((1,), (1,)), ((), ()))
TN = (((0,), (0,)), ((), ()))
NN = (((1,), (0,)), ((), ()))


def dot(left, right, dims=NN):
    return lax.dot_general(left, right, dims, preferred_element_type=F32)


def spin(value, cosine, sine):
    lane = lax.broadcasted_iota(jnp.int32, value.shape, 1) % HEAD_DIM
    half = ROT // 2
    ahead = pltpu.roll(value, LANES - half, 1)
    behind = pltpu.roll(value, half, 1)
    return value * cosine + jnp.where(lane < half, ahead, behind) * sine


def attention_kernel(
    index, earlier, split_ref, qkv_ref, grad_ref, cos_ref, sin_ref, *refs
):
    (att_ref, dqkv_ref, *scratch) = refs[earlier:]
    attention_body(index, split_ref, qkv_ref, grad_ref, cos_ref, sin_ref, att_ref, dqkv_ref, *scratch)


def attention_body(
    index, split_ref, qkv_ref, grad_ref, cos_ref, sin_ref, att_ref, dqkv_ref,
    q_s, k_s, v_s, g_s, b_s, dq_s, dk_s, dv_s, cos_s, sin_s,
):
    seq_len, width = grad_ref.shape
    first = split_ref[index] // BLOCK
    scale = HEAD_DIM ** (-0.5)
    per = LANES // HEAD_DIM
    rest = jnp.zeros((HEAD_DIM - ROT, seq_len), F32)
    cos_part, sin_part = cos_ref[...], sin_ref[...]
    cos_s[...] = jnp.concatenate([cos_part, cos_part, rest + 1.0] * per, 0).T
    sin_s[...] = jnp.concatenate([-sin_part, sin_part, rest] * per, 0).T

    def one_pair(pair, carry):
        def cols(part):
            return pl.ds(pl.multiple_of(part * width + pair * LANES, LANES), LANES)

        cosine, sine = cos_s[...], sin_s[...]
        head_of = lax.broadcasted_iota(jnp.int32, (seq_len, LANES), 1) // HEAD_DIM
        query = spin(qkv_ref[:, cols(0)], cosine, sine).astype(BF16)
        key = spin(qkv_ref[:, cols(1)], cosine, sine).astype(BF16)
        value = qkv_ref[:, cols(2)].astype(BF16)
        grad = grad_ref[:, cols(0)]
        query = (query.astype(F32) * scale).astype(BF16)
        turned_back = (key.astype(F32) * scale).astype(BF16)
        for head in range(per):
            here = head_of == head
            q_s[head] = jnp.where(here, query, 0).astype(BF16)
            k_s[head] = jnp.where(here, key, 0).astype(BF16)
            b_s[head] = jnp.where(here, turned_back, 0).astype(BF16)
            v_s[head] = jnp.where(here, value, 0).astype(BF16)
            g_s[head] = jnp.where(here, grad, 0).astype(BF16)
        dk_s[...] = jnp.zeros_like(dk_s)
        dv_s[...] = jnp.zeros_like(dv_s)

        def one_block(block, inner):
            begin = jnp.where(block >= first, first, 0)
            rows = pl.ds(pl.multiple_of(block * BLOCK, BLOCK), BLOCK)

            def work(count):
                span = pl.ds(pl.multiple_of(begin * BLOCK, BLOCK), count * BLOCK)
                held = None
                for head in range(per):
                    q, g = q_s[head, rows, :], g_s[head, rows, :]
                    scores = dot(k_s[head, span, :], q, NT)
                    top = jnp.max(scores, 0, keepdims=True)
                    power = jnp.exp(scores - top)
                    prob = power * (1.0 / jnp.sum(power, 0, keepdims=True))
                    low = prob.astype(BF16)
                    dprob = dot(v_s[head, span, :], g, NT)
                    mean = jnp.sum(prob * dprob, 0, keepdims=True)
                    dscore = (prob * (dprob - mean)).astype(BF16)
                    parts = (
                        dot(dscore, q), dot(low, g),
                        dot(dscore, b_s[head, span, :], TN), dot(low, v_s[head, span, :], TN),
                    )
                    held = parts if held is None else [a + b for a, b in zip(held, parts)]
                dk, dv, dq, found = held
                dq_s[rows, :] = dq
                att_ref[rows, cols(0)] = found.astype(BF16)
                dk_s[span, :] += dk
                dv_s[span, :] += dv

            for count in range(1, seq_len // BLOCK):
                pl.when(block - begin == count - 1)(functools.partial(work, count))
            return inner

        lax.fori_loop(0, seq_len // BLOCK, one_block, 0)
        dqkv_ref[:, cols(0)] = spin(dq_s[...], cosine, -sine).astype(BF16)
        dqkv_ref[:, cols(1)] = spin(dk_s[...], cosine, -sine).astype(BF16)
        dqkv_ref[:, cols(2)] = dv_s[...].astype(BF16)
        return carry

    lax.fori_loop(0, width // LANES, one_pair, 0)


def attention(index, splits, qkv, grad, cosine, sine, earlier):
    count = splits.shape[0]
    rows, width = grad.shape
    seq_len = rows // count
    per = LANES // HEAD_DIM

    def spec(columns):
        return pl.BlockSpec((seq_len, columns), lambda i, split: (index, 0))

    table = pl.BlockSpec((ROT // 2, seq_len), lambda i, split: (0, index))
    masked = pltpu.VMEM((per, seq_len, LANES), BF16)
    return pl.pallas_call(
        functools.partial(attention_kernel, index, len(earlier)),
        grid_spec=pltpu.PrefetchScalarGridSpec(
            num_scalar_prefetch=1,
            grid=(1,),
            in_specs=[spec(3 * width), spec(width), table, table]
            + [pl.BlockSpec(memory_space=pl.ANY)] * len(earlier),
            out_specs=[spec(width), spec(3 * width)],
            scratch_shapes=[
                masked, masked, masked, masked, masked,
                pltpu.VMEM((seq_len, LANES), F32),
                pltpu.VMEM((seq_len, LANES), F32),
                pltpu.VMEM((seq_len, LANES), F32),
                pltpu.VMEM((seq_len, LANES), F32),
                pltpu.VMEM((seq_len, LANES), F32),
            ],
        ),
        out_shape=[
            jax.ShapeDtypeStruct((rows, width), BF16),
            jax.ShapeDtypeStruct((rows, 3 * width), BF16),
        ],
        cost_estimate=pl.CostEstimate(
            flops=40 * seq_len * seq_len * width // 4,
            transcendentals=seq_len * seq_len * width // HEAD_DIM // 2,
            bytes_accessed=seq_len * width * 24,
        ),
        input_output_aliases={5 + i: i for i in range(len(earlier))},
        compiler_params=pltpu.CompilerParams(vmem_limit_bytes=48 << 20),
        name="attention",
    )(splits, qkv, grad, cosine, sine, *earlier)


def turn_tables(splits, seq_len):
    shape = (ROT // 2, splits.shape[0], seq_len)
    token = lax.broadcasted_iota(jnp.int32, shape, 2)
    start = splits[None, :, None]
    position = (token - jnp.where(token >= start, start, 0)).astype(F32)
    entry = jnp.arange(ROT // 2, dtype=F32)
    angle = position * (10000.0 ** (-(2.0 * entry) / ROT))[:, None, None]
    return jnp.cos(angle).reshape(ROT // 2, -1), jnp.sin(angle).reshape(ROT // 2, -1)


def sum_dots_kernel(count, *refs):
    out_ref = refs[-1]
    total = None
    for i in range(count):
        part = dot(refs[i][...], refs[count + i][...], NT)
        total = part if total is None else total + part
    out_ref[...] = total.astype(out_ref.dtype)


def sum_dots(lefts, rights, tile=512):
    rows, columns = lefts[0].shape[0], rights[0][0].shape[0]
    tile = min(tile, rows)
    depth = sum(left.shape[1] for left in lefts)
    return pl.pallas_call(
        functools.partial(sum_dots_kernel, len(lefts)),
        grid=(rows // tile,),
        in_specs=[pl.BlockSpec((tile, left.shape[1]), lambda i: (i, 0)) for left in lefts] + [
            pl.BlockSpec((columns, size), functools.partial(lambda at, i: (0, at), at))
            for _, size, at in rights
        ],
        out_specs=pl.BlockSpec((tile, columns), lambda i: (i, 0)),
        out_shape=jax.ShapeDtypeStruct((rows, columns), BF16),
        cost_estimate=pl.CostEstimate(
            flops=2 * rows * columns * depth, transcendentals=0,
            bytes_accessed=2 * (rows * columns + depth * (rows + columns)),
        ),
        compiler_params=pltpu.CompilerParams(vmem_limit_bytes=56 << 20),
        name="sum_dots",
    )(*lefts, *(right[0] for right in rights))


def hidden_kernel(n_ref, c_ref, w_ref, bias_ref, act_ref, dh_ref, sum_ref):
    piece = act_ref.shape[1]
    hidden = dot(n_ref[...], w_ref[:, :piece]) + bias_ref[...]
    grad = dot(c_ref[...], w_ref[:, piece:])
    rate = (2.0 / jnp.pi) ** 0.5
    square = hidden * hidden
    bent = jnp.tanh(rate * hidden * (1.0 + 0.044715 * square))
    act_ref[...] = (0.5 * hidden * (1.0 + bent)).astype(BF16)
    slope = 0.5 * (1.0 + bent) + 0.5 * hidden * (1.0 - bent * bent) * (
        rate * (1.0 + 3.0 * 0.044715 * square)
    )
    low = (grad * slope).astype(BF16)
    dh_ref[...] = low

    @pl.when(pl.program_id(0) == 0)
    def _():
        sum_ref[...] = jnp.zeros_like(sum_ref)

    sum_ref[...] += jnp.sum(low.astype(F32), 0, keepdims=True)


def hidden_part(normed_all, cot_all, weights, bias, tile=512):
    rows, depth = normed_all.shape
    piece = weights.shape[1] // 2
    tile = min(tile, rows)
    wide = pl.BlockSpec((tile, depth), lambda i: (i, 0))
    thin = pl.BlockSpec((tile, piece), lambda i: (i, 0))
    line = pl.BlockSpec((1, piece), lambda i: (0, 0))
    return pl.pallas_call(
        hidden_kernel,
        grid=(rows // tile,),
        in_specs=[wide, wide, pl.BlockSpec(weights.shape, lambda i: (0, 0)), line],
        out_specs=[thin, thin, line],
        out_shape=[
            jax.ShapeDtypeStruct((rows, piece), BF16),
            jax.ShapeDtypeStruct((rows, piece), BF16),
            jax.ShapeDtypeStruct((1, piece), F32),
        ],
        cost_estimate=pl.CostEstimate(
            flops=4 * rows * depth * piece, transcendentals=rows * piece,
            bytes_accessed=4 * rows * depth + 4 * depth * piece + 4 * rows * piece,
        ),
        compiler_params=pltpu.CompilerParams(vmem_limit_bytes=48 << 20),
        name="hidden_part",
    )(normed_all, cot_all, weights, bias)


def gather_kernel(
    n, q_ref, k_ref, v_ref, o_ref, up_ref, down_ref, norm_ref, cot_ref,
    w_ref, unit_ref, right_ref, left_ref, last_ref, n_ref, c_ref,
    rows_s, first_s, unit_s, last_s, send_sem, recv_sem, local_sem, store_sem,
):
    z, y, x, c = (lax.axis_index(name) for name in ("z", "y", "x", "c"))
    rows = norm_ref.shape[0]
    half = 3 * rows // 4
    mine = y * 4 + x * 2 + c
    has_right, has_left = z < n - 1, z > 0
    number = {}

    def remote(key, src, dst, axis, target):
        slot = number.setdefault(key, len(number))
        return pltpu.make_async_remote_copy(
            src_ref=src, dst_ref=dst, send_sem=send_sem.at[slot], recv_sem=recv_sem.at[slot],
            device_id={axis: target}, device_id_type=pl.DeviceIdType.MESH,
        )

    def when(condition, action):
        if condition is None:
            action()
        else:
            pl.when(condition)(action)

    started = []

    def start(condition, copy):
        when(condition, copy.start)
        started.append((condition, copy))

    def shard(index, unit):
        return w_ref.at[index * 2 + (y if unit == 0 else 1 - y)]

    width, hidden = q_ref.shape[1] // 2, up_ref.shape[1] // 2
    piece = hidden // 2

    def parts(kind, side):
        if kind == 2:
            sources, size, begin = (q_ref, k_ref, v_ref, o_ref), width, side * width
        else:
            sources, size, begin = (up_ref, down_ref), piece, side * hidden + kind * piece
        span = pl.ds(pl.multiple_of(begin, LANES), size)
        return [(ref.at[:, span], pl.ds(i * size, size)) for i, ref in enumerate(sources)]

    def packed(key, kind, side, block, axis, target):
        return [
            remote(key + (i,), source, block.at[:, columns], axis, target)
            for i, (source, columns) in enumerate(parts(kind, side))
        ]

    def along(step, unit, sign, receiving=False):
        index = z - sign * step if receiving else z - sign * (step - 1)
        if step == 1 and unit == 0:
            return packed((step, unit, sign), 0, y, shard(index, unit), "z", z + sign)
        return [remote((step, unit, sign), shard(index, unit), shard(index, unit), "z", z + sign)]

    def start_all(condition, copies):
        for copy in copies:
            start(condition, copy)

    def wait_all(copies):
        for copy in copies:
            copy.wait_recv()


    full, top, low = pl.ds(0, rows), pl.ds(0, half), pl.ds(half, rows - half)
    arrays = ((n_ref, norm_ref, "n"), (c_ref, cot_ref, "c"))
    at_x, at_y, at_xy = y * 4 + (1 - x) * 2 + c, (1 - y) * 4 + x * 2 + c, (1 - y) * 4 + (1 - x) * 2 + c

    barrier = pltpu.get_barrier_semaphore()
    for axis, target in (("x", 1 - x), ("y", 1 - y), ("c", 1 - c)):
        pl.semaphore_signal(
            barrier, inc=1, device_id={axis: target}, device_id_type=pl.DeviceIdType.MESH
        )
    for condition, target in ((has_right, z + 1), (has_left, z - 1)):
        when(condition, functools.partial(
            pl.semaphore_signal, barrier, inc=1, device_id={"z": target},
            device_id_type=pl.DeviceIdType.MESH,
        ))
    pl.semaphore_wait(barrier, 3 + has_right.astype(jnp.int32) + has_left.astype(jnp.int32))

    for condition, sign in ((has_right, 1), (has_left, -1)):
        start_all(condition, along(1, 0, sign))
    start_all(None, packed(("swap",), 0, 1 - y, shard(z, 0), "y", 1 - y))
    swap_in = packed(("swap",), 0, 1 - y, shard(z, 1), "y", 1 - y)
    for array, source, name in arrays:
        for axis in ("x", "y", "c"):
            start(None, remote((name, axis), source, array.at[mine], axis,
                               {"x": 1 - x, "y": 1 - y, "c": 1 - c}[axis]))
    start_all(None, packed(("unit",), 2, 1 - y, unit_ref.at[y], "y", 1 - y))
    unit_swap_in = packed(("unit",), 2, 1 - y, unit_ref.at[1 - y], "y", 1 - y)
    start_all(None, packed(("late",), 1, 1 - y, last_ref.at[y], "y", 1 - y))
    late_swap = packed(("late",), 1, 1 - y, last_ref.at[1 - y], "y", 1 - y)
    pairs = [(norm_ref, rows_s.at[0]), (cot_ref, rows_s.at[1])]
    for kind, block in ((0, first_s), (2, unit_s), (1, last_s)):
        pairs += [(source, block.at[:, columns]) for source, columns in parts(kind, y)]
    loads = [
        pltpu.make_async_copy(source, target, local_sem.at[i])
        for i, (source, target) in enumerate(pairs)
    ]
    stores = [
        pltpu.make_async_copy(source, target, store_sem.at[i])
        for i, (source, target) in enumerate((
            (first_s, shard(z, 0)), (unit_s, unit_ref.at[y]), (last_s, last_ref.at[y]),
            (rows_s.at[0], n_ref.at[mine]), (rows_s.at[1], c_ref.at[mine]),
        ))
    ]
    for load in loads:
        load.start()
    for load in loads:
        load.wait()
    for store in stores:
        store.start()

    def arrive_swap():
        wait_all(swap_in)
        for condition, sign in ((has_right, 1), (has_left, -1)):
            start_all(condition, along(1, 1, sign))

    def arrive_shard(step, unit, sign):
        inside = z - sign * step >= 0 if sign > 0 else z + step < n
        further = has_right if sign > 0 else has_left
        when(inside, functools.partial(wait_all, along(step, unit, sign, True)))
        if step + 1 < n:
            start_all(inside & further, along(step + 1, unit, sign))

    def arrive_rows(array, name, axis):
        index = {"x": at_x, "y": at_y, "c": None}[axis]
        block = array.at[index]
        remote((name, axis), block, block, axis, 0).wait_recv()
        part, on = (low, "y") if axis == "x" else (top, "x")
        piece = array.at[index, part]
        start(None, remote((name, "far", on), piece, piece, on, {"x": 1 - x, "y": 1 - y}[on]))
        start(None, remote((name, "core", axis), block, block, "c", 1 - c))

    def arrive_far(array, name, on):
        part = low if on == "y" else top
        piece = array.at[at_xy, part]
        remote((name, "far", on), piece, piece, on, 0).wait_recv()
        start(None, remote((name, "core", "far", on), piece, piece, "c", 1 - c))

    def arrive_steps(step):
        for unit in (0, 1):
            for sign in (1, -1):
                arrive_shard(step, unit, sign)

    def second_step(half_of, receiving):
        index = y if half_of == 0 else 1 - y
        ways = ((1, has_left if receiving else has_right, right_ref),
                (-1, has_right if receiving else has_left, left_ref))
        for sign, condition, target in ways:
            key = ("second", half_of, sign)
            if half_of == 0:
                copies = packed(key, 2, y, target.at[index], "z", z + sign)
            else:
                copies = [remote(key, unit_ref.at[index], target.at[index], "z", z + sign)]
            if receiving:
                when(condition, functools.partial(wait_all, copies))
            else:
                start_all(condition, copies)

    (norm, _, norm_name), (cot, _, cot_name) = arrays
    arrive_swap()
    arrive_rows(norm, norm_name, "x")
    for sign in (1, -1):
        arrive_shard(1, 0, sign)
    arrive_rows(norm, norm_name, "y")
    for sign in (1, -1):
        arrive_shard(1, 1, sign)
    arrive_rows(cot, cot_name, "x")
    if n > 2:
        arrive_steps(2)
    second_step(0, False)
    arrive_rows(cot, cot_name, "y")
    wait_all(unit_swap_in)
    second_step(1, False)
    for step in range(3, n):
        arrive_steps(step)
    for array, _, name in arrays:
        for on in ("x", "y"):
            arrive_far(array, name, on)
    for array, _, name in arrays:
        for key, index, part in (
            ((name, "c"), y * 4 + x * 2 + 1 - c, full),
            ((name, "core", "x"), y * 4 + (1 - x) * 2 + 1 - c, full),
            ((name, "core", "y"), (1 - y) * 4 + x * 2 + 1 - c, full),
            ((name, "core", "far", "x"), (1 - y) * 4 + (1 - x) * 2 + 1 - c, top),
            ((name, "core", "far", "y"), (1 - y) * 4 + (1 - x) * 2 + 1 - c, low),
        ):
            piece = array.at[index, part]
            remote(key, piece, piece, "c", 0).wait_recv()
    wait_all(late_swap)
    for half_of in (0, 1):
        second_step(half_of, True)
    for store in stores:
        store.wait()
    for condition, copy in started:
        when(condition, copy.wait_send)


def gather_all(n, query, key, value, output_turned, up, down_turned, normed, cotangent):
    rows, columns = normed.shape
    copies = 4 * (n - 1) + 46
    anywhere = pl.BlockSpec(memory_space=pl.ANY)
    heads = 2 * query.shape[1]
    hidden, depth = up.shape[1] // 2, query.shape[0]
    pair = jax.ShapeDtypeStruct((2, depth, heads), query.dtype)
    weights, unit, right, left, last, normed_all, cot_all = pl.pallas_call(
        functools.partial(gather_kernel, n),
        in_specs=[anywhere] * 8,
        out_specs=[anywhere] * 7,
        out_shape=[
            jax.ShapeDtypeStruct((2 * n, depth, hidden), up.dtype),
            pair, pair, pair,
            jax.ShapeDtypeStruct((2, depth, hidden), up.dtype),
            jax.ShapeDtypeStruct((8, rows, columns), normed.dtype),
            jax.ShapeDtypeStruct((8, rows, columns), cotangent.dtype),
        ],
        scratch_shapes=[
            pltpu.VMEM((2, rows, columns), normed.dtype),
            pltpu.VMEM((depth, hidden), up.dtype),
            pltpu.VMEM((depth, heads), query.dtype),
            pltpu.VMEM((depth, hidden), up.dtype),
            pltpu.SemaphoreType.DMA((copies,)),
            pltpu.SemaphoreType.DMA((copies,)),
            pltpu.SemaphoreType.DMA((10,)),
            pltpu.SemaphoreType.DMA((5,)),
        ],
        cost_estimate=pl.CostEstimate(flops=0, transcendentals=0, bytes_accessed=200 << 20),
        compiler_params=pltpu.CompilerParams(collective_id=0, has_side_effects=True),
        name="gather_rows",
    )(query, key, value, output_turned, up, down_turned, normed, cotangent)
    flat = lambda array: array.reshape(-1, array.shape[-1])
    return tuple(map(flat, (weights, unit, right, left, last, normed_all, cot_all)))


def chain_step(step, n, right, left):
    return (
        lax.ppermute(right, "z", [(i, i + 1) for i in range(step - 1, n - 1)]),
        lax.ppermute(left, "z", [(i, i - 1) for i in range(1, n - step + 1)]),
    )


def assemble(unit, right, left, n, z):
    rows, columns = unit.shape
    whole = jnp.zeros((n * rows, columns), unit.dtype)
    for k in range(n):
        piece = unit if k == 0 else jnp.where(z >= k, right[k], left[n - k])
        row = lax.rem(z - k + n, n) * rows
        whole = lax.dynamic_update_slice(whole, piece, (row, jnp.int32(0)))
    return whole


def scatter_pieces(k, grads, n, z, received):
    rows = grads.shape[0] // n

    def piece(index, got):
        own = lax.dynamic_slice_in_dim(grads, jnp.clip(index, 0, n - 1) * rows, rows, 0)
        return own if got is None else add_low(own, got)

    return piece(z - k, received[0]), piece(z + k, received[1])


def scatter_step(k, grads, n, z, received):
    to_left, to_right = scatter_pieces(k, grads, n, z, received)
    return (
        lax.ppermute(to_left, "z", [(r, r - 1) for r in range(k, n)]),
        lax.ppermute(to_right, "z", [(r, r + 1) for r in range(0, n - k)]),
    )


def scatter_end(grads, n, z, received):
    rows = grads.shape[0] // n
    own = lax.dynamic_slice_in_dim(grads, z * rows, rows, 0).astype(F32)
    return own + received[0].astype(F32) + received[1].astype(F32)


def tail_kernel(
    n, g_any, hw_ref, fw_ref, lw_ref, dq_ref, d0_ref, d1_ref, at_ref, a0_ref, a1_ref,
    left_ref, right_ref, own_ref, std_any, vec_ref,
    keep_ref, take_ref, heads_keep_ref, heads_take_ref, out_ref, mixed_ref, sums_ref,
    g_ref, std_ref, hw_s, fw_s, lw_s, rows_s, stage, zrecv, give, heads_recv, heads_own, heads_give, both, xtop_2, ylow_2, ytop_2, xlow_2,
    top_2, low_2, vstage, vrecv, send_sem, recv_sem, load_sem, rows_sem,
):
    z, y, x, c = (lax.axis_index(name) for name in ("z", "y", "x", "c"))
    rows, columns = out_ref.shape
    wide, wide_heads = give.shape[0], heads_give.shape[0]
    half = rows // 2
    rest = rows - half
    number, started = {}, []

    def remote(key, src, dst, axis, target):
        slot = number.setdefault(key, len(number))
        return pltpu.make_async_remote_copy(
            src_ref=src, dst_ref=dst, send_sem=send_sem.at[slot], recv_sem=recv_sem.at[slot],
            device_id={axis: target}, device_id_type=pl.DeviceIdType.MESH,
        )

    def when(condition, action):
        if condition is None:
            action()
        else:
            pl.when(condition)(action)

    def start(condition, copy):
        when(condition, copy.start)
        started.append((condition, copy))

    def each(count, size, body):
        def step(i, carry):
            body(pl.ds(pl.multiple_of(i * size, size), size))
            return carry
        lax.fori_loop(0, count // size, step, 0)

    barrier = pltpu.get_barrier_semaphore()
    greet = [(None, "x", 1 - x), (None, "y", 1 - y), (None, "c", 1 - c)]
    greet += [(z < n - 1, "z", z + 1), (z > 0, "z", z - 1)]
    for step in (2 ** i for i in range(1, n.bit_length() - 1)):
        greet.append((None, "z", jnp.bitwise_xor(z, step)))
    for condition, axis, target in greet:
        when(condition, functools.partial(
            pl.semaphore_signal, barrier, inc=1, device_id={axis: target},
            device_id_type=pl.DeviceIdType.MESH))

    loads = [
        pltpu.make_async_copy(source, target, load_sem.at[i])
        for i, (source, target) in enumerate(
            ((hw_ref, hw_s), (fw_ref, fw_s), (lw_ref, lw_s), (g_any, g_ref), (std_any, std_ref),
             (own_ref, heads_own)))
    ]
    for load in loads:
        load.start()

    firsts, lasts = fw_ref.shape[1] // 2, lw_ref.shape[1] // 2
    heads = dq_ref.shape[1]
    sums = (
        ((dq_ref, heads, hw_s, 0), (d0_ref, firsts, fw_s, 0), (d1_ref, lasts, lw_s, 0)),
        ((at_ref, heads // 3, hw_s, heads), (a0_ref, firsts, fw_s, firsts),
         (a1_ref, lasts, lw_s, lasts)),
    )
    sides = (1 - y, y)
    jobs = [(a, own, j) for a in (0, 1) for own in (False, True) for j in sides]

    def row_loads(number_of):
        a, own, j = jobs[number_of]
        slot, core, copies, at = number_of % 2, c if own else 1 - c, [], 0
        for p, (left, width, _, _) in enumerate(sums[a]):
            for i in (0, 1):
                block = j * 4 + i * 2 + core
                source = left.at[pl.ds(pl.multiple_of(block * rows, rows), rows)]
                target = rows_s.at[slot, pl.ds(i * rows, rows), pl.ds(at, width)]
                copies.append(pltpu.make_async_copy(source, target, rows_sem.at[slot, p * 2 + i]))
            at += width
        return copies

    def job(number_of):
        a, own, j = jobs[number_of]
        slot = number_of % 2
        if number_of + 1 < len(jobs):
            for copy in row_loads(number_of + 1):
                copy.start()
        for copy in row_loads(number_of):
            copy.wait()
        if own:
            for i in (0, 1):
                core_copy(a, number_of % 2, i).wait_recv()
        elif a == 1:
            for i in (0, 1):
                core_copy(0, number_of % 2, i).wait_send()
        size = min(512, columns)

        def tile(t, carry):
            span = pl.ds(pl.multiple_of(t * size, size), size)
            acc, at = None, 0
            for left, width, weights, column in sums[a]:
                part = dot(
                    rows_s[slot, :, at : at + width], weights[span, column : column + width], NT)
                acc = part if acc is None else acc + part
                at += width
            for i in (0, 1):
                piece = acc[i * rows : (i + 1) * rows]
                if own:
                    both[a, j * 2 + i, :, span] = (
                        piece + both[a, j * 2 + i, :, span].astype(F32)).astype(BF16)
                else:
                    stage[j * 2 + i, :, span] = piece.astype(BF16)
            return carry

        lax.fori_loop(0, columns // size, tile, 0)
        if own and a == 0:
            start(None, first_copy(a, "xtop", number_of % 2))
            if number_of % 2 == 0:
                for i in (0, 1):
                    start(None, first_copy(a, "ylow", i))
        if not own:
            for i in (0, 1):
                copy = core_copy(a, number_of % 2, i)
                copy.start()
                if a == 1:
                    started.append((None, copy))

    def core_copy(a, u, i):
        place = sides[u] * 2 + i
        return remote(("core", a, u, i), stage.at[place], both.at[a, place], "c", 1 - c)

    for copy in row_loads(0):
        copy.start()
    always = sum(condition is None for condition, _, _ in greet)
    pl.semaphore_wait(barrier, always + sum(
        condition.astype(jnp.int32) for condition, _, _ in greet if condition is not None))

    def first_copy(a, name, j):
        if name == "xtop":
            source = both.at[a, sides[j] * 2 + 1 - x, pl.ds(0, half)]
            return remote((name, a, j), source, xtop_2.at[a, j], "x", 1 - x)
        source = both.at[a, (1 - y) * 2 + j, pl.ds(half, rest)]
        return remote((name, a, j), source, ylow_2.at[a, j], "y", 1 - y)

    def second_copy(a, name):
        if name == "ytop":
            return remote((name, a), top_2.at[a], ytop_2.at[a], "y", 1 - y)
        return remote((name, a), low_2.at[a], xlow_2.at[a], "x", 1 - x)

    def first_send(a):
        for j in (0, 1):
            start(None, first_copy(a, "xtop", j))
            start(None, first_copy(a, "ylow", j))

    def first_arrive(a):
        for j in (0, 1):
            first_copy(a, "xtop", j).wait_recv()
            first_copy(a, "ylow", j).wait_recv()

        def upper(part):
            top_2[a, part, :] = (
                both[a, (1 - y) * 2 + x, part, :].astype(F32)
                + xtop_2[a, 0, part, :].astype(F32)
            ).astype(BF16)

        def lower(part):
            low_part = pl.ds(part.start + half, part.size)
            low_2[a, part, :] = (
                both[a, y * 2 + 1 - x, low_part, :].astype(F32)
                + ylow_2[a, 1 - x, part, :].astype(F32)
            ).astype(BF16)

        each(half, 32, upper)
        each(rest, 32, lower)
        start(None, second_copy(a, "ytop"))
        start(None, second_copy(a, "xlow"))

    def second_arrive(a):
        second_copy(a, "ytop").wait_recv()
        second_copy(a, "xlow").wait_recv()
        target = (out_ref, mixed_ref)[a]

        def finish(first, part, placed, last):
            value = (
                both[a, y * 2 + x, placed, :].astype(F32) + first[part, :].astype(F32)
                + last[part, :].astype(F32)
            )
            target[placed, :] = value
            if a == 0:
                scaled = value * std_ref[placed, :]
                vstage[0, 0:1, :] += jnp.sum(scaled, 0, keepdims=True)
                vstage[0, 1:2, :] += jnp.sum(value, 0, keepdims=True)

        def upper(part):
            finish(xtop_2.at[a, 1], part, part, ytop_2.at[a])

        def lower(part):
            finish(ylow_2.at[a, x], part, pl.ds(part.start + half, part.size), xlow_2.at[a])

        each(half, 32, upper)
        each(rest, 32, lower)

    def block_of(direction, k, u):
        index = (z - k if direction == 0 else z + k) * 2 + sides[u]
        return pl.ds(pl.multiple_of(index * rows, rows), rows)

    def z_copy(direction, k, u, src):
        target = z - 1 if direction == 0 else z + 1
        return remote((direction, k, u), src, zrecv.at[direction, k - 1, u], "z", target)

    def z_first(direction):
        edge = z == n - 1 if direction == 0 else z == 0
        for k in range(n - 1, 0, -1):
            for u in (0, 1):
                start(edge, z_copy(direction, k, u, g_any.at[:, block_of(direction, k, u)]))

    def z_step(k, u):
        for direction in (0, 1):
            if direction == 0:
                inside = (z >= k) & (z < n - 1)
            else:
                inside = (n - 1 - z >= k) & (z > 0)
            held = zrecv.at[direction, k, u]

            def add():
                z_copy(direction, k + 1, u, held).wait_recv()
                block = block_of(direction, k, u)

                def body(part):
                    held[part, :] = (
                        g_ref[part, block].astype(F32) + held[part, :].astype(F32)
                    ).astype(BF16)

                each(wide, 256, body)

            when(inside, add)
            start(inside, z_copy(direction, k, u, held))

    def z_last(u, target):
        block = block_of(0, 0, u)

        def first(part):
            target[part, :] = g_ref[part, block].astype(F32)

        each(wide, 256, first)
        for direction in (0, 1):
            held = zrecv.at[direction, 0, u]

            def add():
                z_copy(direction, 1, u, held).wait_recv()

                def body(part):
                    target[part, :] += held[part, :].astype(F32)

                each(wide, 256, body)

            when(z < n - 1 if direction == 0 else z > 0, add)

    def heads_copy(direction, u):
        span = pl.ds(pl.multiple_of(sides[u] * rows, rows), rows)
        source = (left_ref, right_ref)[direction].at[:, span]
        return remote(
            ("heads", direction, u), source, heads_recv.at[direction, :, span], "z",
            z - 1 if direction == 0 else z + 1)

    def heads_send():
        for u in (0, 1):
            start(z > 0, heads_copy(0, u))
            start(z < n - 1, heads_copy(1, u))

    def heads_last(u, target):
        span = pl.ds(pl.multiple_of(sides[u] * rows, rows), rows)

        def first(part):
            target[part, :] = heads_own[part, span].astype(F32)

        each(wide_heads, 256, first)
        for direction in (0, 1):
            def add():
                heads_copy(direction, u).wait_recv()

                def body(part):
                    target[part, :] += heads_recv[direction, part, span].astype(F32)

                each(wide_heads, 256, body)

            when(z < n - 1 if direction == 0 else z > 0, add)

    steps = [(k, u) for k in range(n - 2, 0, -1) for u in (0, 1)]

    def z_next():
        if steps:
            z_step(*steps.pop(0))

    for direction in (0, 1):
        z_first(direction)
    vstage[0] = vec_ref[...]
    for load in loads[:3]:
        load.wait()
    job(0)
    job(1)
    for load in loads[3:]:
        load.wait()
    z_next()
    job(2)
    job(3)
    heads_send()
    z_next()
    job(4)
    job(5)
    z_next()
    job(6)
    job(7)
    first_arrive(0)
    first_send(1)
    while steps:
        z_next()
    second_arrive(0)

    turns = [("z", jnp.bitwise_xor(z, 2 ** i)) for i in range(n.bit_length() - 1)]
    turns += [("y", 1 - y), ("x", 1 - x), ("c", 1 - c)]
    line = lax.broadcasted_iota(jnp.int32, vec_ref.shape, 0)

    def exchange(i):
        axis, target = turns[i]
        return remote(("vec", i), vstage.at[i], vrecv.at[i], axis, target)

    def turn(i):
        exchange(i).wait_recv()
        axis, _ = turns[i]
        old, new = vstage[i], vrecv[i]
        result = sums_ref if i == len(turns) - 1 else vstage.at[i + 1]
        result[...] = old + jnp.where((line < 3) | (axis == "z"), new, 0.0)
        if axis == "y":
            result[4:5, :] = new[3:4, :]
        if i + 1 < len(turns):
            start(None, exchange(i + 1))

    start(None, exchange(0))

    def swapped(key, source, target, length, received):
        def lower_precision(part):
            target[part, :] = source[part, :].astype(BF16)

        each(length, 256, lower_precision)
        copy = remote(key, target, received, "y", 1 - y)
        start(None, copy)
        return copy

    first_arrive(1)
    z_last(0, keep_ref)
    swap = swapped("swap", keep_ref, give, wide, take_ref)
    turn(0)
    turn(1)
    heads_last(0, heads_keep_ref)
    heads_swap = swapped("heads swap", heads_keep_ref, heads_give, wide_heads, heads_take_ref)
    turn(2)
    z_last(1, keep_ref)
    turn(3)
    heads_last(1, heads_keep_ref)
    for i in range(4, len(turns)):
        turn(i)
    second_arrive(1)
    swap.wait_recv()
    heads_swap.wait_recv()
    for condition, copy in started:
        when(condition, copy.wait_send)


def tail(n, grads_turned, weights, lefts, lefts_out, heads_turned, standard, vector):
    rows, columns = standard.shape
    wide, wide_heads = grads_turned.shape[0], heads_turned[0].shape[0]
    half = rows // 2
    inside = pl.BlockSpec(memory_space=pltpu.VMEM)
    anywhere = pl.BlockSpec(memory_space=pl.ANY)
    copies = 4 * (n - 1) + 46
    low = lambda *shape: pltpu.VMEM(shape, BF16)
    small = vector.shape
    depth = sum(left.shape[1] for left in lefts)
    return pl.pallas_call(
        functools.partial(tail_kernel, n),
        in_specs=[anywhere] * 14 + [inside],
        out_specs=[inside] * 7,
        out_shape=[
            jax.ShapeDtypeStruct((wide, rows), F32),
            jax.ShapeDtypeStruct((wide, rows), BF16),
            jax.ShapeDtypeStruct((wide_heads, rows), F32),
            jax.ShapeDtypeStruct((wide_heads, rows), BF16),
            jax.ShapeDtypeStruct((rows, columns), F32),
            jax.ShapeDtypeStruct((rows, columns), F32),
            jax.ShapeDtypeStruct(small, F32),
        ],
        scratch_shapes=[low(*grads_turned.shape), pltpu.VMEM(standard.shape, F32)] + [
            low(*array.shape) for array in weights
        ] + [
            low(2, 2 * rows, depth), low(4, rows, columns),
            low(2, n - 1, 2, wide, rows), low(wide, rows),
            low(2, wide_heads, 2 * rows), low(wide_heads, 2 * rows), low(wide_heads, rows),
            low(2, 4, rows, columns),
            low(2, 2, half, columns), low(2, 2, rows - half, columns),
            low(2, half, columns), low(2, rows - half, columns),
            low(2, half, columns), low(2, rows - half, columns),
            pltpu.VMEM((8,) + small, F32), pltpu.VMEM((8,) + small, F32),
            pltpu.SemaphoreType.DMA((copies,)),
            pltpu.SemaphoreType.DMA((copies,)),
            pltpu.SemaphoreType.DMA((6,)),
            pltpu.SemaphoreType.DMA((2, 6)),
        ],
        cost_estimate=pl.CostEstimate(flops=0, transcendentals=0, bytes_accessed=200 << 20),
        compiler_params=pltpu.CompilerParams(
            collective_id=1, has_side_effects=True, vmem_limit_bytes=63 << 20
        ),
        name="scatter_rest",
    )(grads_turned, *weights, *lefts, *lefts_out, *heads_turned, standard, vector)


def sum_small(array, axes):
    for axis in axes:
        size = lax.axis_size(axis)
        if size & (size - 1):
            array = lax.psum(array, axis)
            continue
        step = 1
        while step < size:
            array = array + lax.ppermute(array, axis, [(i, i ^ step) for i in range(size)])
            step *= 2
    return array


def pick(array, index, axis):
    return lax.dynamic_index_in_dim(array, index, axis, keepdims=False)


def add_low(left, right):
    return (left.astype(F32) + right.astype(F32)).astype(BF16)


def plane_scatter(partial, y, x, c):
    rows, columns = partial.shape[0] // 8, partial.shape[1]
    half = rows // 2
    parts = partial.reshape(2, 2, 2, rows, columns)
    acc = add_low(pick(parts, c, 2), lax.ppermute(pick(parts, 1 - c, 2), "c", SWAP))
    top, low = acc[:, :, :half], acc[:, :, half:]
    top = add_low(pick(top, x, 1), lax.ppermute(pick(top, 1 - x, 1), "x", SWAP))
    low = add_low(pick(low, y, 0), lax.ppermute(pick(low, 1 - y, 0), "y", SWAP))
    top = pick(top, y, 0).astype(F32) + lax.ppermute(pick(top, 1 - y, 0), "y", SWAP).astype(F32)
    low = pick(low, x, 0).astype(F32) + lax.ppermute(pick(low, 1 - x, 0), "x", SWAP).astype(F32)
    return jnp.concatenate([top, low], 0)


def in_order(y, own, other, axis):
    return jnp.where(
        y == 0, jnp.concatenate([own, other], axis), jnp.concatenate([other, own], axis)
    )


def on_device(
    n,
    tokens, norm_gain, norm_bias,
    query_weight, query_bias, key_weight, key_bias, value_weight, value_bias,
    output_weight, output_bias, up_weight, up_bias, down_weight, down_bias,
    doc_split, cotangent,
):
    z, y, x, c = (lax.axis_index(name) for name in ("z", "y", "x", "c"))
    shard_rows = query_weight.shape[0]
    width = query_weight.shape[1] // 2
    hidden_width = up_weight.shape[1] // 2
    chunks = 2
    piece = hidden_width // chunks

    def row(array, start, size):
        return lax.dynamic_slice_in_dim(array, start, size, 0)

    gain_wide = norm_gain.astype(F32)
    tokens_wide = tokens.astype(F32)
    row_mean = jnp.mean(tokens_wide, -1, keepdims=True)
    centred = tokens_wide - row_mean
    inv_scale = lax.rsqrt(jnp.mean(centred * centred, -1, keepdims=True) + EPS)
    standard = centred * inv_scale
    normed = (standard * gain_wide + norm_bias.astype(F32)).astype(BF16)
    phase = lax.optimization_barrier
    other_split = lax.ppermute(doc_split, "y", SWAP)
    splits = in_order(y, doc_split, other_split, 0)
    seq_len = 4 * normed.shape[0]
    cosine, sine = turn_tables(splits, seq_len)

    right, left = [None] * n, [None] * n
    first_weights, heads_unit, right[1], left[1], last_unit, normed_all, cot_all = gather_all(
        n, query_weight, key_weight, value_weight, output_weight.T, up_weight, down_weight.T,
        normed, cotangent,
    )
    first_weights, heads_unit, last_unit, normed_all, cot_all, right[1], left[1], cosine, sine = phase(
        (first_weights, heads_unit, last_unit, normed_all, cot_all, right[1], left[1], cosine, sine)
    )

    def hidden_local(weights, chunk):
        bias = row(up_bias, y * hidden_width + chunk * piece, piece).astype(F32)[None]
        return hidden_part(normed_all, cot_all, weights, bias)

    def weight_grads(grad_columns, columns):
        return jnp.concatenate(
            [dot(normed_all, grad_columns, TN).astype(BF16), dot(cot_all, columns, TN).astype(BF16)], 1
        )

    def gather_step(step, source):
        return chain_step(step, n, right[step - 1], left[step - 1]) if step > 1 else chain_step(
            1, n, source, source)

    activated_0, grad_hidden_0, hidden_sum_0 = hidden_local(first_weights, 0)
    right[2], left[2] = gather_step(2, None)
    activated_0, grad_hidden_0, normed_all, cot_all, right[2], left[2] = phase(
        (activated_0, grad_hidden_0, normed_all, cot_all, right[2], left[2])
    )
    grads_first = weight_grads(grad_hidden_0, activated_0)
    for step in range(3, n):
        right[step], left[step] = gather_step(step, None)
    grads_first, activated_0, last_unit, normed_all, cot_all, right[3:], left[3:] = phase(
        (grads_first, activated_0, last_unit, normed_all, cot_all, right[3:], left[3:])
    )
    head_weights = assemble(heads_unit, right, left, n, z)
    qkv_weight, output_turned = head_weights[:, : 3 * width], head_weights[:, 3 * width :]

    qkv_bias = jnp.concatenate(
        [row(b, y * width, width) for b in (query_bias, key_bias, value_bias)]
    ).astype(F32)
    qkv = dot(normed_all, qkv_weight) + qkv_bias
    grad_attended = dot(cot_all, output_turned).astype(BF16)
    right[1], left[1] = gather_step(1, last_unit)
    qkv, grad_attended, normed_all, cot_all, right[1], left[1] = phase(
        (qkv, grad_attended, normed_all, cot_all, right[1], left[1])
    )
    found = attention(0, splits, qkv, grad_attended, cosine, sine, ())
    right[2], left[2] = gather_step(2, None)
    first_in = scatter_step(n - 1, grads_first, n, z, (None, None))
    found, qkv, grad_attended, normed_all, cot_all, right[2], left[2], first_in, grads_first = phase(
        (found, qkv, grad_attended, normed_all, cot_all, right[2], left[2], first_in, grads_first)
    )
    for index in range(1, splits.shape[0]):
        found = attention(index, splits, qkv, grad_attended, cosine, sine, found)
    for step in range(3, n):
        right[step], left[step] = gather_step(step, None)
    for k in range(n - 2, n - 3, -1):
        first_in = scatter_step(k, grads_first, n, z, first_in)
    found, normed_all, cot_all, right[3:], left[3:], first_in, grads_first = phase(
        (found, normed_all, cot_all, right[3:], left[3:], first_in, grads_first)
    )
    attended, grad_qkv = found
    grads_heads = weight_grads(grad_qkv, attended)
    for k in range(n - 3, 0, -1):
        first_in = scatter_step(k, grads_first, n, z, first_in)
    grads_heads, attended, grad_qkv, normed_all, cot_all, last_unit, first_in, grads_first = phase(
        (grads_heads, attended, grad_qkv, normed_all, cot_all, last_unit, first_in, grads_first)
    )
    first_sum = scatter_end(grads_first, n, z, first_in)

    last_weights = assemble(last_unit, right, left, n, z)
    activated_1, grad_hidden_1, hidden_sum_1 = hidden_local(last_weights, 1)
    heads_in = scatter_step(n - 1, grads_heads, n, z, (None, None))
    (last_weights, activated_1, grad_hidden_1, attended, grad_qkv, heads_in, grads_heads,
     normed_all, cot_all) = phase(
        (last_weights, activated_1, grad_hidden_1, attended, grad_qkv, heads_in, grads_heads,
         normed_all, cot_all)
    )
    for k in range(n - 2, max(n - 3, 1), -1):
        heads_in = scatter_step(k, grads_heads, n, z, heads_in)
    grads_last = weight_grads(grad_hidden_1, activated_1)
    qkv_sum = jnp.sum(grad_qkv, 0, dtype=F32)[None]
    bias_row = jnp.concatenate([qkv_sum, hidden_sum_0, hidden_sum_1], 1)
    cot_wide = cotangent.astype(F32)
    cot_sum = jnp.sum(cot_wide, 0)[None]
    grads_last, heads_in, grads_heads, bias_row, cot_sum = phase(
        (grads_last, heads_in, grads_heads, bias_row, cot_sum)
    )
    def halves(total):
        keep = row(total, y * shard_rows, shard_rows)
        give = row(total, (1 - y) * shard_rows, shard_rows).astype(BF16)
        return keep, lax.ppermute(give, "y", SWAP).astype(F32)

    first_keep, first_take = halves(first_sum)

    if n == 4 and bias_row.shape[1] <= cot_sum.shape[1]:
        spread = cot_sum.shape[1]
        vector = jnp.concatenate([
            jnp.zeros((2, spread), F32), cot_sum,
            jnp.pad(bias_row, ((0, 0), (0, spread - bias_row.shape[1]))),
            jnp.zeros((4, spread), F32),
        ])
        left_piece, right_piece = scatter_pieces(1, grads_heads, n, z, heads_in)
        own_piece = row(grads_heads, z * 2 * shard_rows, 2 * shard_rows)
        last_keep, last_take, heads_keep, heads_take, grad_normed, mixed, sums = tail(
            n, grads_last.T, (head_weights, first_weights, last_weights),
            (grad_qkv, grad_hidden_0, grad_hidden_1), (attended, activated_0, activated_1),
            (left_piece.T, right_piece.T, own_piece.T), standard, vector,
        )
        last_keep, last_take = last_keep.T, last_take.astype(F32).T
        heads_keep, heads_take = heads_keep.T, heads_take.astype(F32).T
        norm_sums = sums[:3]
        bias_rows = in_order(y, sums[3:4], sums[4:5], 0)[:, : bias_row.shape[1]]
    else:
        for k in range(n - 3, 0, -1):
            heads_in = scatter_step(k, grads_heads, n, z, heads_in)
        heads_keep, heads_take = halves(scatter_end(grads_heads, n, z, heads_in))
        partial_out = sum_dots(
            (attended, activated_0, activated_1),
            ((head_weights, width, 3), (first_weights, piece, 1), (last_weights, piece, 1)),
        )
        grad_normed_part = sum_dots(
            (grad_qkv, grad_hidden_0, grad_hidden_1),
            ((head_weights, 3 * width, 0), (first_weights, piece, 0), (last_weights, piece, 0)),
        )
        last_in = (None, None)
        for k in range(n - 1, 0, -1):
            last_in = scatter_step(k, grads_last, n, z, last_in)
        last_keep, last_take = halves(scatter_end(grads_last, n, z, last_in))
        grad_normed = plane_scatter(grad_normed_part, y, x, c)
        mixed = plane_scatter(partial_out, y, x, c)
        norm_sums = sum_small(
            jnp.concatenate([
                jnp.sum(grad_normed * standard, 0)[None], jnp.sum(grad_normed, 0)[None], cot_sum
            ]),
            ("c", "x", "y", "z"),
        )
        bias_row = sum_small(bias_row, ("z",))
        bias_rows = in_order(y, bias_row, lax.ppermute(bias_row, "y", SWAP), 0)
    grad_norm_gain, grad_norm_bias, grad_out_bias = norm_sums

    out_bias = output_bias.astype(F32) + down_bias.astype(F32)
    out = (tokens_wide + mixed + out_bias).astype(BF16)

    def joined(start, size):
        return in_order(
            y, heads_keep[:, start : start + size], heads_take[:, start : start + size], 1
        )

    grad_query_weight, grad_key_weight, grad_value_weight, grad_output_turned = (
        joined(part * width, width) for part in range(4)
    )
    hidden_halves = [(first_keep, first_take), (last_keep, last_take)]

    def side(which, start):
        return jnp.concatenate([pair[which][:, start : start + piece] for pair in hidden_halves], 1)

    grad_up_weight = in_order(y, side(0, 0), side(1, 0), 1)
    grad_down_turned = in_order(y, side(0, piece), side(1, piece), 1)

    grad_query_bias, grad_key_bias, grad_value_bias = (
        bias_rows[:, part * width : (part + 1) * width].reshape(-1) for part in range(3)
    )
    grad_up_bias = bias_rows[:, 3 * width :].reshape(-1)

    grad_scaled = grad_normed * gain_wide
    grad_tokens = cot_wide + inv_scale * (
        grad_scaled
        - jnp.mean(grad_scaled, -1, keepdims=True)
        - standard * jnp.mean(grad_scaled * standard, -1, keepdims=True)
    )
    return (
        out, grad_tokens, grad_norm_gain, grad_norm_bias,
        grad_query_weight, grad_query_bias, grad_key_weight, grad_key_bias,
        grad_value_weight, grad_value_bias, grad_output_turned.T, grad_out_bias,
        grad_up_weight, grad_up_bias, grad_down_turned.T, grad_out_bias,
    )


def solution(mesh):
    n = mesh.shape["dp"] // 2
    grid = Mesh(mesh.devices.reshape(n, 2, mesh.shape["tensor"] // 2, 2), ("z", "y", "x", "c"))
    dp, tensor = ("z", "y"), ("x", "c")
    rows = P(dp + tensor, None)
    whole, split = P(), P(tensor)
    wide, tall = P(dp, tensor), P(tensor, dp)
    in_specs = (
        rows, whole, whole, wide, split, wide, split, wide, split,
        tall, whole, wide, split, tall, whole, P(dp), rows,
    )
    out_specs = (
        rows, rows, whole, whole, wide, split, wide, split, wide, split,
        tall, whole, wide, split, tall, whole,
    )
    return jax.shard_map(
        functools.partial(on_device, n),
        mesh=grid, in_specs=in_specs, out_specs=out_specs, check_vma=False,
    )
```

```python
import functools

import jax
import jax.numpy as jnp
from jax import lax
from jax.experimental import pallas as pl
from jax.experimental.pallas import tpu as pltpu
from jax.sharding import Mesh, PartitionSpec as P

HEAD_DIM = 64
ROT = 32
BLOCK = 256
EPS = 1e-05
LANES = 128
F32 = jnp.float32
BF16 = jnp.bfloat16


SWAP = [(0, 1), (1, 0)]
NT = (((1,), (1,)), ((), ()))
TN = (((0,), (0,)), ((), ()))
NN = (((1,), (0,)), ((), ()))


def dot(left, right, dims=NN):
    return lax.dot_general(left, right, dims, preferred_element_type=F32)


def spin(value, cosine, sine):
    lane = lax.broadcasted_iota(jnp.int32, value.shape, 1) % HEAD_DIM
    half = ROT // 2
    ahead = pltpu.roll(value, LANES - half, 1)
    behind = pltpu.roll(value, half, 1)
    return value * cosine + jnp.where(lane < half, ahead, behind) * sine


def attention_kernel(
    index, earlier, split_ref, qkv_ref, grad_ref, cos_ref, sin_ref, *refs
):
    (att_ref, dqkv_ref, *scratch) = refs[earlier:]
    attention_body(index, split_ref, qkv_ref, grad_ref, cos_ref, sin_ref, att_ref, dqkv_ref, *scratch)


def attention_body(
    index, split_ref, qkv_ref, grad_ref, cos_ref, sin_ref, att_ref, dqkv_ref,
    q_s, k_s, v_s, g_s, b_s, dq_s, dk_s, dv_s, cos_s, sin_s,
):
    seq_len, width = grad_ref.shape
    first = split_ref[index] // BLOCK
    scale = HEAD_DIM ** (-0.5)
    per = LANES // HEAD_DIM
    rest = jnp.zeros((HEAD_DIM - ROT, seq_len), F32)
    cos_part, sin_part = cos_ref[...], sin_ref[...]
    cos_s[...] = jnp.concatenate([cos_part, cos_part, rest + 1.0] * per, 0).T
    sin_s[...] = jnp.concatenate([-sin_part, sin_part, rest] * per, 0).T

    def one_pair(pair, carry):
        def cols(part):
            return pl.ds(pl.multiple_of(part * width + pair * LANES, LANES), LANES)

        cosine, sine = cos_s[...], sin_s[...]
        head_of = lax.broadcasted_iota(jnp.int32, (seq_len, LANES), 1) // HEAD_DIM
        query = spin(qkv_ref[:, cols(0)], cosine, sine).astype(BF16)
        key = spin(qkv_ref[:, cols(1)], cosine, sine).astype(BF16)
        value = qkv_ref[:, cols(2)].astype(BF16)
        grad = grad_ref[:, cols(0)]
        query = (query.astype(F32) * scale).astype(BF16)
        turned_back = (key.astype(F32) * scale).astype(BF16)
        for head in range(per):
            here = head_of == head
            q_s[head] = jnp.where(here, query, 0).astype(BF16)
            k_s[head] = jnp.where(here, key, 0).astype(BF16)
            b_s[head] = jnp.where(here, turned_back, 0).astype(BF16)
            v_s[head] = jnp.where(here, value, 0).astype(BF16)
            g_s[head] = jnp.where(here, grad, 0).astype(BF16)
        dk_s[...] = jnp.zeros_like(dk_s)
        dv_s[...] = jnp.zeros_like(dv_s)

        def one_block(block, inner):
            begin = jnp.where(block >= first, first, 0)
            rows = pl.ds(pl.multiple_of(block * BLOCK, BLOCK), BLOCK)

            def work(count):
                span = pl.ds(pl.multiple_of(begin * BLOCK, BLOCK), count * BLOCK)
                held = None
                for head in range(per):
                    q, g = q_s[head, rows, :], g_s[head, rows, :]
                    scores = dot(k_s[head, span, :], q, NT)
                    top = jnp.max(scores, 0, keepdims=True)
                    power = jnp.exp(scores - top)
                    prob = power * (1.0 / jnp.sum(power, 0, keepdims=True))
                    low = prob.astype(BF16)
                    dprob = dot(v_s[head, span, :], g, NT)
                    mean = jnp.sum(prob * dprob, 0, keepdims=True)
                    dscore = (prob * (dprob - mean)).astype(BF16)
                    parts = (
                        dot(dscore, q), dot(low, g),
                        dot(dscore, b_s[head, span, :], TN), dot(low, v_s[head, span, :], TN),
                    )
                    held = parts if held is None else [a + b for a, b in zip(held, parts)]
                dk, dv, dq, found = held
                dq_s[rows, :] = dq
                att_ref[rows, cols(0)] = found.astype(BF16)
                dk_s[span, :] += dk
                dv_s[span, :] += dv

            for count in range(1, seq_len // BLOCK):
                pl.when(block - begin == count - 1)(functools.partial(work, count))
            return inner

        lax.fori_loop(0, seq_len // BLOCK, one_block, 0)
        dqkv_ref[:, cols(0)] = spin(dq_s[...], cosine, -sine).astype(BF16)
        dqkv_ref[:, cols(1)] = spin(dk_s[...], cosine, -sine).astype(BF16)
        dqkv_ref[:, cols(2)] = dv_s[...].astype(BF16)
        return carry

    lax.fori_loop(0, width // LANES, one_pair, 0)


def attention(index, splits, qkv, grad, cosine, sine, earlier):
    count = splits.shape[0]
    rows, width = grad.shape
    seq_len = rows // count
    per = LANES // HEAD_DIM

    def spec(columns):
        return pl.BlockSpec((seq_len, columns), lambda i, split: (index, 0))

    table = pl.BlockSpec((ROT // 2, seq_len), lambda i, split: (0, index))
    masked = pltpu.VMEM((per, seq_len, LANES), BF16)
    return pl.pallas_call(
        functools.partial(attention_kernel, index, len(earlier)),
        grid_spec=pltpu.PrefetchScalarGridSpec(
            num_scalar_prefetch=1,
            grid=(1,),
            in_specs=[spec(3 * width), spec(width), table, table]
            + [pl.BlockSpec(memory_space=pl.ANY)] * len(earlier),
            out_specs=[spec(width), spec(3 * width)],
            scratch_shapes=[
                masked, masked, masked, masked, masked,
                pltpu.VMEM((seq_len, LANES), F32),
                pltpu.VMEM((seq_len, LANES), F32),
                pltpu.VMEM((seq_len, LANES), F32),
                pltpu.VMEM((seq_len, LANES), F32),
                pltpu.VMEM((seq_len, LANES), F32),
            ],
        ),
        out_shape=[
            jax.ShapeDtypeStruct((rows, width), BF16),
            jax.ShapeDtypeStruct((rows, 3 * width), BF16),
        ],
        cost_estimate=pl.CostEstimate(
            flops=40 * seq_len * seq_len * width // 4,
            transcendentals=seq_len * seq_len * width // HEAD_DIM // 2,
            bytes_accessed=seq_len * width * 24,
        ),
        input_output_aliases={5 + i: i for i in range(len(earlier))},
        compiler_params=pltpu.CompilerParams(vmem_limit_bytes=48 << 20),
        name="attention",
    )(splits, qkv, grad, cosine, sine, *earlier)


def turn_tables(splits, seq_len):
    shape = (ROT // 2, splits.shape[0], seq_len)
    token = lax.broadcasted_iota(jnp.int32, shape, 2)
    start = splits[None, :, None]
    position = (token - jnp.where(token >= start, start, 0)).astype(F32)
    entry = jnp.arange(ROT // 2, dtype=F32)
    angle = position * (10000.0 ** (-(2.0 * entry) / ROT))[:, None, None]
    return jnp.cos(angle).reshape(ROT // 2, -1), jnp.sin(angle).reshape(ROT // 2, -1)


def sum_dots_kernel(count, *refs):
    out_ref = refs[-1]
    total = None
    for i in range(count):
        part = dot(refs[i][...], refs[count + i][...], NT)
        total = part if total is None else total + part
    out_ref[...] = total.astype(out_ref.dtype)


def sum_dots(lefts, rights, tile=512):
    rows, columns = lefts[0].shape[0], rights[0][0].shape[0]
    tile = min(tile, rows)
    depth = sum(left.shape[1] for left in lefts)
    return pl.pallas_call(
        functools.partial(sum_dots_kernel, len(lefts)),
        grid=(rows // tile,),
        in_specs=[pl.BlockSpec((tile, left.shape[1]), lambda i: (i, 0)) for left in lefts] + [
            pl.BlockSpec((columns, size), functools.partial(lambda at, i: (0, at), at))
            for _, size, at in rights
        ],
        out_specs=pl.BlockSpec((tile, columns), lambda i: (i, 0)),
        out_shape=jax.ShapeDtypeStruct((rows, columns), BF16),
        cost_estimate=pl.CostEstimate(
            flops=2 * rows * columns * depth, transcendentals=0,
            bytes_accessed=2 * (rows * columns + depth * (rows + columns)),
        ),
        compiler_params=pltpu.CompilerParams(vmem_limit_bytes=56 << 20),
        name="sum_dots",
    )(*lefts, *(right[0] for right in rights))


def hidden_kernel(n_ref, c_ref, w_ref, bias_ref, act_ref, dh_ref, sum_ref):
    piece = act_ref.shape[1]
    hidden = dot(n_ref[...], w_ref[:, :piece]) + bias_ref[...]
    grad = dot(c_ref[...], w_ref[:, piece:])
    rate = (2.0 / jnp.pi) ** 0.5
    square = hidden * hidden
    bent = jnp.tanh(rate * hidden * (1.0 + 0.044715 * square))
    act_ref[...] = (0.5 * hidden * (1.0 + bent)).astype(BF16)
    slope = 0.5 * (1.0 + bent) + 0.5 * hidden * (1.0 - bent * bent) * (
        rate * (1.0 + 3.0 * 0.044715 * square)
    )
    low = (grad * slope).astype(BF16)
    dh_ref[...] = low

    @pl.when(pl.program_id(0) == 0)
    def _():
        sum_ref[...] = jnp.zeros_like(sum_ref)

    sum_ref[...] += jnp.sum(low.astype(F32), 0, keepdims=True)


def hidden_part(normed_all, cot_all, weights, bias, tile=512):
    rows, depth = normed_all.shape
    piece = weights.shape[1] // 2
    tile = min(tile, rows)
    wide = pl.BlockSpec((tile, depth), lambda i: (i, 0))
    thin = pl.BlockSpec((tile, piece), lambda i: (i, 0))
    line = pl.BlockSpec((1, piece), lambda i: (0, 0))
    return pl.pallas_call(
        hidden_kernel,
        grid=(rows // tile,),
        in_specs=[wide, wide, pl.BlockSpec(weights.shape, lambda i: (0, 0)), line],
        out_specs=[thin, thin, line],
        out_shape=[
            jax.ShapeDtypeStruct((rows, piece), BF16),
            jax.ShapeDtypeStruct((rows, piece), BF16),
            jax.ShapeDtypeStruct((1, piece), F32),
        ],
        cost_estimate=pl.CostEstimate(
            flops=4 * rows * depth * piece, transcendentals=rows * piece,
            bytes_accessed=4 * rows * depth + 4 * depth * piece + 4 * rows * piece,
        ),
        compiler_params=pltpu.CompilerParams(vmem_limit_bytes=48 << 20),
        name="hidden_part",
    )(normed_all, cot_all, weights, bias)


def gather_kernel(
    n, q_ref, k_ref, v_ref, o_ref, up_ref, down_ref, norm_ref, cot_ref,
    w_ref, unit_ref, right_ref, left_ref, last_ref, n_ref, c_ref,
    rows_s, first_s, unit_s, last_s, send_sem, recv_sem, local_sem, store_sem,
):
    z, y, x, c = (lax.axis_index(name) for name in ("z", "y", "x", "c"))
    rows = norm_ref.shape[0]
    half = 3 * rows // 4
    mine = y * 4 + x * 2 + c
    has_right, has_left = z < n - 1, z > 0
    number = {}

    def remote(key, src, dst, axis, target):
        slot = number.setdefault(key, len(number))
        return pltpu.make_async_remote_copy(
            src_ref=src, dst_ref=dst, send_sem=send_sem.at[slot], recv_sem=recv_sem.at[slot],
            device_id={axis: target}, device_id_type=pl.DeviceIdType.MESH,
        )

    def when(condition, action):
        if condition is None:
            action()
        else:
            pl.when(condition)(action)

    started = []

    def start(condition, copy):
        when(condition, copy.start)
        started.append((condition, copy))

    def shard(index, unit):
        return w_ref.at[index * 2 + (y if unit == 0 else 1 - y)]

    width, hidden = q_ref.shape[1] // 2, up_ref.shape[1] // 2
    piece = hidden // 2

    def parts(kind, side):
        if kind == 2:
            sources, size, begin = (q_ref, k_ref, v_ref, o_ref), width, side * width
        else:
            sources, size, begin = (up_ref, down_ref), piece, side * hidden + kind * piece
        span = pl.ds(pl.multiple_of(begin, LANES), size)
        return [(ref.at[:, span], pl.ds(i * size, size)) for i, ref in enumerate(sources)]

    def packed(key, kind, side, block, axis, target):
        return [
            remote(key + (i,), source, block.at[:, columns], axis, target)
            for i, (source, columns) in enumerate(parts(kind, side))
        ]

    def along(step, unit, sign, receiving=False):
        index = z - sign * step if receiving else z - sign * (step - 1)
        if step == 1 and unit == 0:
            return packed((step, unit, sign), 0, y, shard(index, unit), "z", z + sign)
        return [remote((step, unit, sign), shard(index, unit), shard(index, unit), "z", z + sign)]

    def start_all(condition, copies):
        for copy in copies:
            start(condition, copy)

    def wait_all(copies):
        for copy in copies:
            copy.wait_recv()


    full, top, low = pl.ds(0, rows), pl.ds(0, half), pl.ds(half, rows - half)
    arrays = ((n_ref, norm_ref, "n"), (c_ref, cot_ref, "c"))
    at_x, at_y, at_xy = y * 4 + (1 - x) * 2 + c, (1 - y) * 4 + x * 2 + c, (1 - y) * 4 + (1 - x) * 2 + c

    barrier = pltpu.get_barrier_semaphore()
    for axis, target in (("x", 1 - x), ("y", 1 - y), ("c", 1 - c)):
        pl.semaphore_signal(
            barrier, inc=1, device_id={axis: target}, device_id_type=pl.DeviceIdType.MESH
        )
    for condition, target in ((has_right, z + 1), (has_left, z - 1)):
        when(condition, functools.partial(
            pl.semaphore_signal, barrier, inc=1, device_id={"z": target},
            device_id_type=pl.DeviceIdType.MESH,
        ))
    pl.semaphore_wait(barrier, 3 + has_right.astype(jnp.int32) + has_left.astype(jnp.int32))

    for condition, sign in ((has_right, 1), (has_left, -1)):
        start_all(condition, along(1, 0, sign))
    start_all(None, packed(("swap",), 0, 1 - y, shard(z, 0), "y", 1 - y))
    swap_in = packed(("swap",), 0, 1 - y, shard(z, 1), "y", 1 - y)
    for array, source, name in arrays:
        for axis in ("x", "y", "c"):
            start(None, remote((name, axis), source, array.at[mine], axis,
                               {"x": 1 - x, "y": 1 - y, "c": 1 - c}[axis]))
    start_all(None, packed(("unit",), 2, 1 - y, unit_ref.at[y], "y", 1 - y))
    unit_swap_in = packed(("unit",), 2, 1 - y, unit_ref.at[1 - y], "y", 1 - y)
    start_all(None, packed(("late",), 1, 1 - y, last_ref.at[y], "y", 1 - y))
    late_swap = packed(("late",), 1, 1 - y, last_ref.at[1 - y], "y", 1 - y)
    pairs = [(norm_ref, rows_s.at[0]), (cot_ref, rows_s.at[1])]
    for kind, block in ((0, first_s), (2, unit_s), (1, last_s)):
        pairs += [(source, block.at[:, columns]) for source, columns in parts(kind, y)]
    loads = [
        pltpu.make_async_copy(source, target, local_sem.at[i])
        for i, (source, target) in enumerate(pairs)
    ]
    stores = [
        pltpu.make_async_copy(source, target, store_sem.at[i])
        for i, (source, target) in enumerate((
            (first_s, shard(z, 0)), (unit_s, unit_ref.at[y]), (last_s, last_ref.at[y]),
            (rows_s.at[0], n_ref.at[mine]), (rows_s.at[1], c_ref.at[mine]),
        ))
    ]
    for load in loads:
        load.start()
    for load in loads:
        load.wait()
    for store in stores:
        store.start()

    def arrive_swap():
        wait_all(swap_in)
        for condition, sign in ((has_right, 1), (has_left, -1)):
            start_all(condition, along(1, 1, sign))

    def arrive_shard(step, unit, sign):
        inside = z - sign * step >= 0 if sign > 0 else z + step < n
        further = has_right if sign > 0 else has_left
        when(inside, functools.partial(wait_all, along(step, unit, sign, True)))
        if step + 1 < n:
            start_all(inside & further, along(step + 1, unit, sign))

    def arrive_rows(array, name, axis):
        index = {"x": at_x, "y": at_y, "c": None}[axis]
        block = array.at[index]
        remote((name, axis), block, block, axis, 0).wait_recv()
        part, on = (low, "y") if axis == "x" else (top, "x")
        piece = array.at[index, part]
        start(None, remote((name, "far", on), piece, piece, on, {"x": 1 - x, "y": 1 - y}[on]))
        start(None, remote((name, "core", axis), block, block, "c", 1 - c))

    def arrive_far(array, name, on):
        part = low if on == "y" else top
        piece = array.at[at_xy, part]
        remote((name, "far", on), piece, piece, on, 0).wait_recv()
        start(None, remote((name, "core", "far", on), piece, piece, "c", 1 - c))

    def arrive_steps(step):
        for unit in (0, 1):
            for sign in (1, -1):
                arrive_shard(step, unit, sign)

    def second_step(half_of, receiving):
        index = y if half_of == 0 else 1 - y
        ways = ((1, has_left if receiving else has_right, right_ref),
                (-1, has_right if receiving else has_left, left_ref))
        for sign, condition, target in ways:
            key = ("second", half_of, sign)
            if half_of == 0:
                copies = packed(key, 2, y, target.at[index], "z", z + sign)
            else:
                copies = [remote(key, unit_ref.at[index], target.at[index], "z", z + sign)]
            if receiving:
                when(condition, functools.partial(wait_all, copies))
            else:
                start_all(condition, copies)

    (norm, _, norm_name), (cot, _, cot_name) = arrays
    arrive_swap()
    arrive_rows(norm, norm_name, "x")
    for sign in (1, -1):
        arrive_shard(1, 0, sign)
    arrive_rows(norm, norm_name, "y")
    for sign in (1, -1):
        arrive_shard(1, 1, sign)
    arrive_rows(cot, cot_name, "x")
    if n > 2:
        arrive_steps(2)
    second_step(0, False)
    arrive_rows(cot, cot_name, "y")
    wait_all(unit_swap_in)
    second_step(1, False)
    for step in range(3, n):
        arrive_steps(step)
    for array, _, name in arrays:
        for on in ("x", "y"):
            arrive_far(array, name, on)
    for array, _, name in arrays:
        for key, index, part in (
            ((name, "c"), y * 4 + x * 2 + 1 - c, full),
            ((name, "core", "x"), y * 4 + (1 - x) * 2 + 1 - c, full),
            ((name, "core", "y"), (1 - y) * 4 + x * 2 + 1 - c, full),
            ((name, "core", "far", "x"), (1 - y) * 4 + (1 - x) * 2 + 1 - c, top),
            ((name, "core", "far", "y"), (1 - y) * 4 + (1 - x) * 2 + 1 - c, low),
        ):
            piece = array.at[index, part]
            remote(key, piece, piece, "c", 0).wait_recv()
    wait_all(late_swap)
    for half_of in (0, 1):
        second_step(half_of, True)
    for store in stores:
        store.wait()
    for condition, copy in started:
        when(condition, copy.wait_send)


def gather_all(n, query, key, value, output_turned, up, down_turned, normed, cotangent):
    rows, columns = normed.shape
    copies = 4 * (n - 1) + 46
    anywhere = pl.BlockSpec(memory_space=pl.ANY)
    heads = 2 * query.shape[1]
    hidden, depth = up.shape[1] // 2, query.shape[0]
    pair = jax.ShapeDtypeStruct((2, depth, heads), query.dtype)
    weights, unit, right, left, last, normed_all, cot_all = pl.pallas_call(
        functools.partial(gather_kernel, n),
        in_specs=[anywhere] * 8,
        out_specs=[anywhere] * 7,
        out_shape=[
            jax.ShapeDtypeStruct((2 * n, depth, hidden), up.dtype),
            pair, pair, pair,
            jax.ShapeDtypeStruct((2, depth, hidden), up.dtype),
            jax.ShapeDtypeStruct((8, rows, columns), normed.dtype),
            jax.ShapeDtypeStruct((8, rows, columns), cotangent.dtype),
        ],
        scratch_shapes=[
            pltpu.VMEM((2, rows, columns), normed.dtype),
            pltpu.VMEM((depth, hidden), up.dtype),
            pltpu.VMEM((depth, heads), query.dtype),
            pltpu.VMEM((depth, hidden), up.dtype),
            pltpu.SemaphoreType.DMA((copies,)),
            pltpu.SemaphoreType.DMA((copies,)),
            pltpu.SemaphoreType.DMA((10,)),
            pltpu.SemaphoreType.DMA((5,)),
        ],
        cost_estimate=pl.CostEstimate(flops=0, transcendentals=0, bytes_accessed=200 << 20),
        compiler_params=pltpu.CompilerParams(collective_id=0, has_side_effects=True),
        name="gather_rows",
    )(query, key, value, output_turned, up, down_turned, normed, cotangent)
    flat = lambda array: array.reshape(-1, array.shape[-1])
    return tuple(map(flat, (weights, unit, right, left, last, normed_all, cot_all)))


def chain_step(step, n, right, left):
    return (
        lax.ppermute(right, "z", [(i, i + 1) for i in range(step - 1, n - 1)]),
        lax.ppermute(left, "z", [(i, i - 1) for i in range(1, n - step + 1)]),
    )


def assemble(unit, right, left, n, z):
    rows, columns = unit.shape
    whole = jnp.zeros((n * rows, columns), unit.dtype)
    for k in range(n):
        piece = unit if k == 0 else jnp.where(z >= k, right[k], left[n - k])
        row = lax.rem(z - k + n, n) * rows
        whole = lax.dynamic_update_slice(whole, piece, (row, jnp.int32(0)))
    return whole


def scatter_pieces(k, grads, n, z, received):
    rows = grads.shape[0] // n

    def piece(index, got):
        own = lax.dynamic_slice_in_dim(grads, jnp.clip(index, 0, n - 1) * rows, rows, 0)
        return own if got is None else add_low(own, got)

    return piece(z - k, received[0]), piece(z + k, received[1])


def scatter_step(k, grads, n, z, received):
    to_left, to_right = scatter_pieces(k, grads, n, z, received)
    return (
        lax.ppermute(to_left, "z", [(r, r - 1) for r in range(k, n)]),
        lax.ppermute(to_right, "z", [(r, r + 1) for r in range(0, n - k)]),
    )


def scatter_end(grads, n, z, received):
    rows = grads.shape[0] // n
    own = lax.dynamic_slice_in_dim(grads, z * rows, rows, 0).astype(F32)
    return own + received[0].astype(F32) + received[1].astype(F32)


def tail_kernel(
    n, g_any, hw_ref, fw_ref, lw_ref, dq_ref, d0_ref, d1_ref, at_ref, a0_ref, a1_ref,
    left_ref, right_ref, own_ref, std_any, cot_any, tokens_any, vec_ref, lines_ref, inv_ref,
    keep_ref, take_ref, heads_keep_ref, heads_take_ref, out_ref, mixed_ref, sums_ref,
    g_ref, std_ref, hw_s, fw_s, lw_s, rows_s, stage, zrecv, give, heads_recv, heads_own, heads_give, both, xtop_2, ylow_2, ytop_2, xlow_2,
    top_2, low_2, vstage, vrecv, send_sem, recv_sem, load_sem, rows_sem,
):
    z, y, x, c = (lax.axis_index(name) for name in ("z", "y", "x", "c"))
    rows, columns = out_ref.shape
    wide, wide_heads = give.shape[0], heads_give.shape[0]
    half = rows // 2
    rest = rows - half
    number, started = {}, []

    def remote(key, src, dst, axis, target):
        slot = number.setdefault(key, len(number))
        return pltpu.make_async_remote_copy(
            src_ref=src, dst_ref=dst, send_sem=send_sem.at[slot], recv_sem=recv_sem.at[slot],
            device_id={axis: target}, device_id_type=pl.DeviceIdType.MESH,
        )

    def when(condition, action):
        if condition is None:
            action()
        else:
            pl.when(condition)(action)

    def start(condition, copy):
        when(condition, copy.start)
        started.append((condition, copy))

    def each(count, size, body):
        def step(i, carry):
            body(pl.ds(pl.multiple_of(i * size, size), size))
            return carry
        lax.fori_loop(0, count // size, step, 0)

    barrier = pltpu.get_barrier_semaphore()
    greet = [(None, "x", 1 - x), (None, "y", 1 - y), (None, "c", 1 - c)]
    greet += [(z < n - 1, "z", z + 1), (z > 0, "z", z - 1)]
    for step in (2 ** i for i in range(1, n.bit_length() - 1)):
        greet.append((None, "z", jnp.bitwise_xor(z, step)))
    for condition, axis, target in greet:
        when(condition, functools.partial(
            pl.semaphore_signal, barrier, inc=1, device_id={axis: target},
            device_id_type=pl.DeviceIdType.MESH))

    loads = [
        pltpu.make_async_copy(source, target, load_sem.at[i])
        for i, (source, target) in enumerate(
            ((hw_ref, hw_s), (fw_ref, fw_s), (lw_ref, lw_s), (g_any, g_ref), (std_any, std_ref),
             (own_ref, heads_own)))
    ]
    for load in loads:
        load.start()

    firsts, lasts = fw_ref.shape[1] // 2, lw_ref.shape[1] // 2
    heads = dq_ref.shape[1]
    sums = (
        ((dq_ref, heads, hw_s, 0), (d0_ref, firsts, fw_s, 0), (d1_ref, lasts, lw_s, 0)),
        ((at_ref, heads // 3, hw_s, heads), (a0_ref, firsts, fw_s, firsts),
         (a1_ref, lasts, lw_s, lasts)),
    )
    sides = (1 - y, y)
    jobs = [(a, own, j) for a in (0, 1) for own in (False, True) for j in sides]

    def row_loads(number_of):
        a, own, j = jobs[number_of]
        slot, core, copies, at = number_of % 2, c if own else 1 - c, [], 0
        for p, (left, width, _, _) in enumerate(sums[a]):
            for i in (0, 1):
                block = j * 4 + i * 2 + core
                source = left.at[pl.ds(pl.multiple_of(block * rows, rows), rows)]
                target = rows_s.at[slot, pl.ds(i * rows, rows), pl.ds(at, width)]
                copies.append(pltpu.make_async_copy(source, target, rows_sem.at[slot, p * 2 + i]))
            at += width
        return copies

    def job(number_of):
        a, own, j = jobs[number_of]
        slot = number_of % 2
        if number_of + 1 < len(jobs):
            for copy in row_loads(number_of + 1):
                copy.start()
        for copy in row_loads(number_of):
            copy.wait()
        if own:
            for i in (0, 1):
                core_copy(a, number_of % 2, i).wait_recv()
        elif a == 1:
            for i in (0, 1):
                core_copy(0, number_of % 2, i).wait_send()
        size = min(512, columns)

        def tile(t, carry):
            span = pl.ds(pl.multiple_of(t * size, size), size)
            acc, at = None, 0
            for left, width, weights, column in sums[a]:
                part = dot(
                    rows_s[slot, :, at : at + width], weights[span, column : column + width], NT)
                acc = part if acc is None else acc + part
                at += width
            for i in (0, 1):
                piece = acc[i * rows : (i + 1) * rows]
                if own:
                    both[a, j * 2 + i, :, span] = (
                        piece + both[a, j * 2 + i, :, span].astype(F32)).astype(BF16)
                else:
                    stage[j * 2 + i, :, span] = piece.astype(BF16)
            return carry

        lax.fori_loop(0, columns // size, tile, 0)
        if own and a == 0:
            start(None, first_copy(a, "xtop", number_of % 2))
            if number_of % 2 == 0:
                for i in (0, 1):
                    start(None, first_copy(a, "ylow", i))
        if not own:
            for i in (0, 1):
                copy = core_copy(a, number_of % 2, i)
                copy.start()

    def core_copy(a, u, i):
        place = sides[u] * 2 + i
        return remote(("core", a, u, i), stage.at[place], both.at[a, place], "c", 1 - c)

    for copy in row_loads(0):
        copy.start()
    always = sum(condition is None for condition, _, _ in greet)
    pl.semaphore_wait(barrier, always + sum(
        condition.astype(jnp.int32) for condition, _, _ in greet if condition is not None))

    def first_copy(a, name, j):
        if name == "xtop":
            source = both.at[a, sides[j] * 2 + 1 - x, pl.ds(0, half)]
            return remote((name, a, j), source, xtop_2.at[a, j], "x", 1 - x)
        source = both.at[a, (1 - y) * 2 + j, pl.ds(half, rest)]
        return remote((name, a, j), source, ylow_2.at[a, j], "y", 1 - y)

    def second_copy(a, name):
        if name == "ytop":
            return remote((name, a), top_2.at[a], ytop_2.at[a], "y", 1 - y)
        return remote((name, a), low_2.at[a], xlow_2.at[a], "x", 1 - x)

    def first_send(a):
        for j in (0, 1):
            start(None, first_copy(a, "xtop", j))
            start(None, first_copy(a, "ylow", j))

    def first_arrive(a):
        for j in (0, 1):
            first_copy(a, "xtop", j).wait_recv()
            first_copy(a, "ylow", j).wait_recv()

        def upper(part):
            top_2[a, part, :] = (
                both[a, (1 - y) * 2 + x, part, :].astype(F32)
                + xtop_2[a, 0, part, :].astype(F32)
            ).astype(BF16)

        def lower(part):
            low_part = pl.ds(part.start + half, part.size)
            low_2[a, part, :] = (
                both[a, y * 2 + 1 - x, low_part, :].astype(F32)
                + ylow_2[a, 1 - x, part, :].astype(F32)
            ).astype(BF16)

        each(half, 32, upper)
        each(rest, 32, lower)
        start(None, second_copy(a, "ytop"))
        start(None, second_copy(a, "xlow"))

    def second_arrive(a):
        second_copy(a, "ytop").wait_recv()
        second_copy(a, "xlow").wait_recv()
        target = (out_ref, mixed_ref)[a]

        def finish(first, part, placed, last):
            value = (
                both[a, y * 2 + x, placed, :].astype(F32) + first[part, :].astype(F32)
                + last[part, :].astype(F32)
            )
            if a == 0:
                standard = std_ref[placed, :]
                vstage[0, 0:1, :] += jnp.sum(value * standard, 0, keepdims=True)
                vstage[0, 1:2, :] += jnp.sum(value, 0, keepdims=True)
                scaled = value * lines_ref[0:1, :]
                mean = jnp.mean(scaled, 1, keepdims=True)
                along = jnp.mean(scaled * standard, 1, keepdims=True)
                target[placed, :] = stage[0, placed, :].astype(F32) + inv_ref[placed, :] * (
                    scaled - mean - standard * along)
            else:
                whole = stage[1, placed, :].astype(F32) + value + lines_ref[1:2, :]
                target[placed, :] = whole.astype(BF16)

        def upper(part):
            finish(xtop_2.at[a, 1], part, part, ytop_2.at[a])

        def lower(part):
            finish(ylow_2.at[a, x], part, pl.ds(part.start + half, part.size), xlow_2.at[a])

        each(half, 32, upper)
        each(rest, 32, lower)

    def block_of(direction, k, u):
        index = (z - k if direction == 0 else z + k) * 2 + sides[u]
        return pl.ds(pl.multiple_of(index * rows, rows), rows)

    def z_copy(direction, k, u, src):
        target = z - 1 if direction == 0 else z + 1
        return remote((direction, k, u), src, zrecv.at[direction, k - 1, u], "z", target)

    def z_first(direction):
        edge = z == n - 1 if direction == 0 else z == 0
        for k in range(n - 1, 0, -1):
            for u in (0, 1):
                start(edge, z_copy(direction, k, u, g_any.at[:, block_of(direction, k, u)]))

    def z_step(k, u):
        for direction in (0, 1):
            if direction == 0:
                inside = (z >= k) & (z < n - 1)
            else:
                inside = (n - 1 - z >= k) & (z > 0)
            held = zrecv.at[direction, k, u]

            def add():
                z_copy(direction, k + 1, u, held).wait_recv()
                block = block_of(direction, k, u)

                def body(part):
                    held[part, :] = (
                        g_ref[part, block].astype(F32) + held[part, :].astype(F32)
                    ).astype(BF16)

                each(wide, 256, body)

            when(inside, add)
            start(inside, z_copy(direction, k, u, held))

    def z_last(u, target):
        block = block_of(0, 0, u)

        def first(part):
            target[part, :] = g_ref[part, block].astype(F32)

        each(wide, 256, first)
        for direction in (0, 1):
            held = zrecv.at[direction, 0, u]

            def add():
                z_copy(direction, 1, u, held).wait_recv()

                def body(part):
                    target[part, :] += held[part, :].astype(F32)

                each(wide, 256, body)

            when(z < n - 1 if direction == 0 else z > 0, add)

    def heads_copy(direction, u):
        span = pl.ds(pl.multiple_of(sides[u] * rows, rows), rows)
        source = (left_ref, right_ref)[direction].at[:, span]
        return remote(
            ("heads", direction, u), source, heads_recv.at[direction, :, span], "z",
            z - 1 if direction == 0 else z + 1)

    def heads_send():
        for u in (0, 1):
            start(z > 0, heads_copy(0, u))
            start(z < n - 1, heads_copy(1, u))

    def heads_last(u, target):
        span = pl.ds(pl.multiple_of(sides[u] * rows, rows), rows)

        def first(part):
            target[part, :] = heads_own[part, span].astype(F32)

        each(wide_heads, 256, first)
        for direction in (0, 1):
            def add():
                heads_copy(direction, u).wait_recv()

                def body(part):
                    target[part, :] += heads_recv[direction, part, span].astype(F32)

                each(wide_heads, 256, body)

            when(z < n - 1 if direction == 0 else z > 0, add)

    steps = [(k, u) for k in range(n - 2, 0, -1) for u in (0, 1)]

    def z_next():
        if steps:
            z_step(*steps.pop(0))

    for direction in (0, 1):
        z_first(direction)
    vstage[0] = vec_ref[...]
    for load in loads[:3]:
        load.wait()
    job(0)
    job(1)
    for load in loads[3:]:
        load.wait()
    z_next()
    job(2)
    job(3)
    heads_send()
    z_next()
    job(4)
    job(5)
    z_next()
    job(6)
    job(7)
    first_arrive(0)
    first_send(1)
    for u in (0, 1):
        for i in (0, 1):
            core_copy(1, u, i).wait_send()
    late = [
        pltpu.make_async_copy(source, stage.at[i], load_sem.at[6 + i])
        for i, source in enumerate((cot_any, tokens_any))
    ]
    for load in late:
        load.start()
    for load in late:
        load.wait()
    while steps:
        z_next()
    second_arrive(0)

    turns = [("z", jnp.bitwise_xor(z, 2 ** i)) for i in range(n.bit_length() - 1)]
    turns += [("y", 1 - y), ("x", 1 - x), ("c", 1 - c)]
    line = lax.broadcasted_iota(jnp.int32, vec_ref.shape, 0)

    def exchange(i):
        axis, target = turns[i]
        return remote(("vec", i), vstage.at[i], vrecv.at[i], axis, target)

    def turn(i):
        exchange(i).wait_recv()
        axis, _ = turns[i]
        old, new = vstage[i], vrecv[i]
        result = sums_ref if i == len(turns) - 1 else vstage.at[i + 1]
        result[...] = old + jnp.where((line < 3) | (axis == "z"), new, 0.0)
        if axis == "y":
            result[4:5, :] = new[3:4, :]
        if i + 1 < len(turns):
            start(None, exchange(i + 1))

    start(None, exchange(0))

    def swapped(key, source, target, length, received):
        def lower_precision(part):
            target[part, :] = source[part, :].astype(BF16)

        each(length, 256, lower_precision)
        copy = remote(key, target, received, "y", 1 - y)
        start(None, copy)
        return copy

    first_arrive(1)
    z_last(0, keep_ref)
    swap = swapped("swap", keep_ref, give, wide, take_ref)
    turn(0)
    turn(1)
    heads_last(0, heads_keep_ref)
    heads_swap = swapped("heads swap", heads_keep_ref, heads_give, wide_heads, heads_take_ref)
    turn(2)
    z_last(1, keep_ref)
    turn(3)
    heads_last(1, heads_keep_ref)
    for i in range(4, len(turns)):
        turn(i)
    second_arrive(1)
    swap.wait_recv()
    heads_swap.wait_recv()
    for condition, copy in started:
        when(condition, copy.wait_send)


def tail(
    n, grads_turned, weights, lefts, lefts_out, heads_turned, standard, cotangent, tokens, vector,
    lines, inv_scale,
):
    rows, columns = standard.shape
    wide, wide_heads = grads_turned.shape[0], heads_turned[0].shape[0]
    half = rows // 2
    inside = pl.BlockSpec(memory_space=pltpu.VMEM)
    anywhere = pl.BlockSpec(memory_space=pl.ANY)
    copies = 4 * (n - 1) + 46
    low = lambda *shape: pltpu.VMEM(shape, BF16)
    small = vector.shape
    depth = sum(left.shape[1] for left in lefts)
    return pl.pallas_call(
        functools.partial(tail_kernel, n),
        in_specs=[anywhere] * 16 + [inside] * 3,
        out_specs=[inside] * 7,
        out_shape=[
            jax.ShapeDtypeStruct((wide, rows), F32),
            jax.ShapeDtypeStruct((wide, rows), BF16),
            jax.ShapeDtypeStruct((wide_heads, rows), F32),
            jax.ShapeDtypeStruct((wide_heads, rows), BF16),
            jax.ShapeDtypeStruct((rows, columns), F32),
            jax.ShapeDtypeStruct((rows, columns), BF16),
            jax.ShapeDtypeStruct(small, F32),
        ],
        scratch_shapes=[low(*grads_turned.shape), pltpu.VMEM(standard.shape, F32)] + [
            low(*array.shape) for array in weights
        ] + [
            low(2, 2 * rows, depth), low(4, rows, columns),
            low(2, n - 1, 2, wide, rows), low(wide, rows),
            low(2, wide_heads, 2 * rows), low(wide_heads, 2 * rows), low(wide_heads, rows),
            low(2, 4, rows, columns),
            low(2, 2, half, columns), low(2, 2, rows - half, columns),
            low(2, half, columns), low(2, rows - half, columns),
            low(2, half, columns), low(2, rows - half, columns),
            pltpu.VMEM((8,) + small, F32), pltpu.VMEM((8,) + small, F32),
            pltpu.SemaphoreType.DMA((copies,)),
            pltpu.SemaphoreType.DMA((copies,)),
            pltpu.SemaphoreType.DMA((8,)),
            pltpu.SemaphoreType.DMA((2, 6)),
        ],
        cost_estimate=pl.CostEstimate(flops=0, transcendentals=0, bytes_accessed=200 << 20),
        compiler_params=pltpu.CompilerParams(
            collective_id=1, has_side_effects=True, vmem_limit_bytes=63 << 20
        ),
        name="scatter_rest",
    )(
        grads_turned, *weights, *lefts, *lefts_out, *heads_turned, standard, cotangent, tokens,
        vector, lines, inv_scale,
    )


def sum_small(array, axes):
    for axis in axes:
        size = lax.axis_size(axis)
        if size & (size - 1):
            array = lax.psum(array, axis)
            continue
        step = 1
        while step < size:
            array = array + lax.ppermute(array, axis, [(i, i ^ step) for i in range(size)])
            step *= 2
    return array


def pick(array, index, axis):
    return lax.dynamic_index_in_dim(array, index, axis, keepdims=False)


def add_low(left, right):
    return (left.astype(F32) + right.astype(F32)).astype(BF16)


def plane_scatter(partial, y, x, c):
    rows, columns = partial.shape[0] // 8, partial.shape[1]
    half = rows // 2
    parts = partial.reshape(2, 2, 2, rows, columns)
    acc = add_low(pick(parts, c, 2), lax.ppermute(pick(parts, 1 - c, 2), "c", SWAP))
    top, low = acc[:, :, :half], acc[:, :, half:]
    top = add_low(pick(top, x, 1), lax.ppermute(pick(top, 1 - x, 1), "x", SWAP))
    low = add_low(pick(low, y, 0), lax.ppermute(pick(low, 1 - y, 0), "y", SWAP))
    top = pick(top, y, 0).astype(F32) + lax.ppermute(pick(top, 1 - y, 0), "y", SWAP).astype(F32)
    low = pick(low, x, 0).astype(F32) + lax.ppermute(pick(low, 1 - x, 0), "x", SWAP).astype(F32)
    return jnp.concatenate([top, low], 0)


def in_order(y, own, other, axis):
    return jnp.where(
        y == 0, jnp.concatenate([own, other], axis), jnp.concatenate([other, own], axis)
    )


def on_device(
    n,
    tokens, norm_gain, norm_bias,
    query_weight, query_bias, key_weight, key_bias, value_weight, value_bias,
    output_weight, output_bias, up_weight, up_bias, down_weight, down_bias,
    doc_split, cotangent,
):
    z, y, x, c = (lax.axis_index(name) for name in ("z", "y", "x", "c"))
    shard_rows = query_weight.shape[0]
    width = query_weight.shape[1] // 2
    hidden_width = up_weight.shape[1] // 2
    chunks = 2
    piece = hidden_width // chunks

    def row(array, start, size):
        return lax.dynamic_slice_in_dim(array, start, size, 0)

    gain_wide = norm_gain.astype(F32)
    tokens_wide = tokens.astype(F32)
    row_mean = jnp.mean(tokens_wide, -1, keepdims=True)
    centred = tokens_wide - row_mean
    inv_scale = lax.rsqrt(jnp.mean(centred * centred, -1, keepdims=True) + EPS)
    standard = centred * inv_scale
    normed = (standard * gain_wide + norm_bias.astype(F32)).astype(BF16)
    phase = lax.optimization_barrier
    other_split = lax.ppermute(doc_split, "y", SWAP)
    splits = in_order(y, doc_split, other_split, 0)
    seq_len = 4 * normed.shape[0]
    cosine, sine = turn_tables(splits, seq_len)

    right, left = [None] * n, [None] * n
    first_weights, heads_unit, right[1], left[1], last_unit, normed_all, cot_all = gather_all(
        n, query_weight, key_weight, value_weight, output_weight.T, up_weight, down_weight.T,
        normed, cotangent,
    )
    first_weights, heads_unit, last_unit, normed_all, cot_all, right[1], left[1], cosine, sine = phase(
        (first_weights, heads_unit, last_unit, normed_all, cot_all, right[1], left[1], cosine, sine)
    )

    def hidden_local(weights, chunk):
        bias = row(up_bias, y * hidden_width + chunk * piece, piece).astype(F32)[None]
        return hidden_part(normed_all, cot_all, weights, bias)

    def weight_grads(grad_columns, columns):
        return jnp.concatenate(
            [dot(normed_all, grad_columns, TN).astype(BF16), dot(cot_all, columns, TN).astype(BF16)], 1
        )

    def gather_step(step, source):
        return chain_step(step, n, right[step - 1], left[step - 1]) if step > 1 else chain_step(
            1, n, source, source)

    activated_0, grad_hidden_0, hidden_sum_0 = hidden_local(first_weights, 0)
    right[2], left[2] = gather_step(2, None)
    activated_0, grad_hidden_0, normed_all, cot_all, right[2], left[2] = phase(
        (activated_0, grad_hidden_0, normed_all, cot_all, right[2], left[2])
    )
    grads_first = weight_grads(grad_hidden_0, activated_0)
    for step in range(3, n):
        right[step], left[step] = gather_step(step, None)
    grads_first, activated_0, last_unit, normed_all, cot_all, right[3:], left[3:] = phase(
        (grads_first, activated_0, last_unit, normed_all, cot_all, right[3:], left[3:])
    )
    head_weights = assemble(heads_unit, right, left, n, z)
    qkv_weight, output_turned = head_weights[:, : 3 * width], head_weights[:, 3 * width :]

    qkv_bias = jnp.concatenate(
        [row(b, y * width, width) for b in (query_bias, key_bias, value_bias)]
    ).astype(F32)
    qkv = dot(normed_all, qkv_weight) + qkv_bias
    grad_attended = dot(cot_all, output_turned).astype(BF16)
    right[1], left[1] = gather_step(1, last_unit)
    qkv, grad_attended, normed_all, cot_all, right[1], left[1] = phase(
        (qkv, grad_attended, normed_all, cot_all, right[1], left[1])
    )
    found = attention(0, splits, qkv, grad_attended, cosine, sine, ())
    right[2], left[2] = gather_step(2, None)
    first_in = scatter_step(n - 1, grads_first, n, z, (None, None))
    found, qkv, grad_attended, normed_all, cot_all, right[2], left[2], first_in, grads_first = phase(
        (found, qkv, grad_attended, normed_all, cot_all, right[2], left[2], first_in, grads_first)
    )
    for index in range(1, splits.shape[0]):
        found = attention(index, splits, qkv, grad_attended, cosine, sine, found)
    for step in range(3, n):
        right[step], left[step] = gather_step(step, None)
    for k in range(n - 2, n - 3, -1):
        first_in = scatter_step(k, grads_first, n, z, first_in)
    found, normed_all, cot_all, right[3:], left[3:], first_in, grads_first = phase(
        (found, normed_all, cot_all, right[3:], left[3:], first_in, grads_first)
    )
    attended, grad_qkv = found
    grads_heads = weight_grads(grad_qkv, attended)
    for k in range(n - 3, 0, -1):
        first_in = scatter_step(k, grads_first, n, z, first_in)
    grads_heads, attended, grad_qkv, normed_all, cot_all, last_unit, first_in, grads_first = phase(
        (grads_heads, attended, grad_qkv, normed_all, cot_all, last_unit, first_in, grads_first)
    )
    first_sum = scatter_end(grads_first, n, z, first_in)

    last_weights = assemble(last_unit, right, left, n, z)
    activated_1, grad_hidden_1, hidden_sum_1 = hidden_local(last_weights, 1)
    heads_in = scatter_step(n - 1, grads_heads, n, z, (None, None))
    (last_weights, activated_1, grad_hidden_1, attended, grad_qkv, heads_in, grads_heads,
     normed_all, cot_all) = phase(
        (last_weights, activated_1, grad_hidden_1, attended, grad_qkv, heads_in, grads_heads,
         normed_all, cot_all)
    )
    for k in range(n - 2, max(n - 3, 1), -1):
        heads_in = scatter_step(k, grads_heads, n, z, heads_in)
    grads_last = weight_grads(grad_hidden_1, activated_1)
    qkv_sum = jnp.sum(grad_qkv, 0, dtype=F32)[None]
    bias_row = jnp.concatenate([qkv_sum, hidden_sum_0, hidden_sum_1], 1)
    cot_wide = cotangent.astype(F32)
    cot_sum = jnp.sum(cot_wide, 0)[None]
    grads_last, heads_in, grads_heads, bias_row, cot_sum = phase(
        (grads_last, heads_in, grads_heads, bias_row, cot_sum)
    )
    def halves(total):
        keep = row(total, y * shard_rows, shard_rows)
        give = row(total, (1 - y) * shard_rows, shard_rows).astype(BF16)
        return keep, lax.ppermute(give, "y", SWAP).astype(F32)

    first_keep, first_take = halves(first_sum)

    out_bias = output_bias.astype(F32) + down_bias.astype(F32)
    if n == 4 and bias_row.shape[1] <= cot_sum.shape[1]:
        spread = cot_sum.shape[1]
        vector = jnp.concatenate([
            jnp.zeros((2, spread), F32), cot_sum,
            jnp.pad(bias_row, ((0, 0), (0, spread - bias_row.shape[1]))),
            jnp.zeros((4, spread), F32),
        ])
        left_piece, right_piece = scatter_pieces(1, grads_heads, n, z, heads_in)
        own_piece = row(grads_heads, z * 2 * shard_rows, 2 * shard_rows)
        lines = jnp.concatenate(
            [gain_wide[None], out_bias[None], jnp.zeros((6, spread), F32)]
        )
        last_keep, last_take, heads_keep, heads_take, grad_tokens, out, sums = tail(
            n, grads_last.T, (head_weights, first_weights, last_weights),
            (grad_qkv, grad_hidden_0, grad_hidden_1), (attended, activated_0, activated_1),
            (left_piece.T, right_piece.T, own_piece.T), standard, cotangent, tokens, vector,
            lines, inv_scale,
        )
        last_keep, last_take = last_keep.T, last_take.astype(F32).T
        heads_keep, heads_take = heads_keep.T, heads_take.astype(F32).T
        norm_sums = sums[:3]
        bias_rows = in_order(y, sums[3:4], sums[4:5], 0)[:, : bias_row.shape[1]]
    else:
        for k in range(n - 3, 0, -1):
            heads_in = scatter_step(k, grads_heads, n, z, heads_in)
        heads_keep, heads_take = halves(scatter_end(grads_heads, n, z, heads_in))
        partial_out = sum_dots(
            (attended, activated_0, activated_1),
            ((head_weights, width, 3), (first_weights, piece, 1), (last_weights, piece, 1)),
        )
        grad_normed_part = sum_dots(
            (grad_qkv, grad_hidden_0, grad_hidden_1),
            ((head_weights, 3 * width, 0), (first_weights, piece, 0), (last_weights, piece, 0)),
        )
        last_in = (None, None)
        for k in range(n - 1, 0, -1):
            last_in = scatter_step(k, grads_last, n, z, last_in)
        last_keep, last_take = halves(scatter_end(grads_last, n, z, last_in))
        grad_normed = plane_scatter(grad_normed_part, y, x, c)
        mixed = plane_scatter(partial_out, y, x, c)
        norm_sums = sum_small(
            jnp.concatenate([
                jnp.sum(grad_normed * standard, 0)[None], jnp.sum(grad_normed, 0)[None], cot_sum
            ]),
            ("c", "x", "y", "z"),
        )
        grad_scaled = grad_normed * gain_wide
        grad_tokens = cot_wide + inv_scale * (
            grad_scaled
            - jnp.mean(grad_scaled, -1, keepdims=True)
            - standard * jnp.mean(grad_scaled * standard, -1, keepdims=True)
        )
        out = (tokens_wide + mixed + out_bias).astype(BF16)
        bias_row = sum_small(bias_row, ("z",))
        bias_rows = in_order(y, bias_row, lax.ppermute(bias_row, "y", SWAP), 0)
    grad_norm_gain, grad_norm_bias, grad_out_bias = norm_sums

    def joined(start, size):
        return in_order(
            y, heads_keep[:, start : start + size], heads_take[:, start : start + size], 1
        )

    grad_query_weight, grad_key_weight, grad_value_weight, grad_output_turned = (
        joined(part * width, width) for part in range(4)
    )
    hidden_halves = [(first_keep, first_take), (last_keep, last_take)]

    def side(which, start):
        return jnp.concatenate([pair[which][:, start : start + piece] for pair in hidden_halves], 1)

    grad_up_weight = in_order(y, side(0, 0), side(1, 0), 1)
    grad_down_turned = in_order(y, side(0, piece), side(1, piece), 1)

    grad_query_bias, grad_key_bias, grad_value_bias = (
        bias_rows[:, part * width : (part + 1) * width].reshape(-1) for part in range(3)
    )
    grad_up_bias = bias_rows[:, 3 * width :].reshape(-1)

    return (
        out, grad_tokens, grad_norm_gain, grad_norm_bias,
        grad_query_weight, grad_query_bias, grad_key_weight, grad_key_bias,
        grad_value_weight, grad_value_bias, grad_output_turned.T, grad_out_bias,
        grad_up_weight, grad_up_bias, grad_down_turned.T, grad_out_bias,
    )


def solution(mesh):
    n = mesh.shape["dp"] // 2
    grid = Mesh(mesh.devices.reshape(n, 2, mesh.shape["tensor"] // 2, 2), ("z", "y", "x", "c"))
    dp, tensor = ("z", "y"), ("x", "c")
    rows = P(dp + tensor, None)
    whole, split = P(), P(tensor)
    wide, tall = P(dp, tensor), P(tensor, dp)
    in_specs = (
        rows, whole, whole, wide, split, wide, split, wide, split,
        tall, whole, wide, split, tall, whole, P(dp), rows,
    )
    out_specs = (
        rows, rows, whole, whole, wide, split, wide, split, wide, split,
        tall, whole, wide, split, tall, whole,
    )
    return jax.shard_map(
        functools.partial(on_device, n),
        mesh=grid, in_specs=in_specs, out_specs=out_specs, check_vma=False,
    )
```

```python
import functools

import jax
import jax.numpy as jnp
from jax import lax
from jax.experimental import pallas as pl
from jax.experimental.pallas import tpu as pltpu
from jax.sharding import Mesh, PartitionSpec as P

HEAD_DIM = 64
ROT = 32
BLOCK = 256
EPS = 1e-05
LANES = 128
F32 = jnp.float32
BF16 = jnp.bfloat16


SWAP = [(0, 1), (1, 0)]
NT = (((1,), (1,)), ((), ()))
TN = (((0,), (0,)), ((), ()))
NN = (((1,), (0,)), ((), ()))


def dot(left, right, dims=NN):
    return lax.dot_general(left, right, dims, preferred_element_type=F32)


def spin(value, cosine, sine):
    lane = lax.broadcasted_iota(jnp.int32, value.shape, 1) % HEAD_DIM
    half = ROT // 2
    ahead = pltpu.roll(value, LANES - half, 1)
    behind = pltpu.roll(value, half, 1)
    return value * cosine + jnp.where(lane < half, ahead, behind) * sine


def attention_kernel(
    index, earlier, split_ref, qkv_ref, grad_ref, cos_ref, sin_ref, *refs
):
    (att_ref, dqkv_ref, *scratch) = refs[earlier:]
    attention_body(index, split_ref, qkv_ref, grad_ref, cos_ref, sin_ref, att_ref, dqkv_ref, *scratch)


def attention_body(
    index, split_ref, qkv_ref, grad_ref, cos_ref, sin_ref, att_ref, dqkv_ref,
    q_s, k_s, v_s, g_s, b_s, dq_s, dk_s, dv_s, cos_s, sin_s,
):
    seq_len, width = grad_ref.shape
    first = split_ref[index] // BLOCK
    scale = HEAD_DIM ** (-0.5)
    per = LANES // HEAD_DIM
    rest = jnp.zeros((HEAD_DIM - ROT, seq_len), F32)
    cos_part, sin_part = cos_ref[...], sin_ref[...]
    cos_s[...] = jnp.concatenate([cos_part, cos_part, rest + 1.0] * per, 0).T
    sin_s[...] = jnp.concatenate([-sin_part, sin_part, rest] * per, 0).T

    def one_pair(pair, carry):
        def cols(part):
            return pl.ds(pl.multiple_of(part * width + pair * LANES, LANES), LANES)

        cosine, sine = cos_s[...], sin_s[...]
        head_of = lax.broadcasted_iota(jnp.int32, (seq_len, LANES), 1) // HEAD_DIM
        query = spin(qkv_ref[:, cols(0)], cosine, sine).astype(BF16)
        key = spin(qkv_ref[:, cols(1)], cosine, sine).astype(BF16)
        value = qkv_ref[:, cols(2)].astype(BF16)
        grad = grad_ref[:, cols(0)]
        query = (query.astype(F32) * scale).astype(BF16)
        turned_back = (key.astype(F32) * scale).astype(BF16)
        for head in range(per):
            here = head_of == head
            q_s[head] = jnp.where(here, query, 0).astype(BF16)
            k_s[head] = jnp.where(here, key, 0).astype(BF16)
            b_s[head] = jnp.where(here, turned_back, 0).astype(BF16)
            v_s[head] = jnp.where(here, value, 0).astype(BF16)
            g_s[head] = jnp.where(here, grad, 0).astype(BF16)
        dk_s[...] = jnp.zeros_like(dk_s)
        dv_s[...] = jnp.zeros_like(dv_s)

        def one_block(block, inner):
            begin = jnp.where(block >= first, first, 0)
            rows = pl.ds(pl.multiple_of(block * BLOCK, BLOCK), BLOCK)

            def work(count):
                span = pl.ds(pl.multiple_of(begin * BLOCK, BLOCK), count * BLOCK)
                held = None
                for head in range(per):
                    q, g = q_s[head, rows, :], g_s[head, rows, :]
                    scores = dot(k_s[head, span, :], q, NT)
                    top = jnp.max(scores, 0, keepdims=True)
                    power = jnp.exp(scores - top)
                    prob = power * (1.0 / jnp.sum(power, 0, keepdims=True))
                    low = prob.astype(BF16)
                    dprob = dot(v_s[head, span, :], g, NT)
                    mean = jnp.sum(prob * dprob, 0, keepdims=True)
                    dscore = (prob * (dprob - mean)).astype(BF16)
                    parts = (
                        dot(dscore, q), dot(low, g),
                        dot(dscore, b_s[head, span, :], TN), dot(low, v_s[head, span, :], TN),
                    )
                    held = parts if held is None else [a + b for a, b in zip(held, parts)]
                dk, dv, dq, found = held
                dq_s[rows, :] = dq
                att_ref[rows, cols(0)] = found.astype(BF16)
                dk_s[span, :] += dk
                dv_s[span, :] += dv

            for count in range(1, seq_len // BLOCK):
                pl.when(block - begin == count - 1)(functools.partial(work, count))
            return inner

        lax.fori_loop(0, seq_len // BLOCK, one_block, 0)
        dqkv_ref[:, cols(0)] = spin(dq_s[...], cosine, -sine).astype(BF16)
        dqkv_ref[:, cols(1)] = spin(dk_s[...], cosine, -sine).astype(BF16)
        dqkv_ref[:, cols(2)] = dv_s[...].astype(BF16)
        return carry

    lax.fori_loop(0, width // LANES, one_pair, 0)


def attention(index, splits, qkv, grad, cosine, sine, earlier):
    count = splits.shape[0]
    rows, width = grad.shape
    seq_len = rows // count
    per = LANES // HEAD_DIM

    def spec(columns):
        return pl.BlockSpec((seq_len, columns), lambda i, split: (index, 0))

    table = pl.BlockSpec((ROT // 2, seq_len), lambda i, split: (0, index))
    masked = pltpu.VMEM((per, seq_len, LANES), BF16)
    return pl.pallas_call(
        functools.partial(attention_kernel, index, len(earlier)),
        grid_spec=pltpu.PrefetchScalarGridSpec(
            num_scalar_prefetch=1,
            grid=(1,),
            in_specs=[spec(3 * width), spec(width), table, table]
            + [pl.BlockSpec(memory_space=pl.ANY)] * len(earlier),
            out_specs=[spec(width), spec(3 * width)],
            scratch_shapes=[
                masked, masked, masked, masked, masked,
                pltpu.VMEM((seq_len, LANES), F32),
                pltpu.VMEM((seq_len, LANES), F32),
                pltpu.VMEM((seq_len, LANES), F32),
                pltpu.VMEM((seq_len, LANES), F32),
                pltpu.VMEM((seq_len, LANES), F32),
            ],
        ),
        out_shape=[
            jax.ShapeDtypeStruct((rows, width), BF16),
            jax.ShapeDtypeStruct((rows, 3 * width), BF16),
        ],
        cost_estimate=pl.CostEstimate(
            flops=40 * seq_len * seq_len * width // 4,
            transcendentals=seq_len * seq_len * width // HEAD_DIM // 2,
            bytes_accessed=seq_len * width * 24,
        ),
        input_output_aliases={5 + i: i for i in range(len(earlier))},
        compiler_params=pltpu.CompilerParams(vmem_limit_bytes=48 << 20),
        name="attention",
    )(splits, qkv, grad, cosine, sine, *earlier)


def turn_tables(splits, seq_len):
    shape = (ROT // 2, splits.shape[0], seq_len)
    token = lax.broadcasted_iota(jnp.int32, shape, 2)
    start = splits[None, :, None]
    position = (token - jnp.where(token >= start, start, 0)).astype(F32)
    entry = jnp.arange(ROT // 2, dtype=F32)
    angle = position * (10000.0 ** (-(2.0 * entry) / ROT))[:, None, None]
    return jnp.cos(angle).reshape(ROT // 2, -1), jnp.sin(angle).reshape(ROT // 2, -1)


def sum_dots_kernel(count, *refs):
    out_ref = refs[-1]
    total = None
    for i in range(count):
        part = dot(refs[i][...], refs[count + i][...], NT)
        total = part if total is None else total + part
    out_ref[...] = total.astype(out_ref.dtype)


def sum_dots(lefts, rights, tile=512):
    rows, columns = lefts[0].shape[0], rights[0][0].shape[0]
    tile = min(tile, rows)
    depth = sum(left.shape[1] for left in lefts)
    return pl.pallas_call(
        functools.partial(sum_dots_kernel, len(lefts)),
        grid=(rows // tile,),
        in_specs=[pl.BlockSpec((tile, left.shape[1]), lambda i: (i, 0)) for left in lefts] + [
            pl.BlockSpec((columns, size), functools.partial(lambda at, i: (0, at), at))
            for _, size, at in rights
        ],
        out_specs=pl.BlockSpec((tile, columns), lambda i: (i, 0)),
        out_shape=jax.ShapeDtypeStruct((rows, columns), BF16),
        cost_estimate=pl.CostEstimate(
            flops=2 * rows * columns * depth, transcendentals=0,
            bytes_accessed=2 * (rows * columns + depth * (rows + columns)),
        ),
        compiler_params=pltpu.CompilerParams(vmem_limit_bytes=56 << 20),
        name="sum_dots",
    )(*lefts, *(right[0] for right in rights))


def hidden_kernel(n_ref, c_ref, w_ref, bias_ref, act_ref, dh_ref, sum_ref):
    piece = act_ref.shape[1]
    hidden = dot(n_ref[...], w_ref[:, :piece]) + bias_ref[...]
    grad = dot(c_ref[...], w_ref[:, piece:])
    rate = (2.0 / jnp.pi) ** 0.5
    square = hidden * hidden
    bent = jnp.tanh(rate * hidden * (1.0 + 0.044715 * square))
    act_ref[...] = (0.5 * hidden * (1.0 + bent)).astype(BF16)
    slope = 0.5 * (1.0 + bent) + 0.5 * hidden * (1.0 - bent * bent) * (
        rate * (1.0 + 3.0 * 0.044715 * square)
    )
    low = (grad * slope).astype(BF16)
    dh_ref[...] = low

    @pl.when(pl.program_id(0) == 0)
    def _():
        sum_ref[...] = jnp.zeros_like(sum_ref)

    sum_ref[...] += jnp.sum(low.astype(F32), 0, keepdims=True)


def hidden_part(normed_all, cot_all, weights, bias, tile=512):
    rows, depth = normed_all.shape
    piece = weights.shape[1] // 2
    tile = min(tile, rows)
    wide = pl.BlockSpec((tile, depth), lambda i: (i, 0))
    thin = pl.BlockSpec((tile, piece), lambda i: (i, 0))
    line = pl.BlockSpec((1, piece), lambda i: (0, 0))
    return pl.pallas_call(
        hidden_kernel,
        grid=(rows // tile,),
        in_specs=[wide, wide, pl.BlockSpec(weights.shape, lambda i: (0, 0)), line],
        out_specs=[thin, thin, line],
        out_shape=[
            jax.ShapeDtypeStruct((rows, piece), BF16),
            jax.ShapeDtypeStruct((rows, piece), BF16),
            jax.ShapeDtypeStruct((1, piece), F32),
        ],
        cost_estimate=pl.CostEstimate(
            flops=4 * rows * depth * piece, transcendentals=rows * piece,
            bytes_accessed=4 * rows * depth + 4 * depth * piece + 4 * rows * piece,
        ),
        compiler_params=pltpu.CompilerParams(vmem_limit_bytes=48 << 20),
        name="hidden_part",
    )(normed_all, cot_all, weights, bias)


def grads_kernel(left_ref, other_ref, n_ref, c_ref, out_ref, turned_s):
    count = left_ref.shape[1]

    @pl.when(pl.program_id(0) == 0)
    def _():
        turned_s[:count] = left_ref[...].T
        turned_s[count:] = other_ref[...].T

    out_ref[:count] = dot(turned_s[:count], n_ref[...]).astype(BF16)
    out_ref[count:] = dot(turned_s[count:], c_ref[...]).astype(BF16)


def turned_grads(left, other, normed_all, cot_all, tile=512):
    rows, depth = normed_all.shape
    tile = min(tile, depth)
    count = left.shape[1] + other.shape[1]
    fixed = lambda array: pl.BlockSpec(array.shape, lambda i: (0, 0))
    part = pl.BlockSpec((rows, tile), lambda i: (0, i))
    return pl.pallas_call(
        grads_kernel,
        grid=(depth // tile,),
        in_specs=[fixed(left), fixed(other), part, part],
        out_specs=pl.BlockSpec((count, tile), lambda i: (0, i)),
        out_shape=jax.ShapeDtypeStruct((count, depth), BF16),
        scratch_shapes=[pltpu.VMEM((count, rows), BF16)],
        cost_estimate=pl.CostEstimate(
            flops=2 * rows * depth * count, transcendentals=0,
            bytes_accessed=4 * rows * depth + 2 * count * (rows + depth),
        ),
        compiler_params=pltpu.CompilerParams(vmem_limit_bytes=48 << 20),
        name="turned_grads",
    )(left, other, normed_all, cot_all)


def gather_kernel(
    n, q_ref, k_ref, v_ref, o_ref, up_ref, down_ref, norm_ref, cot_ref,
    w_ref, unit_ref, right_ref, left_ref, last_ref, n_ref, c_ref,
    rows_s, first_s, unit_s, last_s, send_sem, recv_sem, local_sem, store_sem,
):
    z, y, x, c = (lax.axis_index(name) for name in ("z", "y", "x", "c"))
    rows = norm_ref.shape[0]
    half = 3 * rows // 4
    mine = y * 4 + x * 2 + c
    has_right, has_left = z < n - 1, z > 0
    number = {}

    def remote(key, src, dst, axis, target):
        slot = number.setdefault(key, len(number))
        return pltpu.make_async_remote_copy(
            src_ref=src, dst_ref=dst, send_sem=send_sem.at[slot], recv_sem=recv_sem.at[slot],
            device_id={axis: target}, device_id_type=pl.DeviceIdType.MESH,
        )

    def when(condition, action):
        if condition is None:
            action()
        else:
            pl.when(condition)(action)

    started = []

    def start(condition, copy):
        when(condition, copy.start)
        started.append((condition, copy))

    def shard(index, unit):
        return w_ref.at[index * 2 + (y if unit == 0 else 1 - y)]

    width, hidden = q_ref.shape[1] // 2, up_ref.shape[1] // 2
    piece = hidden // 2

    def parts(kind, side):
        if kind == 2:
            sources, size, begin = (q_ref, k_ref, v_ref, o_ref), width, side * width
        else:
            sources, size, begin = (up_ref, down_ref), piece, side * hidden + kind * piece
        span = pl.ds(pl.multiple_of(begin, LANES), size)
        return [(ref.at[:, span], pl.ds(i * size, size)) for i, ref in enumerate(sources)]

    def packed(key, kind, side, block, axis, target):
        return [
            remote(key + (i,), source, block.at[:, columns], axis, target)
            for i, (source, columns) in enumerate(parts(kind, side))
        ]

    def along(step, unit, sign, receiving=False):
        index = z - sign * step if receiving else z - sign * (step - 1)
        if step == 1 and unit == 0:
            return packed((step, unit, sign), 0, y, shard(index, unit), "z", z + sign)
        return [remote((step, unit, sign), shard(index, unit), shard(index, unit), "z", z + sign)]

    def start_all(condition, copies):
        for copy in copies:
            start(condition, copy)

    def wait_all(copies):
        for copy in copies:
            copy.wait_recv()


    full, top, low = pl.ds(0, rows), pl.ds(0, half), pl.ds(half, rows - half)
    arrays = ((n_ref, norm_ref, "n"), (c_ref, cot_ref, "c"))
    at_x, at_y, at_xy = y * 4 + (1 - x) * 2 + c, (1 - y) * 4 + x * 2 + c, (1 - y) * 4 + (1 - x) * 2 + c

    barrier = pltpu.get_barrier_semaphore()
    for axis, target in (("x", 1 - x), ("y", 1 - y), ("c", 1 - c)):
        pl.semaphore_signal(
            barrier, inc=1, device_id={axis: target}, device_id_type=pl.DeviceIdType.MESH
        )
    for condition, target in ((has_right, z + 1), (has_left, z - 1)):
        when(condition, functools.partial(
            pl.semaphore_signal, barrier, inc=1, device_id={"z": target},
            device_id_type=pl.DeviceIdType.MESH,
        ))
    pl.semaphore_wait(barrier, 3 + has_right.astype(jnp.int32) + has_left.astype(jnp.int32))

    for condition, sign in ((has_right, 1), (has_left, -1)):
        start_all(condition, along(1, 0, sign))
    start_all(None, packed(("swap",), 0, 1 - y, shard(z, 0), "y", 1 - y))
    swap_in = packed(("swap",), 0, 1 - y, shard(z, 1), "y", 1 - y)
    for array, source, name in arrays:
        for axis in ("x", "y", "c"):
            start(None, remote((name, axis), source, array.at[mine], axis,
                               {"x": 1 - x, "y": 1 - y, "c": 1 - c}[axis]))
    start_all(None, packed(("unit",), 2, 1 - y, unit_ref.at[y], "y", 1 - y))
    unit_swap_in = packed(("unit",), 2, 1 - y, unit_ref.at[1 - y], "y", 1 - y)
    start_all(None, packed(("late",), 1, 1 - y, last_ref.at[y], "y", 1 - y))
    late_swap = packed(("late",), 1, 1 - y, last_ref.at[1 - y], "y", 1 - y)
    pairs = [(norm_ref, rows_s.at[0]), (cot_ref, rows_s.at[1])]
    for kind, block in ((0, first_s), (2, unit_s), (1, last_s)):
        pairs += [(source, block.at[:, columns]) for source, columns in parts(kind, y)]
    loads = [
        pltpu.make_async_copy(source, target, local_sem.at[i])
        for i, (source, target) in enumerate(pairs)
    ]
    stores = [
        pltpu.make_async_copy(source, target, store_sem.at[i])
        for i, (source, target) in enumerate((
            (first_s, shard(z, 0)), (unit_s, unit_ref.at[y]), (last_s, last_ref.at[y]),
            (rows_s.at[0], n_ref.at[mine]), (rows_s.at[1], c_ref.at[mine]),
        ))
    ]
    for load in loads:
        load.start()
    for load in loads:
        load.wait()
    for store in stores:
        store.start()

    def arrive_swap():
        wait_all(swap_in)
        for condition, sign in ((has_right, 1), (has_left, -1)):
            start_all(condition, along(1, 1, sign))

    def arrive_shard(step, unit, sign):
        inside = z - sign * step >= 0 if sign > 0 else z + step < n
        further = has_right if sign > 0 else has_left
        when(inside, functools.partial(wait_all, along(step, unit, sign, True)))
        if step + 1 < n:
            start_all(inside & further, along(step + 1, unit, sign))

    def arrive_rows(array, name, axis):
        index = {"x": at_x, "y": at_y, "c": None}[axis]
        block = array.at[index]
        remote((name, axis), block, block, axis, 0).wait_recv()
        part, on = (low, "y") if axis == "x" else (top, "x")
        piece = array.at[index, part]
        start(None, remote((name, "far", on), piece, piece, on, {"x": 1 - x, "y": 1 - y}[on]))
        start(None, remote((name, "core", axis), block, block, "c", 1 - c))

    def arrive_far(array, name, on):
        part = low if on == "y" else top
        piece = array.at[at_xy, part]
        remote((name, "far", on), piece, piece, on, 0).wait_recv()
        start(None, remote((name, "core", "far", on), piece, piece, "c", 1 - c))

    def arrive_steps(step):
        for unit in (0, 1):
            for sign in (1, -1):
                arrive_shard(step, unit, sign)

    def second_step(half_of, receiving):
        index = y if half_of == 0 else 1 - y
        ways = ((1, has_left if receiving else has_right, right_ref),
                (-1, has_right if receiving else has_left, left_ref))
        for sign, condition, target in ways:
            key = ("second", half_of, sign)
            if half_of == 0:
                copies = packed(key, 2, y, target.at[index], "z", z + sign)
            else:
                copies = [remote(key, unit_ref.at[index], target.at[index], "z", z + sign)]
            if receiving:
                when(condition, functools.partial(wait_all, copies))
            else:
                start_all(condition, copies)

    (norm, _, norm_name), (cot, _, cot_name) = arrays
    arrive_swap()
    arrive_rows(norm, norm_name, "x")
    for sign in (1, -1):
        arrive_shard(1, 0, sign)
    arrive_rows(norm, norm_name, "y")
    for sign in (1, -1):
        arrive_shard(1, 1, sign)
    arrive_rows(cot, cot_name, "x")
    if n > 2:
        arrive_steps(2)
    second_step(0, False)
    arrive_rows(cot, cot_name, "y")
    wait_all(unit_swap_in)
    second_step(1, False)
    for step in range(3, n):
        arrive_steps(step)
    for array, _, name in arrays:
        for on in ("x", "y"):
            arrive_far(array, name, on)
    for array, _, name in arrays:
        for key, index, part in (
            ((name, "c"), y * 4 + x * 2 + 1 - c, full),
            ((name, "core", "x"), y * 4 + (1 - x) * 2 + 1 - c, full),
            ((name, "core", "y"), (1 - y) * 4 + x * 2 + 1 - c, full),
            ((name, "core", "far", "x"), (1 - y) * 4 + (1 - x) * 2 + 1 - c, top),
            ((name, "core", "far", "y"), (1 - y) * 4 + (1 - x) * 2 + 1 - c, low),
        ):
            piece = array.at[index, part]
            remote(key, piece, piece, "c", 0).wait_recv()
    wait_all(late_swap)
    for half_of in (0, 1):
        second_step(half_of, True)
    for store in stores:
        store.wait()
    for condition, copy in started:
        when(condition, copy.wait_send)


def gather_all(n, query, key, value, output_turned, up, down_turned, normed, cotangent):
    rows, columns = normed.shape
    copies = 4 * (n - 1) + 46
    anywhere = pl.BlockSpec(memory_space=pl.ANY)
    heads = 2 * query.shape[1]
    hidden, depth = up.shape[1] // 2, query.shape[0]
    pair = jax.ShapeDtypeStruct((2, depth, heads), query.dtype)
    weights, unit, right, left, last, normed_all, cot_all = pl.pallas_call(
        functools.partial(gather_kernel, n),
        in_specs=[anywhere] * 8,
        out_specs=[anywhere] * 7,
        out_shape=[
            jax.ShapeDtypeStruct((2 * n, depth, hidden), up.dtype),
            pair, pair, pair,
            jax.ShapeDtypeStruct((2, depth, hidden), up.dtype),
            jax.ShapeDtypeStruct((8, rows, columns), normed.dtype),
            jax.ShapeDtypeStruct((8, rows, columns), cotangent.dtype),
        ],
        scratch_shapes=[
            pltpu.VMEM((2, rows, columns), normed.dtype),
            pltpu.VMEM((depth, hidden), up.dtype),
            pltpu.VMEM((depth, heads), query.dtype),
            pltpu.VMEM((depth, hidden), up.dtype),
            pltpu.SemaphoreType.DMA((copies,)),
            pltpu.SemaphoreType.DMA((copies,)),
            pltpu.SemaphoreType.DMA((10,)),
            pltpu.SemaphoreType.DMA((5,)),
        ],
        cost_estimate=pl.CostEstimate(flops=0, transcendentals=0, bytes_accessed=200 << 20),
        compiler_params=pltpu.CompilerParams(collective_id=0, has_side_effects=True),
        name="gather_rows",
    )(query, key, value, output_turned, up, down_turned, normed, cotangent)
    flat = lambda array: array.reshape(-1, array.shape[-1])
    return tuple(map(flat, (weights, unit, right, left, last, normed_all, cot_all)))


def chain_step(step, n, right, left):
    return (
        lax.ppermute(right, "z", [(i, i + 1) for i in range(step - 1, n - 1)]),
        lax.ppermute(left, "z", [(i, i - 1) for i in range(1, n - step + 1)]),
    )


def assemble(unit, right, left, n, z):
    rows, columns = unit.shape
    whole = jnp.zeros((n * rows, columns), unit.dtype)
    for k in range(n):
        piece = unit if k == 0 else jnp.where(z >= k, right[k], left[n - k])
        row = lax.rem(z - k + n, n) * rows
        whole = lax.dynamic_update_slice(whole, piece, (row, jnp.int32(0)))
    return whole


def scatter_pieces(k, grads, n, z, received):
    rows = grads.shape[0] // n

    def piece(index, got):
        own = lax.dynamic_slice_in_dim(grads, jnp.clip(index, 0, n - 1) * rows, rows, 0)
        return own if got is None else add_low(own, got)

    return piece(z - k, received[0]), piece(z + k, received[1])


def scatter_step(k, grads, n, z, received):
    to_left, to_right = scatter_pieces(k, grads, n, z, received)
    return (
        lax.ppermute(to_left, "z", [(r, r - 1) for r in range(k, n)]),
        lax.ppermute(to_right, "z", [(r, r + 1) for r in range(0, n - k)]),
    )


def scatter_end(grads, n, z, received):
    rows = grads.shape[0] // n
    own = lax.dynamic_slice_in_dim(grads, z * rows, rows, 0).astype(F32)
    return own + received[0].astype(F32) + received[1].astype(F32)


def tail_kernel(
    n, g_any, hw_ref, fw_ref, lw_ref, dq_ref, d0_ref, d1_ref, at_ref, a0_ref, a1_ref,
    left_ref, right_ref, own_ref, std_any, cot_any, tokens_any, vec_ref, lines_ref, inv_ref,
    keep_ref, take_ref, heads_keep_ref, heads_take_ref, out_ref, mixed_ref, sums_ref,
    g_ref, std_ref, hw_s, fw_s, lw_s, rows_s, stage, zrecv, give, heads_recv, heads_own, heads_give, both, xtop_2, ylow_2, ytop_2, xlow_2,
    top_2, low_2, vstage, vrecv, send_sem, recv_sem, load_sem, rows_sem,
):
    z, y, x, c = (lax.axis_index(name) for name in ("z", "y", "x", "c"))
    rows, columns = out_ref.shape
    wide, wide_heads = give.shape[0], heads_give.shape[0]
    half = rows // 2
    rest = rows - half
    number, started = {}, []

    def remote(key, src, dst, axis, target):
        slot = number.setdefault(key, len(number))
        return pltpu.make_async_remote_copy(
            src_ref=src, dst_ref=dst, send_sem=send_sem.at[slot], recv_sem=recv_sem.at[slot],
            device_id={axis: target}, device_id_type=pl.DeviceIdType.MESH,
        )

    def when(condition, action):
        if condition is None:
            action()
        else:
            pl.when(condition)(action)

    def start(condition, copy):
        when(condition, copy.start)
        started.append((condition, copy))

    def each(count, size, body):
        def step(i, carry):
            body(pl.ds(pl.multiple_of(i * size, size), size))
            return carry
        lax.fori_loop(0, count // size, step, 0)

    barrier = pltpu.get_barrier_semaphore()
    greet = [(None, "x", 1 - x), (None, "y", 1 - y), (None, "c", 1 - c)]
    greet += [(z < n - 1, "z", z + 1), (z > 0, "z", z - 1)]
    for step in (2 ** i for i in range(1, n.bit_length() - 1)):
        greet.append((None, "z", jnp.bitwise_xor(z, step)))
    for condition, axis, target in greet:
        when(condition, functools.partial(
            pl.semaphore_signal, barrier, inc=1, device_id={axis: target},
            device_id_type=pl.DeviceIdType.MESH))

    loads = [
        pltpu.make_async_copy(source, target, load_sem.at[i])
        for i, (source, target) in enumerate(
            ((hw_ref, hw_s), (fw_ref, fw_s), (lw_ref, lw_s), (g_any, g_ref), (std_any, std_ref),
             (own_ref, heads_own)))
    ]
    for load in loads:
        load.start()

    firsts, lasts = fw_ref.shape[1] // 2, lw_ref.shape[1] // 2
    heads = dq_ref.shape[1]
    sums = (
        ((dq_ref, heads, hw_s, 0), (d0_ref, firsts, fw_s, 0), (d1_ref, lasts, lw_s, 0)),
        ((at_ref, heads // 3, hw_s, heads), (a0_ref, firsts, fw_s, firsts),
         (a1_ref, lasts, lw_s, lasts)),
    )
    sides = (1 - y, y)
    jobs = [(a, own, j) for a in (0, 1) for own in (False, True) for j in sides]

    def row_loads(number_of):
        a, own, j = jobs[number_of]
        slot, core, copies, at = number_of % 2, c if own else 1 - c, [], 0
        for p, (left, width, _, _) in enumerate(sums[a]):
            for i in (0, 1):
                block = j * 4 + i * 2 + core
                source = left.at[pl.ds(pl.multiple_of(block * rows, rows), rows)]
                target = rows_s.at[slot, pl.ds(i * rows, rows), pl.ds(at, width)]
                copies.append(pltpu.make_async_copy(source, target, rows_sem.at[slot, p * 2 + i]))
            at += width
        return copies

    def job(number_of):
        a, own, j = jobs[number_of]
        slot = number_of % 2
        if number_of + 1 < len(jobs):
            for copy in row_loads(number_of + 1):
                copy.start()
        for copy in row_loads(number_of):
            copy.wait()
        if own:
            for i in (0, 1):
                core_copy(a, number_of % 2, i).wait_recv()
        elif a == 1:
            for i in (0, 1):
                core_copy(0, number_of % 2, i).wait_send()
        size = min(512, columns)

        def tile(t, carry):
            span = pl.ds(pl.multiple_of(t * size, size), size)
            acc, at = None, 0
            for left, width, weights, column in sums[a]:
                part = dot(
                    rows_s[slot, :, at : at + width], weights[span, column : column + width], NT)
                acc = part if acc is None else acc + part
                at += width
            for i in (0, 1):
                piece = acc[i * rows : (i + 1) * rows]
                if own:
                    both[a, j * 2 + i, :, span] = (
                        piece + both[a, j * 2 + i, :, span].astype(F32)).astype(BF16)
                else:
                    stage[j * 2 + i, :, span] = piece.astype(BF16)
            return carry

        lax.fori_loop(0, columns // size, tile, 0)
        if own and a == 0:
            start(None, first_copy(a, "xtop", number_of % 2))
            if number_of % 2 == 0:
                for i in (0, 1):
                    start(None, first_copy(a, "ylow", i))
        if not own:
            for i in (0, 1):
                copy = core_copy(a, number_of % 2, i)
                copy.start()

    def core_copy(a, u, i):
        place = sides[u] * 2 + i
        return remote(("core", a, u, i), stage.at[place], both.at[a, place], "c", 1 - c)

    for copy in row_loads(0):
        copy.start()
    always = sum(condition is None for condition, _, _ in greet)
    pl.semaphore_wait(barrier, always + sum(
        condition.astype(jnp.int32) for condition, _, _ in greet if condition is not None))

    def first_copy(a, name, j):
        if name == "xtop":
            source = both.at[a, sides[j] * 2 + 1 - x, pl.ds(0, half)]
            return remote((name, a, j), source, xtop_2.at[a, j], "x", 1 - x)
        source = both.at[a, (1 - y) * 2 + j, pl.ds(half, rest)]
        return remote((name, a, j), source, ylow_2.at[a, j], "y", 1 - y)

    def second_copy(a, name):
        if name == "ytop":
            return remote((name, a), top_2.at[a], ytop_2.at[a], "y", 1 - y)
        return remote((name, a), low_2.at[a], xlow_2.at[a], "x", 1 - x)

    def first_send(a):
        for j in (0, 1):
            start(None, first_copy(a, "xtop", j))
            start(None, first_copy(a, "ylow", j))

    def first_arrive(a):
        for j in (0, 1):
            first_copy(a, "xtop", j).wait_recv()
            first_copy(a, "ylow", j).wait_recv()

        def upper(part):
            top_2[a, part, :] = (
                both[a, (1 - y) * 2 + x, part, :].astype(F32)
                + xtop_2[a, 0, part, :].astype(F32)
            ).astype(BF16)

        def lower(part):
            low_part = pl.ds(part.start + half, part.size)
            low_2[a, part, :] = (
                both[a, y * 2 + 1 - x, low_part, :].astype(F32)
                + ylow_2[a, 1 - x, part, :].astype(F32)
            ).astype(BF16)

        each(half, 32, upper)
        each(rest, 32, lower)
        start(None, second_copy(a, "ytop"))
        start(None, second_copy(a, "xlow"))

    def second_arrive(a):
        second_copy(a, "ytop").wait_recv()
        second_copy(a, "xlow").wait_recv()
        target = (out_ref, mixed_ref)[a]

        def finish(first, part, placed, last):
            value = (
                both[a, y * 2 + x, placed, :].astype(F32) + first[part, :].astype(F32)
                + last[part, :].astype(F32)
            )
            if a == 0:
                standard = std_ref[placed, :]
                vstage[0, 0:1, :] += jnp.sum(value * standard, 0, keepdims=True)
                vstage[0, 1:2, :] += jnp.sum(value, 0, keepdims=True)
                scaled = value * lines_ref[0:1, :]
                mean = jnp.mean(scaled, 1, keepdims=True)
                along = jnp.mean(scaled * standard, 1, keepdims=True)
                target[placed, :] = stage[0, placed, :].astype(F32) + inv_ref[placed, :] * (
                    scaled - mean - standard * along)
            else:
                whole = stage[1, placed, :].astype(F32) + value + lines_ref[1:2, :]
                target[placed, :] = whole.astype(BF16)

        def upper(part):
            finish(xtop_2.at[a, 1], part, part, ytop_2.at[a])

        def lower(part):
            finish(ylow_2.at[a, x], part, pl.ds(part.start + half, part.size), xlow_2.at[a])

        each(half, 32, upper)
        each(rest, 32, lower)

    def block_of(direction, k, u):
        index = (z - k if direction == 0 else z + k) * 2 + sides[u]
        return pl.ds(pl.multiple_of(index * rows, rows), rows)

    def z_copy(direction, k, u, src):
        target = z - 1 if direction == 0 else z + 1
        return remote((direction, k, u), src, zrecv.at[direction, k - 1, u], "z", target)

    def z_first(direction):
        edge = z == n - 1 if direction == 0 else z == 0
        for k in range(n - 1, 0, -1):
            for u in (0, 1):
                start(edge, z_copy(direction, k, u, g_any.at[:, block_of(direction, k, u)]))

    def z_step(k, u):
        for direction in (0, 1):
            if direction == 0:
                inside = (z >= k) & (z < n - 1)
            else:
                inside = (n - 1 - z >= k) & (z > 0)
            held = zrecv.at[direction, k, u]

            def add():
                z_copy(direction, k + 1, u, held).wait_recv()
                block = block_of(direction, k, u)

                def body(part):
                    held[part, :] = (
                        g_ref[part, block].astype(F32) + held[part, :].astype(F32)
                    ).astype(BF16)

                each(wide, 256, body)

            when(inside, add)
            start(inside, z_copy(direction, k, u, held))

    def z_last(u, target):
        block = block_of(0, 0, u)

        def first(part):
            target[part, :] = g_ref[part, block].astype(F32)

        each(wide, 256, first)
        for direction in (0, 1):
            held = zrecv.at[direction, 0, u]

            def add():
                z_copy(direction, 1, u, held).wait_recv()

                def body(part):
                    target[part, :] += held[part, :].astype(F32)

                each(wide, 256, body)

            when(z < n - 1 if direction == 0 else z > 0, add)

    def heads_copy(direction, u):
        span = pl.ds(pl.multiple_of(sides[u] * rows, rows), rows)
        source = (left_ref, right_ref)[direction].at[:, span]
        return remote(
            ("heads", direction, u), source, heads_recv.at[direction, :, span], "z",
            z - 1 if direction == 0 else z + 1)

    def heads_send():
        for u in (0, 1):
            start(z > 0, heads_copy(0, u))
            start(z < n - 1, heads_copy(1, u))

    def heads_last(u, target):
        span = pl.ds(pl.multiple_of(sides[u] * rows, rows), rows)

        def first(part):
            target[part, :] = heads_own[part, span].astype(F32)

        each(wide_heads, 256, first)
        for direction in (0, 1):
            def add():
                heads_copy(direction, u).wait_recv()

                def body(part):
                    target[part, :] += heads_recv[direction, part, span].astype(F32)

                each(wide_heads, 256, body)

            when(z < n - 1 if direction == 0 else z > 0, add)

    steps = [(k, u) for k in range(n - 2, 0, -1) for u in (0, 1)]

    def z_next():
        if steps:
            z_step(*steps.pop(0))

    for direction in (0, 1):
        z_first(direction)
    vstage[0] = vec_ref[...]
    for load in loads[:3]:
        load.wait()
    job(0)
    job(1)
    for load in loads[3:]:
        load.wait()
    z_next()
    job(2)
    job(3)
    heads_send()
    z_next()
    job(4)
    job(5)
    z_next()
    job(6)
    job(7)
    first_arrive(0)
    first_send(1)
    for u in (0, 1):
        for i in (0, 1):
            core_copy(1, u, i).wait_send()
    late = [
        pltpu.make_async_copy(source, stage.at[i], load_sem.at[6 + i])
        for i, source in enumerate((cot_any, tokens_any))
    ]
    for load in late:
        load.start()
    for load in late:
        load.wait()
    while steps:
        z_next()
    second_arrive(0)

    turns = [("z", jnp.bitwise_xor(z, 2 ** i)) for i in range(n.bit_length() - 1)]
    turns += [("y", 1 - y), ("x", 1 - x), ("c", 1 - c)]
    line = lax.broadcasted_iota(jnp.int32, vec_ref.shape, 0)

    def exchange(i):
        axis, target = turns[i]
        return remote(("vec", i), vstage.at[i], vrecv.at[i], axis, target)

    def turn(i):
        exchange(i).wait_recv()
        axis, _ = turns[i]
        old, new = vstage[i], vrecv[i]
        result = sums_ref if i == len(turns) - 1 else vstage.at[i + 1]
        result[...] = old + jnp.where((line < 3) | (axis == "z"), new, 0.0)
        if axis == "y":
            result[4:5, :] = new[3:4, :]
        if i + 1 < len(turns):
            start(None, exchange(i + 1))

    start(None, exchange(0))

    def swapped(key, source, target, length, received):
        def lower_precision(part):
            target[part, :] = source[part, :].astype(BF16)

        each(length, 256, lower_precision)
        copy = remote(key, target, received, "y", 1 - y)
        start(None, copy)
        return copy

    first_arrive(1)
    z_last(0, keep_ref)
    swap = swapped("swap", keep_ref, give, wide, take_ref)
    turn(0)
    turn(1)
    heads_last(0, heads_keep_ref)
    heads_swap = swapped("heads swap", heads_keep_ref, heads_give, wide_heads, heads_take_ref)
    turn(2)
    z_last(1, keep_ref)
    turn(3)
    heads_last(1, heads_keep_ref)
    for i in range(4, len(turns)):
        turn(i)
    second_arrive(1)
    swap.wait_recv()
    heads_swap.wait_recv()
    for condition, copy in started:
        when(condition, copy.wait_send)


def tail(
    n, grads_turned, weights, lefts, lefts_out, heads_turned, standard, cotangent, tokens, vector,
    lines, inv_scale,
):
    rows, columns = standard.shape
    wide, wide_heads = grads_turned.shape[0], heads_turned[0].shape[0]
    half = rows // 2
    inside = pl.BlockSpec(memory_space=pltpu.VMEM)
    anywhere = pl.BlockSpec(memory_space=pl.ANY)
    copies = 4 * (n - 1) + 46
    low = lambda *shape: pltpu.VMEM(shape, BF16)
    small = vector.shape
    depth = sum(left.shape[1] for left in lefts)
    return pl.pallas_call(
        functools.partial(tail_kernel, n),
        in_specs=[anywhere] * 16 + [inside] * 3,
        out_specs=[inside] * 7,
        out_shape=[
            jax.ShapeDtypeStruct((wide, rows), F32),
            jax.ShapeDtypeStruct((wide, rows), BF16),
            jax.ShapeDtypeStruct((wide_heads, rows), F32),
            jax.ShapeDtypeStruct((wide_heads, rows), BF16),
            jax.ShapeDtypeStruct((rows, columns), F32),
            jax.ShapeDtypeStruct((rows, columns), BF16),
            jax.ShapeDtypeStruct(small, F32),
        ],
        scratch_shapes=[low(*grads_turned.shape), pltpu.VMEM(standard.shape, F32)] + [
            low(*array.shape) for array in weights
        ] + [
            low(2, 2 * rows, depth), low(4, rows, columns),
            low(2, n - 1, 2, wide, rows), low(wide, rows),
            low(2, wide_heads, 2 * rows), low(wide_heads, 2 * rows), low(wide_heads, rows),
            low(2, 4, rows, columns),
            low(2, 2, half, columns), low(2, 2, rows - half, columns),
            low(2, half, columns), low(2, rows - half, columns),
            low(2, half, columns), low(2, rows - half, columns),
            pltpu.VMEM((8,) + small, F32), pltpu.VMEM((8,) + small, F32),
            pltpu.SemaphoreType.DMA((copies,)),
            pltpu.SemaphoreType.DMA((copies,)),
            pltpu.SemaphoreType.DMA((8,)),
            pltpu.SemaphoreType.DMA((2, 6)),
        ],
        cost_estimate=pl.CostEstimate(flops=0, transcendentals=0, bytes_accessed=200 << 20),
        compiler_params=pltpu.CompilerParams(
            collective_id=1, has_side_effects=True, vmem_limit_bytes=63 << 20
        ),
        name="scatter_rest",
    )(
        grads_turned, *weights, *lefts, *lefts_out, *heads_turned, standard, cotangent, tokens,
        vector, lines, inv_scale,
    )


def sum_small(array, axes):
    for axis in axes:
        size = lax.axis_size(axis)
        if size & (size - 1):
            array = lax.psum(array, axis)
            continue
        step = 1
        while step < size:
            array = array + lax.ppermute(array, axis, [(i, i ^ step) for i in range(size)])
            step *= 2
    return array


def pick(array, index, axis):
    return lax.dynamic_index_in_dim(array, index, axis, keepdims=False)


def add_low(left, right):
    return (left.astype(F32) + right.astype(F32)).astype(BF16)


def plane_scatter(partial, y, x, c):
    rows, columns = partial.shape[0] // 8, partial.shape[1]
    half = rows // 2
    parts = partial.reshape(2, 2, 2, rows, columns)
    acc = add_low(pick(parts, c, 2), lax.ppermute(pick(parts, 1 - c, 2), "c", SWAP))
    top, low = acc[:, :, :half], acc[:, :, half:]
    top = add_low(pick(top, x, 1), lax.ppermute(pick(top, 1 - x, 1), "x", SWAP))
    low = add_low(pick(low, y, 0), lax.ppermute(pick(low, 1 - y, 0), "y", SWAP))
    top = pick(top, y, 0).astype(F32) + lax.ppermute(pick(top, 1 - y, 0), "y", SWAP).astype(F32)
    low = pick(low, x, 0).astype(F32) + lax.ppermute(pick(low, 1 - x, 0), "x", SWAP).astype(F32)
    return jnp.concatenate([top, low], 0)


def in_order(y, own, other, axis):
    return jnp.where(
        y == 0, jnp.concatenate([own, other], axis), jnp.concatenate([other, own], axis)
    )


def on_device(
    n,
    tokens, norm_gain, norm_bias,
    query_weight, query_bias, key_weight, key_bias, value_weight, value_bias,
    output_weight, output_bias, up_weight, up_bias, down_weight, down_bias,
    doc_split, cotangent,
):
    z, y, x, c = (lax.axis_index(name) for name in ("z", "y", "x", "c"))
    shard_rows = query_weight.shape[0]
    width = query_weight.shape[1] // 2
    hidden_width = up_weight.shape[1] // 2
    chunks = 2
    piece = hidden_width // chunks

    def row(array, start, size):
        return lax.dynamic_slice_in_dim(array, start, size, 0)

    gain_wide = norm_gain.astype(F32)
    tokens_wide = tokens.astype(F32)
    row_mean = jnp.mean(tokens_wide, -1, keepdims=True)
    centred = tokens_wide - row_mean
    inv_scale = lax.rsqrt(jnp.mean(centred * centred, -1, keepdims=True) + EPS)
    standard = centred * inv_scale
    normed = (standard * gain_wide + norm_bias.astype(F32)).astype(BF16)
    phase = lax.optimization_barrier
    other_split = lax.ppermute(doc_split, "y", SWAP)
    splits = in_order(y, doc_split, other_split, 0)
    seq_len = 4 * normed.shape[0]
    cosine, sine = turn_tables(splits, seq_len)

    right, left = [None] * n, [None] * n
    first_weights, heads_unit, right[1], left[1], last_unit, normed_all, cot_all = gather_all(
        n, query_weight, key_weight, value_weight, output_weight.T, up_weight, down_weight.T,
        normed, cotangent,
    )
    first_weights, heads_unit, last_unit, normed_all, cot_all, right[1], left[1], cosine, sine = phase(
        (first_weights, heads_unit, last_unit, normed_all, cot_all, right[1], left[1], cosine, sine)
    )

    def hidden_local(weights, chunk):
        bias = row(up_bias, y * hidden_width + chunk * piece, piece).astype(F32)[None]
        return hidden_part(normed_all, cot_all, weights, bias)

    def weight_grads(grad_columns, columns):
        return turned_grads(grad_columns, columns, normed_all, cot_all).T

    def gather_step(step, source):
        return chain_step(step, n, right[step - 1], left[step - 1]) if step > 1 else chain_step(
            1, n, source, source)

    activated_0, grad_hidden_0, hidden_sum_0 = hidden_local(first_weights, 0)
    right[2], left[2] = gather_step(2, None)
    activated_0, grad_hidden_0, normed_all, cot_all, right[2], left[2] = phase(
        (activated_0, grad_hidden_0, normed_all, cot_all, right[2], left[2])
    )
    grads_first = weight_grads(grad_hidden_0, activated_0)
    for step in range(3, n):
        right[step], left[step] = gather_step(step, None)
    grads_first, activated_0, last_unit, normed_all, cot_all, right[3:], left[3:] = phase(
        (grads_first, activated_0, last_unit, normed_all, cot_all, right[3:], left[3:])
    )
    head_weights = assemble(heads_unit, right, left, n, z)
    qkv_weight, output_turned = head_weights[:, : 3 * width], head_weights[:, 3 * width :]

    qkv_bias = jnp.concatenate(
        [row(b, y * width, width) for b in (query_bias, key_bias, value_bias)]
    ).astype(F32)
    qkv = dot(normed_all, qkv_weight) + qkv_bias
    grad_attended = dot(cot_all, output_turned).astype(BF16)
    right[1], left[1] = gather_step(1, last_unit)
    qkv, grad_attended, normed_all, cot_all, right[1], left[1] = phase(
        (qkv, grad_attended, normed_all, cot_all, right[1], left[1])
    )
    found = attention(0, splits, qkv, grad_attended, cosine, sine, ())
    right[2], left[2] = gather_step(2, None)
    first_in = scatter_step(n - 1, grads_first, n, z, (None, None))
    found, qkv, grad_attended, normed_all, cot_all, right[2], left[2], first_in, grads_first = phase(
        (found, qkv, grad_attended, normed_all, cot_all, right[2], left[2], first_in, grads_first)
    )
    for index in range(1, splits.shape[0]):
        found = attention(index, splits, qkv, grad_attended, cosine, sine, found)
    for step in range(3, n):
        right[step], left[step] = gather_step(step, None)
    for k in range(n - 2, n - 3, -1):
        first_in = scatter_step(k, grads_first, n, z, first_in)
    found, normed_all, cot_all, right[3:], left[3:], first_in, grads_first = phase(
        (found, normed_all, cot_all, right[3:], left[3:], first_in, grads_first)
    )
    attended, grad_qkv = found
    grads_heads = weight_grads(grad_qkv, attended)
    for k in range(n - 3, 0, -1):
        first_in = scatter_step(k, grads_first, n, z, first_in)
    grads_heads, attended, grad_qkv, normed_all, cot_all, last_unit, first_in, grads_first = phase(
        (grads_heads, attended, grad_qkv, normed_all, cot_all, last_unit, first_in, grads_first)
    )
    first_sum = scatter_end(grads_first, n, z, first_in)

    last_weights = assemble(last_unit, right, left, n, z)
    activated_1, grad_hidden_1, hidden_sum_1 = hidden_local(last_weights, 1)
    heads_in = scatter_step(n - 1, grads_heads, n, z, (None, None))
    (last_weights, activated_1, grad_hidden_1, attended, grad_qkv, heads_in, grads_heads,
     normed_all, cot_all) = phase(
        (last_weights, activated_1, grad_hidden_1, attended, grad_qkv, heads_in, grads_heads,
         normed_all, cot_all)
    )
    for k in range(n - 2, max(n - 3, 1), -1):
        heads_in = scatter_step(k, grads_heads, n, z, heads_in)
    grads_last = weight_grads(grad_hidden_1, activated_1)
    qkv_sum = jnp.sum(grad_qkv, 0, dtype=F32)[None]
    bias_row = jnp.concatenate([qkv_sum, hidden_sum_0, hidden_sum_1], 1)
    cot_wide = cotangent.astype(F32)
    cot_sum = jnp.sum(cot_wide, 0)[None]
    grads_last, heads_in, grads_heads, bias_row, cot_sum = phase(
        (grads_last, heads_in, grads_heads, bias_row, cot_sum)
    )
    def halves(total):
        keep = row(total, y * shard_rows, shard_rows)
        give = row(total, (1 - y) * shard_rows, shard_rows).astype(BF16)
        return keep, lax.ppermute(give, "y", SWAP).astype(F32)

    first_keep, first_take = halves(first_sum)

    out_bias = output_bias.astype(F32) + down_bias.astype(F32)
    if n == 4 and bias_row.shape[1] <= cot_sum.shape[1]:
        spread = cot_sum.shape[1]
        vector = jnp.concatenate([
            jnp.zeros((2, spread), F32), cot_sum,
            jnp.pad(bias_row, ((0, 0), (0, spread - bias_row.shape[1]))),
            jnp.zeros((4, spread), F32),
        ])
        left_piece, right_piece = scatter_pieces(1, grads_heads, n, z, heads_in)
        own_piece = row(grads_heads, z * 2 * shard_rows, 2 * shard_rows)
        lines = jnp.concatenate(
            [gain_wide[None], out_bias[None], jnp.zeros((6, spread), F32)]
        )
        last_keep, last_take, heads_keep, heads_take, grad_tokens, out, sums = tail(
            n, grads_last.T, (head_weights, first_weights, last_weights),
            (grad_qkv, grad_hidden_0, grad_hidden_1), (attended, activated_0, activated_1),
            (left_piece.T, right_piece.T, own_piece.T), standard, cotangent, tokens, vector,
            lines, inv_scale,
        )
        last_keep, last_take = last_keep.T, last_take.astype(F32).T
        heads_keep, heads_take = heads_keep.T, heads_take.astype(F32).T
        norm_sums = sums[:3]
        bias_rows = in_order(y, sums[3:4], sums[4:5], 0)[:, : bias_row.shape[1]]
    else:
        for k in range(n - 3, 0, -1):
            heads_in = scatter_step(k, grads_heads, n, z, heads_in)
        heads_keep, heads_take = halves(scatter_end(grads_heads, n, z, heads_in))
        partial_out = sum_dots(
            (attended, activated_0, activated_1),
            ((head_weights, width, 3), (first_weights, piece, 1), (last_weights, piece, 1)),
        )
        grad_normed_part = sum_dots(
            (grad_qkv, grad_hidden_0, grad_hidden_1),
            ((head_weights, 3 * width, 0), (first_weights, piece, 0), (last_weights, piece, 0)),
        )
        last_in = (None, None)
        for k in range(n - 1, 0, -1):
            last_in = scatter_step(k, grads_last, n, z, last_in)
        last_keep, last_take = halves(scatter_end(grads_last, n, z, last_in))
        grad_normed = plane_scatter(grad_normed_part, y, x, c)
        mixed = plane_scatter(partial_out, y, x, c)
        norm_sums = sum_small(
            jnp.concatenate([
                jnp.sum(grad_normed * standard, 0)[None], jnp.sum(grad_normed, 0)[None], cot_sum
            ]),
            ("c", "x", "y", "z"),
        )
        grad_scaled = grad_normed * gain_wide
        grad_tokens = cot_wide + inv_scale * (
            grad_scaled
            - jnp.mean(grad_scaled, -1, keepdims=True)
            - standard * jnp.mean(grad_scaled * standard, -1, keepdims=True)
        )
        out = (tokens_wide + mixed + out_bias).astype(BF16)
        bias_row = sum_small(bias_row, ("z",))
        bias_rows = in_order(y, bias_row, lax.ppermute(bias_row, "y", SWAP), 0)
    grad_norm_gain, grad_norm_bias, grad_out_bias = norm_sums

    def joined(start, size):
        return in_order(
            y, heads_keep[:, start : start + size], heads_take[:, start : start + size], 1
        )

    grad_query_weight, grad_key_weight, grad_value_weight, grad_output_turned = (
        joined(part * width, width) for part in range(4)
    )
    hidden_halves = [(first_keep, first_take), (last_keep, last_take)]

    def side(which, start):
        return jnp.concatenate([pair[which][:, start : start + piece] for pair in hidden_halves], 1)

    grad_up_weight = in_order(y, side(0, 0), side(1, 0), 1)
    grad_down_turned = in_order(y, side(0, piece), side(1, piece), 1)

    grad_query_bias, grad_key_bias, grad_value_bias = (
        bias_rows[:, part * width : (part + 1) * width].reshape(-1) for part in range(3)
    )
    grad_up_bias = bias_rows[:, 3 * width :].reshape(-1)

    return (
        out, grad_tokens, grad_norm_gain, grad_norm_bias,
        grad_query_weight, grad_query_bias, grad_key_weight, grad_key_bias,
        grad_value_weight, grad_value_bias, grad_output_turned.T, grad_out_bias,
        grad_up_weight, grad_up_bias, grad_down_turned.T, grad_out_bias,
    )


def solution(mesh):
    n = mesh.shape["dp"] // 2
    grid = Mesh(mesh.devices.reshape(n, 2, mesh.shape["tensor"] // 2, 2), ("z", "y", "x", "c"))
    dp, tensor = ("z", "y"), ("x", "c")
    rows = P(dp + tensor, None)
    whole, split = P(), P(tensor)
    wide, tall = P(dp, tensor), P(tensor, dp)
    in_specs = (
        rows, whole, whole, wide, split, wide, split, wide, split,
        tall, whole, wide, split, tall, whole, P(dp), rows,
    )
    out_specs = (
        rows, rows, whole, whole, wide, split, wide, split, wide, split,
        tall, whole, wide, split, tall, whole,
    )
    return jax.shard_map(
        functools.partial(on_device, n),
        mesh=grid, in_specs=in_specs, out_specs=out_specs, check_vma=False,
    )
```
